32 devices in a mesh: rep: 8 (over y, x, core), shard: 4 (over z).
Axes of the slice: x: 2, y: 2, z: 4, core: 2. Of those that a mesh axis runs over, the one named last changes fastest.
Arguments:
- tokens: bfloat16 [4096, 2048], P(('rep', 'shard')), may hold values from -6 to 6
- segments: int32 [32, 128], P(('rep', 'shard')), may hold values from 0 to 7, never falling along the last dimension, each value on 1 to 64 neighbouring positions
- routes: int32 [4096, 8], P(('rep', 'shard')), may hold values from 0 to 31, all different within a row; in each aligned block of 128 rows (0 to 127, 128 to 255, ...) at most 64 rows name the same one
- attn_gain: bfloat16 [2048], P('shard'), may hold values from 0.5 to 1.5
- w_query: bfloat16 [2048, 4096], P('shard'), may hold values from -0.125 to 0.125
- key_weight: bfloat16 [2048, 512], P('shard'), may hold values from -0.125 to 0.125
- value_weight: bfloat16 [2048, 512], P('shard'), may hold values from -0.125 to 0.125
- w_out: bfloat16 [4096, 2048], P('shard'), may hold values from -0.75 to 0.75
- query_gain: bfloat16 [128], P('shard'), may hold values from 0.099609375 to 1.8984375
- key_gain: bfloat16 [128], P('shard'), may hold values from 0.099609375 to 1.8984375
- ffn_gain: bfloat16 [2048], P('shard'), may hold values from 0.5 to 1.5
- w_router: bfloat16 [2048, 32], P('shard'), may hold values from -0.125 to 0.125
- w_gate: bfloat16 [32, 2048, 768], P(('rep', 'shard')), may hold values from -0.125 to 0.125
- w_up: bfloat16 [32, 2048, 768], P(('rep', 'shard')), may hold values from -0.125 to 0.125
- w_down: bfloat16 [32, 768, 2048], P(('rep', 'shard')), may hold values from -0.875 to 0.875
- cotangent: bfloat16 [4096, 2048], P(('rep', 'shard')), may hold values from -6 to 6
Outputs:
- output: bfloat16 [4096, 2048], P(('rep', 'shard'))
- grad_tokens: float32 [4096, 2048], P(('rep', 'shard'))
- grad_attn_gain: float32 [2048], P('shard')
- grad_w_query: float32 [2048, 4096], P('shard')
- grad_w_key: float32 [2048, 512], P('shard')
- grad_w_value: float32 [2048, 512], P('shard')
- grad_w_out: float32 [4096, 2048], P('shard')
- grad_query_gain: float32 [128], P('shard')
- grad_key_gain: float32 [128], P('shard')
- grad_ffn_gain: float32 [2048], P('shard')
- grad_w_router: float32 [2048, 32], P('shard')
- grad_w_gate: float32 [32, 2048, 768], P(('rep', 'shard'))
- grad_w_up: float32 [32, 2048, 768], P(('rep', 'shard'))
- grad_w_down: float32 [32, 768, 2048], P(('rep', 'shard'))
The draws below stay inside these ranges and needn't reach their ends.
Inputs may be any that keep to these rules, and one draw needn't show every extreme that they name: `segments`: each device's row never falls, and each sequence has 1 to 64 tokens. `routes`: each token names 8 different experts; among the tokens of one device no expert is named by more than 64 of them.
All inputs are finite; a program needn't handle non-finite values.
Results may differ from the reference program's by a relative error of at most 0.02.
Values may be sent and summed in bfloat16 or wider, within the bound.
A program may use at most 384 MiB of HBM per device.

```python
import math
import jax
import jax.numpy as jnp
import numpy as np
from jax import lax

MODEL_WIDTH = 2048
QUERY_HEADS = 32
KEY_VALUE_HEADS = 4
HEAD_SIZE = 128
FFE = 768
TOP = 8
SEQS_DEV = 8
TOK_DEV = 128
EXPERTS = 32
TOKENS = 4096
CAP = 64
SEQ_MOST = 64
N_REP = 8
N_SHARD = 4


def block_levels(stream_key, dims, split, least, high):
    def one(axis_at, blocks):
        steps = jax.random.uniform(jax.random.fold_in(jax.random.fold_in(stream_key, 6), axis_at), (blocks,), jnp.float32, least / len(split), high / len(split))
        return jnp.repeat(jnp.exp(steps), dims[axis_at] // blocks).reshape((-1,) + (1,) * (len(dims) - axis_at - 1))

    level = one(*split[0])
    for cut in split[1:]:
        level = level * one(*cut)
    return level


def profile(amount, total, bound, skew):
    loads = [(1 << 20) // math.isqrt(grade ** skew) + 1 for grade in range(2, amount + 1)]
    surplus, given = total - bound - (amount - 1), [1] * (amount - 1)
    while surplus > 0:
        candidates = [i for i in range(amount - 1) if given[i] < bound]
        whole, remaining = sum([loads[i] for i in candidates]), surplus
        for i in candidates:
            addition = min(bound - given[i], max(1, remaining * loads[i] // whole), surplus)
            given[i] = given[i] + addition
            surplus = surplus - addition
    return np.array([bound] + given)


def ragged(stream_key, amount, total, bound, lean):
    if amount == 2:
        one = jax.random.randint(stream_key, (), max(1, total - bound), min(bound, total - 1) + 1)
        return jnp.stack([one, total - one])
    tallies = jnp.asarray(profile(amount, total, bound, lean), jnp.int32)
    pairs = (amount - 1) // 2
    donor, sink = tallies[1:1 + 2 * pairs:2], tallies[2:2 + 2 * pairs:2]
    margin = jnp.minimum(donor - 1, bound - sink)
    shifted = jax.random.randint(jax.random.fold_in(stream_key, 1), (pairs,), 0, 1 << 20) % (margin + 1)
    tallies = tallies.at[1:1 + 2 * pairs:2].set(donor - shifted).at[2:2 + 2 * pairs:2].set(sink + shifted)
    return tallies[jax.random.permutation(jax.random.fold_in(stream_key, 2), amount)]


def shared_out(stream_key, own, number, rows, count, top, most, lean):
    order = jax.random.permutation(stream_key, count)
    heavy_load, ordinary = load_shares(count, rows * top, most, lean, True), load_shares(count, rows * top, most, lean, False)
    places = jnp.arange(count)

    def named(sizes, turn):
        used = int((sizes > 0).sum())
        fixed = max(1, used // 4)
        moved = fixed + (places - fixed + turn * (used - fixed)) % max(1, count - fixed)
        return jnp.zeros((count,), jnp.int32).at[order[jnp.where(places < fixed, places, moved)]].set(jnp.asarray(sizes, jnp.int32))

    sizes = jnp.where(number % 4 == 0, named(heavy_load, number // 4), named(ordinary, number - number // 4 - 1))
    mixed = jax.random.permutation(jax.random.fold_in(own, 3), count)
    giver, taker = mixed[0:count // 2 * 2:2], mixed[1:count // 2 * 2:2]
    slack = jnp.minimum(sizes[giver] - 1, most - sizes[taker]) // 2
    slack = jnp.where((giver == order[0]) | (taker == order[0]) | (sizes[taker] == 0), 0, jnp.maximum(slack, 0))
    moved = jax.random.randint(jax.random.fold_in(own, 4), (count // 2,), 0, 1 << 20) % (slack + 1)
    sizes = sizes.at[giver].add(-moved).at[taker].add(moved)
    items = jnp.searchsorted(jnp.cumsum(sizes), jnp.arange(rows * top), side="right").astype(jnp.int32)
    table = items.reshape(top, rows).T
    table = table[jax.random.permutation(jax.random.fold_in(own, 1), rows)]
    turn = jax.random.randint(jax.random.fold_in(own, 2), (rows, 1), 0, top)
    return jnp.take_along_axis(table, (jnp.arange(top)[None, :] + turn) % top, axis=1)


def load_shares(number_of, total, reach, lean, full):
    portions = [(1 << 20) // math.isqrt(rank ** lean) + 1 for rank in range(1, number_of + 1)]
    largest = reach if full else min(reach, max(-(-total // number_of), total * portions[0] // sum(portions)))
    least = 1 if total - largest >= number_of - 1 else 0
    given, surplus = [largest] + [least] * (number_of - 1), total - largest - least * (number_of - 1)
    while surplus > 0:
        candidates = [i for i in range(1, number_of) if given[i] < largest] or [i for i in range(1, number_of) if given[i] < reach]
        whole, left = sum([portions[i] for i in candidates]), surplus
        for i in candidates:
            more = min(reach - given[i], max(1, left * portions[i] // whole), surplus)
            given[i] = given[i] + more
            surplus = surplus - more
    return np.array(given)


def normal_values(rng, shape, spread, limit, pieces=(), kind=jnp.bfloat16):
    array = jax.random.normal(rng, shape, jnp.float32) * spread
    if len(pieces) > 0:
        array = block_levels(rng, shape, pieces, -0.22, 0.18) * array
    return jnp.clip(array, min=-limit, max=limit).astype(kind)


def setup_inputs(seed: int = 0) -> dict:
    streams_of = jax.random.split(jax.random.key(seed), 17)
    tokens = normal_values(streams_of[0], (TOKENS, MODEL_WIDTH), 1.0, 6.0, ((0, 32),))
    segments = jax.vmap(lambda own: jnp.searchsorted(jnp.cumsum(ragged(own, SEQS_DEV, TOK_DEV, SEQ_MOST, 2)), jnp.arange(TOK_DEV), side="right"))(jax.random.split(streams_of[1], (N_REP * N_SHARD))).reshape((N_REP * N_SHARD, TOK_DEV)).astype(jnp.int32)
    routes_keys = jax.random.split(jax.random.fold_in(streams_of[2], 1), TOKENS // TOK_DEV)
    routes_turns = jax.random.permutation(jax.random.fold_in(streams_of[2], 3), TOKENS // TOK_DEV)
    routes = jax.vmap(lambda own, number: shared_out(jax.random.fold_in(streams_of[2], 2), own, number, TOK_DEV, EXPERTS, TOP, CAP, 2))(routes_keys, routes_turns).reshape((TOKENS, TOP))
    attn_gain = jnp.clip(1.0 + 0.1 * jax.random.normal(streams_of[3], (MODEL_WIDTH,), jnp.float32), 0.5, 1.5).astype(jnp.bfloat16)
    w_query = normal_values(streams_of[4], (MODEL_WIDTH, QUERY_HEADS * HEAD_SIZE), MODEL_WIDTH ** -0.5, 0.125, ((0, 4),))
    key_weight = normal_values(streams_of[5], (MODEL_WIDTH, KEY_VALUE_HEADS * HEAD_SIZE), MODEL_WIDTH ** -0.5, 0.125, ((0, 4),))
    value_weight = normal_values(streams_of[6], (MODEL_WIDTH, KEY_VALUE_HEADS * HEAD_SIZE), MODEL_WIDTH ** -0.5, 0.125, ((0, 4),))
    w_out = normal_values(streams_of[7], (QUERY_HEADS * HEAD_SIZE, MODEL_WIDTH), (QUERY_HEADS * HEAD_SIZE // 64) ** -0.5, 0.75, ((0, 4),))
    query_gain = jnp.clip(1.0 + 0.18 * jax.random.normal(streams_of[8], (HEAD_SIZE,), jnp.float32), 0.099609375, 1.8984375).astype(jnp.bfloat16)
    key_gain = jnp.clip(1.0 + 0.18 * jax.random.normal(streams_of[9], (HEAD_SIZE,), jnp.float32), 0.099609375, 1.8984375).astype(jnp.bfloat16)
    ffn_gain = jnp.clip(1.0 + 0.1 * jax.random.normal(streams_of[10], (MODEL_WIDTH,), jnp.float32), 0.5, 1.5).astype(jnp.bfloat16)
    w_router = normal_values(streams_of[11], (MODEL_WIDTH, EXPERTS), MODEL_WIDTH ** -0.5, 0.125, ((0, 4),))
    w_gate = normal_values(streams_of[12], (EXPERTS, MODEL_WIDTH, FFE), MODEL_WIDTH ** -0.5, 0.125, ((0, 32),))
    w_up = normal_values(streams_of[13], (EXPERTS, MODEL_WIDTH, FFE), MODEL_WIDTH ** -0.5, 0.125, ((0, 32),))
    w_down = normal_values(streams_of[14], (EXPERTS, FFE, MODEL_WIDTH), (FFE // 16) ** -0.5, 0.875, ((0, 32),))
    cotangent = normal_values(streams_of[15], (TOKENS, MODEL_WIDTH), 1.0, 6.0, ((0, 32),))
    return dict(tokens=tokens, segments=segments, routes=routes, attn_gain=attn_gain, w_query=w_query, key_weight=key_weight, value_weight=value_weight, w_out=w_out, query_gain=query_gain, key_gain=key_gain, ffn_gain=ffn_gain, w_router=w_router, w_gate=w_gate, w_up=w_up, w_down=w_down, cotangent=cotangent)


epsilon = 1e-06
rope_base = 1000000.0
masked_score = -1e+30

def inverse_rms(values):
    return lax.rsqrt(lax.optimization_barrier(jnp.mean(values * values, axis=-1, keepdims=True)) + epsilon)

def widen(values):
    return lax.optimization_barrier(values).astype(jnp.float32)

def rotate(values):
    half = values.shape[-1] // 2
    return jnp.concatenate([-values[..., half:], values[..., :half]], axis=-1)

def rope_tables(segment_row, width):
    length = segment_row.shape[0]
    places = jnp.arange(length, dtype=jnp.int32)
    same = segment_row[:, None] == segment_row[None, :]
    first = lax.optimization_barrier(jnp.min(jnp.where(same, places[None, :], length), axis=1))
    offset = (places - first).astype(jnp.float32)
    half = width // 2
    frequency = rope_base ** (-2.0 * jnp.arange(half, dtype=jnp.float32) / width)
    angle = offset[:, None] * frequency[None, :]
    cosine = jnp.concatenate([jnp.cos(angle), jnp.cos(angle)], axis=1)[:, None, :]
    sine = jnp.concatenate([jnp.sin(angle), jnp.sin(angle)], axis=1)[:, None, :]
    allowed = same & (places[None, :] <= places[:, None])
    return (cosine, sine, allowed)

def norm_back(grad_scaled, unit, inverse, gain):
    gained = grad_scaled * gain
    return inverse * (gained - unit * lax.optimization_barrier(jnp.mean(gained * unit, axis=-1, keepdims=True)))

def score_block(query_rot, key_rot, allowed, kv_heads, group):
    length, heads, head_dim = query_rot.shape
    grouped = widen(query_rot).reshape(length, kv_heads, group, head_dim)
    scores = jnp.einsum('tkgh,skh->kgts', grouped, widen(key_rot)) * head_dim ** (-0.5)
    return jnp.where(allowed[None, None], scores, masked_score)

def attention_forward(block, segment_row, weights):
    gain_one, w_query, key_weight, value_weight, w_out, query_gain, key_gain = weights
    length = block.shape[0]
    head_dim = query_gain.shape[0]
    heads = w_query.shape[1] // head_dim
    kv_heads = key_weight.shape[1] // head_dim
    group = heads // kv_heads
    wide_tokens = block.astype(jnp.float32)
    inverse_one = inverse_rms(wide_tokens)
    normed_one = wide_tokens * inverse_one
    hidden_in = (normed_one * gain_one.astype(jnp.float32)).astype(jnp.bfloat16)
    query_raw = jnp.dot(hidden_in, w_query, preferred_element_type=jnp.float32).reshape(length, heads, head_dim)
    key_raw = jnp.dot(hidden_in, key_weight, preferred_element_type=jnp.float32).reshape(length, kv_heads, head_dim)
    values = jnp.dot(hidden_in, value_weight, preferred_element_type=jnp.float32).astype(jnp.bfloat16).reshape(length, kv_heads, head_dim)
    inverse_query = inverse_rms(query_raw)
    query_unit = query_raw * inverse_query
    inverse_key = inverse_rms(key_raw)
    key_unit = key_raw * inverse_key
    cosine, sine, allowed = rope_tables(segment_row, head_dim)
    query_scaled = query_unit * query_gain.astype(jnp.float32)
    key_scaled = key_unit * key_gain.astype(jnp.float32)
    query_rot = (query_scaled * cosine + rotate(query_scaled) * sine).astype(jnp.bfloat16)
    key_rot = (key_scaled * cosine + rotate(key_scaled) * sine).astype(jnp.bfloat16)
    scores = score_block(query_rot, key_rot, allowed, kv_heads, group)
    highest = lax.optimization_barrier(jnp.max(scores, axis=-1, keepdims=True))
    log_total = highest + jnp.log(lax.optimization_barrier(jnp.sum(jnp.exp(scores - highest), axis=-1, keepdims=True)))
    probs_low = jnp.exp(scores - log_total).astype(jnp.bfloat16)
    mixed = jnp.einsum('kgts,skh->tkgh', widen(probs_low), widen(values))
    attn_out = mixed.reshape(length, heads * head_dim).astype(jnp.bfloat16)
    resid = wide_tokens + jnp.dot(attn_out, w_out, preferred_element_type=jnp.float32)
    return (inverse_one, normed_one, hidden_in, values, inverse_query, query_unit, inverse_key, key_unit, cosine, sine, allowed, query_rot, key_rot, log_total, attn_out, resid)

def attention_backward(saved, grad_resid, weights):
    gain_one, w_query, key_weight, value_weight, w_out, query_gain, key_gain = weights
    inverse_one, normed_one, hidden_in, values, inverse_query, query_unit, inverse_key, key_unit, cosine, sine, allowed, query_rot, key_rot, log_total, attn_out, resid = saved
    length, heads, head_dim = query_rot.shape
    kv_heads = key_rot.shape[1]
    group = heads // kv_heads
    grad_attn = grad_resid.astype(jnp.bfloat16)
    grad_w_out = jnp.dot(attn_out.T, grad_attn, preferred_element_type=jnp.float32)
    grad_mixed = jnp.dot(grad_attn, w_out.T, preferred_element_type=jnp.float32).astype(jnp.bfloat16)
    grad_mixed = grad_mixed.reshape(length, kv_heads, group, head_dim)
    scores = score_block(query_rot, key_rot, allowed, kv_heads, group)
    probs = jnp.exp(scores - log_total)
    grad_weights = jnp.einsum('tkgh,skh->kgts', widen(grad_mixed), widen(values))
    centre = lax.optimization_barrier(jnp.sum(probs * grad_weights, axis=-1, keepdims=True))
    grad_scores = (probs * (grad_weights - centre) * head_dim ** (-0.5)).astype(jnp.bfloat16)
    grad_values = jnp.einsum('kgts,tkgh->skh', widen(probs.astype(jnp.bfloat16)), widen(grad_mixed))
    grad_query_rot = jnp.einsum('kgts,skh->tkgh', widen(grad_scores), widen(key_rot)).reshape(length, heads, head_dim)
    grad_key_rot = jnp.einsum('kgts,tkgh->skh', widen(grad_scores), widen(query_rot).reshape(length, kv_heads, group, head_dim))
    grad_query_scaled = grad_query_rot * cosine - rotate(grad_query_rot * sine)
    grad_key_scaled = grad_key_rot * cosine - rotate(grad_key_rot * sine)
    grad_query_gain = lax.optimization_barrier(jnp.sum(grad_query_scaled * query_unit, axis=(0, 1)))
    grad_key_gain = lax.optimization_barrier(jnp.sum(grad_key_scaled * key_unit, axis=(0, 1)))
    grad_query = norm_back(grad_query_scaled, query_unit, inverse_query, query_gain.astype(jnp.float32))
    grad_query = grad_query.reshape(length, heads * head_dim).astype(jnp.bfloat16)
    grad_key = norm_back(grad_key_scaled, key_unit, inverse_key, key_gain.astype(jnp.float32))
    grad_key = grad_key.reshape(length, kv_heads * head_dim).astype(jnp.bfloat16)
    grad_value = grad_values.reshape(length, kv_heads * head_dim).astype(jnp.bfloat16)
    grad_w_query = jnp.dot(hidden_in.T, grad_query, preferred_element_type=jnp.float32)
    grad_w_key = jnp.dot(hidden_in.T, grad_key, preferred_element_type=jnp.float32)
    grad_w_value = jnp.dot(hidden_in.T, grad_value, preferred_element_type=jnp.float32)
    grad_hidden_in = jnp.dot(grad_query, w_query.T, preferred_element_type=jnp.float32) + jnp.dot(grad_key, key_weight.T, preferred_element_type=jnp.float32) + jnp.dot(grad_value, value_weight.T, preferred_element_type=jnp.float32)
    grad_attn_gain = lax.optimization_barrier(jnp.sum(grad_hidden_in * normed_one, axis=0))
    grad_tokens = grad_resid + norm_back(grad_hidden_in, normed_one, inverse_one, gain_one.astype(jnp.float32))
    return (grad_tokens, (grad_attn_gain, grad_w_query, grad_w_key, grad_w_value, grad_w_out, grad_query_gain, grad_key_gain))

def block_slots(route_block):
    flat_routes = route_block.reshape(-1)
    onehot = (flat_routes[:, None] == jnp.arange(EXPERTS, dtype=jnp.int32)[None, :]).astype(jnp.int32)
    before = jnp.cumsum(onehot, axis=0, dtype=jnp.int32) - onehot
    return lax.optimization_barrier(jnp.sum(before * onehot, axis=1)).astype(jnp.int32)

def reference(tokens, segments, routes, attn_gain, w_query, key_weight, value_weight, w_out, query_gain, key_gain, ffn_gain, w_router, w_gate, w_up, w_down, cotangent):
    device_count = N_REP * N_SHARD
    weights = (attn_gain, w_query, key_weight, value_weight, w_out, query_gain, key_gain)
    token_blocks = tokens.reshape(device_count, TOK_DEV, MODEL_WIDTH)

    def forward_block(state, item):
        block, segment_row = item
        saved = attention_forward(block, segment_row, weights)
        resid = saved[-1]
        normed_two = resid * inverse_rms(resid)
        hidden_two = (normed_two * ffn_gain.astype(jnp.float32)).astype(jnp.bfloat16)
        return (state, (resid, hidden_two))
    _, (resid_all, hidden_all) = lax.scan(forward_block, jnp.zeros((), jnp.float32), (token_blocks, segments))
    resid_all = resid_all.reshape(TOKENS, MODEL_WIDTH)
    hidden_all = hidden_all.reshape(TOKENS, MODEL_WIDTH)
    inverse_two = inverse_rms(resid_all)
    normed_two = resid_all * inverse_two
    logits = jnp.dot(hidden_all, w_router, preferred_element_type=jnp.float32)
    gate_probs = jax.nn.softmax(logits, axis=-1)
    chosen = routes[:, :, None] == jnp.arange(EXPERTS, dtype=jnp.int32)[None, None, :]
    picked = lax.optimization_barrier(jnp.sum(jnp.where(chosen, gate_probs[:, None, :], 0.0), axis=-1))
    picked_total = lax.optimization_barrier(jnp.sum(picked, axis=-1, keepdims=True))
    mix_weights = picked / picked_total
    slots = lax.map(block_slots, routes.reshape(device_count, TOK_DEV, TOP)).reshape(-1)
    flat_routes = routes.reshape(-1)
    pair_index = jnp.arange(TOKENS * TOP, dtype=jnp.int32)
    owner = pair_index // (TOK_DEV * TOP)
    place = flat_routes * (device_count * CAP) + owner * CAP + slots
    table = jnp.full((EXPERTS * device_count * CAP,), TOKENS * TOP, dtype=jnp.int32)
    table = table.at[place].set(pair_index).reshape(EXPERTS, device_count * CAP)
    zero_row = jnp.zeros((1, MODEL_WIDTH), jnp.bfloat16)
    hidden_pad = jnp.concatenate([hidden_all, zero_row], axis=0)
    grad_pad = jnp.concatenate([cotangent, zero_row], axis=0)
    weight_pad = jnp.concatenate([mix_weights.reshape(-1), jnp.zeros((1,), jnp.float32)])

    def expert_step(carry, item):
        moe_sum, grad_hidden, grad_mix = carry
        pairs, gate_weight, up_weight, down_weight = item
        rows = pairs // TOP
        inputs = hidden_pad[rows]
        weight = weight_pad[pairs][:, None]
        gate = jnp.dot(inputs, gate_weight, preferred_element_type=jnp.float32)
        up = jnp.dot(inputs, up_weight, preferred_element_type=jnp.float32)
        sigmoid_gate = jax.nn.sigmoid(gate)
        activated = (gate * sigmoid_gate * up).astype(jnp.bfloat16)
        produced = jnp.dot(activated, down_weight, preferred_element_type=jnp.float32).astype(jnp.bfloat16)
        produced_wide = produced.astype(jnp.float32)
        moe_sum = moe_sum.at[rows].add(weight * produced_wide)
        grad_rows_out = grad_pad[rows].astype(jnp.float32)
        grad_mix = grad_mix.at[pairs].add(lax.optimization_barrier(jnp.sum(grad_rows_out * produced_wide, axis=1)))
        grad_pair = (weight * grad_rows_out).astype(jnp.bfloat16)
        grad_act = jnp.dot(grad_pair, down_weight.T, preferred_element_type=jnp.float32)
        grad_down = jnp.dot(activated.T, grad_pair, preferred_element_type=jnp.float32)
        grad_gate = (grad_act * up * sigmoid_gate * (1.0 + gate * (1.0 - sigmoid_gate))).astype(jnp.bfloat16)
        grad_up = (grad_act * gate * sigmoid_gate).astype(jnp.bfloat16)
        grad_gate_w = jnp.dot(inputs.T, grad_gate, preferred_element_type=jnp.float32)
        grad_up_w = jnp.dot(inputs.T, grad_up, preferred_element_type=jnp.float32)
        grad_in = (jnp.dot(grad_gate, gate_weight.T, preferred_element_type=jnp.float32) + jnp.dot(grad_up, up_weight.T, preferred_element_type=jnp.float32)).astype(jnp.bfloat16)
        grad_hidden = grad_hidden.at[rows].add(grad_in.astype(jnp.float32))
        return ((moe_sum, grad_hidden, grad_mix), (grad_gate_w, grad_up_w, grad_down))
    start = (jnp.zeros((TOKENS + 1, MODEL_WIDTH), jnp.float32), jnp.zeros((TOKENS + 1, MODEL_WIDTH), jnp.float32), jnp.zeros((TOKENS * TOP + 1,), jnp.float32))
    (moe_sum, grad_hidden, grad_mix), (grad_w_gate, grad_w_up, grad_w_down) = lax.scan(expert_step, start, (table, w_gate, w_up, w_down))
    output = (resid_all + moe_sum[:TOKENS]).astype(jnp.bfloat16)
    grad_mix = grad_mix[:TOKENS * TOP].reshape(TOKENS, TOP)
    grad_picked = (grad_mix - lax.optimization_barrier(jnp.sum(grad_mix * mix_weights, axis=-1, keepdims=True))) / picked_total
    grad_probs = lax.optimization_barrier(jnp.sum(jnp.where(chosen, grad_picked[:, :, None], 0.0), axis=1))
    grad_logits = (gate_probs * (grad_probs - lax.optimization_barrier(jnp.sum(grad_picked * picked, axis=-1, keepdims=True)))).astype(jnp.bfloat16)
    grad_w_router = jnp.dot(hidden_all.T, grad_logits, preferred_element_type=jnp.float32)
    grad_hidden_two = grad_hidden[:TOKENS] + jnp.dot(grad_logits, w_router.T, preferred_element_type=jnp.float32)
    grad_ffn_gain = lax.optimization_barrier(jnp.sum(grad_hidden_two * normed_two, axis=0))
    grad_resid = cotangent.astype(jnp.float32) + norm_back(grad_hidden_two, normed_two, inverse_two, ffn_gain.astype(jnp.float32))

    def backward_block(carry, item):
        block, segment_row, grad_block = item
        saved = attention_forward(block, segment_row, weights)
        grad_tokens_block, grads = attention_backward(saved, grad_block, weights)
        return (jax.tree.map(jnp.add, carry, grads), grad_tokens_block)
    zero_filled = (jnp.zeros((MODEL_WIDTH,), jnp.float32), jnp.zeros((MODEL_WIDTH, QUERY_HEADS * HEAD_SIZE), jnp.float32), jnp.zeros((MODEL_WIDTH, KEY_VALUE_HEADS * HEAD_SIZE), jnp.float32), jnp.zeros((MODEL_WIDTH, KEY_VALUE_HEADS * HEAD_SIZE), jnp.float32), jnp.zeros((QUERY_HEADS * HEAD_SIZE, MODEL_WIDTH), jnp.float32), jnp.zeros((HEAD_SIZE,), jnp.float32), jnp.zeros((HEAD_SIZE,), jnp.float32))
    sums, grad_tokens = lax.scan(backward_block, zero_filled, (token_blocks, segments, grad_resid.reshape(device_count, TOK_DEV, MODEL_WIDTH)))
    grad_attn_gain, grad_w_query, grad_w_key, grad_w_value, grad_w_out, grad_query_gain, grad_key_gain = sums
    return (output, grad_tokens.reshape(TOKENS, MODEL_WIDTH), grad_attn_gain, grad_w_query, grad_w_key, grad_w_value, grad_w_out, grad_query_gain, grad_key_gain, grad_ffn_gain, grad_w_router, grad_w_gate, grad_w_up, grad_w_down)
```

```python
import functools
import jax
import jax.numpy as jnp
from jax import lax
from jax.experimental import pallas as pl
from jax.experimental.pallas import tpu as pltpu
from jax.sharding import PartitionSpec as P

bf16 = jnp.bfloat16
f32 = jnp.float32
vmem_cap = 62 * 1024 * 1024
epsilon = 1e-06
rope_base = 1000000.0
masked_score = -1e30


class Grid:
    def __init__(self, reps, shards):
        self.reps, self.shards = reps, shards
        self.devices = reps * shards
        self.places = reps // 2
        self.los = self.places // 2

    def here(self):
        self.r = lax.axis_index("rep")
        self.z = lax.axis_index("shard")
        self.core = self.r % 2
        place = self.r // 2
        self.hi = place // self.los
        self.lo = place % self.los
        return self

    def rep_of(self, hi, lo, core):
        return (hi * self.los + lo) * 2 + core

    def device(self, rep, shard):
        return {"rep": rep, "shard": shard}

    def other_lo(self, step):
        return (self.lo + step) % self.los

    def nearest(self):
        n = self.shards
        rows = [sorted(range(n), key=lambda p: (abs(p - z), p)) for z in range(n)]
        return [pick(self.z, [rows[z][turn] for z in range(n)]) for turn in range(n)]


def pick(index, values):
    out = jnp.int32(values[0])
    for i in range(1, len(values)):
        out = jnp.where(index == i, jnp.int32(values[i]), out)
    return out


class Sends:
    def __init__(self, sems):
        self.sems, self.used, self.open = sems, 0, []

    def start(self, src, dst, recv, device, when=None):
        copy = pltpu.make_async_remote_copy(
            src_ref=src,
            dst_ref=dst,
            send_sem=self.sems.at[self.used],
            recv_sem=recv,
            device_id=device,
            device_id_type=pl.DeviceIdType.MESH,
        )
        self.used += 1
        self.open.append((copy, when))
        if when is None:
            copy.start()
        else:
            pl.when(when)(copy.start)

    def arrived(self, dst, recv, device, when=None):
        copy = pltpu.make_async_remote_copy(
            src_ref=dst,
            dst_ref=dst,
            send_sem=self.sems.at[0],
            recv_sem=recv,
            device_id=device,
            device_id_type=pl.DeviceIdType.MESH,
        )
        if when is None:
            copy.wait_recv()
        else:
            pl.when(when)(copy.wait_recv)

    def drain(self):
        for copy, when in self.open:
            if when is None:
                copy.wait_send()
            else:
                pl.when(when)(copy.wait_send)
        self.open = []


def greet_line(g):
    barrier = pltpu.get_barrier_semaphore()
    for step in range(1, g.shards):
        pl.semaphore_signal(
            barrier,
            inc=1,
            device_id=g.device(g.r, (g.z + step) % g.shards),
            device_id_type=pl.DeviceIdType.MESH,
        )
    pl.semaphore_wait(barrier, g.shards - 1)


def greet_all(g):
    barrier = pltpu.get_barrier_semaphore()
    me = g.r * g.shards + g.z

    def one(step, carry):
        peer = (me + step) % g.devices
        pl.semaphore_signal(
            barrier,
            inc=1,
            device_id=g.device(peer // g.shards, peer % g.shards),
            device_id_type=pl.DeviceIdType.MESH,
        )
        return carry

    lax.fori_loop(1, g.devices, one, 0)
    pl.semaphore_wait(barrier, g.devices - 1)


def push_rows(g, src, dst, send_sems, recv_sems):
    me = g.r * g.shards + g.z

    def one(step, carry):
        peer = (me + step) % g.devices
        pltpu.make_async_remote_copy(
            src_ref=src.at[peer],
            dst_ref=dst.at[me],
            send_sem=send_sems.at[step],
            recv_sem=recv_sems.at[step],
            device_id=g.device(peer // g.shards, peer % g.shards),
            device_id_type=pl.DeviceIdType.MESH,
        ).start()
        return carry

    lax.fori_loop(1, g.devices, one, 0)


def push_wait(g, src, dst, send_sems, recv_sems):
    me = g.r * g.shards + g.z

    def one(step, carry):
        peer = (me + g.devices - step) % g.devices
        copy = pltpu.make_async_remote_copy(
            src_ref=src.at[peer],
            dst_ref=dst.at[peer],
            send_sem=send_sems.at[step],
            recv_sem=recv_sems.at[step],
            device_id=g.device(peer // g.shards, peer % g.shards),
            device_id_type=pl.DeviceIdType.MESH,
        )
        copy.wait_send()
        copy.wait_recv()
        return carry

    lax.fori_loop(1, g.devices, one, 0)


def gather_all_kernel(reps, shards, x_ref, slab_ref, out_ref, slabs_ref, sems, zr, lr, hr, dr, cr, ps, pr, ls):
    g = Grid(reps, shards).here()
    s = Sends(sems)
    rows = x_ref.shape[0]
    half = rows // 2
    n = g.shards
    parts = (pl.ds(0, half), pl.ds(half, half))
    order = g.nearest()

    def block(hi, lo, core, zp):
        return out_ref.at[g.rep_of(hi, lo, core) * n + zp]

    partner = g.device(g.rep_of(g.hi, g.lo, 1 - g.core), g.z)
    far = 1 - g.hi

    def at(hi, lo):
        return g.device(g.rep_of(hi, lo, g.core), g.z)

    keep = pltpu.make_async_copy(x_ref, block(g.hi, g.lo, g.core, g.z), ls.at[0])
    keep.start()
    greet_all(g)
    push_rows(g, slab_ref, slabs_ref, ps, pr)
    me = g.r * n + g.z
    keep_slab = pltpu.make_async_copy(slab_ref.at[me], slabs_ref.at[me], ls.at[1])
    keep_slab.start()

    def own_line(turn):
        zp = order[turn]
        dst = block(g.hi, g.lo, g.core, zp)
        if turn == 0:
            src = x_ref
        else:
            src = dst
            s.arrived(dst, zr.at[zp], g.device(g.r, zp))
        s.start(src, dst, zr.at[zp], g.device(g.r, jnp.minimum(g.z + 1, n - 1)), (zp <= g.z) & (g.z + 1 < n))
        s.start(src, dst, zr.at[zp], g.device(g.r, jnp.maximum(g.z - 1, 0)), (zp >= g.z) & (g.z > 0))
        for part in (0, 1):
            for step in range(1, g.los):
                s.start(src.at[parts[part]], dst.at[parts[part]], lr.at[zp, part, step - 1], at(g.hi, g.other_lo(step)))
            s.start(src.at[parts[1 - part]], dst.at[parts[1 - part]], hr.at[zp, 1 - part], at(far, g.lo))
        s.start(src, dst, cr.at[zp, 0], partner)

    def first(turn):
        zp = order[turn]
        for step in range(1, g.los):
            frm = (g.lo + g.los - step) % g.los
            dst = block(g.hi, frm, g.core, zp)
            s.arrived(dst.at[parts[0]], lr.at[zp, 0, step - 1], at(g.hi, frm))
            s.start(dst.at[parts[0]], dst.at[parts[0]], dr.at[zp, 0, step - 1], at(far, g.lo))
            s.start(dst.at[parts[0]], dst.at[parts[0]], cr.at[zp, 5 * step], partner)
        dst = block(far, g.lo, g.core, zp)
        s.arrived(dst.at[parts[1]], hr.at[zp, 1], at(far, g.lo))
        for step in range(1, g.los):
            s.start(dst.at[parts[1]], dst.at[parts[1]], dr.at[zp, 1, step - 1], at(g.hi, g.other_lo(step)))
        s.start(dst.at[parts[1]], dst.at[parts[1]], cr.at[zp, 1], partner)
        for step in range(1, g.los):
            frm = (g.lo + g.los - step) % g.los
            dst = block(g.hi, frm, g.core, zp)
            s.arrived(dst.at[parts[1]], lr.at[zp, 1, step - 1], at(g.hi, frm))
            s.start(dst.at[parts[1]], dst.at[parts[1]], cr.at[zp, 5 * step + 1], partner)
        dst = block(far, g.lo, g.core, zp)
        s.arrived(dst.at[parts[0]], hr.at[zp, 0], at(far, g.lo))
        s.start(dst.at[parts[0]], dst.at[parts[0]], cr.at[zp, 2], partner)

    def second(turn):
        zp = order[turn]
        for step in range(1, g.los):
            frm = (g.lo + g.los - step) % g.los
            dst = block(far, frm, g.core, zp)
            s.arrived(dst.at[parts[0]], dr.at[zp, 0, step - 1], at(far, g.lo))
            s.start(dst.at[parts[0]], dst.at[parts[0]], cr.at[zp, 5 * step + 2], partner)
            s.arrived(dst.at[parts[1]], dr.at[zp, 1, step - 1], at(g.hi, frm))
            s.start(dst.at[parts[1]], dst.at[parts[1]], cr.at[zp, 5 * step + 3], partner)

    def from_partner(turn):
        zp = order[turn]
        other = 1 - g.core
        s.arrived(block(g.hi, g.lo, other, zp), cr.at[zp, 0], partner)
        dst = block(far, g.lo, other, zp)
        s.arrived(dst.at[parts[1]], cr.at[zp, 1], partner)
        s.arrived(dst.at[parts[0]], cr.at[zp, 2], partner)
        for step in range(1, g.los):
            frm = (g.lo + g.los - step) % g.los
            dst = block(g.hi, frm, other, zp)
            s.arrived(dst.at[parts[0]], cr.at[zp, 5 * step], partner)
            s.arrived(dst.at[parts[1]], cr.at[zp, 5 * step + 1], partner)
            dst = block(far, frm, other, zp)
            s.arrived(dst.at[parts[0]], cr.at[zp, 5 * step + 2], partner)
            s.arrived(dst.at[parts[1]], cr.at[zp, 5 * step + 3], partner)

    for turn in range(n + 2):
        if turn < n:
            own_line(turn)
        if 0 <= turn - 1 < n:
            first(turn - 1)
        if 0 <= turn - 2 < n:
            second(turn - 2)
    for turn in range(n):
        from_partner(turn)
    keep.wait()
    keep_slab.wait()
    push_wait(g, slab_ref, slabs_ref, ps, pr)
    s.drain()


def gather_all(reps, shards, x, slab, ident):
    g = Grid(reps, shards)
    n, los = shards, g.los
    per_turn = 2 + 2 * los + 1 + (3 * (los - 1)) + los + 1 + 1 + 2 * (los - 1) + los
    dma = pltpu.SemaphoreType.DMA
    return pl.pallas_call(
        functools.partial(gather_all_kernel, reps, shards),
        out_shape=(
            jax.ShapeDtypeStruct((g.devices,) + x.shape, x.dtype),
            jax.ShapeDtypeStruct(slab.shape, slab.dtype),
        ),
        in_specs=[pl.BlockSpec(memory_space=pltpu.VMEM)] * 2,
        out_specs=(pl.BlockSpec(memory_space=pl.ANY), pl.BlockSpec(memory_space=pltpu.VMEM)),
        scratch_shapes=[
            dma((n * (per_turn + 4),)),
            dma((n,)),
            dma((n, 2, max(1, los - 1))),
            dma((n, 2)),
            dma((n, 2, max(1, los - 1))),
            dma((n, 5 * los)),
            dma((g.devices,)),
            dma((g.devices,)),
            dma((2,)),
        ],
        compiler_params=pltpu.CompilerParams(collective_id=ident, has_side_effects=True, vmem_limit_bytes=vmem_cap),
        name="gather_all",
    )(x, slab)


def add_rows(dst, *srcs, rows):
    def one(i, carry):
        at = pl.ds(pl.multiple_of(i * 16, 16), 16)
        total = srcs[0][at, :].astype(f32)
        for src in srcs[1:]:
            total = total + src[at, :].astype(f32)
        dst[at, :] = total.astype(dst.dtype)
        return carry

    lax.fori_loop(0, rows // 16, one, 0)


def scatter_all_kernel(reps, shards, slabbed, *refs):
    if slabbed:
        p_ref, slab_ref, out_ref, slabs_ref, *rest = refs
    else:
        p_ref, out_ref, *rest = refs
    own, ra, rb0, rb1, rc0, rc1, rl, rr, sems, sa, sb0, sb1, sc0, sc1, sl, sr, ps, pr, ls = rest
    g = Grid(reps, shards).here()
    s = Sends(sems)
    n, los = g.shards, g.los
    rows = out_ref.shape[0]
    half = rows // 2
    top, bottom = pl.ds(0, half), pl.ds(half, half)
    order = g.nearest()[::-1]
    partner = g.device(g.rep_of(g.hi, g.lo, 1 - g.core), g.z)
    far = 1 - g.hi

    def at(hi, lo):
        return g.device(g.rep_of(hi, lo, g.core), g.z)

    loads = []
    for turn in range(n):
        load = pltpu.make_async_copy(p_ref.at[:, g.core, order[turn]], own.at[turn], ls.at[turn])
        load.start()
        loads.append(load)
    greet_all(g)
    if slabbed:
        push_rows(g, slab_ref, slabs_ref, ps, pr)
        me = g.r * n + g.z
        keep_slab = pltpu.make_async_copy(slab_ref.at[me], slabs_ref.at[me], ls.at[n])
        keep_slab.start()
    for turn in range(n):
        s.start(p_ref.at[:, 1 - g.core, order[turn]], ra.at[turn], sa.at[turn], partner)

    def stage_a(turn):
        loads[turn].wait()
        s.arrived(ra.at[turn], sa.at[turn], partner)

        def one(i, carry):
            a = pl.ds(pl.multiple_of(i * 16, 16), 16)
            for q in range(g.places):
                own[turn, q, a, :] = (own[turn, q, a, :].astype(f32) + ra[turn, q, a, :].astype(f32)).astype(own.dtype)
            return carry

        lax.fori_loop(0, rows // 16, one, 0)
        s.start(own.at[turn, pl.ds(far * los, los), top], rb0.at[turn], sb0.at[turn], at(far, g.lo))
        for step in range(1, los):
            to = g.other_lo(step)
            for hi in range(2):
                s.start(own.at[turn, hi * los + to, bottom], rb1.at[turn, step - 1, hi], sb1.at[turn, step - 1, hi], at(g.hi, to))

    def stage_b(turn):
        s.arrived(rb0.at[turn], sb0.at[turn], at(far, g.lo))
        for lo in range(los):
            line = own.at[turn, g.hi * los + lo, top]
            add_rows(line, line, rb0.at[turn, lo], rows=half)
        for step in range(1, los):
            frm = (g.lo + los - step) % los
            for hi in range(2):
                s.arrived(rb1.at[turn, step - 1, hi], sb1.at[turn, step - 1, hi], at(g.hi, frm))
        for hi in range(2):
            line = own.at[turn, hi * los + g.lo, bottom]
            add_rows(line, line, *[rb1.at[turn, step, hi] for step in range(los - 1)], rows=half)
        for step in range(1, los):
            to = g.other_lo(step)
            s.start(own.at[turn, g.hi * los + to, top], rc0.at[turn, step - 1], sc0.at[turn, step - 1], at(g.hi, to))
        s.start(own.at[turn, far * los + g.lo, bottom], rc1.at[turn], sc1.at[turn], at(far, g.lo))

    def stage_c(turn):
        mine = g.hi * los + g.lo
        for step in range(1, los):
            s.arrived(rc0.at[turn, step - 1], sc0.at[turn, step - 1], at(g.hi, (g.lo + los - step) % los))
        line = own.at[turn, mine, top]
        add_rows(line, line, *[rc0.at[turn, step] for step in range(los - 1)], rows=half)
        s.arrived(rc1.at[turn], sc1.at[turn], at(far, g.lo))
        line = own.at[turn, mine, bottom]
        add_rows(line, line, rc1.at[turn], rows=half)
        send_line(g, s, order[turn], own.at[turn, mine], out_ref, rl, rr, sl, sr, last=turn == n - 1)

    for turn in range(n + 2):
        if turn < n:
            stage_a(turn)
        if 0 <= turn - 1 < n:
            stage_b(turn - 1)
        if 0 <= turn - 2 < n:
            stage_c(turn - 2)
    if slabbed:
        keep_slab.wait()
        push_wait(g, slab_ref, slabs_ref, ps, pr)
    s.drain()


def send_line(g, s, zp, line, out_ref, rl, rr, sl, sr, last):
    n, rows = g.shards, line.shape[0]
    left, right = g.device(g.r, jnp.maximum(g.z - 1, 0)), g.device(g.r, jnp.minimum(g.z + 1, n - 1))
    has_left, has_right = g.z > 0, g.z + 1 < n
    if last:
        s.arrived(rl.at[g.z], sl.at[g.z], left, has_left)
        s.arrived(rr.at[g.z], sr.at[g.z], right, has_right)

        @pl.when(has_left & has_right)
        def _():
            add_rows(out_ref, line, rl.at[g.z], rr.at[g.z], rows=rows)

        @pl.when(has_left & jnp.logical_not(has_right))
        def _():
            add_rows(out_ref, line, rl.at[g.z], rows=rows)

        @pl.when(has_right & jnp.logical_not(has_left))
        def _():
            add_rows(out_ref, line, rr.at[g.z], rows=rows)
    else:
        onward_right, onward_left = zp > g.z, zp < g.z

        @pl.when(onward_right & has_left)
        def _():
            s.arrived(rl.at[zp], sl.at[zp], left)
            add_rows(line, line, rl.at[zp], rows=rows)

        @pl.when(onward_left & has_right)
        def _():
            s.arrived(rr.at[zp], sr.at[zp], right)
            add_rows(line, line, rr.at[zp], rows=rows)

        s.start(line, rl.at[zp], sl.at[zp], right, onward_right)
        s.start(line, rr.at[zp], sr.at[zp], left, onward_left)


def scatter_all(reps, shards, p, slab, ident):
    g = Grid(reps, shards)
    n, los, places = shards, g.los, g.places
    _, rows, width = p.shape
    half = rows // 2
    lo_others = max(1, los - 1)
    dma = pltpu.SemaphoreType.DMA
    v = pltpu.VMEM
    slabbed = slab is not None
    out_shape = (jax.ShapeDtypeStruct((rows, width), f32),)
    if slabbed:
        out_shape += (jax.ShapeDtypeStruct(slab.shape, slab.dtype),)
    vmem = pl.BlockSpec(memory_space=pltpu.VMEM)
    done = pl.pallas_call(
        functools.partial(scatter_all_kernel, reps, shards, slabbed),
        out_shape=out_shape,
        in_specs=[pl.BlockSpec(memory_space=pl.ANY)] + [vmem] * slabbed,
        out_specs=(vmem,) * len(out_shape),
        scratch_shapes=[
            v((n, places, rows, width), p.dtype),
            v((n, places, rows, width), p.dtype),
            v((n, los, half, width), p.dtype),
            v((n, lo_others, 2, half, width), p.dtype),
            v((n, lo_others, half, width), p.dtype),
            v((n, half, width), p.dtype),
            v((n, rows, width), p.dtype),
            v((n, rows, width), p.dtype),
            dma((n * (6 + 3 * los),)),
            dma((n,)),
            dma((n,)),
            dma((n, lo_others, 2)),
            dma((n, lo_others)),
            dma((n,)),
            dma((n,)),
            dma((n,)),
            dma((g.devices,)),
            dma((g.devices,)),
            dma((n + 1,)),
        ],
        compiler_params=pltpu.CompilerParams(collective_id=ident, has_side_effects=True, vmem_limit_bytes=vmem_cap),
        name="scatter_all",
    )(p.reshape(places, 2, n, rows, width), *([slab] if slabbed else []))
    return done if slabbed else done[0]


def scatter_wide(reps, shards, p, slab, ident, chunks):
    if chunks == 1:
        return scatter_all(reps, shards, p, slab, ident)
    step = p.shape[2] // chunks
    parts = [
        scatter_all(reps, shards, p[:, :, i * step : (i + 1) * step], slab if i == 0 else None, ident + i)
        for i in range(chunks)
    ]
    if slab is None:
        return jnp.concatenate(parts, axis=1)
    first, slabs = parts[0]
    return jnp.concatenate([first] + parts[1:], axis=1), slabs


def gather_line_kernel(reps, shards, x_ref, out_ref, sems, zr, ls):
    g = Grid(reps, shards).here()
    s = Sends(sems)
    n = g.shards
    order = g.nearest()
    keep = pltpu.make_async_copy(x_ref, out_ref.at[g.z], ls.at[0])
    keep.start()
    greet_line(g)
    for turn in range(n):
        zp = order[turn]
        dst = out_ref.at[zp]
        src = x_ref if turn == 0 else dst
        if turn:
            s.arrived(dst, zr.at[zp], g.device(g.r, zp))
        s.start(src, dst, zr.at[zp], g.device(g.r, jnp.minimum(g.z + 1, n - 1)), (zp <= g.z) & (g.z + 1 < n))
        s.start(src, dst, zr.at[zp], g.device(g.r, jnp.maximum(g.z - 1, 0)), (zp >= g.z) & (g.z > 0))
    keep.wait()
    s.drain()


def gather_line(reps, shards, x, ident):
    dma = pltpu.SemaphoreType.DMA
    return pl.pallas_call(
        functools.partial(gather_line_kernel, reps, shards),
        out_shape=jax.ShapeDtypeStruct((shards,) + x.shape, x.dtype),
        in_specs=[pl.BlockSpec(memory_space=pltpu.VMEM)],
        out_specs=pl.BlockSpec(memory_space=pltpu.VMEM),
        scratch_shapes=[dma((2 * shards,)), dma((shards,)), dma((1,))],
        compiler_params=pltpu.CompilerParams(collective_id=ident, has_side_effects=True),
        name="gather_line",
    )(x)


def scatter_line_kernel(reps, shards, p_ref, out_ref, own, rl, rr, sems, sl, sr, ls):
    g = Grid(reps, shards).here()
    s = Sends(sems)
    n = g.shards
    order = g.nearest()[::-1]
    loads = []
    for turn in range(n):
        load = pltpu.make_async_copy(p_ref.at[order[turn]], own.at[turn], ls.at[turn])
        load.start()
        loads.append(load)
    greet_line(g)
    for turn in range(n):
        loads[turn].wait()
        send_line(g, s, order[turn], own.at[turn], out_ref, rl, rr, sl, sr, last=turn == n - 1)
    s.drain()


def scatter_line(reps, shards, p, ident):
    dma = pltpu.SemaphoreType.DMA
    _, rows, width = p.shape
    return pl.pallas_call(
        functools.partial(scatter_line_kernel, reps, shards),
        out_shape=jax.ShapeDtypeStruct((rows, width), f32),
        in_specs=[pl.BlockSpec(memory_space=pl.ANY)],
        out_specs=pl.BlockSpec(memory_space=pltpu.VMEM),
        scratch_shapes=[
            pltpu.VMEM((shards, rows, width), p.dtype),
            pltpu.VMEM((shards, rows, width), p.dtype),
            pltpu.VMEM((shards, rows, width), p.dtype),
            dma((2 * shards,)),
            dma((shards,)),
            dma((shards,)),
            dma((shards,)),
        ],
        compiler_params=pltpu.CompilerParams(collective_id=ident, has_side_effects=True),
        name="scatter_line",
    )(p)


def inverse_rms(values):
    return lax.rsqrt(jnp.mean(values * values, axis=-1, keepdims=True) + epsilon)


def rotate(values):
    half = values.shape[-1] // 2
    return jnp.concatenate([-values[..., half:], values[..., :half]], axis=-1)


def rope_tables(segment_rows, width):
    length = segment_rows.shape[1]
    places = jnp.arange(length, dtype=jnp.int32)
    same = segment_rows[:, :, None] == segment_rows[:, None, :]
    first = jnp.min(jnp.where(same, places[None, None, :], length), axis=2)
    offset = (places[None] - first).astype(f32)
    half = width // 2
    frequency = rope_base ** (-2.0 * jnp.arange(half, dtype=f32) / width)
    angle = offset[..., None] * frequency[None, None, :]
    cosine, sine = jnp.cos(angle), jnp.sin(angle)
    cosine = jnp.concatenate([cosine, cosine], axis=-1)
    sine = jnp.concatenate([sine, sine], axis=-1)
    allowed = same & (places[None, None, :] <= places[None, :, None])
    return cosine, sine, allowed


def norm_back(grad_scaled, unit, inverse, gain):
    gained = grad_scaled * gain
    return inverse * (gained - unit * jnp.mean(gained * unit, axis=-1, keepdims=True))


def matmul(a, b, dims=((1,), (0,))):
    return lax.dot_general(a, b, (dims, ((), ())), preferred_element_type=f32)


def local(
    tokens,
    segments,
    routes,
    attn_gain,
    w_query,
    key_weight,
    value_weight,
    w_out,
    query_gain,
    key_gain,
    ffn_gain,
    w_router,
    w_gate,
    w_up,
    w_down,
    cotangent,
):
    reps, shards = lax.axis_size("rep"), lax.axis_size("shard")
    devices = reps * shards
    r, z = lax.axis_index("rep"), lax.axis_index("shard")
    length, width = tokens.shape
    deep = w_query.shape[0]
    head_dim = query_gain.shape[0] * shards
    heads = w_query.shape[1] // head_dim
    kv_heads = key_weight.shape[1] // head_dim
    experts = w_router.shape[1]
    top = routes.shape[1]
    capacity = 2 * length * top // experts
    my_heads = heads // shards
    my_kv = max(1, kv_heads // shards)
    shared_by = max(1, shards // kv_heads)
    group = my_heads // my_kv
    q_cols, kv_cols = my_heads * head_dim, my_kv * head_dim
    cols = q_cols + 2 * kv_cols
    piece = deep // reps
    chunks = max(1, devices // 32)
    part = head_dim // shards

    def column(values, rows=deep):
        return jnp.pad(values.reshape(-1, 1), ((0, rows - values.size), (0, 0)))

    small = jnp.concatenate(
        [
            w_router,
            column(attn_gain),
            column(ffn_gain),
            column(query_gain),
            column(key_gain),
            column(segments[0].astype(bf16)),
        ],
        axis=1,
    )
    small_cols = -(-small.shape[1] // 128) * 128
    small = jnp.pad(small, ((0, 0), (0, small_cols - small.shape[1])))
    small_all = gather_line(reps, shards, small, 1)
    router_full = small_all[:, :, :experts].reshape(width, experts)
    gain_one = small_all[:, :, experts].reshape(1, width).astype(f32)
    gain_two = small_all[:, :, experts + 1].reshape(1, width).astype(f32)
    qgain = small_all[:, :part, experts + 2].reshape(head_dim).astype(f32)
    kgain = small_all[:, :part, experts + 3].reshape(head_dim).astype(f32)
    segment_rows = small_all[:, :length, experts + 4].astype(jnp.int32)

    def by_shard(weight, count):
        mine = lax.dynamic_slice_in_dim(weight, r * piece, piece, 0)
        mine = mine.reshape(piece, -1, count)
        if mine.shape[1] < shards:
            mine = jnp.repeat(mine, shards // mine.shape[1], axis=1)
        return mine.transpose(1, 0, 2)

    packed = jnp.concatenate(
        [by_shard(w_query, q_cols), by_shard(key_weight, kv_cols), by_shard(value_weight, kv_cols)], axis=2
    )
    packed = lax.all_to_all(packed, "shard", split_axis=0, concat_axis=0, tiled=True)
    packed = lax.all_gather(packed, "rep", axis=0)
    w_in = packed.transpose(1, 0, 2, 3).reshape(width, cols)

    cotangents = lax.all_gather(cotangent, ("rep", "shard"), axis=0)
    block_tokens = gather_line(reps, shards, tokens, 2).reshape(shards * length, width)

    wide = block_tokens.astype(f32)
    inverse_one = inverse_rms(wide)
    normed_one = wide * inverse_one
    hidden_in = (normed_one * gain_one).astype(bf16)
    qkv = matmul(hidden_in, w_in)
    query_raw = qkv[:, :q_cols].reshape(shards, length, my_heads, head_dim)
    key_raw = qkv[:, q_cols : q_cols + kv_cols].reshape(shards, length, my_kv, head_dim)
    values = qkv[:, q_cols + kv_cols :].astype(bf16).reshape(shards, length, my_kv, head_dim)
    inverse_query = inverse_rms(query_raw)
    query_unit = query_raw * inverse_query
    inverse_key = inverse_rms(key_raw)
    key_unit = key_raw * inverse_key
    cosine, sine, allowed = rope_tables(segment_rows, head_dim)
    cosine, sine = cosine[:, :, None, :], sine[:, :, None, :]
    query_scaled = query_unit * qgain
    key_scaled = key_unit * kgain
    query_rot = (query_scaled * cosine + rotate(query_scaled) * sine).astype(bf16)
    key_rot = (key_scaled * cosine + rotate(key_scaled) * sine).astype(bf16)
    grouped = query_rot.reshape(shards, length, my_kv, group, head_dim)
    scores = jnp.einsum("btkgh,bskh->bkgts", grouped, key_rot, preferred_element_type=f32) * head_dim ** (-0.5)
    scores = jnp.where(allowed[:, None, None], scores, masked_score)
    highest = jnp.max(scores, axis=-1, keepdims=True)
    raised = jnp.exp(scores - highest)
    probs = raised / jnp.sum(raised, axis=-1, keepdims=True)
    probs_low = probs.astype(bf16)
    mixed = jnp.einsum("bkgts,bskh->btkgh", probs_low, values, preferred_element_type=f32)
    attn_out = mixed.reshape(shards * length, q_cols).astype(bf16)
    projected = matmul(attn_out, w_out).astype(bf16)
    own_tokens = tokens.astype(f32)
    resid = own_tokens + scatter_line(reps, shards, projected.reshape(shards, length, width), 3)

    inverse_two = inverse_rms(resid)
    normed_two = resid * inverse_two
    hidden_two = (normed_two * gain_two).astype(bf16)
    logits = matmul(hidden_two, router_full)
    gate_probs = jax.nn.softmax(logits, axis=-1)
    chosen = jnp.any(routes[:, :, None] == jnp.arange(experts, dtype=jnp.int32)[None, None, :], axis=1)
    picked = jnp.where(chosen, gate_probs, 0.0)
    picked_total = jnp.sum(picked, axis=-1, keepdims=True)
    mix = picked / picked_total
    slab = jnp.where(chosen, mix, -1.0).T.reshape(experts, 1, length)
    slab = jnp.broadcast_to(slab, (experts, 8, length))
    hiddens, slabs = gather_all(reps, shards, hidden_two, slab, 4)

    share = slabs[:, 0, :]
    member = share >= 0.0
    earlier = jnp.arange(length)[:, None] < jnp.arange(length)[None, :]
    slot = matmul(member.astype(bf16), earlier.astype(bf16))
    place = (jnp.arange(capacity, dtype=f32)[None, :, None] == slot[:, None, :]) & member[:, None, :]
    row_weight = jnp.sum(jnp.where(place, share[:, None, :], 0.0), axis=2, keepdims=True)
    onehot = place.astype(bf16)

    def dispatch(blocks):
        taken = jnp.einsum("bst,btd->bsd", onehot, blocks, preferred_element_type=f32)
        return taken.astype(bf16).reshape(devices * capacity, width)

    rows = dispatch(hiddens)
    row_grads = dispatch(cotangents)
    row_weight = row_weight.reshape(devices * capacity, 1)
    gate = matmul(rows, w_gate[0])
    up = matmul(rows, w_up[0])
    sigmoid_gate = jax.nn.sigmoid(gate)
    activated = (gate * sigmoid_gate * up).astype(bf16)
    produced = matmul(activated, w_down[0]).astype(bf16).astype(f32)
    row_grads = row_grads.astype(f32)
    weighted = (row_weight * produced).astype(bf16)
    row_mix = jnp.sum(row_grads * produced, axis=1).reshape(devices, capacity, 1)
    back_mix = jnp.sum(jnp.where(place, row_mix, 0.0), axis=1).reshape(devices, 1, length)
    back_mix = jnp.broadcast_to(back_mix, (devices, 8, length))
    grad_pair = (row_weight * row_grads).astype(bf16)
    grad_act = matmul(grad_pair, w_down[0], ((1,), (1,)))
    grad_gate = (grad_act * up * sigmoid_gate * (1.0 + gate * (1.0 - sigmoid_gate))).astype(bf16)
    grad_up = (grad_act * gate * sigmoid_gate).astype(bf16)
    grad_in = matmul(grad_gate, w_gate[0], ((1,), (1,))) + matmul(grad_up, w_up[0], ((1,), (1,)))
    grad_w_down = matmul(activated, grad_pair, ((0,), (0,)))
    grad_w_gate = matmul(rows, grad_gate, ((0,), (0,)))
    grad_w_up = matmul(rows, grad_up, ((0,), (0,)))

    def combine(values):
        values = values.reshape(devices, capacity, width)
        return jnp.einsum("bst,bsd->btd", onehot, values, preferred_element_type=f32).astype(bf16)

    grad_hidden, mixes = scatter_wide(reps, shards, combine(grad_in.astype(bf16)), back_mix, 8, chunks)
    output = (resid + scatter_wide(reps, shards, combine(weighted), None, 16, chunks)).astype(bf16)

    grad_out = cotangent.astype(f32)
    grad_mix = mixes[:, 0, :].T
    grad_picked = jnp.where(chosen, grad_mix - jnp.sum(grad_mix * mix, axis=-1, keepdims=True), 0.0) / picked_total
    grad_logits = (gate_probs * (grad_picked - jnp.sum(grad_picked * picked, axis=-1, keepdims=True))).astype(bf16)
    grad_hidden = grad_hidden + matmul(grad_logits, router_full, ((1,), (1,)))
    grad_ffn_gain = jnp.sum(grad_hidden * normed_two, axis=0)
    grad_resid = grad_out + norm_back(grad_hidden, normed_two, inverse_two, gain_two)
    grad_w_router = matmul(hidden_two, grad_logits, ((0,), (0,)))
    grad_attn = gather_line(reps, shards, grad_resid.astype(bf16), 5).reshape(shards * length, width)

    grad_w_out = matmul(attn_out, grad_attn, ((0,), (0,)))
    grad_mixed = matmul(grad_attn, w_out, ((1,), (1,))).astype(bf16)
    grad_mixed = grad_mixed.reshape(shards, length, my_kv, group, head_dim)
    grad_weights = jnp.einsum("btkgh,bskh->bkgts", grad_mixed, values, preferred_element_type=f32)
    centre = jnp.sum(probs * grad_weights, axis=-1, keepdims=True)
    grad_scores = (probs * (grad_weights - centre) * head_dim ** (-0.5)).astype(bf16)
    grad_values = jnp.einsum("bkgts,btkgh->bskh", probs_low, grad_mixed, preferred_element_type=f32)
    grad_query_rot = jnp.einsum("bkgts,bskh->btkgh", grad_scores, key_rot, preferred_element_type=f32)
    grad_query_rot = grad_query_rot.reshape(shards, length, my_heads, head_dim)
    grad_key_rot = jnp.einsum("bkgts,btkgh->bskh", grad_scores, grouped, preferred_element_type=f32)
    grad_query_scaled = grad_query_rot * cosine - rotate(grad_query_rot * sine)
    grad_key_scaled = grad_key_rot * cosine - rotate(grad_key_rot * sine)
    grad_query_gain = jnp.sum(grad_query_scaled * query_unit, axis=(0, 1, 2))
    grad_key_gain = jnp.sum(grad_key_scaled * key_unit, axis=(0, 1, 2))
    grad_query = norm_back(grad_query_scaled, query_unit, inverse_query, qgain)
    grad_key = norm_back(grad_key_scaled, key_unit, inverse_key, kgain)
    grad_qkv = jnp.concatenate(
        [
            grad_query.reshape(shards * length, q_cols).astype(bf16),
            grad_key.reshape(shards * length, kv_cols).astype(bf16),
            grad_values.reshape(shards * length, kv_cols).astype(bf16),
        ],
        axis=1,
    )
    grad_part = matmul(grad_qkv, w_in, ((1,), (1,)))
    grad_attn_gain = jnp.sum(grad_part * normed_one, axis=0)
    grad_hidden_in = scatter_line(reps, shards, grad_part.astype(bf16).reshape(shards, length, width), 6)
    own_inverse = inverse_rms(own_tokens)
    own_normed = own_tokens * own_inverse
    grad_tokens = grad_resid + norm_back(grad_hidden_in, own_normed, own_inverse, gain_one)

    grad_w_in = matmul(hidden_in, grad_qkv, ((0,), (0,)))

    def spread(values):
        return jnp.pad(values.reshape(shards, part), ((0, 0), (0, deep - part))).reshape(width, 1)

    small_grads = jnp.concatenate(
        [
            grad_w_router,
            grad_attn_gain.reshape(width, 1),
            grad_ffn_gain.reshape(width, 1),
            spread(grad_query_gain),
            spread(grad_key_gain),
        ],
        axis=1,
    )
    small_grads = jnp.pad(small_grads, ((0, 0), (0, small_cols - small_grads.shape[1])))
    sent = jnp.concatenate([grad_w_in, small_grads], axis=1).astype(bf16)
    sent = sent.reshape(shards, reps, piece, cols + small_cols).transpose(1, 0, 2, 3)
    sent = lax.psum_scatter(sent, "rep", scatter_dimension=0, tiled=True)[0]
    sent = lax.all_to_all(sent, "shard", split_axis=0, concat_axis=0, tiled=True)
    sent = lax.all_gather(sent, "rep", axis=1, tiled=True)
    owned_out = lax.psum(grad_w_out.astype(bf16), "rep").astype(f32)

    def joined(values):
        if shared_by > 1:
            values = values.astype(f32).reshape(-1, shared_by, deep, values.shape[-1]).sum(axis=1)
        return values.transpose(1, 0, 2).reshape(deep, -1).astype(f32)

    owned_small = jnp.sum(sent[:, :, cols:].astype(f32), axis=0)
    return (
        output,
        grad_tokens,
        owned_small[:, experts],
        sent[:, :, :q_cols].transpose(1, 0, 2).reshape(deep, -1).astype(f32),
        joined(sent[:, :, q_cols : q_cols + kv_cols]),
        joined(sent[:, :, q_cols + kv_cols : cols]),
        owned_out,
        owned_small[:part, experts + 2],
        owned_small[:part, experts + 3],
        owned_small[:, experts + 1],
        owned_small[:, :experts],
        grad_w_gate[None],
        grad_w_up[None],
        grad_w_down[None],
    )


def solution(mesh):
    split = P(("rep", "shard"))
    row = P("shard")
    return jax.shard_map(
        local,
        mesh=mesh,
        in_specs=(split,) * 3 + (row,) * 9 + (split,) * 4,
        out_specs=(split,) * 2 + (row,) * 9 + (split,) * 3,
        check_vma=False,
    )
```

```python
import functools
import jax
import jax.numpy as jnp
from jax import lax
from jax.experimental import pallas as pl
from jax.experimental.pallas import tpu as pltpu
from jax.sharding import PartitionSpec as P

bf16 = jnp.bfloat16
f32 = jnp.float32
vmem_cap = 62 * 1024 * 1024
epsilon = 1e-06
rope_base = 1000000.0
masked_score = -1e30


class Grid:
    def __init__(self, reps, shards):
        self.reps, self.shards = reps, shards
        self.devices = reps * shards
        self.places = reps // 2
        self.los = self.places // 2

    def here(self):
        self.r = lax.axis_index("rep")
        self.z = lax.axis_index("shard")
        self.core = self.r % 2
        place = self.r // 2
        self.hi = place // self.los
        self.lo = place % self.los
        return self

    def rep_of(self, hi, lo, core):
        return (hi * self.los + lo) * 2 + core

    def device(self, rep, shard):
        return {"rep": rep, "shard": shard}

    def other_lo(self, step):
        return (self.lo + step) % self.los

    def nearest(self):
        n = self.shards
        rows = [sorted(range(n), key=lambda p: (abs(p - z), p)) for z in range(n)]
        return [pick(self.z, [rows[z][turn] for z in range(n)]) for turn in range(n)]


def pick(index, values):
    out = jnp.int32(values[0])
    for i in range(1, len(values)):
        out = jnp.where(index == i, jnp.int32(values[i]), out)
    return out


class Sends:
    def __init__(self, sems):
        self.sems, self.used, self.open = sems, 0, []

    def start(self, src, dst, recv, device, when=None):
        copy = pltpu.make_async_remote_copy(
            src_ref=src,
            dst_ref=dst,
            send_sem=self.sems.at[self.used],
            recv_sem=recv,
            device_id=device,
            device_id_type=pl.DeviceIdType.MESH,
        )
        self.used += 1
        self.open.append((copy, when))
        if when is None:
            copy.start()
        else:
            pl.when(when)(copy.start)

    def arrived(self, dst, recv, device, when=None):
        copy = pltpu.make_async_remote_copy(
            src_ref=dst,
            dst_ref=dst,
            send_sem=self.sems.at[0],
            recv_sem=recv,
            device_id=device,
            device_id_type=pl.DeviceIdType.MESH,
        )
        if when is None:
            copy.wait_recv()
        else:
            pl.when(when)(copy.wait_recv)

    def drain(self):
        for copy, when in self.open:
            if when is None:
                copy.wait_send()
            else:
                pl.when(when)(copy.wait_send)
        self.open = []


def greet_line(g):
    barrier = pltpu.get_barrier_semaphore()
    for step in range(1, g.shards):
        pl.semaphore_signal(
            barrier,
            inc=1,
            device_id=g.device(g.r, (g.z + step) % g.shards),
            device_id_type=pl.DeviceIdType.MESH,
        )
    pl.semaphore_wait(barrier, g.shards - 1)


def greet_all(g):
    barrier = pltpu.get_barrier_semaphore()
    me = g.r * g.shards + g.z

    def one(step, carry):
        peer = (me + step) % g.devices
        pl.semaphore_signal(
            barrier,
            inc=1,
            device_id=g.device(peer // g.shards, peer % g.shards),
            device_id_type=pl.DeviceIdType.MESH,
        )
        return carry

    lax.fori_loop(1, g.devices, one, 0)
    pl.semaphore_wait(barrier, g.devices - 1)


def push_rows(g, src, dst, send_sems, recv_sems):
    me = g.r * g.shards + g.z

    def one(step, carry):
        peer = (me + step) % g.devices
        pltpu.make_async_remote_copy(
            src_ref=src.at[peer],
            dst_ref=dst.at[me],
            send_sem=send_sems.at[step],
            recv_sem=recv_sems.at[step],
            device_id=g.device(peer // g.shards, peer % g.shards),
            device_id_type=pl.DeviceIdType.MESH,
        ).start()
        return carry

    lax.fori_loop(1, g.devices, one, 0)


def push_wait(g, src, dst, send_sems, recv_sems):
    me = g.r * g.shards + g.z

    def one(step, carry):
        peer = (me + g.devices - step) % g.devices
        copy = pltpu.make_async_remote_copy(
            src_ref=src.at[peer],
            dst_ref=dst.at[peer],
            send_sem=send_sems.at[step],
            recv_sem=recv_sems.at[step],
            device_id=g.device(peer // g.shards, peer % g.shards),
            device_id_type=pl.DeviceIdType.MESH,
        )
        copy.wait_send()
        copy.wait_recv()
        return carry

    lax.fori_loop(1, g.devices, one, 0)


class PlaneGather:
    def __init__(self, g, s, view, lr, hr, dr, cr):
        self.g, self.s, self.view = g, s, view
        self.lr, self.hr, self.dr, self.cr = lr, hr, dr, cr

    @staticmethod
    def scratch(g, units):
        dma, others = pltpu.SemaphoreType.DMA, max(1, g.los - 1)
        return [dma((units, 2, others)), dma((units, 2)), dma((units, 2, others)), dma((units, 5 * g.los))]

    @staticmethod
    def sends(g, units):
        return 9 * g.los * units

    def at(self, hi, lo):
        return self.g.device(self.g.rep_of(hi, lo, self.g.core), self.g.z)

    def partner(self):
        g = self.g
        return g.device(g.rep_of(g.hi, g.lo, 1 - g.core), g.z)

    def own(self, u, src=None):
        g, s = self.g, self.s

        def dst(part):
            return self.view(u, g.hi, g.lo, g.core, part)

        src = src or dst
        for part in (0, 1):
            for step in range(1, g.los):
                s.start(src(part), dst(part), self.lr.at[u, part, step - 1], self.at(g.hi, g.other_lo(step)))
            s.start(src(1 - part), dst(1 - part), self.hr.at[u, 1 - part], self.at(1 - g.hi, g.lo))
        s.start(src(None), dst(None), self.cr.at[u, 0], self.partner())

    def take(self, u, hi, lo, part, recv, frm, partner_slot, onward=()):
        ref = self.view(u, hi, lo, self.g.core, part)
        self.s.arrived(ref, recv, frm)
        for sem, device in onward:
            self.s.start(ref, ref, sem, device)
        self.s.start(ref, ref, self.cr.at[u, partner_slot], self.partner())

    def first(self, u):
        g = self.g
        far = 1 - g.hi
        for step in range(1, g.los):
            frm = (g.lo + g.los - step) % g.los
            onward = [(self.dr.at[u, 0, step - 1], self.at(far, g.lo))]
            self.take(u, g.hi, frm, 0, self.lr.at[u, 0, step - 1], self.at(g.hi, frm), 5 * step, onward)
        onward = [(self.dr.at[u, 1, step - 1], self.at(g.hi, g.other_lo(step))) for step in range(1, g.los)]
        self.take(u, far, g.lo, 1, self.hr.at[u, 1], self.at(far, g.lo), 1, onward)
        for step in range(1, g.los):
            frm = (g.lo + g.los - step) % g.los
            self.take(u, g.hi, frm, 1, self.lr.at[u, 1, step - 1], self.at(g.hi, frm), 5 * step + 1)
        self.take(u, far, g.lo, 0, self.hr.at[u, 0], self.at(far, g.lo), 2)

    def second(self, u):
        g = self.g
        far = 1 - g.hi
        for step in range(1, g.los):
            frm = (g.lo + g.los - step) % g.los
            self.take(u, far, frm, 0, self.dr.at[u, 0, step - 1], self.at(far, g.lo), 5 * step + 2)
            self.take(u, far, frm, 1, self.dr.at[u, 1, step - 1], self.at(g.hi, frm), 5 * step + 3)

    def from_partner(self, u):
        g = self.g
        far, other = 1 - g.hi, 1 - g.core

        def got(hi, lo, part, slot):
            self.s.arrived(self.view(u, hi, lo, other, part), self.cr.at[u, slot], self.partner())

        got(g.hi, g.lo, None, 0)
        got(far, g.lo, 1, 1)
        got(far, g.lo, 0, 2)
        for step in range(1, g.los):
            frm = (g.lo + g.los - step) % g.los
            got(g.hi, frm, 0, 5 * step)
            got(g.hi, frm, 1, 5 * step + 1)
            got(far, frm, 0, 5 * step + 2)
            got(far, frm, 1, 5 * step + 3)


def add_rows(dst, *srcs, step=16):
    def one(i, carry):
        at = pl.ds(pl.multiple_of(i * step, step), step)
        total = srcs[0][at, :].astype(f32)
        for src in srcs[1:]:
            total = total + src[at, :].astype(f32)
        dst[at, :] = total.astype(dst.dtype)
        return carry

    lax.fori_loop(0, dst.shape[0] // step, one, 0)


class PlaneScatter:
    def __init__(self, g, s, p, cut, own, ra, rb0, rb1, rc0, rc1, sa, sb0, sb1, sc0, sc1, ls):
        self.g, self.s, self.p, self.cut, self.owned = g, s, p, cut, own
        self.ra, self.rb0, self.rb1, self.rc0, self.rc1 = ra, rb0, rb1, rc0, rc1
        self.sa, self.sb0, self.sb1, self.sc0, self.sc1, self.ls = sa, sb0, sb1, sc0, sc1, ls

    @staticmethod
    def scratch(g, units, block, halves, dtype):
        dma, others, v = pltpu.SemaphoreType.DMA, max(1, g.los - 1), pltpu.VMEM
        first, second = halves
        return [
            v((units, g.places) + block, dtype),
            v((units, g.places) + block, dtype),
            v((units, g.los) + first, dtype),
            v((units, others, 2) + second, dtype),
            v((units, others) + first, dtype),
            v((units,) + second, dtype),
            dma((units,)),
            dma((units,)),
            dma((units, others, 2)),
            dma((units, others)),
            dma((units,)),
            dma((units,)),
        ]

    @staticmethod
    def sends(g, units):
        return units * (3 * g.los + 2)

    def at(self, hi, lo):
        return self.g.device(self.g.rep_of(hi, lo, self.g.core), self.g.z)

    def partner(self):
        g = self.g
        return g.device(g.rep_of(g.hi, g.lo, 1 - g.core), g.z)

    def load(self, units):
        self.loads = []
        for turn in range(units):
            load = pltpu.make_async_copy(self.p(turn, self.g.core), self.owned.at[turn], self.ls.at[turn])
            load.start()
            self.loads.append(load)

    def to_partner(self, turn):
        self.s.start(self.p(turn, 1 - self.g.core), self.ra.at[turn], self.sa.at[turn], self.partner())

    def half(self, turn, place, part):
        return self.owned.at[(turn, place) + self.cut(part)]

    def mine(self, turn):
        return self.owned.at[turn, self.g.hi * self.g.los + self.g.lo]

    def a(self, turn):
        g, s = self.g, self.s
        far = 1 - g.hi
        self.loads[turn].wait()
        s.arrived(self.ra.at[turn], self.sa.at[turn], self.partner())

        def one(q, carry):
            line = self.owned.at[turn, q]
            add_rows(line, line, self.ra.at[turn, q])
            return carry

        lax.fori_loop(0, g.places, one, 0)
        block = self.owned.at[(turn, pl.ds(far * g.los, g.los)) + self.cut(0)]
        s.start(block, self.rb0.at[turn], self.sb0.at[turn], self.at(far, g.lo))
        for step in range(1, g.los):
            to = g.other_lo(step)
            for hi in range(2):
                sem = self.sb1.at[turn, step - 1, hi]
                s.start(self.half(turn, hi * g.los + to, 1), self.rb1.at[turn, step - 1, hi], sem, self.at(g.hi, to))

    def b(self, turn):
        g, s = self.g, self.s
        far = 1 - g.hi
        s.arrived(self.rb0.at[turn], self.sb0.at[turn], self.at(far, g.lo))
        for lo in range(g.los):
            line = self.half(turn, g.hi * g.los + lo, 0)
            add_rows(line, line, self.rb0.at[turn, lo])
        for step in range(1, g.los):
            to = g.other_lo(step)
            sem = self.sc0.at[turn, step - 1]
            s.start(self.half(turn, g.hi * g.los + to, 0), self.rc0.at[turn, step - 1], sem, self.at(g.hi, to))
        for step in range(1, g.los):
            frm = (g.lo + g.los - step) % g.los
            for hi in range(2):
                s.arrived(self.rb1.at[turn, step - 1, hi], self.sb1.at[turn, step - 1, hi], self.at(g.hi, frm))
        for hi in range(2):
            line = self.half(turn, hi * g.los + g.lo, 1)
            add_rows(line, line, *[self.rb1.at[turn, step, hi] for step in range(g.los - 1)])
        s.start(self.half(turn, far * g.los + g.lo, 1), self.rc1.at[turn], self.sc1.at[turn], self.at(far, g.lo))

    def c(self, turn):
        g, s = self.g, self.s
        place = g.hi * g.los + g.lo
        for step in range(1, g.los):
            frm = (g.lo + g.los - step) % g.los
            s.arrived(self.rc0.at[turn, step - 1], self.sc0.at[turn, step - 1], self.at(g.hi, frm))
        line = self.half(turn, place, 0)
        add_rows(line, line, *[self.rc0.at[turn, step] for step in range(g.los - 1)])
        s.arrived(self.rc1.at[turn], self.sc1.at[turn], self.at(1 - g.hi, g.lo))
        line = self.half(turn, place, 1)
        add_rows(line, line, self.rc1.at[turn])


def pass_along(g, s, zp, src, dst, zr):
    n = g.shards
    right, left = g.device(g.r, jnp.minimum(g.z + 1, n - 1)), g.device(g.r, jnp.maximum(g.z - 1, 0))
    s.start(src, dst, zr.at[zp], right, (zp <= g.z) & (g.z + 1 < n))
    s.start(src, dst, zr.at[zp], left, (zp >= g.z) & (g.z > 0))


def send_line(g, s, zp, line, out_ref, rl, rr, sl, sr, last):
    n = g.shards
    left, right = g.device(g.r, jnp.maximum(g.z - 1, 0)), g.device(g.r, jnp.minimum(g.z + 1, n - 1))
    has_left, has_right = g.z > 0, g.z + 1 < n
    if last:
        s.arrived(rl.at[g.z], sl.at[g.z], left, has_left)
        s.arrived(rr.at[g.z], sr.at[g.z], right, has_right)

        @pl.when(has_left & has_right)
        def _():
            add_rows(out_ref, line, rl.at[g.z], rr.at[g.z])

        @pl.when(has_left & jnp.logical_not(has_right))
        def _():
            add_rows(out_ref, line, rl.at[g.z])

        @pl.when(has_right & jnp.logical_not(has_left))
        def _():
            add_rows(out_ref, line, rr.at[g.z])
    else:
        onward_right, onward_left = zp > g.z, zp < g.z

        @pl.when(onward_right & has_left)
        def _():
            s.arrived(rl.at[zp], sl.at[zp], left)
            add_rows(line, line, rl.at[zp])

        @pl.when(onward_left & has_right)
        def _():
            s.arrived(rr.at[zp], sr.at[zp], right)
            add_rows(line, line, rr.at[zp])

        s.start(line, rl.at[zp], sl.at[zp], right, onward_right)
        s.start(line, rr.at[zp], sr.at[zp], left, onward_left)


def line_scratch(shards, block, dtype):
    v, dma = pltpu.VMEM, pltpu.SemaphoreType.DMA
    return [v((shards,) + block, dtype), v((shards,) + block, dtype), dma((shards,)), dma((shards,))]


hbm = pl.BlockSpec(memory_space=pl.ANY)
vmem = pl.BlockSpec(memory_space=pltpu.VMEM)


def params(ident):
    return pltpu.CompilerParams(collective_id=ident, has_side_effects=True, vmem_limit_bytes=vmem_cap)


def gather_line_kernel(reps, shards, x_ref, out_ref, sems, zr, ls):
    g = Grid(reps, shards).here()
    s = Sends(sems)
    keep = pltpu.make_async_copy(x_ref, out_ref.at[g.z], ls.at[0])
    keep.start()
    greet_line(g)
    for turn, zp in enumerate(g.nearest()):
        dst = out_ref.at[zp]
        if turn:
            s.arrived(dst, zr.at[zp], g.device(g.r, zp))
        pass_along(g, s, zp, dst if turn else x_ref, dst, zr)
    keep.wait()
    s.drain()


def gather_line(reps, shards, x, ident):
    dma = pltpu.SemaphoreType.DMA
    return pl.pallas_call(
        functools.partial(gather_line_kernel, reps, shards),
        out_shape=jax.ShapeDtypeStruct((shards,) + x.shape, x.dtype),
        in_specs=[vmem],
        out_specs=vmem,
        scratch_shapes=[dma((2 * shards,)), dma((shards,)), dma((1,))],
        compiler_params=params(ident),
        name="gather_line",
    )(x)


def scatter_line_kernel(reps, shards, p_ref, out_ref, own, rl, rr, sl, sr, sems, ls):
    g = Grid(reps, shards).here()
    s = Sends(sems)
    n = g.shards
    order = g.nearest()[::-1]
    loads = []
    for turn in range(n):
        load = pltpu.make_async_copy(p_ref.at[order[turn]], own.at[turn], ls.at[turn])
        load.start()
        loads.append(load)
    greet_line(g)
    for turn in range(n):
        loads[turn].wait()
        send_line(g, s, order[turn], own.at[turn], out_ref, rl, rr, sl, sr, last=turn == n - 1)
    s.drain()


def scatter_line(reps, shards, p, ident):
    dma = pltpu.SemaphoreType.DMA
    _, rows, width = p.shape
    return pl.pallas_call(
        functools.partial(scatter_line_kernel, reps, shards),
        out_shape=jax.ShapeDtypeStruct((rows, width), f32),
        in_specs=[hbm],
        out_specs=vmem,
        scratch_shapes=[pltpu.VMEM(p.shape, p.dtype)]
        + line_scratch(shards, (rows, width), p.dtype)
        + [dma((2 * shards,)), dma((shards,))],
        compiler_params=params(ident),
        name="scatter_line",
    )(p)


def collect_kernel(reps, shards, layout, x_ref, small_ref, wq_ref, wk_ref, wv_ref, xs_ref, smalls_ref, w_ref, sems, xr, mr, wr, lr, hr, dr, cr, ls):
    g = Grid(reps, shards).here()
    s = Sends(sems)
    n = g.shards
    q_cols, kv_cols, kv_heads, head_dim = layout
    deep = wq_ref.shape[0]
    piece = deep // g.reps
    cols = q_cols + 2 * kv_cols
    first = cols // 2 // 128 * 128
    spans = {0: pl.ds(0, first), 1: pl.ds(first, cols - first), None: pl.ds(0, cols)}
    mine = pl.ds(pl.multiple_of(g.r * piece, piece), piece)

    def view(u, hi, lo, core, part):
        row = pl.multiple_of(u * deep + g.rep_of(hi, lo, core) * piece, piece)
        return w_ref.at[pl.ds(row, piece), spans[part]]

    def pieces(zp, u):
        row = pl.ds(pl.multiple_of(u * deep + g.r * piece, piece), piece)
        at_q = pl.ds(pl.multiple_of(zp * q_cols, 128), q_cols)
        at_kv = pl.ds(pl.multiple_of(zp * kv_heads // n * head_dim, 128), kv_cols)
        return (
            (wq_ref.at[mine, at_q], w_ref.at[row, pl.ds(0, q_cols)]),
            (wk_ref.at[mine, at_kv], w_ref.at[row, pl.ds(q_cols, kv_cols)]),
            (wv_ref.at[mine, at_kv], w_ref.at[row, pl.ds(q_cols + kv_cols, kv_cols)]),
        )

    keeps = [
        pltpu.make_async_copy(x_ref, xs_ref.at[g.z], ls.at[0]),
        pltpu.make_async_copy(small_ref, smalls_ref.at[g.z], ls.at[1]),
    ]
    locals_ = [pltpu.make_async_copy(src, dst, ls.at[2 + i]) for i, (src, dst) in enumerate(pieces(g.z, g.z))]
    for copy in locals_ + keeps:
        copy.start()
    barrier = pltpu.get_barrier_semaphore()
    peers = [g.device(g.r, (g.z + step) % n) for step in range(1, n)]
    peers += [g.device(g.rep_of(g.hi, g.other_lo(step), g.core), g.z) for step in range(1, g.los)]
    peers += [g.device(g.rep_of(1 - g.hi, g.lo, g.core), g.z), g.device(g.rep_of(g.hi, g.lo, 1 - g.core), g.z)]
    for peer in peers:
        pl.semaphore_signal(barrier, inc=1, device_id=peer, device_id_type=pl.DeviceIdType.MESH)
    pl.semaphore_wait(barrier, len(peers))

    plane = PlaneGather(g, s, view, lr, hr, dr, cr)
    for step in range(1, n):
        zp = (g.z + step) % n
        for i, (src, dst) in enumerate(pieces(zp, g.z)):
            s.start(src, dst, wr.at[step, i], g.device(g.r, zp))
    order = g.nearest()

    def line(turn):
        zp = order[turn]
        if turn:
            s.arrived(smalls_ref.at[zp], mr.at[zp], g.device(g.r, zp))
        pass_along(g, s, zp, smalls_ref.at[zp] if turn else small_ref, smalls_ref.at[zp], mr)
        if turn:
            s.arrived(xs_ref.at[zp], xr.at[zp], g.device(g.r, zp))
        pass_along(g, s, zp, xs_ref.at[zp] if turn else x_ref, xs_ref.at[zp], xr)

    line(0)
    for copy in locals_:
        copy.wait()
    plane.own(g.z)

    def unit(step):
        return (g.z + n - step) % n

    for step in range(1, n):
        u = unit(step)
        for i, (_, dst) in enumerate(pieces(g.z, u)):
            s.arrived(dst, wr.at[step, i], g.device(g.r, u))
        plane.own(u)
    line(1)
    for step in range(n):
        plane.first(unit(step))
        if step:
            plane.second(unit(step - 1))
        if 2 + step < n:
            line(2 + step)
    plane.second(unit(n - 1))
    for step in range(n):
        plane.from_partner(unit(step))
    for copy in keeps:
        copy.wait()
    s.drain()


def collect(reps, shards, x, small, wq, wk, wv, layout, ident):
    g = Grid(reps, shards)
    dma = pltpu.SemaphoreType.DMA
    n = shards
    cols = layout[0] + 2 * layout[1]
    return pl.pallas_call(
        functools.partial(collect_kernel, reps, shards, layout),
        out_shape=(
            jax.ShapeDtypeStruct((n,) + x.shape, x.dtype),
            jax.ShapeDtypeStruct((n,) + small.shape, small.dtype),
            jax.ShapeDtypeStruct((n * wq.shape[0], cols), wq.dtype),
        ),
        in_specs=[vmem, vmem, hbm, hbm, hbm],
        out_specs=(vmem, vmem, vmem),
        scratch_shapes=[dma((PlaneGather.sends(g, n) + 7 * n,)), dma((n,)), dma((n,)), dma((n, 3))]
        + PlaneGather.scratch(g, n)
        + [dma((5,))],
        compiler_params=params(ident),
        name="collect",
    )(x, small, wq, wk, wv)


def gather_all_kernel(reps, shards, x_ref, slab_ref, out_ref, slabs_ref, sems, zr, ps, pr, ls, lr, hr, dr, cr):
    g = Grid(reps, shards).here()
    s = Sends(sems)
    half = x_ref.shape[0] // 2
    n = g.shards
    spans = {0: pl.ds(0, half), 1: pl.ds(half, half), None: pl.ds(0, 2 * half)}
    order = g.nearest()

    def view(u, hi, lo, core, part):
        return out_ref.at[g.rep_of(hi, lo, core) * n + u, spans[part]]

    plane = PlaneGather(g, s, view, lr, hr, dr, cr)
    keep = pltpu.make_async_copy(x_ref, view(g.z, g.hi, g.lo, g.core, None), ls.at[0])
    keep.start()
    greet_all(g)
    push_rows(g, slab_ref, slabs_ref, ps, pr)
    me = g.r * n + g.z
    keep_slab = pltpu.make_async_copy(slab_ref.at[me], slabs_ref.at[me], ls.at[1])
    keep_slab.start()
    for turn in range(n + 2):
        if turn < n:
            zp = order[turn]
            dst = view(zp, g.hi, g.lo, g.core, None)
            if turn:
                s.arrived(dst, zr.at[zp], g.device(g.r, zp))
            pass_along(g, s, zp, dst if turn else x_ref, dst, zr)
            plane.own(zp, None if turn else lambda part: x_ref.at[spans[part]])
        if 0 <= turn - 1 < n:
            plane.first(order[turn - 1])
        if 0 <= turn - 2 < n:
            plane.second(order[turn - 2])
    for turn in range(n):
        plane.from_partner(order[turn])
    keep.wait()
    keep_slab.wait()
    push_wait(g, slab_ref, slabs_ref, ps, pr)
    s.drain()


def gather_all(reps, shards, x, slab, ident):
    g = Grid(reps, shards)
    dma = pltpu.SemaphoreType.DMA
    n = shards
    return pl.pallas_call(
        functools.partial(gather_all_kernel, reps, shards),
        out_shape=(
            jax.ShapeDtypeStruct((g.devices,) + x.shape, x.dtype),
            jax.ShapeDtypeStruct(slab.shape, slab.dtype),
        ),
        in_specs=[vmem, vmem],
        out_specs=(hbm, vmem),
        scratch_shapes=[
            dma((PlaneGather.sends(g, n) + 2 * n,)),
            dma((n,)),
            dma((g.devices,)),
            dma((g.devices,)),
            dma((2,)),
        ]
        + PlaneGather.scratch(g, n),
        compiler_params=params(ident),
        name="gather_all",
    )(x, slab)


def scatter_all_kernel(reps, shards, slabbed, *refs):
    if slabbed:
        p_ref, slab_ref, out_ref, slabs_ref, *rest = refs
    else:
        p_ref, out_ref, *rest = refs
    rl, rr, sl, sr, sems, ps, pr, slab_sem, *rest = rest
    g = Grid(reps, shards).here()
    s = Sends(sems)
    n = g.shards
    half = out_ref.shape[0] // 2
    order = g.nearest()[::-1]
    plane = PlaneScatter(
        g, s, lambda turn, core: p_ref.at[:, core, order[turn]], lambda part: (pl.ds(part * half, half),), *rest
    )
    plane.load(n)
    greet_all(g)
    for turn in range(n):
        plane.to_partner(turn)
    if slabbed:
        push_rows(g, slab_ref, slabs_ref, ps, pr)
        me = g.r * n + g.z
        keep_slab = pltpu.make_async_copy(slab_ref.at[me], slabs_ref.at[me], slab_sem.at[0])
        keep_slab.start()
    for turn in range(n + 2):
        if turn < n:
            plane.a(turn)
        if 0 <= turn - 1 < n:
            plane.b(turn - 1)
        if 0 <= turn - 2 < n:
            plane.c(turn - 2)
            send_line(g, s, order[turn - 2], plane.mine(turn - 2), out_ref, rl, rr, sl, sr, last=turn - 2 == n - 1)
    if slabbed:
        keep_slab.wait()
        push_wait(g, slab_ref, slabs_ref, ps, pr)
    s.drain()


def scatter_all(reps, shards, p, slab, ident):
    g = Grid(reps, shards)
    n = shards
    _, rows, width = p.shape
    half = rows // 2
    dma = pltpu.SemaphoreType.DMA
    slabbed = slab is not None
    out_shape = (jax.ShapeDtypeStruct((rows, width), f32),)
    if slabbed:
        out_shape += (jax.ShapeDtypeStruct(slab.shape, slab.dtype),)
    done = pl.pallas_call(
        functools.partial(scatter_all_kernel, reps, shards, slabbed),
        out_shape=out_shape,
        in_specs=[hbm] + [vmem] * slabbed,
        out_specs=(vmem,) * len(out_shape),
        scratch_shapes=line_scratch(n, (rows, width), p.dtype)
        + [dma((PlaneScatter.sends(g, n) + 2 * n,)), dma((g.devices,)), dma((g.devices,)), dma((1,))]
        + PlaneScatter.scratch(g, n, (rows, width), ((half, width), (half, width)), p.dtype),
        compiler_params=params(ident),
        name="scatter_all",
    )(p.reshape(g.places, 2, n, rows, width), *([slab] if slabbed else []))
    return done if slabbed else done[0]


def scatter_wide(reps, shards, p, slab, ident, chunks):
    if chunks == 1:
        return scatter_all(reps, shards, p, slab, ident)
    step = p.shape[2] // chunks
    parts = [
        scatter_all(reps, shards, p[:, :, i * step : (i + 1) * step], slab if i == 0 else None, ident + i)
        for i in range(chunks)
    ]
    if slab is None:
        return jnp.concatenate(parts, axis=1)
    first, slabs = parts[0]
    return jnp.concatenate([first] + parts[1:], axis=1), slabs


def deliver_kernel(reps, shards, p_ref, w_ref, out_ref, ws_ref, line_own, rl, rr, sl, sr, sems, line_loads, wr, keep_sem, *rest):
    g = Grid(reps, shards).here()
    s = Sends(sems)
    n = g.shards
    gather_refs, scatter_refs = rest[:4], rest[4:]
    cols = w_ref.shape[-1]
    first = cols // 2 // 128 * 128
    spans = {0: pl.ds(0, first), 1: pl.ds(first, cols - first), None: pl.ds(0, cols)}
    order = g.nearest()[::-1]
    scatter = PlaneScatter(
        g, s, lambda turn, core: w_ref.at[turn, :, core], lambda part: (slice(None), spans[part]), *scatter_refs
    )
    gather = PlaneGather(
        g, s, lambda u, hi, lo, core, part: ws_ref.at[u, g.rep_of(hi, lo, core), :, spans[part]], *gather_refs
    )
    scatter.load(n)
    loads = []
    for turn in range(n):
        load = pltpu.make_async_copy(p_ref.at[order[turn]], line_own.at[turn], line_loads.at[turn])
        load.start()
        loads.append(load)
    barrier = pltpu.get_barrier_semaphore()
    peers = [g.device(g.r, (g.z + step) % n) for step in range(1, n)]
    peers += [g.device(g.rep_of(g.hi, g.other_lo(step), g.core), g.z) for step in range(1, g.los)]
    peers += [g.device(g.rep_of(1 - g.hi, g.lo, g.core), g.z), g.device(g.rep_of(g.hi, g.lo, 1 - g.core), g.z)]
    for peer in peers:
        pl.semaphore_signal(barrier, inc=1, device_id=peer, device_id_type=pl.DeviceIdType.MESH)
    pl.semaphore_wait(barrier, len(peers))

    for turn in range(n):
        scatter.to_partner(turn)

    def line(turn):
        loads[turn].wait()
        send_line(g, s, order[turn], line_own.at[turn], out_ref, rl, rr, sl, sr, last=turn == n - 1)

    def owner(turn):
        scatter.c(turn)
        dst = ws_ref.at[g.z, g.r]
        keep = pltpu.make_async_copy(scatter.mine(turn), dst, keep_sem.at[0])
        pl.when(g.z == turn)(keep.start)
        s.start(scatter.mine(turn), dst, wr.at[g.z], g.device(g.r, turn), g.z != turn)
        pl.when(g.z == turn)(keep.wait)

    line(0)
    for turn in range(n + 2):
        if turn < n:
            scatter.a(turn)
        if 0 <= turn - 1 < n:
            scatter.b(turn - 1)
        if 1 <= turn < n - 1:
            line(turn)
        if 0 <= turn - 2 < n:
            owner(turn - 2)
    gather.own(g.z)

    def unit(step):
        return (g.z + n - step) % n

    for step in range(1, n):
        u = unit(step)
        s.arrived(ws_ref.at[u, g.r], wr.at[u], g.device(g.r, u))
        gather.own(u)
        gather.first(unit(step - 1))
        if step > 1:
            gather.second(unit(step - 2))
    gather.first(unit(n - 1))
    gather.second(unit(n - 2))
    gather.second(unit(n - 1))
    line(n - 1)
    for step in range(n):
        gather.from_partner(unit(step))
    s.drain()


def deliver(reps, shards, p, w, ident):
    g = Grid(reps, shards)
    n = shards
    dma = pltpu.SemaphoreType.DMA
    _, rows, width = p.shape
    _, _, piece, cols = w.shape
    first = cols // 2 // 128 * 128
    return pl.pallas_call(
        functools.partial(deliver_kernel, reps, shards),
        out_shape=(jax.ShapeDtypeStruct((rows, width), f32), jax.ShapeDtypeStruct(w.shape, w.dtype)),
        in_specs=[hbm, hbm],
        out_specs=(vmem, vmem),
        scratch_shapes=[pltpu.VMEM(p.shape, p.dtype)]
        + line_scratch(n, (rows, width), p.dtype)
        + [
            dma((PlaneGather.sends(g, n) + PlaneScatter.sends(g, n) + 3 * n,)),
            dma((n,)),
            dma((n,)),
            dma((1,)),
        ]
        + PlaneGather.scratch(g, n)
        + PlaneScatter.scratch(g, n, (piece, cols), ((piece, first), (piece, cols - first)), w.dtype),
        compiler_params=params(ident),
        name="deliver",
    )(p, w.reshape(n, g.places, 2, piece, cols))


def inverse_rms(values):
    return lax.rsqrt(jnp.mean(values * values, axis=-1, keepdims=True) + epsilon)


def rotate(values):
    half = values.shape[-1] // 2
    return jnp.concatenate([-values[..., half:], values[..., :half]], axis=-1)


def rope_tables(segment_rows, width):
    length = segment_rows.shape[1]
    places = jnp.arange(length, dtype=jnp.int32)
    same = segment_rows[:, :, None] == segment_rows[:, None, :]
    first = jnp.min(jnp.where(same, places[None, None, :], length), axis=2)
    offset = (places[None] - first).astype(f32)
    half = width // 2
    frequency = rope_base ** (-2.0 * jnp.arange(half, dtype=f32) / width)
    angle = offset[..., None] * frequency[None, None, :]
    cosine, sine = jnp.cos(angle), jnp.sin(angle)
    cosine = jnp.concatenate([cosine, cosine], axis=-1)
    sine = jnp.concatenate([sine, sine], axis=-1)
    allowed = same & (places[None, None, :] <= places[None, :, None])
    return cosine, sine, allowed


def norm_back(grad_scaled, unit, inverse, gain):
    gained = grad_scaled * gain
    return inverse * (gained - unit * jnp.mean(gained * unit, axis=-1, keepdims=True))


def matmul(a, b, dims=((1,), (0,))):
    return lax.dot_general(a, b, (dims, ((), ())), preferred_element_type=f32)


def local(
    tokens,
    segments,
    routes,
    attn_gain,
    w_query,
    key_weight,
    value_weight,
    w_out,
    query_gain,
    key_gain,
    ffn_gain,
    w_router,
    w_gate,
    w_up,
    w_down,
    cotangent,
):
    reps, shards = lax.axis_size("rep"), lax.axis_size("shard")
    devices = reps * shards
    r, z = lax.axis_index("rep"), lax.axis_index("shard")
    length, width = tokens.shape
    deep = w_query.shape[0]
    head_dim = query_gain.shape[0] * shards
    heads = w_query.shape[1] // head_dim
    kv_heads = key_weight.shape[1] // head_dim
    experts = w_router.shape[1]
    top = routes.shape[1]
    capacity = 2 * length * top // experts
    my_heads = heads // shards
    my_kv = max(1, kv_heads // shards)
    shared_by = max(1, shards // kv_heads)
    group = my_heads // my_kv
    q_cols, kv_cols = my_heads * head_dim, my_kv * head_dim
    cols = q_cols + 2 * kv_cols
    piece = deep // reps
    chunks = max(1, devices // 32)
    part = head_dim // shards

    def column(values, rows=deep):
        return jnp.pad(values.reshape(-1, 1), ((0, rows - values.size), (0, 0)))

    small = jnp.concatenate(
        [
            w_router,
            column(attn_gain),
            column(ffn_gain),
            column(query_gain),
            column(key_gain),
            column(segments[0].astype(bf16)),
        ],
        axis=1,
    )
    small_cols = -(-small.shape[1] // 128) * 128
    small = jnp.pad(small, ((0, 0), (0, small_cols - small.shape[1])))
    layout = (q_cols, kv_cols, kv_heads, head_dim)
    block_tokens, small_all, w_in = collect(
        reps, shards, tokens, small, w_query, key_weight, value_weight, layout, 1
    )
    block_tokens = block_tokens.reshape(shards * length, width)
    router_full = small_all[:, :, :experts].reshape(width, experts)
    gain_one = small_all[:, :, experts].reshape(1, width).astype(f32)
    gain_two = small_all[:, :, experts + 1].reshape(1, width).astype(f32)
    qgain = small_all[:, :part, experts + 2].reshape(head_dim).astype(f32)
    kgain = small_all[:, :part, experts + 3].reshape(head_dim).astype(f32)
    segment_rows = small_all[:, :length, experts + 4].astype(jnp.int32)

    cotangents = lax.all_gather(cotangent, ("rep", "shard"), axis=0)

    wide = block_tokens.astype(f32)
    inverse_one = inverse_rms(wide)
    normed_one = wide * inverse_one
    hidden_in = (normed_one * gain_one).astype(bf16)
    qkv = matmul(hidden_in, w_in)
    query_raw = qkv[:, :q_cols].reshape(shards, length, my_heads, head_dim)
    key_raw = qkv[:, q_cols : q_cols + kv_cols].reshape(shards, length, my_kv, head_dim)
    values = qkv[:, q_cols + kv_cols :].astype(bf16).reshape(shards, length, my_kv, head_dim)
    inverse_query = inverse_rms(query_raw)
    query_unit = query_raw * inverse_query
    inverse_key = inverse_rms(key_raw)
    key_unit = key_raw * inverse_key
    cosine, sine, allowed = rope_tables(segment_rows, head_dim)
    cosine, sine = cosine[:, :, None, :], sine[:, :, None, :]
    query_scaled = query_unit * qgain
    key_scaled = key_unit * kgain
    query_rot = (query_scaled * cosine + rotate(query_scaled) * sine).astype(bf16)
    key_rot = (key_scaled * cosine + rotate(key_scaled) * sine).astype(bf16)
    grouped = query_rot.reshape(shards, length, my_kv, group, head_dim)
    scores = jnp.einsum("btkgh,bskh->bkgts", grouped, key_rot, preferred_element_type=f32) * head_dim ** (-0.5)
    scores = jnp.where(allowed[:, None, None], scores, masked_score)
    highest = jnp.max(scores, axis=-1, keepdims=True)
    raised = jnp.exp(scores - highest)
    probs = raised / jnp.sum(raised, axis=-1, keepdims=True)
    probs_low = probs.astype(bf16)
    mixed = jnp.einsum("bkgts,bskh->btkgh", probs_low, values, preferred_element_type=f32)
    attn_out = mixed.reshape(shards * length, q_cols).astype(bf16)
    projected = matmul(attn_out, w_out).astype(bf16)
    own_tokens = tokens.astype(f32)
    resid = own_tokens + scatter_line(reps, shards, projected.reshape(shards, length, width), 3)

    inverse_two = inverse_rms(resid)
    normed_two = resid * inverse_two
    hidden_two = (normed_two * gain_two).astype(bf16)
    logits = matmul(hidden_two, router_full)
    gate_probs = jax.nn.softmax(logits, axis=-1)
    chosen = jnp.any(routes[:, :, None] == jnp.arange(experts, dtype=jnp.int32)[None, None, :], axis=1)
    picked = jnp.where(chosen, gate_probs, 0.0)
    picked_total = jnp.sum(picked, axis=-1, keepdims=True)
    mix = picked / picked_total
    slab = jnp.where(chosen, mix, -1.0).T.reshape(experts, 1, length)
    slab = jnp.broadcast_to(slab, (experts, 8, length))
    hiddens, slabs = gather_all(reps, shards, hidden_two, slab, 4)

    share = slabs[:, 0, :]
    member = share >= 0.0
    earlier = jnp.arange(length)[:, None] < jnp.arange(length)[None, :]
    slot = matmul(member.astype(bf16), earlier.astype(bf16))
    place = (jnp.arange(capacity, dtype=f32)[None, :, None] == slot[:, None, :]) & member[:, None, :]
    row_weight = jnp.sum(jnp.where(place, share[:, None, :], 0.0), axis=2, keepdims=True)
    onehot = place.astype(bf16)

    def dispatch(blocks):
        taken = jnp.einsum("bst,btd->bsd", onehot, blocks, preferred_element_type=f32)
        return taken.astype(bf16).reshape(devices * capacity, width)

    rows = dispatch(hiddens)
    row_grads = dispatch(cotangents)
    row_weight = row_weight.reshape(devices * capacity, 1)
    gate = matmul(rows, w_gate[0])
    up = matmul(rows, w_up[0])
    sigmoid_gate = jax.nn.sigmoid(gate)
    activated = (gate * sigmoid_gate * up).astype(bf16)
    produced = matmul(activated, w_down[0]).astype(bf16).astype(f32)
    row_grads = row_grads.astype(f32)
    weighted = (row_weight * produced).astype(bf16)
    row_mix = jnp.sum(row_grads * produced, axis=1).reshape(devices, capacity, 1)
    back_mix = jnp.sum(jnp.where(place, row_mix, 0.0), axis=1).reshape(devices, 1, length)
    back_mix = jnp.broadcast_to(back_mix, (devices, 8, length))
    grad_pair = (row_weight * row_grads).astype(bf16)
    grad_act = matmul(grad_pair, w_down[0], ((1,), (1,)))
    grad_gate = (grad_act * up * sigmoid_gate * (1.0 + gate * (1.0 - sigmoid_gate))).astype(bf16)
    grad_up = (grad_act * gate * sigmoid_gate).astype(bf16)
    grad_in = matmul(grad_gate, w_gate[0], ((1,), (1,))) + matmul(grad_up, w_up[0], ((1,), (1,)))
    grad_w_down = matmul(activated, grad_pair, ((0,), (0,)))
    grad_w_gate = matmul(rows, grad_gate, ((0,), (0,)))
    grad_w_up = matmul(rows, grad_up, ((0,), (0,)))

    def combine(values):
        values = values.reshape(devices, capacity, width)
        return jnp.einsum("bst,bsd->btd", onehot, values, preferred_element_type=f32).astype(bf16)

    grad_hidden, mixes = scatter_wide(reps, shards, combine(grad_in.astype(bf16)), back_mix, 8, chunks)
    output = (resid + scatter_wide(reps, shards, combine(weighted), None, 16, chunks)).astype(bf16)

    grad_out = cotangent.astype(f32)
    grad_mix = mixes[:, 0, :].T
    grad_picked = jnp.where(chosen, grad_mix - jnp.sum(grad_mix * mix, axis=-1, keepdims=True), 0.0) / picked_total
    grad_logits = (gate_probs * (grad_picked - jnp.sum(grad_picked * picked, axis=-1, keepdims=True))).astype(bf16)
    grad_hidden = grad_hidden + matmul(grad_logits, router_full, ((1,), (1,)))
    grad_ffn_gain = jnp.sum(grad_hidden * normed_two, axis=0)
    grad_resid = grad_out + norm_back(grad_hidden, normed_two, inverse_two, gain_two)
    grad_w_router = matmul(hidden_two, grad_logits, ((0,), (0,)))
    grad_attn = gather_line(reps, shards, grad_resid.astype(bf16), 5).reshape(shards * length, width)

    grad_w_out = matmul(attn_out, grad_attn, ((0,), (0,)))
    owned_out = lax.psum(grad_w_out.astype(bf16), "rep").astype(f32)
    grad_mixed = matmul(grad_attn, w_out, ((1,), (1,))).astype(bf16)
    grad_mixed = grad_mixed.reshape(shards, length, my_kv, group, head_dim)
    grad_weights = jnp.einsum("btkgh,bskh->bkgts", grad_mixed, values, preferred_element_type=f32)
    centre = jnp.sum(probs * grad_weights, axis=-1, keepdims=True)
    grad_scores = (probs * (grad_weights - centre) * head_dim ** (-0.5)).astype(bf16)
    grad_values = jnp.einsum("bkgts,btkgh->bskh", probs_low, grad_mixed, preferred_element_type=f32)
    grad_query_rot = jnp.einsum("bkgts,bskh->btkgh", grad_scores, key_rot, preferred_element_type=f32)
    grad_query_rot = grad_query_rot.reshape(shards, length, my_heads, head_dim)
    grad_key_rot = jnp.einsum("bkgts,btkgh->bskh", grad_scores, grouped, preferred_element_type=f32)
    grad_query_scaled = grad_query_rot * cosine - rotate(grad_query_rot * sine)
    grad_key_scaled = grad_key_rot * cosine - rotate(grad_key_rot * sine)
    grad_query_gain = jnp.sum(grad_query_scaled * query_unit, axis=(0, 1, 2))
    grad_key_gain = jnp.sum(grad_key_scaled * key_unit, axis=(0, 1, 2))
    grad_query = norm_back(grad_query_scaled, query_unit, inverse_query, qgain)
    grad_key = norm_back(grad_key_scaled, key_unit, inverse_key, kgain)
    grad_qkv = jnp.concatenate(
        [
            grad_query.reshape(shards * length, q_cols).astype(bf16),
            grad_key.reshape(shards * length, kv_cols).astype(bf16),
            grad_values.reshape(shards * length, kv_cols).astype(bf16),
        ],
        axis=1,
    )
    grad_part = matmul(grad_qkv, w_in, ((1,), (1,)))
    grad_attn_gain = jnp.sum(grad_part * normed_one, axis=0)
    grad_w_in = matmul(hidden_in, grad_qkv, ((0,), (0,)))

    def spread(values):
        return jnp.pad(values.reshape(shards, part), ((0, 0), (0, deep - part))).reshape(width, 1)

    small_grads = jnp.concatenate(
        [
            grad_w_router,
            grad_attn_gain.reshape(width, 1),
            grad_ffn_gain.reshape(width, 1),
            spread(grad_query_gain),
            spread(grad_key_gain),
        ],
        axis=1,
    )
    small_grads = jnp.pad(small_grads, ((0, 0), (0, small_cols - small_grads.shape[1])))
    sent = jnp.concatenate([grad_w_in, small_grads], axis=1).astype(bf16)
    sent = sent.reshape(shards, reps, piece, cols + small_cols)
    grad_part = grad_part.astype(bf16).reshape(shards, length, width)
    grad_hidden_in, sent = deliver(reps, shards, grad_part, sent, 6)
    sent = sent.reshape(shards, deep, cols + small_cols)
    own_inverse = inverse_rms(own_tokens)
    own_normed = own_tokens * own_inverse
    grad_tokens = grad_resid + norm_back(grad_hidden_in, own_normed, own_inverse, gain_one)

    def joined(values):
        if shared_by > 1:
            values = values.astype(f32).reshape(-1, shared_by, deep, values.shape[-1]).sum(axis=1)
        return values.transpose(1, 0, 2).reshape(deep, -1).astype(f32)

    owned_small = jnp.sum(sent[:, :, cols:].astype(f32), axis=0)
    return (
        output,
        grad_tokens,
        owned_small[:, experts],
        sent[:, :, :q_cols].transpose(1, 0, 2).reshape(deep, -1).astype(f32),
        joined(sent[:, :, q_cols : q_cols + kv_cols]),
        joined(sent[:, :, q_cols + kv_cols : cols]),
        owned_out,
        owned_small[:part, experts + 2],
        owned_small[:part, experts + 3],
        owned_small[:, experts + 1],
        owned_small[:, :experts],
        grad_w_gate[None],
        grad_w_up[None],
        grad_w_down[None],
    )


def solution(mesh):
    split = P(("rep", "shard"))
    row = P("shard")
    return jax.shard_map(
        local,
        mesh=mesh,
        in_specs=(split,) * 3 + (row,) * 9 + (split,) * 4,
        out_specs=(split,) * 2 + (row,) * 9 + (split,) * 3,
        check_vma=False,
    )
```

```python
import functools
import jax
import jax.numpy as jnp
from jax import lax
from jax.experimental import pallas as pl
from jax.experimental.pallas import tpu as pltpu
from jax.sharding import PartitionSpec as P

bf16 = jnp.bfloat16
f32 = jnp.float32
vmem_cap = 62 * 1024 * 1024
epsilon = 1e-06
rope_base = 1000000.0
masked_score = -1e30


class Grid:
    def __init__(self, reps, shards):
        self.reps, self.shards = reps, shards
        self.devices = reps * shards
        self.places = reps // 2
        self.los = self.places // 2

    def here(self):
        self.r = lax.axis_index("rep")
        self.z = lax.axis_index("shard")
        self.core = self.r % 2
        place = self.r // 2
        self.hi = place // self.los
        self.lo = place % self.los
        return self

    def rep_of(self, hi, lo, core):
        return (hi * self.los + lo) * 2 + core

    def device(self, rep, shard):
        return {"rep": rep, "shard": shard}

    def other_lo(self, step):
        return (self.lo + step) % self.los

    def nearest(self):
        n = self.shards
        rows = [sorted(range(n), key=lambda p: (abs(p - z), p)) for z in range(n)]
        return [pick(self.z, [rows[z][turn] for z in range(n)]) for turn in range(n)]


def pick(index, values):
    out = jnp.int32(values[0])
    for i in range(1, len(values)):
        out = jnp.where(index == i, jnp.int32(values[i]), out)
    return out


class Sends:
    def __init__(self, sems):
        self.sems, self.used, self.open = sems, 0, []

    def start(self, src, dst, recv, device, when=None):
        copy = pltpu.make_async_remote_copy(
            src_ref=src,
            dst_ref=dst,
            send_sem=self.sems.at[self.used],
            recv_sem=recv,
            device_id=device,
            device_id_type=pl.DeviceIdType.MESH,
        )
        self.used += 1
        self.open.append((copy, when))
        if when is None:
            copy.start()
        else:
            pl.when(when)(copy.start)

    def arrived(self, dst, recv, device, when=None):
        copy = pltpu.make_async_remote_copy(
            src_ref=dst,
            dst_ref=dst,
            send_sem=self.sems.at[0],
            recv_sem=recv,
            device_id=device,
            device_id_type=pl.DeviceIdType.MESH,
        )
        if when is None:
            copy.wait_recv()
        else:
            pl.when(when)(copy.wait_recv)

    def drain(self):
        for copy, when in self.open:
            if when is None:
                copy.wait_send()
            else:
                pl.when(when)(copy.wait_send)
        self.open = []


def greet_line(g):
    barrier = pltpu.get_barrier_semaphore()
    for step in range(1, g.shards):
        pl.semaphore_signal(
            barrier,
            inc=1,
            device_id=g.device(g.r, (g.z + step) % g.shards),
            device_id_type=pl.DeviceIdType.MESH,
        )
    pl.semaphore_wait(barrier, g.shards - 1)


def greet_all(g):
    barrier = pltpu.get_barrier_semaphore()
    me = g.r * g.shards + g.z

    def one(step, carry):
        peer = (me + step) % g.devices
        pl.semaphore_signal(
            barrier,
            inc=1,
            device_id=g.device(peer // g.shards, peer % g.shards),
            device_id_type=pl.DeviceIdType.MESH,
        )
        return carry

    lax.fori_loop(1, g.devices, one, 0)
    pl.semaphore_wait(barrier, g.devices - 1)


def push_rows(g, src, dst, send_sems, recv_sems):
    me = g.r * g.shards + g.z

    def one(step, carry):
        peer = (me + step) % g.devices
        pltpu.make_async_remote_copy(
            src_ref=src.at[peer],
            dst_ref=dst.at[me],
            send_sem=send_sems.at[step],
            recv_sem=recv_sems.at[step],
            device_id=g.device(peer // g.shards, peer % g.shards),
            device_id_type=pl.DeviceIdType.MESH,
        ).start()
        return carry

    lax.fori_loop(1, g.devices, one, 0)


def push_wait(g, src, dst, send_sems, recv_sems):
    me = g.r * g.shards + g.z

    def one(step, carry):
        peer = (me + g.devices - step) % g.devices
        copy = pltpu.make_async_remote_copy(
            src_ref=src.at[peer],
            dst_ref=dst.at[peer],
            send_sem=send_sems.at[step],
            recv_sem=recv_sems.at[step],
            device_id=g.device(peer // g.shards, peer % g.shards),
            device_id_type=pl.DeviceIdType.MESH,
        )
        copy.wait_send()
        copy.wait_recv()
        return carry

    lax.fori_loop(1, g.devices, one, 0)


class PlaneGather:
    def __init__(self, g, s, view, lr, hr, dr, cr):
        self.g, self.s, self.view = g, s, view
        self.lr, self.hr, self.dr, self.cr = lr, hr, dr, cr

    @staticmethod
    def scratch(g, units):
        dma, others = pltpu.SemaphoreType.DMA, max(1, g.los - 1)
        return [dma((units, 2, others)), dma((units, 2)), dma((units, 2, others)), dma((units, 5 * g.los))]

    @staticmethod
    def sends(g, units):
        return 9 * g.los * units

    def at(self, hi, lo):
        return self.g.device(self.g.rep_of(hi, lo, self.g.core), self.g.z)

    def partner(self):
        g = self.g
        return g.device(g.rep_of(g.hi, g.lo, 1 - g.core), g.z)

    def own(self, u, src=None):
        g, s = self.g, self.s

        def dst(part):
            return self.view(u, g.hi, g.lo, g.core, part)

        src = src or dst
        for part in (0, 1):
            for step in range(1, g.los):
                s.start(src(part), dst(part), self.lr.at[u, part, step - 1], self.at(g.hi, g.other_lo(step)))
            s.start(src(1 - part), dst(1 - part), self.hr.at[u, 1 - part], self.at(1 - g.hi, g.lo))
        s.start(src(None), dst(None), self.cr.at[u, 0], self.partner())

    def take(self, u, hi, lo, part, recv, frm, partner_slot, onward=()):
        ref = self.view(u, hi, lo, self.g.core, part)
        self.s.arrived(ref, recv, frm)
        for sem, device in onward:
            self.s.start(ref, ref, sem, device)
        self.s.start(ref, ref, self.cr.at[u, partner_slot], self.partner())

    def first(self, u):
        g = self.g
        far = 1 - g.hi
        for step in range(1, g.los):
            frm = (g.lo + g.los - step) % g.los
            onward = [(self.dr.at[u, 0, step - 1], self.at(far, g.lo))]
            self.take(u, g.hi, frm, 0, self.lr.at[u, 0, step - 1], self.at(g.hi, frm), 5 * step, onward)
        onward = [(self.dr.at[u, 1, step - 1], self.at(g.hi, g.other_lo(step))) for step in range(1, g.los)]
        self.take(u, far, g.lo, 1, self.hr.at[u, 1], self.at(far, g.lo), 1, onward)
        for step in range(1, g.los):
            frm = (g.lo + g.los - step) % g.los
            self.take(u, g.hi, frm, 1, self.lr.at[u, 1, step - 1], self.at(g.hi, frm), 5 * step + 1)
        self.take(u, far, g.lo, 0, self.hr.at[u, 0], self.at(far, g.lo), 2)

    def second(self, u):
        g = self.g
        far = 1 - g.hi
        for step in range(1, g.los):
            frm = (g.lo + g.los - step) % g.los
            self.take(u, far, frm, 0, self.dr.at[u, 0, step - 1], self.at(far, g.lo), 5 * step + 2)
            self.take(u, far, frm, 1, self.dr.at[u, 1, step - 1], self.at(g.hi, frm), 5 * step + 3)

    def from_partner(self, u):
        g = self.g
        far, other = 1 - g.hi, 1 - g.core

        def got(hi, lo, part, slot):
            self.s.arrived(self.view(u, hi, lo, other, part), self.cr.at[u, slot], self.partner())

        got(g.hi, g.lo, None, 0)
        got(far, g.lo, 1, 1)
        got(far, g.lo, 0, 2)
        for step in range(1, g.los):
            frm = (g.lo + g.los - step) % g.los
            got(g.hi, frm, 0, 5 * step)
            got(g.hi, frm, 1, 5 * step + 1)
            got(far, frm, 0, 5 * step + 2)
            got(far, frm, 1, 5 * step + 3)


def add_rows(dst, *srcs, step=16):
    def one(i, carry):
        at = pl.ds(pl.multiple_of(i * step, step), step)
        total = srcs[0][at, :].astype(f32)
        for src in srcs[1:]:
            total = total + src[at, :].astype(f32)
        dst[at, :] = total.astype(dst.dtype)
        return carry

    lax.fori_loop(0, dst.shape[0] // step, one, 0)


class PlaneScatter:
    def __init__(self, g, s, p, cut, own, ra, rb0, rb1, rc0, rc1, sa, sb0, sb1, sc0, sc1, ls):
        self.g, self.s, self.p, self.cut, self.owned = g, s, p, cut, own
        self.ra, self.rb0, self.rb1, self.rc0, self.rc1 = ra, rb0, rb1, rc0, rc1
        self.sa, self.sb0, self.sb1, self.sc0, self.sc1, self.ls = sa, sb0, sb1, sc0, sc1, ls

    @staticmethod
    def scratch(g, units, block, halves, dtype):
        dma, others, v = pltpu.SemaphoreType.DMA, max(1, g.los - 1), pltpu.VMEM
        first, second = halves
        return [
            v((units, g.places) + block, dtype),
            v((units, g.places) + block, dtype),
            v((units, g.los) + first, dtype),
            v((units, others, 2) + second, dtype),
            v((units, others) + first, dtype),
            v((units,) + second, dtype),
            dma((units,)),
            dma((units,)),
            dma((units, others, 2)),
            dma((units, others)),
            dma((units,)),
            dma((units,)),
        ]

    @staticmethod
    def sends(g, units):
        return units * (3 * g.los + 2)

    def at(self, hi, lo):
        return self.g.device(self.g.rep_of(hi, lo, self.g.core), self.g.z)

    def partner(self):
        g = self.g
        return g.device(g.rep_of(g.hi, g.lo, 1 - g.core), g.z)

    def load(self, units):
        self.loads = []
        for turn in range(units):
            load = pltpu.make_async_copy(self.p(turn, self.g.core), self.owned.at[turn], self.ls.at[turn])
            load.start()
            self.loads.append(load)

    def to_partner(self, turn):
        self.s.start(self.p(turn, 1 - self.g.core), self.ra.at[turn], self.sa.at[turn], self.partner())

    def half(self, turn, place, part):
        return self.owned.at[(turn, place) + self.cut(part)]

    def mine(self, turn):
        return self.owned.at[turn, self.g.hi * self.g.los + self.g.lo]

    def a(self, turn):
        g, s = self.g, self.s
        far = 1 - g.hi
        self.loads[turn].wait()
        s.arrived(self.ra.at[turn], self.sa.at[turn], self.partner())

        def one(q, carry):
            line = self.owned.at[turn, q]
            add_rows(line, line, self.ra.at[turn, q])
            return carry

        lax.fori_loop(0, g.places, one, 0)
        block = self.owned.at[(turn, pl.ds(far * g.los, g.los)) + self.cut(0)]
        s.start(block, self.rb0.at[turn], self.sb0.at[turn], self.at(far, g.lo))
        for step in range(1, g.los):
            to = g.other_lo(step)
            for hi in range(2):
                sem = self.sb1.at[turn, step - 1, hi]
                s.start(self.half(turn, hi * g.los + to, 1), self.rb1.at[turn, step - 1, hi], sem, self.at(g.hi, to))

    def b(self, turn):
        g, s = self.g, self.s
        far = 1 - g.hi
        s.arrived(self.rb0.at[turn], self.sb0.at[turn], self.at(far, g.lo))
        for lo in range(g.los):
            line = self.half(turn, g.hi * g.los + lo, 0)
            add_rows(line, line, self.rb0.at[turn, lo])
        for step in range(1, g.los):
            to = g.other_lo(step)
            sem = self.sc0.at[turn, step - 1]
            s.start(self.half(turn, g.hi * g.los + to, 0), self.rc0.at[turn, step - 1], sem, self.at(g.hi, to))
        for step in range(1, g.los):
            frm = (g.lo + g.los - step) % g.los
            for hi in range(2):
                s.arrived(self.rb1.at[turn, step - 1, hi], self.sb1.at[turn, step - 1, hi], self.at(g.hi, frm))
        for hi in range(2):
            line = self.half(turn, hi * g.los + g.lo, 1)
            add_rows(line, line, *[self.rb1.at[turn, step, hi] for step in range(g.los - 1)])
        s.start(self.half(turn, far * g.los + g.lo, 1), self.rc1.at[turn], self.sc1.at[turn], self.at(far, g.lo))

    def c(self, turn):
        g, s = self.g, self.s
        place = g.hi * g.los + g.lo
        for step in range(1, g.los):
            frm = (g.lo + g.los - step) % g.los
            s.arrived(self.rc0.at[turn, step - 1], self.sc0.at[turn, step - 1], self.at(g.hi, frm))
        line = self.half(turn, place, 0)
        add_rows(line, line, *[self.rc0.at[turn, step] for step in range(g.los - 1)])
        s.arrived(self.rc1.at[turn], self.sc1.at[turn], self.at(1 - g.hi, g.lo))
        line = self.half(turn, place, 1)
        add_rows(line, line, self.rc1.at[turn])


def pass_along(g, s, zp, src, dst, zr):
    n = g.shards
    right, left = g.device(g.r, jnp.minimum(g.z + 1, n - 1)), g.device(g.r, jnp.maximum(g.z - 1, 0))
    s.start(src, dst, zr.at[zp], right, (zp <= g.z) & (g.z + 1 < n))
    s.start(src, dst, zr.at[zp], left, (zp >= g.z) & (g.z > 0))


def send_line(g, s, zp, line, out_ref, rl, rr, sl, sr, last):
    n = g.shards
    left, right = g.device(g.r, jnp.maximum(g.z - 1, 0)), g.device(g.r, jnp.minimum(g.z + 1, n - 1))
    has_left, has_right = g.z > 0, g.z + 1 < n
    if last:
        s.arrived(rl.at[g.z], sl.at[g.z], left, has_left)
        s.arrived(rr.at[g.z], sr.at[g.z], right, has_right)

        @pl.when(has_left & has_right)
        def _():
            add_rows(out_ref, line, rl.at[g.z], rr.at[g.z])

        @pl.when(has_left & jnp.logical_not(has_right))
        def _():
            add_rows(out_ref, line, rl.at[g.z])

        @pl.when(has_right & jnp.logical_not(has_left))
        def _():
            add_rows(out_ref, line, rr.at[g.z])
    else:
        onward_right, onward_left = zp > g.z, zp < g.z

        @pl.when(onward_right & has_left)
        def _():
            s.arrived(rl.at[zp], sl.at[zp], left)
            add_rows(line, line, rl.at[zp])

        @pl.when(onward_left & has_right)
        def _():
            s.arrived(rr.at[zp], sr.at[zp], right)
            add_rows(line, line, rr.at[zp])

        s.start(line, rl.at[zp], sl.at[zp], right, onward_right)
        s.start(line, rr.at[zp], sr.at[zp], left, onward_left)


def line_scratch(shards, block, dtype):
    v, dma = pltpu.VMEM, pltpu.SemaphoreType.DMA
    return [v((shards,) + block, dtype), v((shards,) + block, dtype), dma((shards,)), dma((shards,))]


hbm = pl.BlockSpec(memory_space=pl.ANY)
vmem = pl.BlockSpec(memory_space=pltpu.VMEM)


def params(ident):
    return pltpu.CompilerParams(collective_id=ident, has_side_effects=True, vmem_limit_bytes=vmem_cap)


def collect_kernel(reps, shards, layout, x_ref, small_ref, wq_ref, wk_ref, wv_ref, xs_ref, smalls_ref, w_ref, sems, xr, mr, wr, lr, hr, dr, cr, ls):
    g = Grid(reps, shards).here()
    s = Sends(sems)
    n = g.shards
    q_cols, kv_cols, kv_heads, head_dim = layout
    deep = wq_ref.shape[0]
    piece = deep // g.reps
    cols = q_cols + 2 * kv_cols
    first = cols // 2 // 128 * 128
    spans = {0: pl.ds(0, first), 1: pl.ds(first, cols - first), None: pl.ds(0, cols)}
    mine = pl.ds(pl.multiple_of(g.r * piece, piece), piece)

    def view(u, hi, lo, core, part):
        row = pl.multiple_of(u * deep + g.rep_of(hi, lo, core) * piece, piece)
        return w_ref.at[pl.ds(row, piece), spans[part]]

    def pieces(zp, u):
        row = pl.ds(pl.multiple_of(u * deep + g.r * piece, piece), piece)
        at_q = pl.ds(pl.multiple_of(zp * q_cols, 128), q_cols)
        at_kv = pl.ds(pl.multiple_of(zp * kv_heads // n * head_dim, 128), kv_cols)
        return (
            (wq_ref.at[mine, at_q], w_ref.at[row, pl.ds(0, q_cols)]),
            (wk_ref.at[mine, at_kv], w_ref.at[row, pl.ds(q_cols, kv_cols)]),
            (wv_ref.at[mine, at_kv], w_ref.at[row, pl.ds(q_cols + kv_cols, kv_cols)]),
        )

    keeps = [
        pltpu.make_async_copy(x_ref, xs_ref.at[g.z], ls.at[0]),
        pltpu.make_async_copy(small_ref, smalls_ref.at[g.z], ls.at[1]),
    ]
    locals_ = [pltpu.make_async_copy(src, dst, ls.at[2 + i]) for i, (src, dst) in enumerate(pieces(g.z, g.z))]
    for copy in locals_ + keeps:
        copy.start()
    barrier = pltpu.get_barrier_semaphore()
    peers = [g.device(g.r, (g.z + step) % n) for step in range(1, n)]
    peers += [g.device(g.rep_of(g.hi, g.other_lo(step), g.core), g.z) for step in range(1, g.los)]
    peers += [g.device(g.rep_of(1 - g.hi, g.lo, g.core), g.z), g.device(g.rep_of(g.hi, g.lo, 1 - g.core), g.z)]
    for peer in peers:
        pl.semaphore_signal(barrier, inc=1, device_id=peer, device_id_type=pl.DeviceIdType.MESH)
    pl.semaphore_wait(barrier, len(peers))

    plane = PlaneGather(g, s, view, lr, hr, dr, cr)
    for step in range(1, n):
        zp = (g.z + step) % n
        for i, (src, dst) in enumerate(pieces(zp, g.z)):
            s.start(src, dst, wr.at[step, i], g.device(g.r, zp))
    order = g.nearest()

    def line(turn):
        zp = order[turn]
        if turn:
            s.arrived(smalls_ref.at[zp], mr.at[zp], g.device(g.r, zp))
        pass_along(g, s, zp, smalls_ref.at[zp] if turn else small_ref, smalls_ref.at[zp], mr)
        if turn:
            s.arrived(xs_ref.at[zp], xr.at[zp], g.device(g.r, zp))
        pass_along(g, s, zp, xs_ref.at[zp] if turn else x_ref, xs_ref.at[zp], xr)

    line(0)
    for copy in locals_:
        copy.wait()
    plane.own(g.z)

    def unit(step):
        return (g.z + n - step) % n

    for step in range(1, n):
        u = unit(step)
        for i, (_, dst) in enumerate(pieces(g.z, u)):
            s.arrived(dst, wr.at[step, i], g.device(g.r, u))
        plane.own(u)
    line(1)
    for step in range(n):
        plane.first(unit(step))
        if step:
            plane.second(unit(step - 1))
        if 2 + step < n:
            line(2 + step)
    plane.second(unit(n - 1))
    for step in range(n):
        plane.from_partner(unit(step))
    for copy in keeps:
        copy.wait()
    s.drain()


def collect(reps, shards, x, small, wq, wk, wv, layout, ident):
    g = Grid(reps, shards)
    dma = pltpu.SemaphoreType.DMA
    n = shards
    cols = layout[0] + 2 * layout[1]
    return pl.pallas_call(
        functools.partial(collect_kernel, reps, shards, layout),
        out_shape=(
            jax.ShapeDtypeStruct((n,) + x.shape, x.dtype),
            jax.ShapeDtypeStruct((n,) + small.shape, small.dtype),
            jax.ShapeDtypeStruct((n * wq.shape[0], cols), wq.dtype),
        ),
        in_specs=[vmem, vmem, hbm, hbm, hbm],
        out_specs=(vmem, vmem, vmem),
        scratch_shapes=[dma((PlaneGather.sends(g, n) + 7 * n,)), dma((n,)), dma((n,)), dma((n, 3))]
        + PlaneGather.scratch(g, n)
        + [dma((5,))],
        compiler_params=params(ident),
        name="collect",
    )(x, small, wq, wk, wv)


def gather_all_kernel(reps, shards, x_ref, slab_ref, out_ref, slabs_ref, sems, zr, ps, pr, ls, lr, hr, dr, cr):
    g = Grid(reps, shards).here()
    s = Sends(sems)
    half = x_ref.shape[0] // 2
    n = g.shards
    spans = {0: pl.ds(0, half), 1: pl.ds(half, half), None: pl.ds(0, 2 * half)}
    order = g.nearest()

    def view(u, hi, lo, core, part):
        return out_ref.at[g.rep_of(hi, lo, core) * n + u, spans[part]]

    plane = PlaneGather(g, s, view, lr, hr, dr, cr)
    keep = pltpu.make_async_copy(x_ref, view(g.z, g.hi, g.lo, g.core, None), ls.at[0])
    keep.start()
    greet_all(g)
    push_rows(g, slab_ref, slabs_ref, ps, pr)
    me = g.r * n + g.z
    keep_slab = pltpu.make_async_copy(slab_ref.at[me], slabs_ref.at[me], ls.at[1])
    keep_slab.start()
    for turn in range(n + 2):
        if turn < n:
            zp = order[turn]
            dst = view(zp, g.hi, g.lo, g.core, None)
            if turn:
                s.arrived(dst, zr.at[zp], g.device(g.r, zp))
            pass_along(g, s, zp, dst if turn else x_ref, dst, zr)
            plane.own(zp, None if turn else lambda part: x_ref.at[spans[part]])
        if 0 <= turn - 1 < n:
            plane.first(order[turn - 1])
        if 0 <= turn - 2 < n:
            plane.second(order[turn - 2])
    for turn in range(n):
        plane.from_partner(order[turn])
    keep.wait()
    keep_slab.wait()
    push_wait(g, slab_ref, slabs_ref, ps, pr)
    s.drain()


def gather_all(reps, shards, x, slab, ident):
    g = Grid(reps, shards)
    dma = pltpu.SemaphoreType.DMA
    n = shards
    return pl.pallas_call(
        functools.partial(gather_all_kernel, reps, shards),
        out_shape=(
            jax.ShapeDtypeStruct((g.devices,) + x.shape, x.dtype),
            jax.ShapeDtypeStruct(slab.shape, slab.dtype),
        ),
        in_specs=[vmem, vmem],
        out_specs=(hbm, vmem),
        scratch_shapes=[
            dma((PlaneGather.sends(g, n) + 2 * n,)),
            dma((n,)),
            dma((g.devices,)),
            dma((g.devices,)),
            dma((2,)),
        ]
        + PlaneGather.scratch(g, n),
        compiler_params=params(ident),
        name="gather_all",
    )(x, slab)


def scatter_all_kernel(reps, shards, slabbed, *refs):
    if slabbed:
        p_ref, slab_ref, out_ref, slabs_ref, *rest = refs
    else:
        p_ref, out_ref, *rest = refs
    rl, rr, sl, sr, sems, ps, pr, slab_sem, *rest = rest
    g = Grid(reps, shards).here()
    s = Sends(sems)
    n = g.shards
    half = out_ref.shape[0] // 2
    order = g.nearest()[::-1]
    plane = PlaneScatter(
        g, s, lambda turn, core: p_ref.at[:, core, order[turn]], lambda part: (pl.ds(part * half, half),), *rest
    )
    plane.load(n)
    greet_all(g)
    for turn in range(n):
        plane.to_partner(turn)
    if slabbed:
        push_rows(g, slab_ref, slabs_ref, ps, pr)
        me = g.r * n + g.z
        keep_slab = pltpu.make_async_copy(slab_ref.at[me], slabs_ref.at[me], slab_sem.at[0])
        keep_slab.start()
    for turn in range(n + 2):
        if turn < n:
            plane.a(turn)
        if 0 <= turn - 1 < n:
            plane.b(turn - 1)
        if 0 <= turn - 2 < n:
            plane.c(turn - 2)
            send_line(g, s, order[turn - 2], plane.mine(turn - 2), out_ref, rl, rr, sl, sr, last=turn - 2 == n - 1)
    if slabbed:
        keep_slab.wait()
        push_wait(g, slab_ref, slabs_ref, ps, pr)
    s.drain()


def scatter_all(reps, shards, p, slab, ident):
    g = Grid(reps, shards)
    n = shards
    _, rows, width = p.shape
    half = rows // 2
    dma = pltpu.SemaphoreType.DMA
    slabbed = slab is not None
    out_shape = (jax.ShapeDtypeStruct((rows, width), f32),)
    if slabbed:
        out_shape += (jax.ShapeDtypeStruct(slab.shape, slab.dtype),)
    done = pl.pallas_call(
        functools.partial(scatter_all_kernel, reps, shards, slabbed),
        out_shape=out_shape,
        in_specs=[hbm] + [vmem] * slabbed,
        out_specs=(vmem,) * len(out_shape),
        scratch_shapes=line_scratch(n, (rows, width), p.dtype)
        + [dma((PlaneScatter.sends(g, n) + 2 * n,)), dma((g.devices,)), dma((g.devices,)), dma((1,))]
        + PlaneScatter.scratch(g, n, (rows, width), ((half, width), (half, width)), p.dtype),
        compiler_params=params(ident),
        name="scatter_all",
    )(p.reshape(g.places, 2, n, rows, width), *([slab] if slabbed else []))
    return done if slabbed else done[0]


def scatter_wide(reps, shards, p, slab, ident, chunks):
    if chunks == 1:
        return scatter_all(reps, shards, p, slab, ident)
    step = p.shape[2] // chunks
    parts = [
        scatter_all(reps, shards, p[:, :, i * step : (i + 1) * step], slab if i == 0 else None, ident + i)
        for i in range(chunks)
    ]
    if slab is None:
        return jnp.concatenate(parts, axis=1)
    first, slabs = parts[0]
    return jnp.concatenate([first] + parts[1:], axis=1), slabs


def deliver_kernel(reps, shards, p_ref, w_ref, out_ref, ws_ref, line_own, rl, rr, sl, sr, sems, line_loads, wr, keep_sem, *rest):
    g = Grid(reps, shards).here()
    s = Sends(sems)
    n = g.shards
    gather_refs, scatter_refs = rest[:4], rest[4:]
    cols = w_ref.shape[-1]
    first = cols // 2 // 128 * 128
    spans = {0: pl.ds(0, first), 1: pl.ds(first, cols - first), None: pl.ds(0, cols)}
    order = g.nearest()[::-1]
    scatter = PlaneScatter(
        g, s, lambda turn, core: w_ref.at[turn, :, core], lambda part: (slice(None), spans[part]), *scatter_refs
    )
    gather = PlaneGather(
        g, s, lambda u, hi, lo, core, part: ws_ref.at[u, g.rep_of(hi, lo, core), :, spans[part]], *gather_refs
    )
    scatter.load(n)
    loads = []
    for turn in range(n):
        load = pltpu.make_async_copy(p_ref.at[order[turn]], line_own.at[turn], line_loads.at[turn])
        load.start()
        loads.append(load)
    barrier = pltpu.get_barrier_semaphore()
    peers = [g.device(g.r, (g.z + step) % n) for step in range(1, n)]
    peers += [g.device(g.rep_of(g.hi, g.other_lo(step), g.core), g.z) for step in range(1, g.los)]
    peers += [g.device(g.rep_of(1 - g.hi, g.lo, g.core), g.z), g.device(g.rep_of(g.hi, g.lo, 1 - g.core), g.z)]
    for peer in peers:
        pl.semaphore_signal(barrier, inc=1, device_id=peer, device_id_type=pl.DeviceIdType.MESH)
    pl.semaphore_wait(barrier, len(peers))

    for turn in range(n):
        scatter.to_partner(turn)

    def line(turn):
        loads[turn].wait()
        send_line(g, s, order[turn], line_own.at[turn], out_ref, rl, rr, sl, sr, last=turn == n - 1)

    def owner(turn):
        scatter.c(turn)
        dst = ws_ref.at[g.z, g.r]
        keep = pltpu.make_async_copy(scatter.mine(turn), dst, keep_sem.at[0])
        pl.when(g.z == turn)(keep.start)
        s.start(scatter.mine(turn), dst, wr.at[g.z], g.device(g.r, turn), g.z != turn)
        pl.when(g.z == turn)(keep.wait)

    line(0)
    for turn in range(n + 2):
        if turn < n:
            scatter.a(turn)
        if 0 <= turn - 1 < n:
            scatter.b(turn - 1)
        if 1 <= turn < n - 1:
            line(turn)
        if 0 <= turn - 2 < n:
            owner(turn - 2)
    gather.own(g.z)

    def unit(step):
        return (g.z + n - step) % n

    for step in range(1, n):
        u = unit(step)
        s.arrived(ws_ref.at[u, g.r], wr.at[u], g.device(g.r, u))
        gather.own(u)
        gather.first(unit(step - 1))
        if step > 1:
            gather.second(unit(step - 2))
    gather.first(unit(n - 1))
    gather.second(unit(n - 2))
    gather.second(unit(n - 1))
    line(n - 1)
    for step in range(n):
        gather.from_partner(unit(step))
    s.drain()


def deliver(reps, shards, p, w, ident):
    g = Grid(reps, shards)
    n = shards
    dma = pltpu.SemaphoreType.DMA
    _, rows, width = p.shape
    _, _, piece, cols = w.shape
    first = cols // 2 // 128 * 128
    return pl.pallas_call(
        functools.partial(deliver_kernel, reps, shards),
        out_shape=(jax.ShapeDtypeStruct((rows, width), f32), jax.ShapeDtypeStruct(w.shape, w.dtype)),
        in_specs=[hbm, hbm],
        out_specs=(vmem, vmem),
        scratch_shapes=[pltpu.VMEM(p.shape, p.dtype)]
        + line_scratch(n, (rows, width), p.dtype)
        + [
            dma((PlaneGather.sends(g, n) + PlaneScatter.sends(g, n) + 3 * n,)),
            dma((n,)),
            dma((n,)),
            dma((1,)),
        ]
        + PlaneGather.scratch(g, n)
        + PlaneScatter.scratch(g, n, (piece, cols), ((piece, first), (piece, cols - first)), w.dtype),
        compiler_params=params(ident),
        name="deliver",
    )(p, w.reshape(n, g.places, 2, piece, cols))


def turned(x, cosine, sine):
    return x * cosine + pltpu.roll(x, x.shape[-1] // 2, 1) * sine


def mean_last(x):
    return jnp.sum(x, axis=-1, keepdims=True) * (1.0 / x.shape[-1])


def unit_of(x):
    inverse = lax.rsqrt(mean_last(x * x) + epsilon)
    return inverse, x * inverse


def dot_t(a, b):
    return lax.dot_general(a, b, (((1,), (1,)), ((), ())), preferred_element_type=f32)


def t_dot(a, b):
    return lax.dot_general(a, b, (((0,), (0,)), ((), ())), preferred_element_type=f32)


def softmax_rows(q_rot, k_rot, bias, head_dim):
    scores = dot_t(q_rot, k_rot) * head_dim ** (-0.5) + bias
    raised = jnp.exp(scores - jnp.max(scores, axis=-1, keepdims=True))
    return raised * (1.0 / jnp.sum(raised, axis=-1, keepdims=True))


def back_unit(grad_scaled, unit, inverse, gain):
    gained = grad_scaled * gain
    return inverse * (gained - unit * mean_last(gained * unit))


def attend_block(b, heads, x_ref, w_ref, wo_ref, gain_ref, qg_ref, kg_ref, cos_ref, sin_ref, bias_ref, hid_ref, qkv_ref, att_ref, line):
    my_heads, my_kv, head_dim = heads
    x = x_ref[b].astype(f32)
    _, unit = unit_of(x)
    hid_ref[b] = (unit * gain_ref[...]).astype(bf16)
    qkv_ref[b] = jnp.dot(hid_ref[b], w_ref[...], preferred_element_type=f32)
    cosine, sine, bias = cos_ref[b], sin_ref[b], bias_ref[b]
    group = my_heads // my_kv
    for n in range(my_kv):
        at_k = (my_heads + n) * head_dim
        at_v = (my_heads + my_kv + n) * head_dim
        _, k_unit = unit_of(qkv_ref[b, :, at_k : at_k + head_dim])
        k_rot = turned(k_unit * kg_ref[...], cosine, sine).astype(bf16)
        values = qkv_ref[b, :, at_v : at_v + head_dim].astype(bf16)
        for h in range(n * group, (n + 1) * group):
            span = slice(h * head_dim, (h + 1) * head_dim)
            _, q_unit = unit_of(qkv_ref[b, :, span])
            q_rot = turned(q_unit * qg_ref[...], cosine, sine).astype(bf16)
            probs = softmax_rows(q_rot, k_rot, bias, head_dim)
            mixed = jnp.dot(probs.astype(bf16), values, preferred_element_type=f32)
            att_ref[b, :, span] = mixed.astype(bf16)
    line[...] = jnp.dot(att_ref[b], wo_ref[...], preferred_element_type=f32).astype(bf16)


def attend_back_block(b, heads, ga_ref, qkv_ref, wo_ref, qg_ref, kg_ref, cos_ref, sin_ref, bias_ref, gm_ref, gqkv_ref, qsum_ref, ksum_ref):
    my_heads, my_kv, head_dim = heads
    gm_ref[...] = dot_t(ga_ref[b], wo_ref[...]).astype(bf16)
    cosine, sine, bias = cos_ref[b], sin_ref[b], bias_ref[b]
    group = my_heads // my_kv
    qg, kg = qg_ref[...], kg_ref[...]
    for n in range(my_kv):
        at_k = (my_heads + n) * head_dim
        at_v = (my_heads + my_kv + n) * head_dim
        k_inverse, k_unit = unit_of(qkv_ref[b, :, at_k : at_k + head_dim])
        k_rot = turned(k_unit * kg, cosine, sine).astype(bf16)
        values = qkv_ref[b, :, at_v : at_v + head_dim].astype(bf16)
        grad_k = jnp.zeros(k_unit.shape, f32)
        grad_v = jnp.zeros(k_unit.shape, f32)
        for h in range(n * group, (n + 1) * group):
            span = slice(h * head_dim, (h + 1) * head_dim)
            q_inverse, q_unit = unit_of(qkv_ref[b, :, span])
            q_rot = turned(q_unit * qg, cosine, sine).astype(bf16)
            probs = softmax_rows(q_rot, k_rot, bias, head_dim)
            grad_mixed = gm_ref[:, span]
            grad_weights = dot_t(grad_mixed, values)
            centre = jnp.sum(probs * grad_weights, axis=-1, keepdims=True)
            grad_scores = (probs * (grad_weights - centre) * head_dim ** (-0.5)).astype(bf16)
            grad_v = grad_v + t_dot(probs.astype(bf16), grad_mixed)
            grad_k = grad_k + t_dot(grad_scores, q_rot)
            grad_q = jnp.dot(grad_scores, k_rot, preferred_element_type=f32)
            grad_q = turned(grad_q, cosine, -sine)
            qsum_ref[...] += jnp.sum(grad_q * q_unit, axis=0, keepdims=True)
            gqkv_ref[b, :, span] = back_unit(grad_q, q_unit, q_inverse, qg).astype(bf16)
        grad_k = turned(grad_k, cosine, -sine)
        ksum_ref[...] += jnp.sum(grad_k * k_unit, axis=0, keepdims=True)
        gqkv_ref[b, :, at_k : at_k + head_dim] = back_unit(grad_k, k_unit, k_inverse, kg).astype(bf16)
        gqkv_ref[b, :, at_v : at_v + head_dim] = grad_v.astype(bf16)


class GatherAll:
    def __init__(self, g, s, x_ref, out_ref, zr, plane_sems):
        self.g, self.s, self.x_ref, self.out_ref, self.zr = g, s, x_ref, out_ref, zr
        half = x_ref.shape[0] // 2
        self.spans = {0: pl.ds(0, half), 1: pl.ds(half, half), None: pl.ds(0, 2 * half)}
        self.order = g.nearest()
        self.plane = PlaneGather(g, s, self.view, *plane_sems)

    @staticmethod
    def scratch(g):
        dma = pltpu.SemaphoreType.DMA
        return [dma((g.shards,))] + PlaneGather.scratch(g, g.shards)

    @staticmethod
    def sends(g):
        return PlaneGather.sends(g, g.shards) + 2 * g.shards

    def view(self, u, hi, lo, core, part):
        return self.out_ref.at[self.g.rep_of(hi, lo, core) * self.g.shards + u, self.spans[part]]

    def own(self):
        g = self.g
        return self.view(g.z, g.hi, g.lo, g.core, None)

    def line(self, turn):
        g, zp = self.g, self.order[turn]
        dst = self.view(zp, g.hi, g.lo, g.core, None)
        if turn:
            self.s.arrived(dst, self.zr.at[zp], g.device(g.r, zp))
        pass_along(g, self.s, zp, dst if turn else self.x_ref, dst, self.zr)
        self.plane.own(zp, None if turn else lambda part: self.x_ref.at[self.spans[part]])

    def first(self, turn):
        self.plane.first(self.order[turn])

    def second(self, turn):
        self.plane.second(self.order[turn])

    def finish(self):
        for turn in range(self.g.shards):
            self.plane.from_partner(self.order[turn])


class ScatterAll:
    def __init__(self, g, s, p_ref, out_ref, rl, rr, sl, sr, *plane_refs):
        self.g, self.s, self.out_ref = g, s, out_ref
        self.lines = (rl, rr, sl, sr)
        half = out_ref.shape[0] // 2
        self.order = g.nearest()[::-1]
        self.plane = PlaneScatter(
            g,
            s,
            lambda turn, core: p_ref.at[:, core, self.order[turn]],
            lambda part: (pl.ds(part * half, half),),
            *plane_refs,
        )

    @staticmethod
    def scratch(g, block, dtype):
        rows, width = block
        half = (rows // 2, width)
        return line_scratch(g.shards, block, dtype) + PlaneScatter.scratch(g, g.shards, block, (half, half), dtype)

    @staticmethod
    def sends(g):
        return PlaneScatter.sends(g, g.shards) + 2 * g.shards

    def load(self):
        self.plane.load(self.g.shards)

    def to_partner(self):
        for turn in range(self.g.shards):
            self.plane.to_partner(turn)

    def step(self, turn):
        n = self.g.shards
        if turn < n:
            self.plane.a(turn)
        if 0 <= turn - 1 < n:
            self.plane.b(turn - 1)
        if 0 <= turn - 2 < n:
            t = turn - 2
            self.plane.c(t)
            send_line(self.g, self.s, self.order[t], self.plane.mine(t), self.out_ref, *self.lines, last=t == n - 1)


def attend_kernel(reps, shards, heads, *refs):
    (
        x_ref, w_ref, wo_ref, gain_ref, qg_ref, kg_ref, cos_ref, sin_ref, bias_ref, cot_ref,
        hid_ref, qkv_ref, att_ref, out_ref, cots_ref,
        own, rl, rr, sl, sr, sems, keep_sem, *gather_sems,
    ) = refs
    g = Grid(reps, shards).here()
    s = Sends(sems)
    n = g.shards
    gather = GatherAll(g, s, cot_ref, cots_ref, gather_sems[0], gather_sems[1:])
    keep = pltpu.make_async_copy(cot_ref, gather.own(), keep_sem.at[0])
    keep.start()
    greet_all(g)
    gather.line(0)
    order = g.nearest()[::-1]
    for turn in range(n):
        zp = order[turn]
        attend_block(
            zp, heads, x_ref, w_ref, wo_ref, gain_ref, qg_ref, kg_ref, cos_ref, sin_ref, bias_ref,
            hid_ref, qkv_ref, att_ref, own.at[turn],
        )
        send_line(g, s, zp, own.at[turn], out_ref, rl, rr, sl, sr, last=turn == n - 1)
        if turn + 1 < n:
            gather.line(turn + 1)
            gather.first(turn)
        if turn > 0:
            gather.second(turn - 1)
    gather.first(n - 1)
    gather.second(n - 1)
    gather.finish()
    keep.wait()
    s.drain()


def attend(reps, shards, heads, x, w, wo, gain, qg, kg, cosine, sine, bias, cot, ident):
    g = Grid(reps, shards)
    dma, v = pltpu.SemaphoreType.DMA, pltpu.VMEM
    n, rows, width = x.shape
    cols = w.shape[1]
    return pl.pallas_call(
        functools.partial(attend_kernel, reps, shards, heads),
        out_shape=(
            jax.ShapeDtypeStruct(x.shape, bf16),
            jax.ShapeDtypeStruct((n, rows, cols), f32),
            jax.ShapeDtypeStruct((n, rows, wo.shape[0]), bf16),
            jax.ShapeDtypeStruct((rows, width), f32),
            jax.ShapeDtypeStruct((g.devices, rows, width), bf16),
        ),
        in_specs=[vmem] * 10,
        out_specs=(vmem, vmem, vmem, vmem, hbm),
        scratch_shapes=[v((n, rows, width), bf16)]
        + line_scratch(n, (rows, width), bf16)
        + [dma((GatherAll.sends(g) + 2 * n,)), dma((1,))]
        + GatherAll.scratch(g),
        compiler_params=params(ident),
        name="attend",
    )(x, w, wo, gain, qg, kg, cosine, sine, bias, cot)


def attend_back_kernel(reps, shards, heads, *refs):
    (
        ga_ref, qkv_ref, wo_ref, qg_ref, kg_ref, cos_ref, sin_ref, bias_ref, p_ref,
        gas_ref, gqkv_ref, qsum_ref, ksum_ref, out_ref,
        gm, zr, sems, keep_sem, *scatter_refs,
    ) = refs
    g = Grid(reps, shards).here()
    s = Sends(sems)
    n = g.shards
    scatter = ScatterAll(g, s, p_ref, out_ref, *scatter_refs)
    scatter.load()
    keep = pltpu.make_async_copy(ga_ref, gas_ref.at[g.z], keep_sem.at[0])
    keep.start()
    qsum_ref[...] = jnp.zeros(qsum_ref.shape, f32)
    ksum_ref[...] = jnp.zeros(ksum_ref.shape, f32)
    greet_all(g)
    order = g.nearest()

    def line(turn):
        zp = order[turn]
        dst = gas_ref.at[zp]
        if turn:
            s.arrived(dst, zr.at[zp], g.device(g.r, zp))
        pass_along(g, s, zp, dst if turn else ga_ref, dst, zr)

    line(0)
    scatter.to_partner()
    keep.wait()
    for turn in range(n):
        scatter.step(turn)
        if turn + 1 < n:
            line(turn + 1)
        attend_back_block(
            order[turn], heads, gas_ref, qkv_ref, wo_ref, qg_ref, kg_ref, cos_ref, sin_ref, bias_ref,
            gm, gqkv_ref, qsum_ref, ksum_ref,
        )
    scatter.step(n)
    scatter.step(n + 1)
    s.drain()


def attend_back(reps, shards, heads, ga, qkv, wo, qg, kg, cosine, sine, bias, p, ident):
    g = Grid(reps, shards)
    dma, v = pltpu.SemaphoreType.DMA, pltpu.VMEM
    n = shards
    rows, width = ga.shape
    out_width = p.shape[2]
    row = jax.ShapeDtypeStruct(qg.shape, f32)
    return pl.pallas_call(
        functools.partial(attend_back_kernel, reps, shards, heads),
        out_shape=(
            jax.ShapeDtypeStruct((n, rows, width), bf16),
            jax.ShapeDtypeStruct(qkv.shape, bf16),
            row,
            row,
            jax.ShapeDtypeStruct((rows, out_width), f32),
        ),
        in_specs=[vmem] * 8 + [hbm],
        out_specs=(vmem,) * 5,
        scratch_shapes=[v((rows, wo.shape[0]), bf16), dma((n,)), dma((ScatterAll.sends(g) + 2 * n,)), dma((1,))]
        + ScatterAll.scratch(g, (rows, out_width), p.dtype),
        compiler_params=params(ident),
        name="attend_back",
    )(ga, qkv, wo, qg, kg, cosine, sine, bias, p.reshape(g.places, 2, n, rows, out_width))


def inverse_rms(values):
    return lax.rsqrt(jnp.mean(values * values, axis=-1, keepdims=True) + epsilon)


def rope_tables(segment_rows, width):
    length = segment_rows.shape[1]
    places = jnp.arange(length, dtype=jnp.int32)
    same = segment_rows[:, :, None] == segment_rows[:, None, :]
    first = jnp.min(jnp.where(same, places[None, None, :], length), axis=2)
    offset = (places[None] - first).astype(f32)
    half = width // 2
    frequency = rope_base ** (-2.0 * jnp.arange(half, dtype=f32) / width)
    angle = offset[..., None] * frequency[None, None, :]
    cosine, sine = jnp.cos(angle), jnp.sin(angle)
    cosine = jnp.concatenate([cosine, cosine], axis=-1)
    sine = jnp.concatenate([-sine, sine], axis=-1)
    allowed = same & (places[None, None, :] <= places[None, :, None])
    return cosine, sine, allowed


def norm_back(grad_scaled, unit, inverse, gain):
    gained = grad_scaled * gain
    return inverse * (gained - unit * jnp.mean(gained * unit, axis=-1, keepdims=True))


def matmul(a, b, dims=((1,), (0,))):
    return lax.dot_general(a, b, (dims, ((), ())), preferred_element_type=f32)


def local(
    tokens,
    segments,
    routes,
    attn_gain,
    w_query,
    key_weight,
    value_weight,
    w_out,
    query_gain,
    key_gain,
    ffn_gain,
    w_router,
    w_gate,
    w_up,
    w_down,
    cotangent,
):
    reps, shards = lax.axis_size("rep"), lax.axis_size("shard")
    devices = reps * shards
    r, z = lax.axis_index("rep"), lax.axis_index("shard")
    length, width = tokens.shape
    deep = w_query.shape[0]
    head_dim = query_gain.shape[0] * shards
    heads = w_query.shape[1] // head_dim
    kv_heads = key_weight.shape[1] // head_dim
    experts = w_router.shape[1]
    top = routes.shape[1]
    capacity = 2 * length * top // experts
    my_heads = heads // shards
    my_kv = max(1, kv_heads // shards)
    shared_by = max(1, shards // kv_heads)
    q_cols, kv_cols = my_heads * head_dim, my_kv * head_dim
    cols = q_cols + 2 * kv_cols
    piece = deep // reps
    chunks = max(1, devices // 32)
    part = head_dim // shards

    def column(values, rows=deep):
        return jnp.pad(values.reshape(-1, 1), ((0, rows - values.size), (0, 0)))

    small = jnp.concatenate(
        [
            w_router,
            column(attn_gain),
            column(ffn_gain),
            column(query_gain),
            column(key_gain),
            column(segments[0].astype(bf16)),
        ],
        axis=1,
    )
    small_cols = -(-small.shape[1] // 128) * 128
    small = jnp.pad(small, ((0, 0), (0, small_cols - small.shape[1])))
    layout = (q_cols, kv_cols, kv_heads, head_dim)
    block_tokens, small_all, w_in = collect(
        reps, shards, tokens, small, w_query, key_weight, value_weight, layout, 1
    )
    router_full = small_all[:, :, :experts].reshape(width, experts)
    gain_one = small_all[:, :, experts].reshape(1, width).astype(f32)
    gain_two = small_all[:, :, experts + 1].reshape(1, width).astype(f32)
    qgain = small_all[:, :part, experts + 2].reshape(1, head_dim).astype(f32)
    kgain = small_all[:, :part, experts + 3].reshape(1, head_dim).astype(f32)
    segment_rows = small_all[:, :length, experts + 4].astype(jnp.int32)

    head_sizes = (my_heads, my_kv, head_dim)
    cosine, sine, allowed = rope_tables(segment_rows, head_dim)
    bias = jnp.where(allowed, 0.0, masked_score)
    hidden_in, qkv, attn_out, mixed, cotangents = attend(
        reps, shards, head_sizes, block_tokens, w_in, w_out, gain_one, qgain, kgain, cosine, sine, bias, cotangent, 2
    )
    own_tokens = tokens.astype(f32)
    resid = own_tokens + mixed

    inverse_two = inverse_rms(resid)
    normed_two = resid * inverse_two
    hidden_two = (normed_two * gain_two).astype(bf16)
    logits = matmul(hidden_two, router_full)
    gate_probs = jax.nn.softmax(logits, axis=-1)
    chosen = jnp.any(routes[:, :, None] == jnp.arange(experts, dtype=jnp.int32)[None, None, :], axis=1)
    picked = jnp.where(chosen, gate_probs, 0.0)
    picked_total = jnp.sum(picked, axis=-1, keepdims=True)
    mix = picked / picked_total
    slab = jnp.where(chosen, mix, -1.0).T.reshape(experts, 1, length)
    slab = jnp.broadcast_to(slab, (experts, 8, length))
    hiddens, slabs = gather_all(reps, shards, hidden_two, slab, 4)

    share = slabs[:, 0, :]
    member = share >= 0.0
    earlier = jnp.arange(length)[:, None] < jnp.arange(length)[None, :]
    slot = matmul(member.astype(bf16), earlier.astype(bf16))
    place = (jnp.arange(capacity, dtype=f32)[None, :, None] == slot[:, None, :]) & member[:, None, :]
    row_weight = jnp.sum(jnp.where(place, share[:, None, :], 0.0), axis=2, keepdims=True)
    onehot = place.astype(bf16)

    def dispatch(blocks):
        taken = jnp.einsum("bst,btd->bsd", onehot, blocks, preferred_element_type=f32)
        return taken.astype(bf16).reshape(devices * capacity, width)

    rows = dispatch(hiddens)
    row_grads = dispatch(cotangents)
    row_weight = row_weight.reshape(devices * capacity, 1)
    gate = matmul(rows, w_gate[0])
    up = matmul(rows, w_up[0])
    sigmoid_gate = jax.nn.sigmoid(gate)
    activated = (gate * sigmoid_gate * up).astype(bf16)
    produced = matmul(activated, w_down[0]).astype(bf16).astype(f32)
    row_grads = row_grads.astype(f32)
    weighted = (row_weight * produced).astype(bf16)
    row_mix = jnp.sum(row_grads * produced, axis=1).reshape(devices, capacity, 1)
    back_mix = jnp.sum(jnp.where(place, row_mix, 0.0), axis=1).reshape(devices, 1, length)
    back_mix = jnp.broadcast_to(back_mix, (devices, 8, length))
    grad_pair = (row_weight * row_grads).astype(bf16)
    grad_act = matmul(grad_pair, w_down[0], ((1,), (1,)))
    grad_gate = (grad_act * up * sigmoid_gate * (1.0 + gate * (1.0 - sigmoid_gate))).astype(bf16)
    grad_up = (grad_act * gate * sigmoid_gate).astype(bf16)
    grad_in = matmul(grad_gate, w_gate[0], ((1,), (1,))) + matmul(grad_up, w_up[0], ((1,), (1,)))
    grad_w_down = matmul(activated, grad_pair, ((0,), (0,)))
    grad_w_gate = matmul(rows, grad_gate, ((0,), (0,)))
    grad_w_up = matmul(rows, grad_up, ((0,), (0,)))

    def combine(values):
        values = values.reshape(devices, capacity, width)
        return jnp.einsum("bst,bsd->btd", onehot, values, preferred_element_type=f32).astype(bf16)

    grad_hidden, mixes = scatter_wide(reps, shards, combine(grad_in.astype(bf16)), back_mix, 8, chunks)
    sums = combine(weighted)

    grad_out = cotangent.astype(f32)
    grad_mix = mixes[:, 0, :].T
    grad_picked = jnp.where(chosen, grad_mix - jnp.sum(grad_mix * mix, axis=-1, keepdims=True), 0.0) / picked_total
    grad_logits = (gate_probs * (grad_picked - jnp.sum(grad_picked * picked, axis=-1, keepdims=True))).astype(bf16)
    grad_hidden = grad_hidden + matmul(grad_logits, router_full, ((1,), (1,)))
    grad_ffn_gain = jnp.sum(grad_hidden * normed_two, axis=0)
    grad_resid = grad_out + norm_back(grad_hidden, normed_two, inverse_two, gain_two)
    grad_w_router = matmul(hidden_two, grad_logits, ((0,), (0,)))

    fused = width // chunks
    grad_attn, grad_qkv, grad_query_gain, grad_key_gain, moe = attend_back(
        reps, shards, head_sizes, grad_resid.astype(bf16), qkv, w_out, qgain, kgain, cosine, sine, bias,
        sums[:, :, :fused], 5,
    )
    if chunks > 1:
        rest = scatter_wide(reps, shards, sums[:, :, fused:], None, 16, chunks - 1)
        moe = jnp.concatenate([moe, rest], axis=1)
    output = (resid + moe).astype(bf16)
    grad_attn = grad_attn.reshape(shards * length, width)
    grad_qkv = grad_qkv.reshape(shards * length, cols)
    grad_w_out = matmul(attn_out.reshape(shards * length, q_cols), grad_attn, ((0,), (0,)))
    owned_out = lax.psum(grad_w_out.astype(bf16), "rep").astype(f32)
    hidden_in = hidden_in.reshape(shards * length, width)
    _, normed_one = unit_of(block_tokens.reshape(shards * length, width).astype(f32))
    grad_part = matmul(grad_qkv, w_in, ((1,), (1,)))
    grad_attn_gain = jnp.sum(grad_part * normed_one, axis=0)
    grad_w_in = matmul(hidden_in, grad_qkv, ((0,), (0,)))

    def spread(values):
        return jnp.pad(values.reshape(shards, part), ((0, 0), (0, deep - part))).reshape(width, 1)

    small_grads = jnp.concatenate(
        [
            grad_w_router,
            grad_attn_gain.reshape(width, 1),
            grad_ffn_gain.reshape(width, 1),
            spread(grad_query_gain),
            spread(grad_key_gain),
        ],
        axis=1,
    )
    small_grads = jnp.pad(small_grads, ((0, 0), (0, small_cols - small_grads.shape[1])))
    sent = jnp.concatenate([grad_w_in, small_grads], axis=1).astype(bf16)
    sent = sent.reshape(shards, reps, piece, cols + small_cols)
    grad_part = grad_part.astype(bf16).reshape(shards, length, width)
    grad_hidden_in, sent = deliver(reps, shards, grad_part, sent, 6)
    sent = sent.reshape(shards, deep, cols + small_cols)
    own_inverse = inverse_rms(own_tokens)
    own_normed = own_tokens * own_inverse
    grad_tokens = grad_resid + norm_back(grad_hidden_in, own_normed, own_inverse, gain_one)

    def joined(values):
        if shared_by > 1:
            values = values.astype(f32).reshape(-1, shared_by, deep, values.shape[-1]).sum(axis=1)
        return values.transpose(1, 0, 2).reshape(deep, -1).astype(f32)

    owned_small = jnp.sum(sent[:, :, cols:].astype(f32), axis=0)
    return (
        output,
        grad_tokens,
        owned_small[:, experts],
        sent[:, :, :q_cols].transpose(1, 0, 2).reshape(deep, -1).astype(f32),
        joined(sent[:, :, q_cols : q_cols + kv_cols]),
        joined(sent[:, :, q_cols + kv_cols : cols]),
        owned_out,
        owned_small[:part, experts + 2],
        owned_small[:part, experts + 3],
        owned_small[:, experts + 1],
        owned_small[:, :experts],
        grad_w_gate[None],
        grad_w_up[None],
        grad_w_down[None],
    )


def solution(mesh):
    split = P(("rep", "shard"))
    row = P("shard")
    return jax.shard_map(
        local,
        mesh=mesh,
        in_specs=(split,) * 3 + (row,) * 9 + (split,) * 4,
        out_specs=(split,) * 2 + (row,) * 9 + (split,) * 3,
        check_vma=False,
    )
```

```python
import functools
import jax
import jax.numpy as jnp
from jax import lax
from jax.experimental import pallas as pl
from jax.experimental.pallas import tpu as pltpu
from jax.sharding import PartitionSpec as P

bf16 = jnp.bfloat16
f32 = jnp.float32
vmem_cap = 62 * 1024 * 1024
epsilon = 1e-06
rope_base = 1000000.0
masked_score = -1e30


class Grid:
    def __init__(self, reps, shards):
        self.reps, self.shards = reps, shards
        self.devices = reps * shards
        self.places = reps // 2
        self.los = self.places // 2

    def here(self):
        self.r = lax.axis_index("rep")
        self.z = lax.axis_index("shard")
        self.core = self.r % 2
        place = self.r // 2
        self.hi = place // self.los
        self.lo = place % self.los
        return self

    def rep_of(self, hi, lo, core):
        return (hi * self.los + lo) * 2 + core

    def device(self, rep, shard):
        return {"rep": rep, "shard": shard}

    def other_lo(self, step):
        return (self.lo + step) % self.los

    def nearest(self):
        n = self.shards
        rows = [sorted(range(n), key=lambda p: (abs(p - z), p)) for z in range(n)]
        return [pick(self.z, [rows[z][turn] for z in range(n)]) for turn in range(n)]


def pick(index, values):
    out = jnp.int32(values[0])
    for i in range(1, len(values)):
        out = jnp.where(index == i, jnp.int32(values[i]), out)
    return out


class Sends:
    def __init__(self, sems):
        self.sems, self.used, self.open, self.samples = sems, 0, [], []

    def copy(self, src, dst, sem, recv, device):
        return pltpu.make_async_remote_copy(
            src_ref=src,
            dst_ref=dst,
            send_sem=self.sems.at[sem],
            recv_sem=recv,
            device_id=device,
            device_id_type=pl.DeviceIdType.MESH,
        )

    def start(self, src, dst, recv, device, when=None):
        copy = self.copy(src, dst, self.used, recv, device)
        sample = src
        for other in self.samples:
            if other.shape == src.shape:
                sample = other
        self.open.append((self.used, sample, when))
        self.used += 1
        if when is None:
            copy.start()
        else:
            pl.when(when())(copy.start)

    def arrived(self, dst, recv, device, when=None):
        copy = self.copy(dst, dst, 0, recv, device)
        if when is None:
            copy.wait_recv()
        else:
            pl.when(when())(copy.wait_recv)

    def drain(self):
        here = {"rep": lax.axis_index("rep"), "shard": lax.axis_index("shard")}
        for sem, sample, when in self.open:
            copy = self.copy(sample, sample, sem, self.sems.at[sem], here)
            if when is None:
                copy.wait_send()
            else:
                pl.when(when())(copy.wait_send)
        self.open = []


def greet_all(g):
    barrier = pltpu.get_barrier_semaphore()
    me = g.r * g.shards + g.z

    def one(step, carry):
        peer = (me + step) % g.devices
        pl.semaphore_signal(
            barrier,
            inc=1,
            device_id=g.device(peer // g.shards, peer % g.shards),
            device_id_type=pl.DeviceIdType.MESH,
        )
        return carry

    lax.fori_loop(1, g.devices, one, 0)
    pl.semaphore_wait(barrier, g.devices - 1)


def push_rows(g, src, dst, send_sems, recv_sems):
    me = g.r * g.shards + g.z

    def one(step, carry):
        peer = (me + step) % g.devices
        pltpu.make_async_remote_copy(
            src_ref=src.at[peer],
            dst_ref=dst.at[me],
            send_sem=send_sems.at[step],
            recv_sem=recv_sems.at[step],
            device_id=g.device(peer // g.shards, peer % g.shards),
            device_id_type=pl.DeviceIdType.MESH,
        ).start()
        return carry

    lax.fori_loop(1, g.devices, one, 0)


def push_wait(g, src, dst, send_sems, recv_sems):
    me = g.r * g.shards + g.z

    def one(step, carry):
        peer = (me + g.devices - step) % g.devices
        copy = pltpu.make_async_remote_copy(
            src_ref=src.at[peer],
            dst_ref=dst.at[peer],
            send_sem=send_sems.at[step],
            recv_sem=recv_sems.at[step],
            device_id=g.device(peer // g.shards, peer % g.shards),
            device_id_type=pl.DeviceIdType.MESH,
        )
        copy.wait_send()
        copy.wait_recv()
        return carry

    lax.fori_loop(1, g.devices, one, 0)


class PlaneGather:
    def __init__(self, g, s, view, lr, hr, dr, cr):
        self.g, self.s, self.view = g, s, view
        self.lr, self.hr, self.dr, self.cr = lr, hr, dr, cr

    @staticmethod
    def scratch(g, units):
        dma, others = pltpu.SemaphoreType.DMA, max(1, g.los - 1)
        return [dma((units, 2, others)), dma((units, 2)), dma((units, 2, others)), dma((units, 5 * g.los))]

    @staticmethod
    def sends(g, units):
        return 9 * g.los * units

    def at(self, hi, lo):
        return self.g.device(self.g.rep_of(hi, lo, self.g.core), self.g.z)

    def partner(self):
        g = self.g
        return g.device(g.rep_of(g.hi, g.lo, 1 - g.core), g.z)

    def own(self, u, src=None):
        g, s = self.g, self.s

        def dst(part):
            return self.view(u, g.hi, g.lo, g.core, part)

        src = src or dst
        for part in (0, 1):
            for step in range(1, g.los):
                s.start(src(part), dst(part), self.lr.at[u, part, step - 1], self.at(g.hi, g.other_lo(step)))
            s.start(src(1 - part), dst(1 - part), self.hr.at[u, 1 - part], self.at(1 - g.hi, g.lo))
        s.start(src(None), dst(None), self.cr.at[u, 0], self.partner())

    def take(self, u, hi, lo, part, recv, frm, partner_slot, onward=()):
        ref = self.view(u, hi, lo, self.g.core, part)
        self.s.arrived(ref, recv, frm)
        for sem, device in onward:
            self.s.start(ref, ref, sem, device)
        self.s.start(ref, ref, self.cr.at[u, partner_slot], self.partner())

    def first(self, u):
        g = self.g
        far = 1 - g.hi
        for step in range(1, g.los):
            frm = (g.lo + g.los - step) % g.los
            onward = [(self.dr.at[u, 0, step - 1], self.at(far, g.lo))]
            self.take(u, g.hi, frm, 0, self.lr.at[u, 0, step - 1], self.at(g.hi, frm), 5 * step, onward)
        onward = [(self.dr.at[u, 1, step - 1], self.at(g.hi, g.other_lo(step))) for step in range(1, g.los)]
        self.take(u, far, g.lo, 1, self.hr.at[u, 1], self.at(far, g.lo), 1, onward)
        for step in range(1, g.los):
            frm = (g.lo + g.los - step) % g.los
            self.take(u, g.hi, frm, 1, self.lr.at[u, 1, step - 1], self.at(g.hi, frm), 5 * step + 1)
        self.take(u, far, g.lo, 0, self.hr.at[u, 0], self.at(far, g.lo), 2)

    def second(self, u):
        g = self.g
        far = 1 - g.hi
        for step in range(1, g.los):
            frm = (g.lo + g.los - step) % g.los
            self.take(u, far, frm, 0, self.dr.at[u, 0, step - 1], self.at(far, g.lo), 5 * step + 2)
            self.take(u, far, frm, 1, self.dr.at[u, 1, step - 1], self.at(g.hi, frm), 5 * step + 3)

    def from_partner(self, u):
        g = self.g
        far, other = 1 - g.hi, 1 - g.core

        def got(hi, lo, part, slot):
            self.s.arrived(self.view(u, hi, lo, other, part), self.cr.at[u, slot], self.partner())

        got(g.hi, g.lo, None, 0)
        got(far, g.lo, 1, 1)
        got(far, g.lo, 0, 2)
        for step in range(1, g.los):
            frm = (g.lo + g.los - step) % g.los
            got(g.hi, frm, 0, 5 * step)
            got(g.hi, frm, 1, 5 * step + 1)
            got(far, frm, 0, 5 * step + 2)
            got(far, frm, 1, 5 * step + 3)


def add_rows(dst, *srcs, step=16):
    def one(i, carry):
        at = pl.ds(pl.multiple_of(i * step, step), step)
        total = srcs[0][at, :].astype(f32)
        for src in srcs[1:]:
            total = total + src[at, :].astype(f32)
        dst[at, :] = total.astype(dst.dtype)
        return carry

    lax.fori_loop(0, dst.shape[0] // step, one, 0)


class PlaneScatter:
    def __init__(self, g, s, p, cut, own, ra, rb0, rb1, rc0, rc1, sa, sb0, sb1, sc0, sc1, ls):
        self.g, self.s, self.p, self.cut, self.owned = g, s, p, cut, own
        self.ra, self.rb0, self.rb1, self.rc0, self.rc1 = ra, rb0, rb1, rc0, rc1
        self.sa, self.sb0, self.sb1, self.sc0, self.sc1, self.ls = sa, sb0, sb1, sc0, sc1, ls

    @staticmethod
    def scratch(g, units, block, halves, dtype):
        dma, others, v = pltpu.SemaphoreType.DMA, max(1, g.los - 1), pltpu.VMEM
        first, second = halves
        return [
            v((units, g.places) + block, dtype),
            v((units, g.places) + block, dtype),
            v((units, g.los) + first, dtype),
            v((units, others, 2) + second, dtype),
            v((units, others) + first, dtype),
            v((units,) + second, dtype),
            dma((units,)),
            dma((units,)),
            dma((units, others, 2)),
            dma((units, others)),
            dma((units,)),
            dma((units,)),
        ]

    @staticmethod
    def sends(g, units):
        return units * (3 * g.los + 2)

    def at(self, hi, lo):
        return self.g.device(self.g.rep_of(hi, lo, self.g.core), self.g.z)

    def partner(self):
        g = self.g
        return g.device(g.rep_of(g.hi, g.lo, 1 - g.core), g.z)

    def load(self, units):
        self.loads = []
        for turn in range(units):
            load = pltpu.make_async_copy(self.p(turn, self.g.core), self.owned.at[turn], self.ls.at[turn])
            load.start()
            self.loads.append(load)

    def to_partner(self, turn):
        self.s.start(self.p(turn, 1 - self.g.core), self.ra.at[turn], self.sa.at[turn], self.partner())

    def half(self, turn, place, part):
        return self.owned.at[(turn, place) + self.cut(part)]

    def mine(self, turn):
        return self.owned.at[turn, self.g.hi * self.g.los + self.g.lo]

    def a(self, turn):
        g, s = self.g, self.s
        far = 1 - g.hi
        self.loads[turn].wait()
        s.arrived(self.ra.at[turn], self.sa.at[turn], self.partner())

        def one(q, carry):
            line = self.owned.at[turn, q]
            add_rows(line, line, self.ra.at[turn, q])
            return carry

        lax.fori_loop(0, g.places, one, 0)
        block = self.owned.at[(turn, pl.ds(far * g.los, g.los)) + self.cut(0)]
        s.start(block, self.rb0.at[turn], self.sb0.at[turn], self.at(far, g.lo))
        for step in range(1, g.los):
            to = g.other_lo(step)
            for hi in range(2):
                sem = self.sb1.at[turn, step - 1, hi]
                s.start(self.half(turn, hi * g.los + to, 1), self.rb1.at[turn, step - 1, hi], sem, self.at(g.hi, to))

    def b(self, turn):
        g, s = self.g, self.s
        far = 1 - g.hi
        s.arrived(self.rb0.at[turn], self.sb0.at[turn], self.at(far, g.lo))
        for lo in range(g.los):
            line = self.half(turn, g.hi * g.los + lo, 0)
            add_rows(line, line, self.rb0.at[turn, lo])
        for step in range(1, g.los):
            to = g.other_lo(step)
            sem = self.sc0.at[turn, step - 1]
            s.start(self.half(turn, g.hi * g.los + to, 0), self.rc0.at[turn, step - 1], sem, self.at(g.hi, to))
        for step in range(1, g.los):
            frm = (g.lo + g.los - step) % g.los
            for hi in range(2):
                s.arrived(self.rb1.at[turn, step - 1, hi], self.sb1.at[turn, step - 1, hi], self.at(g.hi, frm))
        for hi in range(2):
            line = self.half(turn, hi * g.los + g.lo, 1)
            add_rows(line, line, *[self.rb1.at[turn, step, hi] for step in range(g.los - 1)])
        s.start(self.half(turn, far * g.los + g.lo, 1), self.rc1.at[turn], self.sc1.at[turn], self.at(far, g.lo))

    def c(self, turn):
        g, s = self.g, self.s
        place = g.hi * g.los + g.lo
        for step in range(1, g.los):
            frm = (g.lo + g.los - step) % g.los
            s.arrived(self.rc0.at[turn, step - 1], self.sc0.at[turn, step - 1], self.at(g.hi, frm))
        line = self.half(turn, place, 0)
        add_rows(line, line, *[self.rc0.at[turn, step] for step in range(g.los - 1)])
        s.arrived(self.rc1.at[turn], self.sc1.at[turn], self.at(1 - g.hi, g.lo))
        line = self.half(turn, place, 1)
        add_rows(line, line, self.rc1.at[turn])


def pass_along(g, s, zp, src, dst, zr):
    n = g.shards
    right, left = g.device(g.r, jnp.minimum(g.z + 1, n - 1)), g.device(g.r, jnp.maximum(g.z - 1, 0))
    s.start(src, dst, zr.at[zp], right, lambda: (zp <= g.z) & (g.z + 1 < n))
    s.start(src, dst, zr.at[zp], left, lambda: (zp >= g.z) & (g.z > 0))


def send_line(g, s, zp, line, out_ref, rl, rr, sl, sr, last):
    n = g.shards
    left, right = g.device(g.r, jnp.maximum(g.z - 1, 0)), g.device(g.r, jnp.minimum(g.z + 1, n - 1))
    has_left, has_right = g.z > 0, g.z + 1 < n
    if last:
        s.arrived(rl.at[g.z], sl.at[g.z], left, lambda: g.z > 0)
        s.arrived(rr.at[g.z], sr.at[g.z], right, lambda: g.z + 1 < n)

        @pl.when(has_left & has_right)
        def _():
            add_rows(out_ref, line, rl.at[g.z], rr.at[g.z])

        @pl.when(has_left & jnp.logical_not(has_right))
        def _():
            add_rows(out_ref, line, rl.at[g.z])

        @pl.when(has_right & jnp.logical_not(has_left))
        def _():
            add_rows(out_ref, line, rr.at[g.z])
    else:
        onward_right, onward_left = zp > g.z, zp < g.z

        @pl.when(onward_right & has_left)
        def _():
            s.arrived(rl.at[zp], sl.at[zp], left)
            add_rows(line, line, rl.at[zp])

        @pl.when(onward_left & has_right)
        def _():
            s.arrived(rr.at[zp], sr.at[zp], right)
            add_rows(line, line, rr.at[zp])

        s.start(line, rl.at[zp], sl.at[zp], right, lambda: zp > g.z)
        s.start(line, rr.at[zp], sr.at[zp], left, lambda: zp < g.z)


def line_scratch(shards, block, dtype):
    v, dma = pltpu.VMEM, pltpu.SemaphoreType.DMA
    return [v((shards,) + block, dtype), v((shards,) + block, dtype), dma((shards,)), dma((shards,))]


def wait_for(copies, k):
    for copy in copies(k):
        copy.wait()


hbm = pl.BlockSpec(memory_space=pl.ANY)
vmem = pl.BlockSpec(memory_space=pltpu.VMEM)


def params(ident):
    return pltpu.CompilerParams(collective_id=ident, has_side_effects=True, vmem_limit_bytes=vmem_cap)


def collect_kernel(reps, shards, layout, x_ref, small_ref, wq_ref, wk_ref, wv_ref, xs_ref, smalls_ref, w_ref, sems, xr, mr, wr, lr, hr, dr, cr, ls):
    g = Grid(reps, shards).here()
    s = Sends(sems)
    n = g.shards
    q_cols, kv_cols, kv_heads, head_dim = layout
    deep = wq_ref.shape[0]
    piece = deep // g.reps
    cols = q_cols + 2 * kv_cols
    first = cols // 2 // 128 * 128
    spans = {0: pl.ds(0, first), 1: pl.ds(first, cols - first), None: pl.ds(0, cols)}
    mine = pl.ds(pl.multiple_of(g.r * piece, piece), piece)

    def view(u, hi, lo, core, part):
        row = pl.multiple_of(u * deep + g.rep_of(hi, lo, core) * piece, piece)
        return w_ref.at[pl.ds(row, piece), spans[part]]

    def pieces(zp, u):
        row = pl.ds(pl.multiple_of(u * deep + g.r * piece, piece), piece)
        at_q = pl.ds(pl.multiple_of(zp * q_cols, 128), q_cols)
        at_kv = pl.ds(pl.multiple_of(zp * kv_heads // n * head_dim, 128), kv_cols)
        return (
            (wq_ref.at[mine, at_q], w_ref.at[row, pl.ds(0, q_cols)]),
            (wk_ref.at[mine, at_kv], w_ref.at[row, pl.ds(q_cols, kv_cols)]),
            (wv_ref.at[mine, at_kv], w_ref.at[row, pl.ds(q_cols + kv_cols, kv_cols)]),
        )

    keeps = [
        pltpu.make_async_copy(x_ref, xs_ref.at[g.z], ls.at[0]),
        pltpu.make_async_copy(small_ref, smalls_ref.at[g.z], ls.at[1]),
    ]
    locals_ = [pltpu.make_async_copy(src, dst, ls.at[2 + i]) for i, (src, dst) in enumerate(pieces(g.z, g.z))]
    for copy in locals_ + keeps:
        copy.start()
    barrier = pltpu.get_barrier_semaphore()
    peers = [g.device(g.r, (g.z + step) % n) for step in range(1, n)]
    peers += [g.device(g.rep_of(g.hi, g.other_lo(step), g.core), g.z) for step in range(1, g.los)]
    peers += [g.device(g.rep_of(1 - g.hi, g.lo, g.core), g.z), g.device(g.rep_of(g.hi, g.lo, 1 - g.core), g.z)]
    for peer in peers:
        pl.semaphore_signal(barrier, inc=1, device_id=peer, device_id_type=pl.DeviceIdType.MESH)
    pl.semaphore_wait(barrier, len(peers))

    plane = PlaneGather(g, s, view, lr, hr, dr, cr)
    for step in range(1, n):
        zp = (g.z + step) % n
        for i, (src, dst) in enumerate(pieces(zp, g.z)):
            s.start(src, dst, wr.at[step, i], g.device(g.r, zp))
    order = g.nearest()

    def line(turn):
        zp = order[turn]
        if turn:
            s.arrived(smalls_ref.at[zp], mr.at[zp], g.device(g.r, zp))
        pass_along(g, s, zp, smalls_ref.at[zp] if turn else small_ref, smalls_ref.at[zp], mr)
        if turn:
            s.arrived(xs_ref.at[zp], xr.at[zp], g.device(g.r, zp))
        pass_along(g, s, zp, xs_ref.at[zp] if turn else x_ref, xs_ref.at[zp], xr)

    line(0)
    for copy in locals_:
        copy.wait()
    plane.own(g.z)

    def unit(step):
        return (g.z + n - step) % n

    for step in range(1, n):
        u = unit(step)
        for i, (_, dst) in enumerate(pieces(g.z, u)):
            s.arrived(dst, wr.at[step, i], g.device(g.r, u))
        plane.own(u)
    line(1)
    for step in range(n):
        plane.first(unit(step))
        if step:
            plane.second(unit(step - 1))
        if 2 + step < n:
            line(2 + step)
    plane.second(unit(n - 1))
    for step in range(n):
        plane.from_partner(unit(step))
    for copy in keeps:
        copy.wait()
    s.drain()


def collect(reps, shards, x, small, wq, wk, wv, layout, ident):
    g = Grid(reps, shards)
    dma = pltpu.SemaphoreType.DMA
    n = shards
    cols = layout[0] + 2 * layout[1]
    return pl.pallas_call(
        functools.partial(collect_kernel, reps, shards, layout),
        out_shape=(
            jax.ShapeDtypeStruct((n,) + x.shape, x.dtype),
            jax.ShapeDtypeStruct((n,) + small.shape, small.dtype),
            jax.ShapeDtypeStruct((n * wq.shape[0], cols), wq.dtype),
        ),
        in_specs=[vmem, vmem, hbm, hbm, hbm],
        out_specs=(vmem, vmem, vmem),
        scratch_shapes=[dma((PlaneGather.sends(g, n) + 7 * n,)), dma((n,)), dma((n,)), dma((n, 3))]
        + PlaneGather.scratch(g, n)
        + [dma((5,))],
        compiler_params=params(ident),
        name="collect",
    )(x, small, wq, wk, wv)


def scatter_all_kernel(reps, shards, slabbed, *refs):
    if slabbed:
        (
            p_ref, slab_ref, x_ref, c_ref, gg_ref, gu_ref, act_ref, out_ref, slabs_ref, wg_ref, wu_ref, wd_ref,
            xt, ct, og, ou, od, tile_sems, out_sems, *rest,
        ) = refs
    else:
        p_ref, out_ref, *rest = refs
    sems, ps, pr, slab_sem, *rest = rest
    g = Grid(reps, shards).here()
    s = Sends(sems)
    n = g.shards
    scatter = ScatterAll(g, s, p_ref, out_ref, *rest)
    half = pl.ds(0, out_ref.shape[0] // 2)
    own = scatter.plane.owned
    s.samples = [own.at[0, 0], own.at[0, 0, half], own.at[0, pl.ds(0, g.los), half]]
    scatter.load()
    if not slabbed:
        greet_all(g)
        scatter.to_partner()
        for turn in range(n + 2):
            scatter.step(turn)
        s.drain()
        return

    tile = xt.shape[2]
    tiles = x_ref.shape[1] // tile

    def tile_in(j, slot):
        span = pl.ds(pl.multiple_of(j * tile, tile), tile)
        return [
            pltpu.make_async_copy(x_ref.at[:, span], xt.at[slot], tile_sems.at[slot, 0]),
            pltpu.make_async_copy(c_ref.at[:, span], ct.at[slot], tile_sems.at[slot, 1]),
        ]

    def tile_out(j):
        span = pl.ds(pl.multiple_of(j * tile, tile), tile)
        return [
            pltpu.make_async_copy(og, wg_ref.at[span, :], out_sems.at[0]),
            pltpu.make_async_copy(ou, wu_ref.at[span, :], out_sems.at[1]),
            pltpu.make_async_copy(od, wd_ref.at[:, span], out_sems.at[2]),
        ]

    for copy in tile_in(0, 0):
        copy.start()
    greet_all(g)
    scatter.to_partner()
    push_rows(g, slab_ref, slabs_ref, ps, pr)
    me = g.r * n + g.z
    keep_slab = pltpu.make_async_copy(slab_ref.at[me], slabs_ref.at[me], slab_sem.at[0])
    keep_slab.start()

    def next_tiles(j):
        for copy in tile_in(j + 1, (j + 1) % 2):
            copy.start()

    def weight_grads(j, carry):
        for turn in range(n):
            pl.when(j == turn * tiles // n)(functools.partial(scatter.step, turn))
        pl.when(j + 1 < tiles)(functools.partial(next_tiles, j))
        slot = j % 2
        for copy in tile_in(j, slot):
            copy.wait()
        pl.when(j > 0)(functools.partial(wait_for, tile_out, j))
        og[...] = t_dot(xt[slot], gg_ref[...])
        ou[...] = t_dot(xt[slot], gu_ref[...])
        od[...] = t_dot(act_ref[...], ct[slot])
        for copy in tile_out(j):
            copy.start()
        return carry

    lax.fori_loop(0, tiles, weight_grads, 0)
    scatter.step(n)
    scatter.step(n + 1)
    wait_for(tile_out, 0)
    keep_slab.wait()
    push_wait(g, slab_ref, slabs_ref, ps, pr)
    s.drain()


def scatter_all(reps, shards, p, slab, fill, ident):
    g = Grid(reps, shards)
    n = shards
    _, rows, width = p.shape
    dma, v = pltpu.SemaphoreType.DMA, pltpu.VMEM
    slabbed = slab is not None
    out_shape = (jax.ShapeDtypeStruct((rows, width), f32),)
    out_specs, in_specs, extra, scratch = (vmem,), [hbm], [], []
    if slabbed:
        x, c, gg, gu, act = fill
        count, wide = x.shape
        inner = gg.shape[1]
        tile = 256
        narrow = jax.ShapeDtypeStruct((wide, inner), f32)
        out_shape += (
            jax.ShapeDtypeStruct(slab.shape, slab.dtype), narrow, narrow, jax.ShapeDtypeStruct((inner, wide), f32)
        )
        out_specs += (vmem, hbm, hbm, hbm)
        in_specs += [vmem, hbm, hbm, vmem, vmem, vmem]
        extra = [slab, *fill]
        scratch = [
            v((2, count, tile), bf16), v((2, count, tile), bf16),
            v((tile, inner), f32), v((tile, inner), f32), v((inner, tile), f32),
            dma((2, 2)), dma((3,)),
        ]
    done = pl.pallas_call(
        functools.partial(scatter_all_kernel, reps, shards, slabbed),
        out_shape=out_shape,
        in_specs=in_specs,
        out_specs=out_specs,
        scratch_shapes=scratch
        + [dma((ScatterAll.sends(g),)), dma((g.devices,)), dma((g.devices,)), dma((1,))]
        + ScatterAll.scratch(g, (rows, width), p.dtype),
        compiler_params=params(ident),
        name="scatter_all",
    )(p.reshape(g.places, 2, n, rows, width), *extra)
    return done if slabbed else done[0]


def scatter_wide(reps, shards, p, slab, fill, ident, chunks):
    if chunks == 1:
        return scatter_all(reps, shards, p, slab, fill, ident)
    step = p.shape[2] // chunks
    parts = [
        scatter_all(reps, shards, p[:, :, i * step : (i + 1) * step], slab if i == 0 else None, fill, ident + i)
        for i in range(chunks)
    ]
    if slab is None:
        return jnp.concatenate(parts, axis=1)
    first, *others = parts[0]
    return jnp.concatenate([first] + parts[1:], axis=1), *others


def deliver_kernel(reps, shards, p_ref, w_ref, out_ref, ws_ref, line_own, rl, rr, sl, sr, sems, line_loads, wr, keep_sem, *rest):
    g = Grid(reps, shards).here()
    s = Sends(sems)
    n = g.shards
    gather_refs, scatter_refs = rest[:4], rest[4:]
    cols = w_ref.shape[-1]
    first = cols // 2 // 128 * 128
    spans = {0: pl.ds(0, first), 1: pl.ds(first, cols - first), None: pl.ds(0, cols)}
    order = g.nearest()[::-1]
    scatter = PlaneScatter(
        g, s, lambda turn, core: w_ref.at[turn, :, core], lambda part: (slice(None), spans[part]), *scatter_refs
    )
    gather = PlaneGather(
        g, s, lambda u, hi, lo, core, part: ws_ref.at[u, g.rep_of(hi, lo, core), :, spans[part]], *gather_refs
    )
    scatter.load(n)
    loads = []
    for turn in range(n):
        load = pltpu.make_async_copy(p_ref.at[order[turn]], line_own.at[turn], line_loads.at[turn])
        load.start()
        loads.append(load)
    barrier = pltpu.get_barrier_semaphore()
    peers = [g.device(g.r, (g.z + step) % n) for step in range(1, n)]
    peers += [g.device(g.rep_of(g.hi, g.other_lo(step), g.core), g.z) for step in range(1, g.los)]
    peers += [g.device(g.rep_of(1 - g.hi, g.lo, g.core), g.z), g.device(g.rep_of(g.hi, g.lo, 1 - g.core), g.z)]
    for peer in peers:
        pl.semaphore_signal(barrier, inc=1, device_id=peer, device_id_type=pl.DeviceIdType.MESH)
    pl.semaphore_wait(barrier, len(peers))

    for turn in range(n):
        scatter.to_partner(turn)

    def line(turn):
        loads[turn].wait()
        send_line(g, s, order[turn], line_own.at[turn], out_ref, rl, rr, sl, sr, last=turn == n - 1)

    def owner(turn):
        scatter.c(turn)
        dst = ws_ref.at[g.z, g.r]
        keep = pltpu.make_async_copy(scatter.mine(turn), dst, keep_sem.at[0])
        pl.when(g.z == turn)(keep.start)
        s.start(scatter.mine(turn), dst, wr.at[g.z], g.device(g.r, turn), lambda: g.z != turn)
        pl.when(g.z == turn)(keep.wait)

    line(0)
    for turn in range(n + 2):
        if turn < n:
            scatter.a(turn)
        if 0 <= turn - 1 < n:
            scatter.b(turn - 1)
        if 1 <= turn < n - 1:
            line(turn)
        if 0 <= turn - 2 < n:
            owner(turn - 2)
    gather.own(g.z)

    def unit(step):
        return (g.z + n - step) % n

    for step in range(1, n):
        u = unit(step)
        s.arrived(ws_ref.at[u, g.r], wr.at[u], g.device(g.r, u))
        gather.own(u)
        gather.first(unit(step - 1))
        if step > 1:
            gather.second(unit(step - 2))
    gather.first(unit(n - 1))
    gather.second(unit(n - 2))
    gather.second(unit(n - 1))
    line(n - 1)
    for step in range(n):
        gather.from_partner(unit(step))
    s.drain()


def deliver(reps, shards, p, w, ident):
    g = Grid(reps, shards)
    n = shards
    dma = pltpu.SemaphoreType.DMA
    _, rows, width = p.shape
    _, _, piece, cols = w.shape
    first = cols // 2 // 128 * 128
    return pl.pallas_call(
        functools.partial(deliver_kernel, reps, shards),
        out_shape=(jax.ShapeDtypeStruct((rows, width), f32), jax.ShapeDtypeStruct(w.shape, w.dtype)),
        in_specs=[hbm, hbm],
        out_specs=(vmem, vmem),
        scratch_shapes=[pltpu.VMEM(p.shape, p.dtype)]
        + line_scratch(n, (rows, width), p.dtype)
        + [
            dma((PlaneGather.sends(g, n) + PlaneScatter.sends(g, n) + 3 * n,)),
            dma((n,)),
            dma((n,)),
            dma((1,)),
        ]
        + PlaneGather.scratch(g, n)
        + PlaneScatter.scratch(g, n, (piece, cols), ((piece, first), (piece, cols - first)), w.dtype),
        compiler_params=params(ident),
        name="deliver",
    )(p, w.reshape(n, g.places, 2, piece, cols))


def turned(x, cosine, sine):
    return x * cosine + pltpu.roll(x, x.shape[-1] // 2, 1) * sine


def mean_last(x):
    return jnp.sum(x, axis=-1, keepdims=True) * (1.0 / x.shape[-1])


def unit_of(x):
    inverse = lax.rsqrt(mean_last(x * x) + epsilon)
    return inverse, x * inverse


def dot_t(a, b):
    return lax.dot_general(a, b, (((1,), (1,)), ((), ())), preferred_element_type=f32)


def t_dot(a, b):
    return lax.dot_general(a, b, (((0,), (0,)), ((), ())), preferred_element_type=f32)


def softmax_rows(q_rot, k_rot, bias, head_dim):
    scores = dot_t(q_rot, k_rot) * head_dim ** (-0.5) + bias
    raised = jnp.exp(scores - jnp.max(scores, axis=-1, keepdims=True))
    return raised * (1.0 / jnp.sum(raised, axis=-1, keepdims=True))


def back_unit(grad_scaled, unit, inverse, gain):
    gained = grad_scaled * gain
    return inverse * (gained - unit * mean_last(gained * unit))


def attend_block(b, heads, x_ref, w_ref, wo_ref, gain_ref, qg_ref, kg_ref, cos_ref, sin_ref, bias_ref, hid_ref, qkv_ref, att_ref, line):
    my_heads, my_kv, head_dim = heads
    x = x_ref[b].astype(f32)
    _, unit = unit_of(x)
    hid_ref[b] = (unit * gain_ref[...]).astype(bf16)
    qkv_ref[b] = jnp.dot(hid_ref[b], w_ref[...], preferred_element_type=f32)
    cosine, sine, bias = cos_ref[b], sin_ref[b], bias_ref[b]
    group = my_heads // my_kv
    for n in range(my_kv):
        at_k = (my_heads + n) * head_dim
        at_v = (my_heads + my_kv + n) * head_dim
        _, k_unit = unit_of(qkv_ref[b, :, at_k : at_k + head_dim])
        k_rot = turned(k_unit * kg_ref[...], cosine, sine).astype(bf16)
        values = qkv_ref[b, :, at_v : at_v + head_dim].astype(bf16)
        for h in range(n * group, (n + 1) * group):
            span = slice(h * head_dim, (h + 1) * head_dim)
            _, q_unit = unit_of(qkv_ref[b, :, span])
            q_rot = turned(q_unit * qg_ref[...], cosine, sine).astype(bf16)
            probs = softmax_rows(q_rot, k_rot, bias, head_dim)
            mixed = jnp.dot(probs.astype(bf16), values, preferred_element_type=f32)
            att_ref[b, :, span] = mixed.astype(bf16)
    line[...] = jnp.dot(att_ref[b], wo_ref[...], preferred_element_type=f32).astype(bf16)


def attend_back_block(b, heads, ga_ref, qkv_ref, wo_ref, qg_ref, kg_ref, cos_ref, sin_ref, bias_ref, gm_ref, gqkv_ref, qsum_ref, ksum_ref):
    my_heads, my_kv, head_dim = heads
    gm_ref[...] = dot_t(ga_ref[b], wo_ref[...]).astype(bf16)
    cosine, sine, bias = cos_ref[b], sin_ref[b], bias_ref[b]
    group = my_heads // my_kv
    qg, kg = qg_ref[...], kg_ref[...]
    for n in range(my_kv):
        at_k = (my_heads + n) * head_dim
        at_v = (my_heads + my_kv + n) * head_dim
        k_inverse, k_unit = unit_of(qkv_ref[b, :, at_k : at_k + head_dim])
        k_rot = turned(k_unit * kg, cosine, sine).astype(bf16)
        values = qkv_ref[b, :, at_v : at_v + head_dim].astype(bf16)
        grad_k = jnp.zeros(k_unit.shape, f32)
        grad_v = jnp.zeros(k_unit.shape, f32)
        for h in range(n * group, (n + 1) * group):
            span = slice(h * head_dim, (h + 1) * head_dim)
            q_inverse, q_unit = unit_of(qkv_ref[b, :, span])
            q_rot = turned(q_unit * qg, cosine, sine).astype(bf16)
            probs = softmax_rows(q_rot, k_rot, bias, head_dim)
            grad_mixed = gm_ref[:, span]
            grad_weights = dot_t(grad_mixed, values)
            centre = jnp.sum(probs * grad_weights, axis=-1, keepdims=True)
            grad_scores = (probs * (grad_weights - centre) * head_dim ** (-0.5)).astype(bf16)
            grad_v = grad_v + t_dot(probs.astype(bf16), grad_mixed)
            grad_k = grad_k + t_dot(grad_scores, q_rot)
            grad_q = jnp.dot(grad_scores, k_rot, preferred_element_type=f32)
            grad_q = turned(grad_q, cosine, -sine)
            qsum_ref[...] += jnp.sum(grad_q * q_unit, axis=0, keepdims=True)
            gqkv_ref[b, :, span] = back_unit(grad_q, q_unit, q_inverse, qg).astype(bf16)
        grad_k = turned(grad_k, cosine, -sine)
        ksum_ref[...] += jnp.sum(grad_k * k_unit, axis=0, keepdims=True)
        gqkv_ref[b, :, at_k : at_k + head_dim] = back_unit(grad_k, k_unit, k_inverse, kg).astype(bf16)
        gqkv_ref[b, :, at_v : at_v + head_dim] = grad_v.astype(bf16)


class GatherAll:
    def __init__(self, g, s, x_ref, out_ref, zr, plane_sems):
        self.g, self.s, self.x_ref, self.out_ref, self.zr = g, s, x_ref, out_ref, zr
        half = x_ref.shape[0] // 2
        self.spans = {0: pl.ds(0, half), 1: pl.ds(half, half), None: pl.ds(0, 2 * half)}
        self.order = g.nearest()
        self.plane = PlaneGather(g, s, self.view, *plane_sems)

    @staticmethod
    def scratch(g):
        dma = pltpu.SemaphoreType.DMA
        return [dma((g.shards,))] + PlaneGather.scratch(g, g.shards)

    @staticmethod
    def sends(g):
        return PlaneGather.sends(g, g.shards) + 2 * g.shards

    def view(self, u, hi, lo, core, part):
        return self.out_ref.at[self.g.rep_of(hi, lo, core) * self.g.shards + u, self.spans[part]]

    def own(self):
        g = self.g
        return self.view(g.z, g.hi, g.lo, g.core, None)

    def line(self, turn):
        g, zp = self.g, self.order[turn]
        dst = self.view(zp, g.hi, g.lo, g.core, None)
        if turn:
            self.s.arrived(dst, self.zr.at[zp], g.device(g.r, zp))
        pass_along(g, self.s, zp, dst if turn else self.x_ref, dst, self.zr)
        self.plane.own(zp, None if turn else lambda part: self.x_ref.at[self.spans[part]])

    def first(self, turn):
        self.plane.first(self.order[turn])

    def second(self, turn):
        self.plane.second(self.order[turn])

    def finish(self):
        for turn in range(self.g.shards):
            self.plane.from_partner(self.order[turn])


class ScatterAll:
    def __init__(self, g, s, p_ref, out_ref, rl, rr, sl, sr, *plane_refs):
        self.g, self.s, self.out_ref = g, s, out_ref
        self.lines = (rl, rr, sl, sr)
        half = out_ref.shape[0] // 2
        self.order = g.nearest()[::-1]
        self.plane = PlaneScatter(
            g,
            s,
            lambda turn, core: p_ref.at[:, core, self.order[turn]],
            lambda part: (pl.ds(part * half, half),),
            *plane_refs,
        )

    @staticmethod
    def scratch(g, block, dtype):
        rows, width = block
        half = (rows // 2, width)
        return line_scratch(g.shards, block, dtype) + PlaneScatter.scratch(g, g.shards, block, (half, half), dtype)

    @staticmethod
    def sends(g):
        return PlaneScatter.sends(g, g.shards) + 2 * g.shards

    def load(self):
        self.plane.load(self.g.shards)

    def to_partner(self):
        for turn in range(self.g.shards):
            self.plane.to_partner(turn)

    def step(self, turn):
        n = self.g.shards
        if turn < n:
            self.plane.a(turn)
        if 0 <= turn - 1 < n:
            self.plane.b(turn - 1)
        if 0 <= turn - 2 < n:
            t = turn - 2
            self.plane.c(t)
            send_line(self.g, self.s, self.order[t], self.plane.mine(t), self.out_ref, *self.lines, last=t == n - 1)


def attend_kernel(reps, shards, heads, *refs):
    (
        x_ref, w_ref, wo_ref, gain_ref, qg_ref, kg_ref, cos_ref, sin_ref, bias_ref, cot_ref,
        hid_ref, qkv_ref, att_ref, out_ref, cots_ref,
        own, rl, rr, sl, sr, sems, keep_sem, *gather_sems,
    ) = refs
    g = Grid(reps, shards).here()
    s = Sends(sems)
    n = g.shards
    gather = GatherAll(g, s, cot_ref, cots_ref, gather_sems[0], gather_sems[1:])
    keep = pltpu.make_async_copy(cot_ref, gather.own(), keep_sem.at[0])
    keep.start()
    greet_all(g)
    gather.line(0)
    order = g.nearest()[::-1]
    for turn in range(n):
        zp = order[turn]
        attend_block(
            zp, heads, x_ref, w_ref, wo_ref, gain_ref, qg_ref, kg_ref, cos_ref, sin_ref, bias_ref,
            hid_ref, qkv_ref, att_ref, own.at[turn],
        )
        send_line(g, s, zp, own.at[turn], out_ref, rl, rr, sl, sr, last=turn == n - 1)
        if turn + 1 < n:
            gather.line(turn + 1)
            gather.first(turn)
        if turn > 0:
            gather.second(turn - 1)
    gather.first(n - 1)
    gather.second(n - 1)
    gather.finish()
    keep.wait()
    s.drain()


def attend(reps, shards, heads, x, w, wo, gain, qg, kg, cosine, sine, bias, cot, ident):
    g = Grid(reps, shards)
    dma, v = pltpu.SemaphoreType.DMA, pltpu.VMEM
    n, rows, width = x.shape
    cols = w.shape[1]
    return pl.pallas_call(
        functools.partial(attend_kernel, reps, shards, heads),
        out_shape=(
            jax.ShapeDtypeStruct(x.shape, bf16),
            jax.ShapeDtypeStruct((n, rows, cols), f32),
            jax.ShapeDtypeStruct((n, rows, wo.shape[0]), bf16),
            jax.ShapeDtypeStruct((rows, width), f32),
            jax.ShapeDtypeStruct((g.devices, rows, width), bf16),
        ),
        in_specs=[vmem] * 10,
        out_specs=(vmem, vmem, vmem, vmem, hbm),
        scratch_shapes=[v((n, rows, width), bf16)]
        + line_scratch(n, (rows, width), bf16)
        + [dma((GatherAll.sends(g) + 2 * n,)), dma((1,))]
        + GatherAll.scratch(g),
        compiler_params=params(ident),
        name="attend",
    )(x, w, wo, gain, qg, kg, cosine, sine, bias, cot)


def attend_back_kernel(reps, shards, heads, *refs):
    (
        ga_ref, qkv_ref, wo_ref, qg_ref, kg_ref, cos_ref, sin_ref, bias_ref, p_ref,
        gas_ref, gqkv_ref, qsum_ref, ksum_ref, out_ref,
        gm, zr, sems, keep_sem, *scatter_refs,
    ) = refs
    g = Grid(reps, shards).here()
    s = Sends(sems)
    n = g.shards
    scatter = ScatterAll(g, s, p_ref, out_ref, *scatter_refs)
    scatter.load()
    keep = pltpu.make_async_copy(ga_ref, gas_ref.at[g.z], keep_sem.at[0])
    keep.start()
    qsum_ref[...] = jnp.zeros(qsum_ref.shape, f32)
    ksum_ref[...] = jnp.zeros(ksum_ref.shape, f32)
    greet_all(g)
    order = g.nearest()

    def line(turn):
        zp = order[turn]
        dst = gas_ref.at[zp]
        if turn:
            s.arrived(dst, zr.at[zp], g.device(g.r, zp))
        pass_along(g, s, zp, dst if turn else ga_ref, dst, zr)

    line(0)
    scatter.to_partner()
    keep.wait()
    for turn in range(n):
        scatter.step(turn)
        if turn + 1 < n:
            line(turn + 1)
        attend_back_block(
            order[turn], heads, gas_ref, qkv_ref, wo_ref, qg_ref, kg_ref, cos_ref, sin_ref, bias_ref,
            gm, gqkv_ref, qsum_ref, ksum_ref,
        )
    scatter.step(n)
    scatter.step(n + 1)
    s.drain()


def attend_back(reps, shards, heads, ga, qkv, wo, qg, kg, cosine, sine, bias, p, ident):
    g = Grid(reps, shards)
    dma, v = pltpu.SemaphoreType.DMA, pltpu.VMEM
    n = shards
    rows, width = ga.shape
    out_width = p.shape[2]
    row = jax.ShapeDtypeStruct(qg.shape, f32)
    return pl.pallas_call(
        functools.partial(attend_back_kernel, reps, shards, heads),
        out_shape=(
            jax.ShapeDtypeStruct((n, rows, width), bf16),
            jax.ShapeDtypeStruct(qkv.shape, bf16),
            row,
            row,
            jax.ShapeDtypeStruct((rows, out_width), f32),
        ),
        in_specs=[vmem] * 8 + [hbm],
        out_specs=(vmem,) * 5,
        scratch_shapes=[v((rows, wo.shape[0]), bf16), dma((n,)), dma((ScatterAll.sends(g) + 2 * n,)), dma((1,))]
        + ScatterAll.scratch(g, (rows, out_width), p.dtype),
        compiler_params=params(ident),
        name="attend_back",
    )(ga, qkv, wo, qg, kg, cosine, sine, bias, p.reshape(g.places, 2, n, rows, out_width))


def slots_of(slab, capacity):
    length = slab.shape[1]
    member = slab >= 0.0
    earlier = lax.broadcasted_iota(jnp.int32, (length, length), 0) < lax.broadcasted_iota(jnp.int32, (length, length), 1)
    ones = jnp.where(member, 1.0, 0.0).astype(bf16)
    slot = jnp.dot(ones, jnp.where(earlier, 1.0, 0.0).astype(bf16), preferred_element_type=f32)
    slot = jnp.where(member, slot, -1.0)[0:1]
    rows = lax.broadcasted_iota(jnp.int32, (capacity, length), 0).astype(f32)
    return jnp.where(rows == slot, 1.0, 0.0), slab[0:1]


def experts_kernel(reps, shards, capacity, held, *refs):
    (
        x_ref, slab_ref, cots_ref, wg_ref, wu_ref, wd_ref,
        back_ref, sums_ref, grads_ref, rows_ref, cs_ref, gg_ref, gu_ref, act_ref, all_ref,
        slabs, cot_buf, hid_buf, d_ref, x_buf, c_buf, gg_buf, gu_buf, act_buf, sum_buf, grad_buf,
        sems, ps, pr, ls, cot_sem, hid_sem, out_sems, zr, *plane_sems,
    ) = refs
    g = Grid(reps, shards).here()
    s = Sends(sems)
    n, places = g.shards, g.places
    length = x_ref.shape[0]
    hidden = hid_buf if held else all_ref
    s.samples = [x_ref, x_ref.at[pl.ds(0, length // 2)]]
    gather = GatherAll(g, s, x_ref, hidden, zr, plane_sems)
    order = gather.order
    groups = 2 * n

    def which(k):
        return jnp.where(k % 2 == 0, g.core, 1 - g.core), pick(k // 2, order)

    def cot_load(k, slot):
        core, zp = which(k)
        return pltpu.make_async_copy(cots_ref.at[:, core, zp], cot_buf.at[slot], cot_sem.at[slot])

    def onehots(k):
        core, zp = which(k)
        return [slots_of(slabs[(q * 2 + core) * n + zp], capacity) for q in range(places)]

    keep = pltpu.make_async_copy(x_ref, gather.own(), ls.at[0])
    keep.start()
    cot_load(0, 0).start()
    greet_all(g)
    push_rows(g, slab_ref, slabs, ps, pr)
    me = g.r * n + g.z
    keep_slab = pltpu.make_async_copy(slab_ref.at[me], slabs.at[me], ls.at[1])
    keep_slab.start()
    gather.line(0)
    keep_slab.wait()
    push_wait(g, slab_ref, slabs, ps, pr)
    keep.wait()

    def turns(k, steps):
        for at, step in steps:
            pl.when(k == at)(step)

    def both(*fs):
        def run():
            for f, turn in fs:
                f(turn)

        return run

    early = [(2, both((gather.first, 0))), (4, both((gather.line, 1), (gather.second, 0))), (6, both((gather.first, 1)))]

    def outs(k):
        return [
            pltpu.make_async_copy(x_buf, rows_ref.at[k], out_sems.at[0]),
            pltpu.make_async_copy(gg_buf, gg_ref.at[k], out_sems.at[1]),
            pltpu.make_async_copy(gu_buf, gu_ref.at[k], out_sems.at[2]),
            pltpu.make_async_copy(act_buf, act_ref.at[k], out_sems.at[3]),
        ]

    def blocks_out(k):
        core, zp = which(k)
        return [
            pltpu.make_async_copy(sum_buf, sums_ref.at[:, core, zp], out_sems.at[4]),
            pltpu.make_async_copy(grad_buf, grads_ref.at[:, core, zp], out_sems.at[5]),
        ]

    def c_out(k):
        return pltpu.make_async_copy(c_buf, cs_ref.at[k], out_sems.at[6])

    def backward_input(k, carry):
        turns(k, early)
        slot = k % 2
        pl.when(k + 1 < groups)(lambda: cot_load(k + 1, 1 - slot).start())
        cot_load(k, slot).wait()
        pl.when(k > 0)(lambda: c_out(k).wait())
        for q, (onehot, _) in enumerate(onehots(k)):
            taken = jnp.dot(onehot.astype(bf16), cot_buf[slot, q], preferred_element_type=f32)
            c_buf[q * capacity : (q + 1) * capacity, :] = taken.astype(bf16)
        c_out(k).start()
        d_ref[k] = dot_t(c_buf[...], wd_ref[...])
        return carry

    lax.fori_loop(0, groups, backward_input, 0)
    c_out(0).wait()

    late = []
    for turn in range(n):
        steps = []
        if turn == 0:
            steps += [(gather.line, 2)] if n > 2 else []
        else:
            if turn + 2 < n:
                steps.append((gather.line, turn + 2))
            if turn > 1:
                steps.append((gather.first, turn))
            steps.append((gather.second, turn))
        if steps:
            late.append((2 * turn, both(*steps)))
        late.append((2 * turn + 1, both((lambda t: gather.plane.from_partner(order[t]), turn))))

    def expert(k, carry):
        turns(k, late)
        core, zp = which(k)
        if not held:
            fetch = pltpu.make_async_copy(all_ref.at[pl.ds(0, places)], hid_buf, hid_sem.at[0])
            for q in range(places):
                pltpu.make_async_copy(all_ref.at[(q * 2 + core) * n + zp], hid_buf.at[q], hid_sem.at[0]).start()
            fetch.wait()
        hots = onehots(k)
        pl.when(k > 0)(functools.partial(wait_for, outs, k))
        for q, (onehot, _) in enumerate(hots):
            block = hid_buf[(q * 2 + core) * n + zp] if held else hid_buf[q]
            taken = jnp.dot(onehot.astype(bf16), block, preferred_element_type=f32)
            x_buf[q * capacity : (q + 1) * capacity, :] = taken.astype(bf16)
        weight = jnp.concatenate(
            [jnp.sum(onehot * share, axis=1, keepdims=True) for onehot, share in hots], axis=0
        )
        gate = jnp.dot(x_buf[...], wg_ref[...], preferred_element_type=f32)
        up = jnp.dot(x_buf[...], wu_ref[...], preferred_element_type=f32)
        sigmoid = 1.0 / (1.0 + jnp.exp(-gate))
        silu = gate * sigmoid
        activated = silu * up
        grad = d_ref[k]
        row_mix = jnp.sum(activated * grad, axis=1, keepdims=True)
        grad = grad * weight
        act_buf[...] = (activated * weight).astype(bf16)
        gg_buf[...] = (grad * up * sigmoid * (1.0 + gate * (1.0 - sigmoid))).astype(bf16)
        gu_buf[...] = (grad * silu).astype(bf16)
        for copy in outs(k):
            copy.start()
        for q, (onehot, _) in enumerate(hots):
            back = jnp.sum(onehot * row_mix[q * capacity : (q + 1) * capacity], axis=0, keepdims=True)
            back_ref[(q * 2 + core) * n + zp] = jnp.broadcast_to(back, slab_ref.shape[1:])
        produced = jnp.dot(act_buf[...], wd_ref[...], preferred_element_type=f32).astype(bf16)
        pl.when(k > 0)(functools.partial(wait_for, blocks_out, k))
        for q, (onehot, _) in enumerate(hots):
            part = produced[q * capacity : (q + 1) * capacity]
            sum_buf[q] = t_dot(onehot.astype(bf16), part).astype(bf16)
        grad_in = (dot_t(gg_buf[...], wg_ref[...]) + dot_t(gu_buf[...], wu_ref[...])).astype(bf16)
        for q, (onehot, _) in enumerate(hots):
            part = grad_in[q * capacity : (q + 1) * capacity]
            grad_buf[q] = t_dot(onehot.astype(bf16), part).astype(bf16)
        for copy in blocks_out(k):
            copy.start()
        return carry

    lax.fori_loop(0, groups, expert, 0)
    for copy in outs(0) + blocks_out(0):
        copy.wait()
    s.drain()


def experts_all(reps, shards, capacity, x, slab, cots, wg, wu, wd, ident):
    g = Grid(reps, shards)
    dma, v = pltpu.SemaphoreType.DMA, pltpu.VMEM
    n, places = shards, g.places
    length, width = x.shape
    inner = wg.shape[1]
    rows = places * capacity
    held = g.devices <= 32
    blocks = jax.ShapeDtypeStruct((places, 2, n, length, width), bf16)
    wide = jax.ShapeDtypeStruct((2 * n, rows, width), bf16)
    narrow = jax.ShapeDtypeStruct((2 * n, rows, inner), bf16)
    gathered = (g.devices, length, width)
    return pl.pallas_call(
        functools.partial(experts_kernel, reps, shards, capacity, held),
        out_shape=(
            jax.ShapeDtypeStruct(slab.shape, f32),
            blocks,
            blocks,
            wide,
            wide,
            narrow,
            narrow,
            narrow,
            jax.ShapeDtypeStruct((1, 16, 128) if held else gathered, bf16),
        ),
        in_specs=[vmem, vmem, hbm, vmem, vmem, vmem],
        out_specs=(vmem,) + (hbm,) * 8,
        scratch_shapes=[
            v(slab.shape, f32),
            v((2, places, length, width), bf16),
            v(gathered if held else (places, length, width), bf16),
            v((2 * n, rows, inner), f32),
            v((rows, width), bf16),
            v((rows, width), bf16),
            v((rows, inner), bf16),
            v((rows, inner), bf16),
            v((rows, inner), bf16),
            v((places, length, width), bf16),
            v((places, length, width), bf16),
            dma((GatherAll.sends(g),)),
            dma((g.devices,)),
            dma((g.devices,)),
            dma((2,)),
            dma((2,)),
            dma((1,)),
            dma((7,)),
        ]
        + GatherAll.scratch(g),
        compiler_params=params(ident),
        name="experts_all",
    )(x, slab, cots.reshape(places, 2, n, length, width), wg, wu, wd)[:-1]


def inverse_rms(values):
    return lax.rsqrt(jnp.mean(values * values, axis=-1, keepdims=True) + epsilon)


def rope_tables(segment_rows, width):
    length = segment_rows.shape[1]
    places = jnp.arange(length, dtype=jnp.int32)
    same = segment_rows[:, :, None] == segment_rows[:, None, :]
    first = jnp.min(jnp.where(same, places[None, None, :], length), axis=2)
    offset = (places[None] - first).astype(f32)
    half = width // 2
    frequency = rope_base ** (-2.0 * jnp.arange(half, dtype=f32) / width)
    angle = offset[..., None] * frequency[None, None, :]
    cosine, sine = jnp.cos(angle), jnp.sin(angle)
    cosine = jnp.concatenate([cosine, cosine], axis=-1)
    sine = jnp.concatenate([-sine, sine], axis=-1)
    allowed = same & (places[None, None, :] <= places[None, :, None])
    return cosine, sine, allowed


def norm_back(grad_scaled, unit, inverse, gain):
    gained = grad_scaled * gain
    return inverse * (gained - unit * jnp.mean(gained * unit, axis=-1, keepdims=True))


def matmul(a, b, dims=((1,), (0,))):
    return lax.dot_general(a, b, (dims, ((), ())), preferred_element_type=f32)


def local(
    tokens,
    segments,
    routes,
    attn_gain,
    w_query,
    key_weight,
    value_weight,
    w_out,
    query_gain,
    key_gain,
    ffn_gain,
    w_router,
    w_gate,
    w_up,
    w_down,
    cotangent,
):
    reps, shards = lax.axis_size("rep"), lax.axis_size("shard")
    devices = reps * shards
    r, z = lax.axis_index("rep"), lax.axis_index("shard")
    length, width = tokens.shape
    deep = w_query.shape[0]
    head_dim = query_gain.shape[0] * shards
    heads = w_query.shape[1] // head_dim
    kv_heads = key_weight.shape[1] // head_dim
    experts = w_router.shape[1]
    top = routes.shape[1]
    capacity = 2 * length * top // experts
    my_heads = heads // shards
    my_kv = max(1, kv_heads // shards)
    shared_by = max(1, shards // kv_heads)
    q_cols, kv_cols = my_heads * head_dim, my_kv * head_dim
    cols = q_cols + 2 * kv_cols
    piece = deep // reps
    chunks = max(1, devices // 32)
    part = head_dim // shards

    def column(values, rows=deep):
        return jnp.pad(values.reshape(-1, 1), ((0, rows - values.size), (0, 0)))

    small = jnp.concatenate(
        [
            w_router,
            column(attn_gain),
            column(ffn_gain),
            column(query_gain),
            column(key_gain),
            column(segments[0].astype(bf16)),
        ],
        axis=1,
    )
    small_cols = -(-small.shape[1] // 128) * 128
    small = jnp.pad(small, ((0, 0), (0, small_cols - small.shape[1])))
    layout = (q_cols, kv_cols, kv_heads, head_dim)
    block_tokens, small_all, w_in = collect(
        reps, shards, tokens, small, w_query, key_weight, value_weight, layout, 1
    )
    router_full = small_all[:, :, :experts].reshape(width, experts)
    gain_one = small_all[:, :, experts].reshape(1, width).astype(f32)
    gain_two = small_all[:, :, experts + 1].reshape(1, width).astype(f32)
    qgain = small_all[:, :part, experts + 2].reshape(1, head_dim).astype(f32)
    kgain = small_all[:, :part, experts + 3].reshape(1, head_dim).astype(f32)
    segment_rows = small_all[:, :length, experts + 4].astype(jnp.int32)

    head_sizes = (my_heads, my_kv, head_dim)
    cosine, sine, allowed = rope_tables(segment_rows, head_dim)
    bias = jnp.where(allowed, 0.0, masked_score)
    hidden_in, qkv, attn_out, mixed, cotangents = attend(
        reps, shards, head_sizes, block_tokens, w_in, w_out, gain_one, qgain, kgain, cosine, sine, bias, cotangent, 2
    )
    own_tokens = tokens.astype(f32)
    resid = own_tokens + mixed

    inverse_two = inverse_rms(resid)
    normed_two = resid * inverse_two
    hidden_two = (normed_two * gain_two).astype(bf16)
    logits = matmul(hidden_two, router_full)
    gate_probs = jax.nn.softmax(logits, axis=-1)
    chosen = jnp.any(routes[:, :, None] == jnp.arange(experts, dtype=jnp.int32)[None, None, :], axis=1)
    picked = jnp.where(chosen, gate_probs, 0.0)
    picked_total = jnp.sum(picked, axis=-1, keepdims=True)
    mix = picked / picked_total
    slab = jnp.where(chosen, mix, -1.0).T.reshape(experts, 1, length)
    slab = jnp.broadcast_to(slab, (experts, 8, length))
    back_mix, sums, grad_sums, rows, row_grads, grad_gate, grad_up, activated = experts_all(
        reps, shards, capacity, hidden_two, slab, cotangents, w_gate[0], w_up[0], w_down[0], 4
    )
    sums = sums.reshape(devices, length, width)
    grad_sums = grad_sums.reshape(devices, length, width)
    rows, row_grads = rows.reshape(-1, width), row_grads.reshape(-1, width)
    fill = (rows, row_grads) + tuple(a.reshape(rows.shape[0], -1) for a in (grad_gate, grad_up, activated))
    grad_hidden, mixes, grad_w_gate, grad_w_up, grad_w_down = scatter_wide(
        reps, shards, grad_sums, back_mix, fill, 8, chunks
    )

    grad_out = cotangent.astype(f32)
    grad_mix = mixes[:, 0, :].T
    grad_picked = jnp.where(chosen, grad_mix - jnp.sum(grad_mix * mix, axis=-1, keepdims=True), 0.0) / picked_total
    grad_logits = (gate_probs * (grad_picked - jnp.sum(grad_picked * picked, axis=-1, keepdims=True))).astype(bf16)
    grad_hidden = grad_hidden + matmul(grad_logits, router_full, ((1,), (1,)))
    grad_ffn_gain = jnp.sum(grad_hidden * normed_two, axis=0)
    grad_resid = grad_out + norm_back(grad_hidden, normed_two, inverse_two, gain_two)
    grad_w_router = matmul(hidden_two, grad_logits, ((0,), (0,)))

    fused = width // chunks
    grad_attn, grad_qkv, grad_query_gain, grad_key_gain, moe = attend_back(
        reps, shards, head_sizes, grad_resid.astype(bf16), qkv, w_out, qgain, kgain, cosine, sine, bias,
        sums[:, :, :fused], 5,
    )
    if chunks > 1:
        rest = scatter_wide(reps, shards, sums[:, :, fused:], None, None, 16, chunks - 1)
        moe = jnp.concatenate([moe, rest], axis=1)
    output = (resid + moe).astype(bf16)
    grad_attn = grad_attn.reshape(shards * length, width)
    grad_qkv = grad_qkv.reshape(shards * length, cols)
    grad_w_out = matmul(attn_out.reshape(shards * length, q_cols), grad_attn, ((0,), (0,)))
    owned_out = lax.psum(grad_w_out.astype(bf16), "rep").astype(f32)
    hidden_in = hidden_in.reshape(shards * length, width)
    _, normed_one = unit_of(block_tokens.reshape(shards * length, width).astype(f32))
    grad_part = matmul(grad_qkv, w_in, ((1,), (1,)))
    grad_attn_gain = jnp.sum(grad_part * normed_one, axis=0)
    grad_w_in = matmul(hidden_in, grad_qkv, ((0,), (0,)))

    def spread(values):
        return jnp.pad(values.reshape(shards, part), ((0, 0), (0, deep - part))).reshape(width, 1)

    small_grads = jnp.concatenate(
        [
            grad_w_router,
            grad_attn_gain.reshape(width, 1),
            grad_ffn_gain.reshape(width, 1),
            spread(grad_query_gain),
            spread(grad_key_gain),
        ],
        axis=1,
    )
    small_grads = jnp.pad(small_grads, ((0, 0), (0, small_cols - small_grads.shape[1])))
    sent = jnp.concatenate([grad_w_in, small_grads], axis=1).astype(bf16)
    sent = sent.reshape(shards, reps, piece, cols + small_cols)
    grad_part = grad_part.astype(bf16).reshape(shards, length, width)
    grad_hidden_in, sent = deliver(reps, shards, grad_part, sent, 6)
    sent = sent.reshape(shards, deep, cols + small_cols)
    own_inverse = inverse_rms(own_tokens)
    own_normed = own_tokens * own_inverse
    grad_tokens = grad_resid + norm_back(grad_hidden_in, own_normed, own_inverse, gain_one)

    def joined(values):
        if shared_by > 1:
            values = values.astype(f32).reshape(-1, shared_by, deep, values.shape[-1]).sum(axis=1)
        return values.transpose(1, 0, 2).reshape(deep, -1).astype(f32)

    owned_small = jnp.sum(sent[:, :, cols:].astype(f32), axis=0)
    return (
        output,
        grad_tokens,
        owned_small[:, experts],
        sent[:, :, :q_cols].transpose(1, 0, 2).reshape(deep, -1).astype(f32),
        joined(sent[:, :, q_cols : q_cols + kv_cols]),
        joined(sent[:, :, q_cols + kv_cols : cols]),
        owned_out,
        owned_small[:part, experts + 2],
        owned_small[:part, experts + 3],
        owned_small[:, experts + 1],
        owned_small[:, :experts],
        grad_w_gate[None],
        grad_w_up[None],
        grad_w_down[None],
    )


def solution(mesh):
    split = P(("rep", "shard"))
    row = P("shard")
    return jax.shard_map(
        local,
        mesh=mesh,
        in_specs=(split,) * 3 + (row,) * 9 + (split,) * 4,
        out_specs=(split,) * 2 + (row,) * 9 + (split,) * 3,
        check_vma=False,
    )
```

```python
import functools
import jax
import jax.numpy as jnp
from jax import lax
from jax.experimental import pallas as pl
from jax.experimental.pallas import tpu as pltpu
from jax.sharding import PartitionSpec as P

bf16 = jnp.bfloat16
f32 = jnp.float32
vmem_cap = 62 * 1024 * 1024
epsilon = 1e-06
rope_base = 1000000.0
masked_score = -1e30


class Grid:
    def __init__(self, reps, shards):
        self.reps, self.shards = reps, shards
        self.devices = reps * shards
        self.places = reps // 2
        self.los = self.places // 2

    def here(self):
        self.r = lax.axis_index("rep")
        self.z = lax.axis_index("shard")
        self.core = self.r % 2
        place = self.r // 2
        self.hi = place // self.los
        self.lo = place % self.los
        return self

    def rep_of(self, hi, lo, core):
        return (hi * self.los + lo) * 2 + core

    def device(self, rep, shard):
        return {"rep": rep, "shard": shard}

    def other_lo(self, step):
        return (self.lo + step) % self.los

    def nearest(self):
        n = self.shards
        rows = [sorted(range(n), key=lambda p: (abs(p - z), p)) for z in range(n)]
        return [pick(self.z, [rows[z][turn] for z in range(n)]) for turn in range(n)]


def pick(index, values):
    out = jnp.int32(values[0])
    for i in range(1, len(values)):
        out = jnp.where(index == i, jnp.int32(values[i]), out)
    return out


class Sends:
    def __init__(self, sems):
        self.sems, self.used, self.open, self.samples = sems, 0, [], []

    def copy(self, src, dst, sem, recv, device):
        return pltpu.make_async_remote_copy(
            src_ref=src,
            dst_ref=dst,
            send_sem=self.sems.at[sem],
            recv_sem=recv,
            device_id=device,
            device_id_type=pl.DeviceIdType.MESH,
        )

    def start(self, src, dst, recv, device, when=None):
        copy = self.copy(src, dst, self.used, recv, device)
        sample = src
        for other in self.samples:
            if other.shape == src.shape:
                sample = other
        self.open.append((self.used, sample, when))
        self.used += 1
        if when is None:
            copy.start()
        else:
            pl.when(when())(copy.start)

    def arrived(self, dst, recv, device, when=None):
        copy = self.copy(dst, dst, 0, recv, device)
        if when is None:
            copy.wait_recv()
        else:
            pl.when(when())(copy.wait_recv)

    def drain(self):
        here = {"rep": lax.axis_index("rep"), "shard": lax.axis_index("shard")}
        for sem, sample, when in self.open:
            copy = self.copy(sample, sample, sem, self.sems.at[sem], here)
            if when is None:
                copy.wait_send()
            else:
                pl.when(when())(copy.wait_send)
        self.open = []


def greet_all(g):
    barrier = pltpu.get_barrier_semaphore()
    me = g.r * g.shards + g.z

    def one(step, carry):
        peer = (me + step) % g.devices
        pl.semaphore_signal(
            barrier,
            inc=1,
            device_id=g.device(peer // g.shards, peer % g.shards),
            device_id_type=pl.DeviceIdType.MESH,
        )
        return carry

    lax.fori_loop(1, g.devices, one, 0)
    pl.semaphore_wait(barrier, g.devices - 1)


def push_rows(g, src, dst, send_sems, recv_sems):
    me = g.r * g.shards + g.z

    def one(step, carry):
        peer = (me + step) % g.devices
        pltpu.make_async_remote_copy(
            src_ref=src.at[peer],
            dst_ref=dst.at[me],
            send_sem=send_sems.at[step],
            recv_sem=recv_sems.at[step],
            device_id=g.device(peer // g.shards, peer % g.shards),
            device_id_type=pl.DeviceIdType.MESH,
        ).start()
        return carry

    lax.fori_loop(1, g.devices, one, 0)


def push_wait(g, src, dst, send_sems, recv_sems):
    me = g.r * g.shards + g.z

    def one(step, carry):
        peer = (me + g.devices - step) % g.devices
        copy = pltpu.make_async_remote_copy(
            src_ref=src.at[peer],
            dst_ref=dst.at[peer],
            send_sem=send_sems.at[step],
            recv_sem=recv_sems.at[step],
            device_id=g.device(peer // g.shards, peer % g.shards),
            device_id_type=pl.DeviceIdType.MESH,
        )
        copy.wait_send()
        copy.wait_recv()
        return carry

    lax.fori_loop(1, g.devices, one, 0)


class PlaneGather:
    def __init__(self, g, s, view, lr, hr, dr, cr):
        self.g, self.s, self.view = g, s, view
        self.lr, self.hr, self.dr, self.cr = lr, hr, dr, cr

    @staticmethod
    def scratch(g, units):
        dma, others = pltpu.SemaphoreType.DMA, max(1, g.los - 1)
        return [dma((units, 2, others)), dma((units, 2)), dma((units, 2, others)), dma((units, 5 * g.los))]

    @staticmethod
    def sends(g, units):
        return 9 * g.los * units

    def at(self, hi, lo):
        return self.g.device(self.g.rep_of(hi, lo, self.g.core), self.g.z)

    def partner(self):
        g = self.g
        return g.device(g.rep_of(g.hi, g.lo, 1 - g.core), g.z)

    def own(self, u, src=None):
        g, s = self.g, self.s

        def dst(part):
            return self.view(u, g.hi, g.lo, g.core, part)

        src = src or dst
        for part in (0, 1):
            for step in range(1, g.los):
                s.start(src(part), dst(part), self.lr.at[u, part, step - 1], self.at(g.hi, g.other_lo(step)))
            s.start(src(1 - part), dst(1 - part), self.hr.at[u, 1 - part], self.at(1 - g.hi, g.lo))
        s.start(src(None), dst(None), self.cr.at[u, 0], self.partner())

    def take(self, u, hi, lo, part, recv, frm, partner_slot, onward=()):
        ref = self.view(u, hi, lo, self.g.core, part)
        self.s.arrived(ref, recv, frm)
        for sem, device in onward:
            self.s.start(ref, ref, sem, device)
        self.s.start(ref, ref, self.cr.at[u, partner_slot], self.partner())

    def first(self, u):
        g = self.g
        far = 1 - g.hi
        for step in range(1, g.los):
            frm = (g.lo + g.los - step) % g.los
            onward = [(self.dr.at[u, 0, step - 1], self.at(far, g.lo))]
            self.take(u, g.hi, frm, 0, self.lr.at[u, 0, step - 1], self.at(g.hi, frm), 5 * step, onward)
        onward = [(self.dr.at[u, 1, step - 1], self.at(g.hi, g.other_lo(step))) for step in range(1, g.los)]
        self.take(u, far, g.lo, 1, self.hr.at[u, 1], self.at(far, g.lo), 1, onward)
        for step in range(1, g.los):
            frm = (g.lo + g.los - step) % g.los
            self.take(u, g.hi, frm, 1, self.lr.at[u, 1, step - 1], self.at(g.hi, frm), 5 * step + 1)
        self.take(u, far, g.lo, 0, self.hr.at[u, 0], self.at(far, g.lo), 2)

    def second(self, u):
        g = self.g
        far = 1 - g.hi
        for step in range(1, g.los):
            frm = (g.lo + g.los - step) % g.los
            self.take(u, far, frm, 0, self.dr.at[u, 0, step - 1], self.at(far, g.lo), 5 * step + 2)
            self.take(u, far, frm, 1, self.dr.at[u, 1, step - 1], self.at(g.hi, frm), 5 * step + 3)

    def from_partner(self, u):
        g = self.g
        far, other = 1 - g.hi, 1 - g.core

        def got(hi, lo, part, slot):
            self.s.arrived(self.view(u, hi, lo, other, part), self.cr.at[u, slot], self.partner())

        got(g.hi, g.lo, None, 0)
        got(far, g.lo, 1, 1)
        got(far, g.lo, 0, 2)
        for step in range(1, g.los):
            frm = (g.lo + g.los - step) % g.los
            got(g.hi, frm, 0, 5 * step)
            got(g.hi, frm, 1, 5 * step + 1)
            got(far, frm, 0, 5 * step + 2)
            got(far, frm, 1, 5 * step + 3)


def add_rows(dst, *srcs, step=16):
    def one(i, carry):
        at = pl.ds(pl.multiple_of(i * step, step), step)
        total = srcs[0][at, :].astype(f32)
        for src in srcs[1:]:
            total = total + src[at, :].astype(f32)
        dst[at, :] = total.astype(dst.dtype)
        return carry

    lax.fori_loop(0, dst.shape[0] // step, one, 0)


class PlaneScatter:
    def __init__(self, g, s, p, cut, own, ra, rb0, rb1, rc0, rc1, sa, sb0, sb1, sc0, sc1, ls):
        self.g, self.s, self.p, self.cut, self.owned = g, s, p, cut, own
        self.ra, self.rb0, self.rb1, self.rc0, self.rc1 = ra, rb0, rb1, rc0, rc1
        self.sa, self.sb0, self.sb1, self.sc0, self.sc1, self.ls = sa, sb0, sb1, sc0, sc1, ls

    @staticmethod
    def scratch(g, units, block, halves, dtype):
        dma, others, v = pltpu.SemaphoreType.DMA, max(1, g.los - 1), pltpu.VMEM
        first, second = halves
        return [
            v((units, g.places) + block, dtype),
            v((units, g.places) + block, dtype),
            v((units, g.los) + first, dtype),
            v((units, others, 2) + second, dtype),
            v((units, others) + first, dtype),
            v((units,) + second, dtype),
            dma((units,)),
            dma((units,)),
            dma((units, others, 2)),
            dma((units, others)),
            dma((units,)),
            dma((units,)),
        ]

    @staticmethod
    def sends(g, units):
        return units * (3 * g.los + 2)

    def at(self, hi, lo):
        return self.g.device(self.g.rep_of(hi, lo, self.g.core), self.g.z)

    def partner(self):
        g = self.g
        return g.device(g.rep_of(g.hi, g.lo, 1 - g.core), g.z)

    def load(self, units):
        self.loads = []
        for turn in range(units):
            load = pltpu.make_async_copy(self.p(turn, self.g.core), self.owned.at[turn], self.ls.at[turn])
            load.start()
            self.loads.append(load)

    def to_partner(self, turn):
        self.s.start(self.p(turn, 1 - self.g.core), self.ra.at[turn], self.sa.at[turn], self.partner())

    def half(self, turn, place, part):
        return self.owned.at[(turn, place) + self.cut(part)]

    def mine(self, turn):
        return self.owned.at[turn, self.g.hi * self.g.los + self.g.lo]

    def a(self, turn):
        g, s = self.g, self.s
        far = 1 - g.hi
        self.loads[turn].wait()
        s.arrived(self.ra.at[turn], self.sa.at[turn], self.partner())

        def one(q, carry):
            line = self.owned.at[turn, q]
            add_rows(line, line, self.ra.at[turn, q])
            return carry

        lax.fori_loop(0, g.places, one, 0)
        block = self.owned.at[(turn, pl.ds(far * g.los, g.los)) + self.cut(0)]
        s.start(block, self.rb0.at[turn], self.sb0.at[turn], self.at(far, g.lo))
        for step in range(1, g.los):
            to = g.other_lo(step)
            for hi in range(2):
                sem = self.sb1.at[turn, step - 1, hi]
                s.start(self.half(turn, hi * g.los + to, 1), self.rb1.at[turn, step - 1, hi], sem, self.at(g.hi, to))

    def b(self, turn):
        g, s = self.g, self.s
        far = 1 - g.hi
        s.arrived(self.rb0.at[turn], self.sb0.at[turn], self.at(far, g.lo))
        for lo in range(g.los):
            line = self.half(turn, g.hi * g.los + lo, 0)
            add_rows(line, line, self.rb0.at[turn, lo])
        for step in range(1, g.los):
            to = g.other_lo(step)
            sem = self.sc0.at[turn, step - 1]
            s.start(self.half(turn, g.hi * g.los + to, 0), self.rc0.at[turn, step - 1], sem, self.at(g.hi, to))
        for step in range(1, g.los):
            frm = (g.lo + g.los - step) % g.los
            for hi in range(2):
                s.arrived(self.rb1.at[turn, step - 1, hi], self.sb1.at[turn, step - 1, hi], self.at(g.hi, frm))
        for hi in range(2):
            line = self.half(turn, hi * g.los + g.lo, 1)
            add_rows(line, line, *[self.rb1.at[turn, step, hi] for step in range(g.los - 1)])
        s.start(self.half(turn, far * g.los + g.lo, 1), self.rc1.at[turn], self.sc1.at[turn], self.at(far, g.lo))

    def c(self, turn):
        g, s = self.g, self.s
        place = g.hi * g.los + g.lo
        for step in range(1, g.los):
            frm = (g.lo + g.los - step) % g.los
            s.arrived(self.rc0.at[turn, step - 1], self.sc0.at[turn, step - 1], self.at(g.hi, frm))
        line = self.half(turn, place, 0)
        add_rows(line, line, *[self.rc0.at[turn, step] for step in range(g.los - 1)])
        s.arrived(self.rc1.at[turn], self.sc1.at[turn], self.at(1 - g.hi, g.lo))
        line = self.half(turn, place, 1)
        add_rows(line, line, self.rc1.at[turn])


def pass_along(g, s, zp, src, dst, zr):
    n = g.shards
    right, left = g.device(g.r, jnp.minimum(g.z + 1, n - 1)), g.device(g.r, jnp.maximum(g.z - 1, 0))
    s.start(src, dst, zr.at[zp], right, lambda: (zp <= g.z) & (g.z + 1 < n))
    s.start(src, dst, zr.at[zp], left, lambda: (zp >= g.z) & (g.z > 0))


def send_line(g, s, zp, line, out_ref, rl, rr, sl, sr, last):
    n = g.shards
    left, right = g.device(g.r, jnp.maximum(g.z - 1, 0)), g.device(g.r, jnp.minimum(g.z + 1, n - 1))
    has_left, has_right = g.z > 0, g.z + 1 < n
    if last:
        s.arrived(rl.at[g.z], sl.at[g.z], left, lambda: g.z > 0)
        s.arrived(rr.at[g.z], sr.at[g.z], right, lambda: g.z + 1 < n)

        @pl.when(has_left & has_right)
        def _():
            add_rows(out_ref, line, rl.at[g.z], rr.at[g.z])

        @pl.when(has_left & jnp.logical_not(has_right))
        def _():
            add_rows(out_ref, line, rl.at[g.z])

        @pl.when(has_right & jnp.logical_not(has_left))
        def _():
            add_rows(out_ref, line, rr.at[g.z])
    else:
        onward_right, onward_left = zp > g.z, zp < g.z

        @pl.when(onward_right & has_left)
        def _():
            s.arrived(rl.at[zp], sl.at[zp], left)
            add_rows(line, line, rl.at[zp])

        @pl.when(onward_left & has_right)
        def _():
            s.arrived(rr.at[zp], sr.at[zp], right)
            add_rows(line, line, rr.at[zp])

        s.start(line, rl.at[zp], sl.at[zp], right, lambda: zp > g.z)
        s.start(line, rr.at[zp], sr.at[zp], left, lambda: zp < g.z)


def line_scratch(shards, block, dtype):
    v, dma = pltpu.VMEM, pltpu.SemaphoreType.DMA
    return [v((shards,) + block, dtype), v((shards,) + block, dtype), dma((shards,)), dma((shards,))]


def wait_for(copies, k):
    for copy in copies(k):
        copy.wait()


hbm = pl.BlockSpec(memory_space=pl.ANY)
vmem = pl.BlockSpec(memory_space=pltpu.VMEM)


def params(ident):
    return pltpu.CompilerParams(collective_id=ident, has_side_effects=True, vmem_limit_bytes=vmem_cap)


def scatter_all_kernel(reps, shards, slabbed, *refs):
    if slabbed:
        (
            p_ref, slab_ref, x_ref, c_ref, gg_ref, gu_ref, act_ref, out_ref, slabs_ref, wg_ref, wu_ref, wd_ref,
            xt, ct, og, ou, od, tile_sems, out_sems, *rest,
        ) = refs
    else:
        p_ref, out_ref, *rest = refs
    sems, ps, pr, slab_sem, *rest = rest
    g = Grid(reps, shards).here()
    s = Sends(sems)
    n = g.shards
    scatter = ScatterAll(g, s, p_ref, out_ref, *rest)
    half = pl.ds(0, out_ref.shape[0] // 2)
    own = scatter.plane.owned
    s.samples = [own.at[0, 0], own.at[0, 0, half], own.at[0, pl.ds(0, g.los), half]]
    scatter.load()
    if not slabbed:
        greet_all(g)
        scatter.to_partner()
        for turn in range(n + 2):
            scatter.step(turn)
        s.drain()
        return

    tile = xt.shape[2]
    tiles = x_ref.shape[1] // tile

    def tile_in(j, slot):
        span = pl.ds(pl.multiple_of(j * tile, tile), tile)
        return [
            pltpu.make_async_copy(x_ref.at[:, span], xt.at[slot], tile_sems.at[slot, 0]),
            pltpu.make_async_copy(c_ref.at[:, span], ct.at[slot], tile_sems.at[slot, 1]),
        ]

    def tile_out(j):
        span = pl.ds(pl.multiple_of(j * tile, tile), tile)
        return [
            pltpu.make_async_copy(og, wg_ref.at[span, :], out_sems.at[0]),
            pltpu.make_async_copy(ou, wu_ref.at[span, :], out_sems.at[1]),
            pltpu.make_async_copy(od, wd_ref.at[:, span], out_sems.at[2]),
        ]

    for copy in tile_in(0, 0):
        copy.start()
    greet_all(g)
    scatter.to_partner()
    push_rows(g, slab_ref, slabs_ref, ps, pr)
    me = g.r * n + g.z
    keep_slab = pltpu.make_async_copy(slab_ref.at[me], slabs_ref.at[me], slab_sem.at[0])
    keep_slab.start()

    def next_tiles(j):
        for copy in tile_in(j + 1, (j + 1) % 2):
            copy.start()

    def weight_grads(j, carry):
        for turn in range(n):
            pl.when(j == turn * tiles // n)(functools.partial(scatter.step, turn))
        pl.when(j + 1 < tiles)(functools.partial(next_tiles, j))
        slot = j % 2
        for copy in tile_in(j, slot):
            copy.wait()
        pl.when(j > 0)(functools.partial(wait_for, tile_out, j))
        og[...] = t_dot(xt[slot], gg_ref[...])
        ou[...] = t_dot(xt[slot], gu_ref[...])
        od[...] = t_dot(act_ref[...], ct[slot])
        for copy in tile_out(j):
            copy.start()
        return carry

    lax.fori_loop(0, tiles, weight_grads, 0)
    scatter.step(n)
    scatter.step(n + 1)
    wait_for(tile_out, 0)
    keep_slab.wait()
    push_wait(g, slab_ref, slabs_ref, ps, pr)
    s.drain()


def scatter_all(reps, shards, p, slab, fill, ident):
    g = Grid(reps, shards)
    n = shards
    _, rows, width = p.shape
    dma, v = pltpu.SemaphoreType.DMA, pltpu.VMEM
    slabbed = slab is not None
    out_shape = (jax.ShapeDtypeStruct((rows, width), f32),)
    out_specs, in_specs, extra, scratch = (vmem,), [hbm], [], []
    if slabbed:
        x, c, gg, gu, act = fill
        count, wide = x.shape
        inner = gg.shape[1]
        tile = 256
        narrow = jax.ShapeDtypeStruct((wide, inner), f32)
        out_shape += (
            jax.ShapeDtypeStruct(slab.shape, slab.dtype), narrow, narrow, jax.ShapeDtypeStruct((inner, wide), f32)
        )
        out_specs += (vmem, hbm, hbm, hbm)
        in_specs += [vmem, hbm, hbm, vmem, vmem, vmem]
        extra = [slab, *fill]
        scratch = [
            v((2, count, tile), bf16), v((2, count, tile), bf16),
            v((tile, inner), f32), v((tile, inner), f32), v((inner, tile), f32),
            dma((2, 2)), dma((3,)),
        ]
    done = pl.pallas_call(
        functools.partial(scatter_all_kernel, reps, shards, slabbed),
        out_shape=out_shape,
        in_specs=in_specs,
        out_specs=out_specs,
        scratch_shapes=scratch
        + [dma((ScatterAll.sends(g),)), dma((g.devices,)), dma((g.devices,)), dma((1,))]
        + ScatterAll.scratch(g, (rows, width), p.dtype),
        compiler_params=params(ident),
        name="scatter_all",
    )(p.reshape(g.places, 2, n, rows, width), *extra)
    return done if slabbed else done[0]


def scatter_wide(reps, shards, p, slab, fill, ident, chunks):
    if chunks == 1:
        return scatter_all(reps, shards, p, slab, fill, ident)
    step = p.shape[2] // chunks
    parts = [
        scatter_all(reps, shards, p[:, :, i * step : (i + 1) * step], slab if i == 0 else None, fill, ident + i)
        for i in range(chunks)
    ]
    if slab is None:
        return jnp.concatenate(parts, axis=1)
    first, *others = parts[0]
    return jnp.concatenate([first] + parts[1:], axis=1), *others


def deliver_kernel(reps, shards, p_ref, w_ref, out_ref, ws_ref, line_own, rl, rr, sl, sr, sems, line_loads, wr, keep_sem, *rest):
    g = Grid(reps, shards).here()
    s = Sends(sems)
    n = g.shards
    gather_refs, scatter_refs = rest[:4], rest[4:]
    cols = w_ref.shape[-1]
    first = cols // 2 // 128 * 128
    spans = {0: pl.ds(0, first), 1: pl.ds(first, cols - first), None: pl.ds(0, cols)}
    order = g.nearest()[::-1]
    scatter = PlaneScatter(
        g, s, lambda turn, core: w_ref.at[turn, :, core], lambda part: (slice(None), spans[part]), *scatter_refs
    )
    gather = PlaneGather(
        g, s, lambda u, hi, lo, core, part: ws_ref.at[u, g.rep_of(hi, lo, core), :, spans[part]], *gather_refs
    )
    scatter.load(n)
    loads = []
    for turn in range(n):
        load = pltpu.make_async_copy(p_ref.at[order[turn]], line_own.at[turn], line_loads.at[turn])
        load.start()
        loads.append(load)
    barrier = pltpu.get_barrier_semaphore()
    peers = [g.device(g.r, (g.z + step) % n) for step in range(1, n)]
    peers += [g.device(g.rep_of(g.hi, g.other_lo(step), g.core), g.z) for step in range(1, g.los)]
    peers += [g.device(g.rep_of(1 - g.hi, g.lo, g.core), g.z), g.device(g.rep_of(g.hi, g.lo, 1 - g.core), g.z)]
    for peer in peers:
        pl.semaphore_signal(barrier, inc=1, device_id=peer, device_id_type=pl.DeviceIdType.MESH)
    pl.semaphore_wait(barrier, len(peers))

    for turn in range(n):
        scatter.to_partner(turn)

    def line(turn):
        loads[turn].wait()
        send_line(g, s, order[turn], line_own.at[turn], out_ref, rl, rr, sl, sr, last=turn == n - 1)

    def owner(turn):
        scatter.c(turn)
        dst = ws_ref.at[g.z, g.r]
        keep = pltpu.make_async_copy(scatter.mine(turn), dst, keep_sem.at[0])
        pl.when(g.z == turn)(keep.start)
        s.start(scatter.mine(turn), dst, wr.at[g.z], g.device(g.r, turn), lambda: g.z != turn)
        pl.when(g.z == turn)(keep.wait)

    line(0)
    for turn in range(n + 2):
        if turn < n:
            scatter.a(turn)
        if 0 <= turn - 1 < n:
            scatter.b(turn - 1)
        if 1 <= turn < n - 1:
            line(turn)
        if 0 <= turn - 2 < n:
            owner(turn - 2)
    gather.own(g.z)

    def unit(step):
        return (g.z + n - step) % n

    for step in range(1, n):
        u = unit(step)
        s.arrived(ws_ref.at[u, g.r], wr.at[u], g.device(g.r, u))
        gather.own(u)
        gather.first(unit(step - 1))
        if step > 1:
            gather.second(unit(step - 2))
    gather.first(unit(n - 1))
    gather.second(unit(n - 2))
    gather.second(unit(n - 1))
    line(n - 1)
    for step in range(n):
        gather.from_partner(unit(step))
    s.drain()


def deliver(reps, shards, p, w, ident):
    g = Grid(reps, shards)
    n = shards
    dma = pltpu.SemaphoreType.DMA
    _, rows, width = p.shape
    _, _, piece, cols = w.shape
    first = cols // 2 // 128 * 128
    return pl.pallas_call(
        functools.partial(deliver_kernel, reps, shards),
        out_shape=(jax.ShapeDtypeStruct((rows, width), f32), jax.ShapeDtypeStruct(w.shape, w.dtype)),
        in_specs=[hbm, hbm],
        out_specs=(vmem, vmem),
        scratch_shapes=[pltpu.VMEM(p.shape, p.dtype)]
        + line_scratch(n, (rows, width), p.dtype)
        + [
            dma((PlaneGather.sends(g, n) + PlaneScatter.sends(g, n) + 3 * n,)),
            dma((n,)),
            dma((n,)),
            dma((1,)),
        ]
        + PlaneGather.scratch(g, n)
        + PlaneScatter.scratch(g, n, (piece, cols), ((piece, first), (piece, cols - first)), w.dtype),
        compiler_params=params(ident),
        name="deliver",
    )(p, w.reshape(n, g.places, 2, piece, cols))


def turned(x, cosine, sine):
    return x * cosine + pltpu.roll(x, x.shape[-1] // 2, 1) * sine


def mean_last(x):
    return jnp.sum(x, axis=-1, keepdims=True) * (1.0 / x.shape[-1])


def unit_of(x):
    inverse = lax.rsqrt(mean_last(x * x) + epsilon)
    return inverse, x * inverse


def dot_t(a, b):
    return lax.dot_general(a, b, (((1,), (1,)), ((), ())), preferred_element_type=f32)


def t_dot(a, b):
    return lax.dot_general(a, b, (((0,), (0,)), ((), ())), preferred_element_type=f32)


def softmax_rows(q_rot, k_rot, bias, head_dim):
    scores = dot_t(q_rot, k_rot) * head_dim ** (-0.5) + bias
    raised = jnp.exp(scores - jnp.max(scores, axis=-1, keepdims=True))
    return raised * (1.0 / jnp.sum(raised, axis=-1, keepdims=True))


def back_unit(grad_scaled, unit, inverse, gain):
    gained = grad_scaled * gain
    return inverse * (gained - unit * mean_last(gained * unit))


def attend_block(b, heads, x_ref, w_ref, wo_ref, gain_ref, qg_ref, kg_ref, cos_ref, sin_ref, bias_ref, hid_ref, qkv_ref, att_ref, line):
    my_heads, my_kv, head_dim = heads
    x = x_ref[b].astype(f32)
    _, unit = unit_of(x)
    hid_ref[b] = (unit * gain_ref[...]).astype(bf16)
    qkv_ref[b] = jnp.dot(hid_ref[b], w_ref[...], preferred_element_type=f32)
    cosine, sine, bias = cos_ref[b], sin_ref[b], bias_ref[b]
    group = my_heads // my_kv
    for n in range(my_kv):
        at_k = (my_heads + n) * head_dim
        at_v = (my_heads + my_kv + n) * head_dim
        _, k_unit = unit_of(qkv_ref[b, :, at_k : at_k + head_dim])
        k_rot = turned(k_unit * kg_ref[...], cosine, sine).astype(bf16)
        values = qkv_ref[b, :, at_v : at_v + head_dim].astype(bf16)
        for h in range(n * group, (n + 1) * group):
            span = slice(h * head_dim, (h + 1) * head_dim)
            _, q_unit = unit_of(qkv_ref[b, :, span])
            q_rot = turned(q_unit * qg_ref[...], cosine, sine).astype(bf16)
            probs = softmax_rows(q_rot, k_rot, bias, head_dim)
            mixed = jnp.dot(probs.astype(bf16), values, preferred_element_type=f32)
            att_ref[b, :, span] = mixed.astype(bf16)
    line[...] = jnp.dot(att_ref[b], wo_ref[...], preferred_element_type=f32).astype(bf16)


def attend_back_block(b, heads, ga_ref, qkv_ref, wo_ref, qg_ref, kg_ref, cos_ref, sin_ref, bias_ref, gm_ref, gqkv_ref, qsum_ref, ksum_ref):
    my_heads, my_kv, head_dim = heads
    gm_ref[...] = dot_t(ga_ref[b], wo_ref[...]).astype(bf16)
    cosine, sine, bias = cos_ref[b], sin_ref[b], bias_ref[b]
    group = my_heads // my_kv
    qg, kg = qg_ref[...], kg_ref[...]
    for n in range(my_kv):
        at_k = (my_heads + n) * head_dim
        at_v = (my_heads + my_kv + n) * head_dim
        k_inverse, k_unit = unit_of(qkv_ref[b, :, at_k : at_k + head_dim])
        k_rot = turned(k_unit * kg, cosine, sine).astype(bf16)
        values = qkv_ref[b, :, at_v : at_v + head_dim].astype(bf16)
        grad_k = jnp.zeros(k_unit.shape, f32)
        grad_v = jnp.zeros(k_unit.shape, f32)
        for h in range(n * group, (n + 1) * group):
            span = slice(h * head_dim, (h + 1) * head_dim)
            q_inverse, q_unit = unit_of(qkv_ref[b, :, span])
            q_rot = turned(q_unit * qg, cosine, sine).astype(bf16)
            probs = softmax_rows(q_rot, k_rot, bias, head_dim)
            grad_mixed = gm_ref[:, span]
            grad_weights = dot_t(grad_mixed, values)
            centre = jnp.sum(probs * grad_weights, axis=-1, keepdims=True)
            grad_scores = (probs * (grad_weights - centre) * head_dim ** (-0.5)).astype(bf16)
            grad_v = grad_v + t_dot(probs.astype(bf16), grad_mixed)
            grad_k = grad_k + t_dot(grad_scores, q_rot)
            grad_q = jnp.dot(grad_scores, k_rot, preferred_element_type=f32)
            grad_q = turned(grad_q, cosine, -sine)
            qsum_ref[...] += jnp.sum(grad_q * q_unit, axis=0, keepdims=True)
            gqkv_ref[b, :, span] = back_unit(grad_q, q_unit, q_inverse, qg).astype(bf16)
        grad_k = turned(grad_k, cosine, -sine)
        ksum_ref[...] += jnp.sum(grad_k * k_unit, axis=0, keepdims=True)
        gqkv_ref[b, :, at_k : at_k + head_dim] = back_unit(grad_k, k_unit, k_inverse, kg).astype(bf16)
        gqkv_ref[b, :, at_v : at_v + head_dim] = grad_v.astype(bf16)


class GatherAll:
    def __init__(self, g, s, x_ref, out_ref, zr, plane_sems):
        self.g, self.s, self.x_ref, self.out_ref, self.zr = g, s, x_ref, out_ref, zr
        half = x_ref.shape[0] // 2
        self.spans = {0: pl.ds(0, half), 1: pl.ds(half, half), None: pl.ds(0, 2 * half)}
        self.order = g.nearest()
        self.plane = PlaneGather(g, s, self.view, *plane_sems)

    @staticmethod
    def scratch(g):
        dma = pltpu.SemaphoreType.DMA
        return [dma((g.shards,))] + PlaneGather.scratch(g, g.shards)

    @staticmethod
    def sends(g):
        return PlaneGather.sends(g, g.shards) + 2 * g.shards

    def view(self, u, hi, lo, core, part):
        return self.out_ref.at[self.g.rep_of(hi, lo, core) * self.g.shards + u, self.spans[part]]

    def own(self):
        g = self.g
        return self.view(g.z, g.hi, g.lo, g.core, None)

    def line(self, turn):
        g, zp = self.g, self.order[turn]
        dst = self.view(zp, g.hi, g.lo, g.core, None)
        if turn:
            self.s.arrived(dst, self.zr.at[zp], g.device(g.r, zp))
        pass_along(g, self.s, zp, dst if turn else self.x_ref, dst, self.zr)
        self.plane.own(zp, None if turn else lambda part: self.x_ref.at[self.spans[part]])

    def first(self, turn):
        self.plane.first(self.order[turn])

    def second(self, turn):
        self.plane.second(self.order[turn])

    def finish(self):
        for turn in range(self.g.shards):
            self.plane.from_partner(self.order[turn])


class ScatterAll:
    def __init__(self, g, s, p_ref, out_ref, rl, rr, sl, sr, *plane_refs):
        self.g, self.s, self.out_ref = g, s, out_ref
        self.lines = (rl, rr, sl, sr)
        half = out_ref.shape[0] // 2
        self.order = g.nearest()[::-1]
        self.plane = PlaneScatter(
            g,
            s,
            lambda turn, core: p_ref.at[:, core, self.order[turn]],
            lambda part: (pl.ds(part * half, half),),
            *plane_refs,
        )

    @staticmethod
    def scratch(g, block, dtype):
        rows, width = block
        half = (rows // 2, width)
        return line_scratch(g.shards, block, dtype) + PlaneScatter.scratch(g, g.shards, block, (half, half), dtype)

    @staticmethod
    def sends(g):
        return PlaneScatter.sends(g, g.shards) + 2 * g.shards

    def load(self):
        self.plane.load(self.g.shards)

    def to_partner(self):
        for turn in range(self.g.shards):
            self.plane.to_partner(turn)

    def step(self, turn):
        n = self.g.shards
        if turn < n:
            self.plane.a(turn)
        if 0 <= turn - 1 < n:
            self.plane.b(turn - 1)
        if 0 <= turn - 2 < n:
            t = turn - 2
            self.plane.c(t)
            send_line(self.g, self.s, self.order[t], self.plane.mine(t), self.out_ref, *self.lines, last=t == n - 1)


def attend_back_kernel(reps, shards, heads, *refs):
    (
        ga_ref, qkv_ref, wo_ref, qg_ref, kg_ref, cos_ref, sin_ref, bias_ref, p_ref,
        gas_ref, gqkv_ref, qsum_ref, ksum_ref, out_ref,
        gm, zr, sems, keep_sem, *scatter_refs,
    ) = refs
    g = Grid(reps, shards).here()
    s = Sends(sems)
    n = g.shards
    scatter = ScatterAll(g, s, p_ref, out_ref, *scatter_refs)
    scatter.load()
    keep = pltpu.make_async_copy(ga_ref, gas_ref.at[g.z], keep_sem.at[0])
    keep.start()
    qsum_ref[...] = jnp.zeros(qsum_ref.shape, f32)
    ksum_ref[...] = jnp.zeros(ksum_ref.shape, f32)
    greet_all(g)
    order = g.nearest()

    def line(turn):
        zp = order[turn]
        dst = gas_ref.at[zp]
        if turn:
            s.arrived(dst, zr.at[zp], g.device(g.r, zp))
        pass_along(g, s, zp, dst if turn else ga_ref, dst, zr)

    line(0)
    scatter.to_partner()
    keep.wait()
    for turn in range(n):
        scatter.step(turn)
        if turn + 1 < n:
            line(turn + 1)
        attend_back_block(
            order[turn], heads, gas_ref, qkv_ref, wo_ref, qg_ref, kg_ref, cos_ref, sin_ref, bias_ref,
            gm, gqkv_ref, qsum_ref, ksum_ref,
        )
    scatter.step(n)
    scatter.step(n + 1)
    s.drain()


def attend_back(reps, shards, heads, ga, qkv, wo, qg, kg, cosine, sine, bias, p, ident):
    g = Grid(reps, shards)
    dma, v = pltpu.SemaphoreType.DMA, pltpu.VMEM
    n = shards
    rows, width = ga.shape
    out_width = p.shape[2]
    row = jax.ShapeDtypeStruct(qg.shape, f32)
    return pl.pallas_call(
        functools.partial(attend_back_kernel, reps, shards, heads),
        out_shape=(
            jax.ShapeDtypeStruct((n, rows, width), bf16),
            jax.ShapeDtypeStruct(qkv.shape, bf16),
            row,
            row,
            jax.ShapeDtypeStruct((rows, out_width), f32),
        ),
        in_specs=[vmem] * 8 + [hbm],
        out_specs=(vmem,) * 5,
        scratch_shapes=[v((rows, wo.shape[0]), bf16), dma((n,)), dma((ScatterAll.sends(g) + 2 * n,)), dma((1,))]
        + ScatterAll.scratch(g, (rows, out_width), p.dtype),
        compiler_params=params(ident),
        name="attend_back",
    )(ga, qkv, wo, qg, kg, cosine, sine, bias, p.reshape(g.places, 2, n, rows, out_width))


def tables_of(segment_column, segment_row, frequency):
    length = segment_row.shape[1]
    rows = lax.broadcasted_iota(jnp.int32, (length, length), 0).astype(f32)
    columns = lax.broadcasted_iota(jnp.int32, (length, length), 1).astype(f32)
    same = segment_column == segment_row
    first = jnp.min(jnp.where(same, columns, float(length)), axis=1, keepdims=True)
    width = frequency.shape[1]
    place = lax.broadcasted_iota(jnp.int32, (length, width), 0).astype(f32)
    angle = (place - first) * frequency
    second_half = lax.broadcasted_iota(jnp.int32, (length, width), 1) >= width // 2
    sine = jnp.sin(angle)
    bias = jnp.where(same & (columns <= rows), 0.0, masked_score)
    return jnp.cos(angle), jnp.where(second_half, sine, -sine), bias


def front_kernel(reps, shards, heads, layout, *refs):
    (
        x_ref, cot_ref, small_ref, freq_ref, wq_ref, wk_ref, wv_ref, wo_in,
        smalls_ref, gains_ref, qk_ref, cos_ref, sin_ref, bias_ref, out_ref,
        xs_out, w_out, hid_out, qkv_out, att_out, cots_ref,
        xs_ref, w_ref, wo_ref, hid_ref, qkv_ref, att_ref, own, rl, rr, sl, sr,
        sems, xr, mr, wr, ls, out_sems, lr, hr, dr, cr, *gather_sems,
    ) = refs
    g = Grid(reps, shards).here()
    s = Sends(sems)
    n = g.shards
    q_cols, kv_cols, kv_heads, experts = layout
    head_dim = heads[2]
    deep = wq_ref.shape[0]
    piece = deep // g.reps
    cols = q_cols + 2 * kv_cols
    first = cols // 2 // 128 * 128
    spans = {0: pl.ds(0, first), 1: pl.ds(first, cols - first), None: pl.ds(0, cols)}
    mine = pl.ds(pl.multiple_of(g.r * piece, piece), piece)

    def view(u, hi, lo, core, part):
        row = pl.multiple_of(u * deep + g.rep_of(hi, lo, core) * piece, piece)
        return w_ref.at[pl.ds(row, piece), spans[part]]

    def pieces(zp, u):
        row = pl.ds(pl.multiple_of(u * deep + g.r * piece, piece), piece)
        at_q = pl.ds(pl.multiple_of(zp * q_cols, 128), q_cols)
        at_kv = pl.ds(pl.multiple_of(zp * kv_heads // n * head_dim, 128), kv_cols)
        return (
            (wq_ref.at[mine, at_q], w_ref.at[row, pl.ds(0, q_cols)]),
            (wk_ref.at[mine, at_kv], w_ref.at[row, pl.ds(q_cols, kv_cols)]),
            (wv_ref.at[mine, at_kv], w_ref.at[row, pl.ds(q_cols + kv_cols, kv_cols)]),
        )

    plane = PlaneGather(g, s, view, lr, hr, dr, cr)
    gather = GatherAll(g, s, cot_ref, cots_ref, gather_sems[0], gather_sems[1:])
    locals_ = [pltpu.make_async_copy(src, dst, ls.at[i]) for i, (src, dst) in enumerate(pieces(g.z, g.z))]
    keeps = [
        pltpu.make_async_copy(x_ref, xs_ref.at[g.z], ls.at[3]),
        pltpu.make_async_copy(small_ref, smalls_ref.at[g.z], ls.at[4]),
        pltpu.make_async_copy(wo_in, wo_ref, ls.at[5]),
        pltpu.make_async_copy(cot_ref, gather.own(), ls.at[6]),
    ]
    for copy in locals_ + keeps:
        copy.start()
    barrier = pltpu.get_barrier_semaphore()
    peers = [g.device(g.r, (g.z + step) % n) for step in range(1, n)]
    peers += [g.device(g.rep_of(g.hi, g.other_lo(step), g.core), g.z) for step in range(1, g.los)]
    peers += [g.device(g.rep_of(1 - g.hi, g.lo, g.core), g.z), g.device(g.rep_of(g.hi, g.lo, 1 - g.core), g.z)]
    for peer in peers:
        pl.semaphore_signal(barrier, inc=1, device_id=peer, device_id_type=pl.DeviceIdType.MESH)
    pl.semaphore_wait(barrier, len(peers))

    order = g.nearest()

    def unit(step):
        return (g.z + n - step) % n

    def line(turn):
        zp = order[turn]
        if turn:
            s.arrived(smalls_ref.at[zp], mr.at[zp], g.device(g.r, zp))
        pass_along(g, s, zp, smalls_ref.at[zp] if turn else small_ref, smalls_ref.at[zp], mr)
        if turn:
            s.arrived(xs_ref.at[zp], xr.at[zp], g.device(g.r, zp))
        pass_along(g, s, zp, xs_ref.at[zp] if turn else x_ref, xs_ref.at[zp], xr)

    for step in range(1, n):
        zp = (g.z + step) % n
        for i, (src, dst) in enumerate(pieces(zp, g.z)):
            s.start(src, dst, wr.at[step, i], g.device(g.r, zp))
    line(0)
    for copy in locals_:
        copy.wait()
    plane.own(g.z)
    for step in range(1, n):
        u = unit(step)
        for i, (_, dst) in enumerate(pieces(g.z, u)):
            s.arrived(dst, wr.at[step, i], g.device(g.r, u))
        plane.own(u)
    gather.plane.own(g.z, lambda part: cot_ref.at[gather.spans[part]])
    line(1)
    for step in range(n):
        plane.first(unit(step))
        if step:
            plane.second(unit(step - 1))
        if 2 + step < n:
            line(2 + step)
        if step == max(0, n - 3):
            pass_along(g, s, g.z, cot_ref, gather.own(), gather.zr)
    plane.second(unit(n - 1))
    for step in range(n):
        plane.from_partner(unit(step))
    for copy in keeps[:3]:
        copy.wait()

    outs = [pltpu.make_async_copy(w_ref, w_out, out_sems.at[0]), pltpu.make_async_copy(xs_ref, xs_out, out_sems.at[1])]
    for copy in outs:
        copy.start()
    length = x_ref.shape[0]
    for zp in range(n):
        rows = smalls_ref[zp].astype(f32)
        gains_ref[:, zp * deep : (zp + 1) * deep] = rows.T[experts : experts + 8]
    for i in range(2):
        qk_ref[i : i + 1] = sum(gains_ref[2 + i : 3 + i, zp * deep : zp * deep + head_dim] for zp in range(n))

    def compute(turn):
        zp = order[turn]
        column = smalls_ref[zp, 0:length, experts + 4 : experts + 5].astype(f32)
        row = gains_ref[4:5, pl.ds(pl.multiple_of(zp * deep, 128), length)]
        cos_ref[zp], sin_ref[zp], bias_ref[zp] = tables_of(column, row, freq_ref[...])
        attend_block(
            zp, heads, xs_ref, w_ref, wo_ref, gains_ref.at[0:1], qk_ref.at[0:1], qk_ref.at[1:2],
            cos_ref, sin_ref, bias_ref, hid_ref, qkv_ref, att_ref, own.at[turn],
        )

    def sums(turn):
        send_line(g, s, order[turn], own.at[turn], out_ref, rl, rr, sl, sr, last=turn == 0)

    compute(n - 1)
    sums(n - 1)
    gather.first(0)
    gather.line(1)
    for turn in range(n - 2, -1, -1):
        compute(turn)
        at = n - 1 - turn
        if turn > 0:
            sums(turn)
            gather.second(at - 1)
            gather.first(at)
            if at + 1 < n:
                gather.line(at + 1)
    late = [
        pltpu.make_async_copy(hid_ref, hid_out, out_sems.at[2]),
        pltpu.make_async_copy(qkv_ref, qkv_out, out_sems.at[3]),
        pltpu.make_async_copy(att_ref, att_out, out_sems.at[4]),
    ]
    for copy in late:
        copy.start()
    gather.second(n - 2)
    gather.first(n - 1)
    gather.second(n - 1)
    sums(0)
    gather.finish()
    for copy in outs + late + keeps[3:]:
        copy.wait()
    s.drain()


def front(reps, shards, heads, layout, x, cot, small, frequency, wq, wk, wv, wo, ident):
    g = Grid(reps, shards)
    dma, v = pltpu.SemaphoreType.DMA, pltpu.VMEM
    n = shards
    rows, width = x.shape
    head_dim = heads[2]
    cols = layout[0] + 2 * layout[1]
    table = jax.ShapeDtypeStruct((n, rows, head_dim), f32)
    lines = (n, rows, width)
    return pl.pallas_call(
        functools.partial(front_kernel, reps, shards, heads, layout),
        out_shape=(
            jax.ShapeDtypeStruct((n,) + small.shape, bf16),
            jax.ShapeDtypeStruct((8, width), f32),
            jax.ShapeDtypeStruct((8, head_dim), f32),
            table,
            table,
            jax.ShapeDtypeStruct((n, rows, rows), f32),
            jax.ShapeDtypeStruct((rows, width), f32),
            jax.ShapeDtypeStruct(lines, bf16),
            jax.ShapeDtypeStruct((width, cols), bf16),
            jax.ShapeDtypeStruct(lines, bf16),
            jax.ShapeDtypeStruct((n, rows, cols), f32),
            jax.ShapeDtypeStruct((n, rows, wo.shape[0]), bf16),
            jax.ShapeDtypeStruct((g.devices, rows, width), bf16),
        ),
        in_specs=[vmem] * 4 + [hbm] * 4,
        out_specs=(vmem,) * 7 + (hbm,) * 6,
        scratch_shapes=[
            v(lines, bf16),
            v((width, cols), bf16),
            v(wo.shape, bf16),
            v(lines, bf16),
            v((n, rows, cols), f32),
            v((n, rows, wo.shape[0]), bf16),
            v(lines, bf16),
        ]
        + line_scratch(n, (rows, width), bf16)
        + [
            dma((PlaneGather.sends(g, n) + GatherAll.sends(g) + 9 * n,)),
            dma((n,)),
            dma((n,)),
            dma((n, 3)),
            dma((7,)),
            dma((5,)),
        ]
        + PlaneGather.scratch(g, n)
        + GatherAll.scratch(g),
        compiler_params=params(ident),
        name="front",
    )(x, cot, small, frequency, wq, wk, wv, wo)


def slots_of(slab, capacity):
    length = slab.shape[1]
    member = slab >= 0.0
    earlier = lax.broadcasted_iota(jnp.int32, (length, length), 0) < lax.broadcasted_iota(jnp.int32, (length, length), 1)
    ones = jnp.where(member, 1.0, 0.0).astype(bf16)
    slot = jnp.dot(ones, jnp.where(earlier, 1.0, 0.0).astype(bf16), preferred_element_type=f32)
    slot = jnp.where(member, slot, -1.0)[0:1]
    rows = lax.broadcasted_iota(jnp.int32, (capacity, length), 0).astype(f32)
    return jnp.where(rows == slot, 1.0, 0.0), slab[0:1]


def experts_kernel(reps, shards, capacity, held, *refs):
    (
        x_ref, slab_ref, cots_ref, wg_ref, wu_ref, wd_ref,
        back_ref, sums_ref, grads_ref, rows_ref, cs_ref, gg_ref, gu_ref, act_ref, all_ref,
        slabs, cot_buf, hid_buf, d_ref, x_buf, c_buf, gg_buf, gu_buf, act_buf, sum_buf, grad_buf,
        sems, ps, pr, ls, cot_sem, hid_sem, out_sems, zr, *plane_sems,
    ) = refs
    g = Grid(reps, shards).here()
    s = Sends(sems)
    n, places = g.shards, g.places
    length = x_ref.shape[0]
    hidden = hid_buf if held else all_ref
    s.samples = [x_ref, x_ref.at[pl.ds(0, length // 2)]]
    gather = GatherAll(g, s, x_ref, hidden, zr, plane_sems)
    order = gather.order
    groups = 2 * n

    def which(k):
        return jnp.where(k % 2 == 0, g.core, 1 - g.core), pick(k // 2, order)

    def cot_load(k, slot):
        core, zp = which(k)
        return pltpu.make_async_copy(cots_ref.at[:, core, zp], cot_buf.at[slot], cot_sem.at[slot])

    def onehots(k):
        core, zp = which(k)
        return [slots_of(slabs[(q * 2 + core) * n + zp], capacity) for q in range(places)]

    keep = pltpu.make_async_copy(x_ref, gather.own(), ls.at[0])
    keep.start()
    cot_load(0, 0).start()
    greet_all(g)
    push_rows(g, slab_ref, slabs, ps, pr)
    me = g.r * n + g.z
    keep_slab = pltpu.make_async_copy(slab_ref.at[me], slabs.at[me], ls.at[1])
    keep_slab.start()
    gather.line(0)
    keep_slab.wait()
    push_wait(g, slab_ref, slabs, ps, pr)
    keep.wait()

    def turns(k, steps):
        for at, step in steps:
            pl.when(k == at)(step)

    def both(*fs):
        def run():
            for f, turn in fs:
                f(turn)

        return run

    early = [(2, both((gather.first, 0))), (3, both((gather.line, 1))), (5, both((gather.second, 0)))]
    if n > 2:
        early.append((7, both((gather.line, 2))))

    def outs(k):
        return [
            pltpu.make_async_copy(x_buf, rows_ref.at[k], out_sems.at[0]),
            pltpu.make_async_copy(gg_buf, gg_ref.at[k], out_sems.at[1]),
            pltpu.make_async_copy(gu_buf, gu_ref.at[k], out_sems.at[2]),
            pltpu.make_async_copy(act_buf, act_ref.at[k], out_sems.at[3]),
        ]

    def blocks_out(k):
        core, zp = which(k)
        return [
            pltpu.make_async_copy(sum_buf, sums_ref.at[:, core, zp], out_sems.at[4]),
            pltpu.make_async_copy(grad_buf, grads_ref.at[:, core, zp], out_sems.at[5]),
        ]

    def c_out(k):
        return pltpu.make_async_copy(c_buf, cs_ref.at[k], out_sems.at[6])

    def backward_input(k, carry):
        turns(k, early)
        slot = k % 2
        pl.when(k + 1 < groups)(lambda: cot_load(k + 1, 1 - slot).start())
        cot_load(k, slot).wait()
        pl.when(k > 0)(lambda: c_out(k).wait())
        for q, (onehot, _) in enumerate(onehots(k)):
            taken = jnp.dot(onehot.astype(bf16), cot_buf[slot, q], preferred_element_type=f32)
            c_buf[q * capacity : (q + 1) * capacity, :] = taken.astype(bf16)
        c_out(k).start()
        d_ref[k] = dot_t(c_buf[...], wd_ref[...])
        return carry

    lax.fori_loop(0, groups, backward_input, 0)
    c_out(0).wait()

    def partner(turn):
        gather.plane.from_partner(order[turn])

    late = [(0, both((gather.first, 1)))]
    for turn in range(n):
        if 0 < turn < n - 1:
            late.append((2 * turn, both((gather.second, turn))))
        steps = [(partner, turn)]
        if turn + 3 < n:
            steps.append((gather.line, turn + 3))
        if turn + 2 < n:
            steps.append((gather.first, turn + 2))
        if turn == n - 2:
            steps.append((gather.second, n - 1))
        late.append((2 * turn + 1, both(*steps)))

    def expert(k, carry):
        turns(k, late)
        core, zp = which(k)
        if not held:
            fetch = pltpu.make_async_copy(all_ref.at[pl.ds(0, places)], hid_buf, hid_sem.at[0])
            for q in range(places):
                pltpu.make_async_copy(all_ref.at[(q * 2 + core) * n + zp], hid_buf.at[q], hid_sem.at[0]).start()
            fetch.wait()
        hots = onehots(k)
        pl.when(k > 0)(functools.partial(wait_for, outs, k))
        for q, (onehot, _) in enumerate(hots):
            block = hid_buf[(q * 2 + core) * n + zp] if held else hid_buf[q]
            taken = jnp.dot(onehot.astype(bf16), block, preferred_element_type=f32)
            x_buf[q * capacity : (q + 1) * capacity, :] = taken.astype(bf16)
        weight = jnp.concatenate(
            [jnp.sum(onehot * share, axis=1, keepdims=True) for onehot, share in hots], axis=0
        )
        gate = jnp.dot(x_buf[...], wg_ref[...], preferred_element_type=f32)
        up = jnp.dot(x_buf[...], wu_ref[...], preferred_element_type=f32)
        sigmoid = 1.0 / (1.0 + jnp.exp(-gate))
        silu = gate * sigmoid
        activated = silu * up
        grad = d_ref[k]
        row_mix = jnp.sum(activated * grad, axis=1, keepdims=True)
        grad = grad * weight
        act_buf[...] = (activated * weight).astype(bf16)
        gg_buf[...] = (grad * up * sigmoid * (1.0 + gate * (1.0 - sigmoid))).astype(bf16)
        gu_buf[...] = (grad * silu).astype(bf16)
        for copy in outs(k):
            copy.start()
        for q, (onehot, _) in enumerate(hots):
            back = jnp.sum(onehot * row_mix[q * capacity : (q + 1) * capacity], axis=0, keepdims=True)
            back_ref[(q * 2 + core) * n + zp] = jnp.broadcast_to(back, slab_ref.shape[1:])
        produced = jnp.dot(act_buf[...], wd_ref[...], preferred_element_type=f32).astype(bf16)
        pl.when(k > 0)(functools.partial(wait_for, blocks_out, k))
        for q, (onehot, _) in enumerate(hots):
            part = produced[q * capacity : (q + 1) * capacity]
            sum_buf[q] = t_dot(onehot.astype(bf16), part).astype(bf16)
        grad_in = (dot_t(gg_buf[...], wg_ref[...]) + dot_t(gu_buf[...], wu_ref[...])).astype(bf16)
        for q, (onehot, _) in enumerate(hots):
            part = grad_in[q * capacity : (q + 1) * capacity]
            grad_buf[q] = t_dot(onehot.astype(bf16), part).astype(bf16)
        for copy in blocks_out(k):
            copy.start()
        return carry

    lax.fori_loop(0, groups, expert, 0)
    for copy in outs(0) + blocks_out(0):
        copy.wait()
    s.drain()


def experts_all(reps, shards, capacity, x, slab, cots, wg, wu, wd, ident):
    g = Grid(reps, shards)
    dma, v = pltpu.SemaphoreType.DMA, pltpu.VMEM
    n, places = shards, g.places
    length, width = x.shape
    inner = wg.shape[1]
    rows = places * capacity
    held = g.devices <= 32
    blocks = jax.ShapeDtypeStruct((places, 2, n, length, width), bf16)
    wide = jax.ShapeDtypeStruct((2 * n, rows, width), bf16)
    narrow = jax.ShapeDtypeStruct((2 * n, rows, inner), bf16)
    gathered = (g.devices, length, width)
    return pl.pallas_call(
        functools.partial(experts_kernel, reps, shards, capacity, held),
        out_shape=(
            jax.ShapeDtypeStruct(slab.shape, f32),
            blocks,
            blocks,
            wide,
            wide,
            narrow,
            narrow,
            narrow,
            jax.ShapeDtypeStruct((1, 16, 128) if held else gathered, bf16),
        ),
        in_specs=[vmem, vmem, hbm, vmem, vmem, vmem],
        out_specs=(vmem,) + (hbm,) * 8,
        scratch_shapes=[
            v(slab.shape, f32),
            v((2, places, length, width), bf16),
            v(gathered if held else (places, length, width), bf16),
            v((2 * n, rows, inner), f32),
            v((rows, width), bf16),
            v((rows, width), bf16),
            v((rows, inner), bf16),
            v((rows, inner), bf16),
            v((rows, inner), bf16),
            v((places, length, width), bf16),
            v((places, length, width), bf16),
            dma((GatherAll.sends(g),)),
            dma((g.devices,)),
            dma((g.devices,)),
            dma((2,)),
            dma((2,)),
            dma((1,)),
            dma((7,)),
        ]
        + GatherAll.scratch(g),
        compiler_params=params(ident),
        name="experts_all",
    )(x, slab, cots.reshape(places, 2, n, length, width), wg, wu, wd)[:-1]


def inverse_rms(values):
    return lax.rsqrt(jnp.mean(values * values, axis=-1, keepdims=True) + epsilon)


def norm_back(grad_scaled, unit, inverse, gain):
    gained = grad_scaled * gain
    return inverse * (gained - unit * jnp.mean(gained * unit, axis=-1, keepdims=True))


def matmul(a, b, dims=((1,), (0,))):
    return lax.dot_general(a, b, (dims, ((), ())), preferred_element_type=f32)


def local(
    tokens,
    segments,
    routes,
    attn_gain,
    w_query,
    key_weight,
    value_weight,
    w_out,
    query_gain,
    key_gain,
    ffn_gain,
    w_router,
    w_gate,
    w_up,
    w_down,
    cotangent,
):
    reps, shards = lax.axis_size("rep"), lax.axis_size("shard")
    devices = reps * shards
    r, z = lax.axis_index("rep"), lax.axis_index("shard")
    length, width = tokens.shape
    deep = w_query.shape[0]
    head_dim = query_gain.shape[0] * shards
    heads = w_query.shape[1] // head_dim
    kv_heads = key_weight.shape[1] // head_dim
    experts = w_router.shape[1]
    top = routes.shape[1]
    capacity = 2 * length * top // experts
    my_heads = heads // shards
    my_kv = max(1, kv_heads // shards)
    shared_by = max(1, shards // kv_heads)
    q_cols, kv_cols = my_heads * head_dim, my_kv * head_dim
    cols = q_cols + 2 * kv_cols
    piece = deep // reps
    chunks = max(1, devices // 32)
    part = head_dim // shards

    def column(values, rows=deep):
        return jnp.pad(values.reshape(-1, 1), ((0, rows - values.size), (0, 0)))

    spot = lax.broadcasted_iota(jnp.int32, (deep, 1), 0) // part == z

    def spotted(values):
        return jnp.where(spot, jnp.tile(column(values, part), (deep // part, 1)), 0)

    small = jnp.concatenate(
        [
            w_router,
            column(attn_gain),
            column(ffn_gain),
            spotted(query_gain),
            spotted(key_gain),
            column(segments[0].astype(bf16)),
        ],
        axis=1,
    )
    small_cols = -(-(experts + 8) // 128) * 128
    small = jnp.pad(small, ((0, 0), (0, small_cols - small.shape[1])))
    half = rope_base ** (-2.0 * jnp.arange(head_dim // 2, dtype=f32) / head_dim)
    frequency = jnp.concatenate([half, half]).reshape(1, head_dim)
    head_sizes = (my_heads, my_kv, head_dim)
    layout = (q_cols, kv_cols, kv_heads, experts)
    (
        small_all, gains, qk_gains, cosine, sine, bias, mixed,
        block_tokens, w_in, hidden_in, qkv, attn_out, cotangents,
    ) = front(
        reps, shards, head_sizes, layout, tokens, cotangent, small, frequency,
        w_query, key_weight, value_weight, w_out, 1,
    )
    router_full = small_all[:, :, :experts].reshape(width, experts)
    gain_one, gain_two = gains[0:1], gains[1:2]
    qgain, kgain = qk_gains[0:1], qk_gains[1:2]
    own_tokens = tokens.astype(f32)
    resid = own_tokens + mixed

    inverse_two = inverse_rms(resid)
    normed_two = resid * inverse_two
    hidden_two = (normed_two * gain_two).astype(bf16)
    logits = matmul(hidden_two, router_full)
    gate_probs = jax.nn.softmax(logits, axis=-1)
    chosen = jnp.any(routes[:, :, None] == jnp.arange(experts, dtype=jnp.int32)[None, None, :], axis=1)
    picked = jnp.where(chosen, gate_probs, 0.0)
    picked_total = jnp.sum(picked, axis=-1, keepdims=True)
    mix = picked / picked_total
    slab = jnp.where(chosen, mix, -1.0).T.reshape(experts, 1, length)
    slab = jnp.broadcast_to(slab, (experts, 8, length))
    back_mix, sums, grad_sums, rows, row_grads, grad_gate, grad_up, activated = experts_all(
        reps, shards, capacity, hidden_two, slab, cotangents, w_gate[0], w_up[0], w_down[0], 4
    )
    sums = sums.reshape(devices, length, width)
    grad_sums = grad_sums.reshape(devices, length, width)
    rows, row_grads = rows.reshape(-1, width), row_grads.reshape(-1, width)
    fill = (rows, row_grads) + tuple(a.reshape(rows.shape[0], -1) for a in (grad_gate, grad_up, activated))
    grad_hidden, mixes, grad_w_gate, grad_w_up, grad_w_down = scatter_wide(
        reps, shards, grad_sums, back_mix, fill, 8, chunks
    )

    grad_out = cotangent.astype(f32)
    grad_mix = mixes[:, 0, :].T
    grad_picked = jnp.where(chosen, grad_mix - jnp.sum(grad_mix * mix, axis=-1, keepdims=True), 0.0) / picked_total
    grad_logits = (gate_probs * (grad_picked - jnp.sum(grad_picked * picked, axis=-1, keepdims=True))).astype(bf16)
    grad_hidden = grad_hidden + matmul(grad_logits, router_full, ((1,), (1,)))
    grad_ffn_gain = jnp.sum(grad_hidden * normed_two, axis=0)
    grad_resid = grad_out + norm_back(grad_hidden, normed_two, inverse_two, gain_two)
    grad_w_router = matmul(hidden_two, grad_logits, ((0,), (0,)))

    fused = width // chunks
    grad_attn, grad_qkv, grad_query_gain, grad_key_gain, moe = attend_back(
        reps, shards, head_sizes, grad_resid.astype(bf16), qkv, w_out, qgain, kgain, cosine, sine, bias,
        sums[:, :, :fused], 5,
    )
    if chunks > 1:
        rest = scatter_wide(reps, shards, sums[:, :, fused:], None, None, 16, chunks - 1)
        moe = jnp.concatenate([moe, rest], axis=1)
    output = (resid + moe).astype(bf16)
    grad_attn = grad_attn.reshape(shards * length, width)
    grad_qkv = grad_qkv.reshape(shards * length, cols)
    grad_w_out = matmul(attn_out.reshape(shards * length, q_cols), grad_attn, ((0,), (0,)))
    owned_out = lax.psum(grad_w_out.astype(bf16), "rep").astype(f32)
    hidden_in = hidden_in.reshape(shards * length, width)
    _, normed_one = unit_of(block_tokens.reshape(shards * length, width).astype(f32))
    grad_part = matmul(grad_qkv, w_in, ((1,), (1,)))
    grad_attn_gain = jnp.sum(grad_part * normed_one, axis=0)
    grad_w_in = matmul(hidden_in, grad_qkv, ((0,), (0,)))

    def spread(values):
        return jnp.pad(values.reshape(shards, part), ((0, 0), (0, deep - part))).reshape(width, 1)

    small_grads = jnp.concatenate(
        [
            grad_w_router,
            grad_attn_gain.reshape(width, 1),
            grad_ffn_gain.reshape(width, 1),
            spread(grad_query_gain),
            spread(grad_key_gain),
        ],
        axis=1,
    )
    small_grads = jnp.pad(small_grads, ((0, 0), (0, small_cols - small_grads.shape[1])))
    sent = jnp.concatenate([grad_w_in, small_grads], axis=1).astype(bf16)
    sent = sent.reshape(shards, reps, piece, cols + small_cols)
    grad_part = grad_part.astype(bf16).reshape(shards, length, width)
    grad_hidden_in, sent = deliver(reps, shards, grad_part, sent, 6)
    sent = sent.reshape(shards, deep, cols + small_cols)
    own_inverse = inverse_rms(own_tokens)
    own_normed = own_tokens * own_inverse
    grad_tokens = grad_resid + norm_back(grad_hidden_in, own_normed, own_inverse, gain_one)

    def joined(values):
        if shared_by > 1:
            values = values.astype(f32).reshape(-1, shared_by, deep, values.shape[-1]).sum(axis=1)
        return values.transpose(1, 0, 2).reshape(deep, -1).astype(f32)

    owned_small = jnp.sum(sent[:, :, cols:].astype(f32), axis=0)
    return (
        output,
        grad_tokens,
        owned_small[:, experts],
        sent[:, :, :q_cols].transpose(1, 0, 2).reshape(deep, -1).astype(f32),
        joined(sent[:, :, q_cols : q_cols + kv_cols]),
        joined(sent[:, :, q_cols + kv_cols : cols]),
        owned_out,
        owned_small[:part, experts + 2],
        owned_small[:part, experts + 3],
        owned_small[:, experts + 1],
        owned_small[:, :experts],
        grad_w_gate[None],
        grad_w_up[None],
        grad_w_down[None],
    )


def solution(mesh):
    split = P(("rep", "shard"))
    row = P("shard")
    return jax.shard_map(
        local,
        mesh=mesh,
        in_specs=(split,) * 3 + (row,) * 9 + (split,) * 4,
        out_specs=(split,) * 2 + (row,) * 9 + (split,) * 3,
        check_vma=False,
    )
```

```python
import functools
import jax
import jax.numpy as jnp
from jax import lax
from jax.experimental import pallas as pl
from jax.experimental.pallas import tpu as pltpu
from jax.sharding import PartitionSpec as P

bf16 = jnp.bfloat16
f32 = jnp.float32
vmem_cap = 62 * 1024 * 1024
epsilon = 1e-06
rope_base = 1000000.0
masked_score = -1e30


class Grid:
    def __init__(self, reps, shards):
        self.reps, self.shards = reps, shards
        self.devices = reps * shards
        self.places = reps // 2
        self.los = self.places // 2

    def here(self):
        self.r = lax.axis_index("rep")
        self.z = lax.axis_index("shard")
        self.core = self.r % 2
        place = self.r // 2
        self.hi = place // self.los
        self.lo = place % self.los
        return self

    def rep_of(self, hi, lo, core):
        return (hi * self.los + lo) * 2 + core

    def device(self, rep, shard):
        return {"rep": rep, "shard": shard}

    def other_lo(self, step):
        return (self.lo + step) % self.los

    def nearest(self):
        n = self.shards
        rows = [sorted(range(n), key=lambda p: (abs(p - z), p)) for z in range(n)]
        return [pick(self.z, [rows[z][turn] for z in range(n)]) for turn in range(n)]


def pick(index, values):
    out = jnp.int32(values[0])
    for i in range(1, len(values)):
        out = jnp.where(index == i, jnp.int32(values[i]), out)
    return out


class Sends:
    def __init__(self, sems):
        self.sems, self.used, self.open, self.samples = sems, 0, [], []

    def copy(self, src, dst, sem, recv, device):
        return pltpu.make_async_remote_copy(
            src_ref=src,
            dst_ref=dst,
            send_sem=self.sems.at[sem],
            recv_sem=recv,
            device_id=device,
            device_id_type=pl.DeviceIdType.MESH,
        )

    def start(self, src, dst, recv, device, when=None):
        copy = self.copy(src, dst, self.used, recv, device)
        sample = src
        for other in self.samples:
            if other.shape == src.shape:
                sample = other
        self.open.append((self.used, sample, when))
        self.used += 1
        if when is None:
            copy.start()
        else:
            pl.when(when())(copy.start)

    def arrived(self, dst, recv, device, when=None):
        copy = self.copy(dst, dst, 0, recv, device)
        if when is None:
            copy.wait_recv()
        else:
            pl.when(when())(copy.wait_recv)

    def drain(self):
        here = {"rep": lax.axis_index("rep"), "shard": lax.axis_index("shard")}
        for sem, sample, when in self.open:
            copy = self.copy(sample, sample, sem, self.sems.at[sem], here)
            if when is None:
                copy.wait_send()
            else:
                pl.when(when())(copy.wait_send)
        self.open = []


def greet_all(g):
    barrier = pltpu.get_barrier_semaphore()
    me = g.r * g.shards + g.z

    def one(step, carry):
        peer = (me + step) % g.devices
        pl.semaphore_signal(
            barrier,
            inc=1,
            device_id=g.device(peer // g.shards, peer % g.shards),
            device_id_type=pl.DeviceIdType.MESH,
        )
        return carry

    lax.fori_loop(1, g.devices, one, 0)
    pl.semaphore_wait(barrier, g.devices - 1)


def push_rows(g, src, dst, send_sems, recv_sems):
    me = g.r * g.shards + g.z

    def one(step, carry):
        peer = (me + step) % g.devices
        pltpu.make_async_remote_copy(
            src_ref=src.at[peer],
            dst_ref=dst.at[me],
            send_sem=send_sems.at[step],
            recv_sem=recv_sems.at[step],
            device_id=g.device(peer // g.shards, peer % g.shards),
            device_id_type=pl.DeviceIdType.MESH,
        ).start()
        return carry

    lax.fori_loop(1, g.devices, one, 0)


def push_wait(g, src, dst, send_sems, recv_sems):
    me = g.r * g.shards + g.z

    def one(step, carry):
        peer = (me + g.devices - step) % g.devices
        copy = pltpu.make_async_remote_copy(
            src_ref=src.at[peer],
            dst_ref=dst.at[peer],
            send_sem=send_sems.at[step],
            recv_sem=recv_sems.at[step],
            device_id=g.device(peer // g.shards, peer % g.shards),
            device_id_type=pl.DeviceIdType.MESH,
        )
        copy.wait_send()
        copy.wait_recv()
        return carry

    lax.fori_loop(1, g.devices, one, 0)


class PlaneGather:
    def __init__(self, g, s, view, lr, hr, dr, cr):
        self.g, self.s, self.view = g, s, view
        self.lr, self.hr, self.dr, self.cr = lr, hr, dr, cr

    @staticmethod
    def scratch(g, units):
        dma, others = pltpu.SemaphoreType.DMA, max(1, g.los - 1)
        return [dma((units, 2, others)), dma((units, 2)), dma((units, 2, others)), dma((units, 5 * g.los))]

    @staticmethod
    def sends(g, units):
        return 9 * g.los * units

    def at(self, hi, lo):
        return self.g.device(self.g.rep_of(hi, lo, self.g.core), self.g.z)

    def partner(self):
        g = self.g
        return g.device(g.rep_of(g.hi, g.lo, 1 - g.core), g.z)

    def own(self, u, src=None):
        g, s = self.g, self.s

        def dst(part):
            return self.view(u, g.hi, g.lo, g.core, part)

        src = src or dst
        for part in (0, 1):
            for step in range(1, g.los):
                s.start(src(part), dst(part), self.lr.at[u, part, step - 1], self.at(g.hi, g.other_lo(step)))
            s.start(src(1 - part), dst(1 - part), self.hr.at[u, 1 - part], self.at(1 - g.hi, g.lo))
        s.start(src(None), dst(None), self.cr.at[u, 0], self.partner())

    def take(self, u, hi, lo, part, recv, frm, partner_slot, onward=()):
        ref = self.view(u, hi, lo, self.g.core, part)
        self.s.arrived(ref, recv, frm)
        for sem, device in onward:
            self.s.start(ref, ref, sem, device)
        self.s.start(ref, ref, self.cr.at[u, partner_slot], self.partner())

    def first(self, u):
        g = self.g
        far = 1 - g.hi
        for step in range(1, g.los):
            frm = (g.lo + g.los - step) % g.los
            onward = [(self.dr.at[u, 0, step - 1], self.at(far, g.lo))]
            self.take(u, g.hi, frm, 0, self.lr.at[u, 0, step - 1], self.at(g.hi, frm), 5 * step, onward)
        onward = [(self.dr.at[u, 1, step - 1], self.at(g.hi, g.other_lo(step))) for step in range(1, g.los)]
        self.take(u, far, g.lo, 1, self.hr.at[u, 1], self.at(far, g.lo), 1, onward)
        for step in range(1, g.los):
            frm = (g.lo + g.los - step) % g.los
            self.take(u, g.hi, frm, 1, self.lr.at[u, 1, step - 1], self.at(g.hi, frm), 5 * step + 1)
        self.take(u, far, g.lo, 0, self.hr.at[u, 0], self.at(far, g.lo), 2)

    def second(self, u):
        g = self.g
        far = 1 - g.hi
        for step in range(1, g.los):
            frm = (g.lo + g.los - step) % g.los
            self.take(u, far, frm, 0, self.dr.at[u, 0, step - 1], self.at(far, g.lo), 5 * step + 2)
            self.take(u, far, frm, 1, self.dr.at[u, 1, step - 1], self.at(g.hi, frm), 5 * step + 3)

    def from_partner(self, u):
        g = self.g
        far, other = 1 - g.hi, 1 - g.core

        def got(hi, lo, part, slot):
            self.s.arrived(self.view(u, hi, lo, other, part), self.cr.at[u, slot], self.partner())

        got(g.hi, g.lo, None, 0)
        got(far, g.lo, 1, 1)
        got(far, g.lo, 0, 2)
        for step in range(1, g.los):
            frm = (g.lo + g.los - step) % g.los
            got(g.hi, frm, 0, 5 * step)
            got(g.hi, frm, 1, 5 * step + 1)
            got(far, frm, 0, 5 * step + 2)
            got(far, frm, 1, 5 * step + 3)


def add_rows(dst, *srcs, step=16):
    def one(i, carry):
        at = pl.ds(pl.multiple_of(i * step, step), step)
        total = srcs[0][at, :].astype(f32)
        for src in srcs[1:]:
            total = total + src[at, :].astype(f32)
        dst[at, :] = total.astype(dst.dtype)
        return carry

    lax.fori_loop(0, dst.shape[0] // step, one, 0)


class PlaneScatter:
    def __init__(self, g, s, p, cut, own, ra, rb0, rb1, rc0, rc1, sa, sb0, sb1, sc0, sc1, ls):
        self.g, self.s, self.p, self.cut, self.owned = g, s, p, cut, own
        self.ra, self.rb0, self.rb1, self.rc0, self.rc1 = ra, rb0, rb1, rc0, rc1
        self.sa, self.sb0, self.sb1, self.sc0, self.sc1, self.ls = sa, sb0, sb1, sc0, sc1, ls

    @staticmethod
    def scratch(g, units, block, halves, dtype):
        dma, others, v = pltpu.SemaphoreType.DMA, max(1, g.los - 1), pltpu.VMEM
        first, second = halves
        return [
            v((units, g.places) + block, dtype),
            v((units, g.places) + block, dtype),
            v((units, g.los) + first, dtype),
            v((units, others, 2) + second, dtype),
            v((units, others) + first, dtype),
            v((units,) + second, dtype),
            dma((units,)),
            dma((units,)),
            dma((units, others, 2)),
            dma((units, others)),
            dma((units,)),
            dma((units,)),
        ]

    @staticmethod
    def sends(g, units):
        return units * (3 * g.los + 2)

    def at(self, hi, lo):
        return self.g.device(self.g.rep_of(hi, lo, self.g.core), self.g.z)

    def partner(self):
        g = self.g
        return g.device(g.rep_of(g.hi, g.lo, 1 - g.core), g.z)

    def load(self, units):
        self.loads = []
        for turn in range(units):
            load = pltpu.make_async_copy(self.p(turn, self.g.core), self.owned.at[turn], self.ls.at[turn])
            load.start()
            self.loads.append(load)

    def to_partner(self, turn):
        self.s.start(self.p(turn, 1 - self.g.core), self.ra.at[turn], self.sa.at[turn], self.partner())

    def half(self, turn, place, part):
        return self.owned.at[(turn, place) + self.cut(part)]

    def mine(self, turn):
        return self.owned.at[turn, self.g.hi * self.g.los + self.g.lo]

    def a(self, turn, waited=False):
        g, s = self.g, self.s
        far = 1 - g.hi
        if self.loads[turn] is not None:
            self.loads[turn].wait()
        if not waited:
            s.arrived(self.ra.at[turn], self.sa.at[turn], self.partner())

        def one(q, carry):
            line = self.owned.at[turn, q]
            add_rows(line, line, self.ra.at[turn, q])
            return carry

        lax.fori_loop(0, g.places, one, 0)
        block = self.owned.at[(turn, pl.ds(far * g.los, g.los)) + self.cut(0)]
        s.start(block, self.rb0.at[turn], self.sb0.at[turn], self.at(far, g.lo))
        for step in range(1, g.los):
            to = g.other_lo(step)
            for hi in range(2):
                sem = self.sb1.at[turn, step - 1, hi]
                s.start(self.half(turn, hi * g.los + to, 1), self.rb1.at[turn, step - 1, hi], sem, self.at(g.hi, to))

    def b(self, turn):
        g, s = self.g, self.s
        far = 1 - g.hi
        s.arrived(self.rb0.at[turn], self.sb0.at[turn], self.at(far, g.lo))
        for lo in range(g.los):
            line = self.half(turn, g.hi * g.los + lo, 0)
            add_rows(line, line, self.rb0.at[turn, lo])
        for step in range(1, g.los):
            to = g.other_lo(step)
            sem = self.sc0.at[turn, step - 1]
            s.start(self.half(turn, g.hi * g.los + to, 0), self.rc0.at[turn, step - 1], sem, self.at(g.hi, to))
        for step in range(1, g.los):
            frm = (g.lo + g.los - step) % g.los
            for hi in range(2):
                s.arrived(self.rb1.at[turn, step - 1, hi], self.sb1.at[turn, step - 1, hi], self.at(g.hi, frm))
        for hi in range(2):
            line = self.half(turn, hi * g.los + g.lo, 1)
            add_rows(line, line, *[self.rb1.at[turn, step, hi] for step in range(g.los - 1)])
        s.start(self.half(turn, far * g.los + g.lo, 1), self.rc1.at[turn], self.sc1.at[turn], self.at(far, g.lo))

    def c(self, turn):
        g, s = self.g, self.s
        place = g.hi * g.los + g.lo
        for step in range(1, g.los):
            frm = (g.lo + g.los - step) % g.los
            s.arrived(self.rc0.at[turn, step - 1], self.sc0.at[turn, step - 1], self.at(g.hi, frm))
        line = self.half(turn, place, 0)
        add_rows(line, line, *[self.rc0.at[turn, step] for step in range(g.los - 1)])
        s.arrived(self.rc1.at[turn], self.sc1.at[turn], self.at(1 - g.hi, g.lo))
        line = self.half(turn, place, 1)
        add_rows(line, line, self.rc1.at[turn])


def pass_along(g, s, zp, src, dst, zr):
    n = g.shards
    right, left = g.device(g.r, jnp.minimum(g.z + 1, n - 1)), g.device(g.r, jnp.maximum(g.z - 1, 0))
    s.start(src, dst, zr.at[zp], right, lambda: (zp <= g.z) & (g.z + 1 < n))
    s.start(src, dst, zr.at[zp], left, lambda: (zp >= g.z) & (g.z > 0))


def send_line(g, s, zp, line, out_ref, rl, rr, sl, sr, last):
    n = g.shards
    left, right = g.device(g.r, jnp.maximum(g.z - 1, 0)), g.device(g.r, jnp.minimum(g.z + 1, n - 1))
    has_left, has_right = g.z > 0, g.z + 1 < n
    if last:
        s.arrived(rl.at[g.z], sl.at[g.z], left, lambda: g.z > 0)
        s.arrived(rr.at[g.z], sr.at[g.z], right, lambda: g.z + 1 < n)

        @pl.when(has_left & has_right)
        def _():
            add_rows(out_ref, line, rl.at[g.z], rr.at[g.z])

        @pl.when(has_left & jnp.logical_not(has_right))
        def _():
            add_rows(out_ref, line, rl.at[g.z])

        @pl.when(has_right & jnp.logical_not(has_left))
        def _():
            add_rows(out_ref, line, rr.at[g.z])
    else:
        onward_right, onward_left = zp > g.z, zp < g.z

        @pl.when(onward_right & has_left)
        def _():
            s.arrived(rl.at[zp], sl.at[zp], left)
            add_rows(line, line, rl.at[zp])

        @pl.when(onward_left & has_right)
        def _():
            s.arrived(rr.at[zp], sr.at[zp], right)
            add_rows(line, line, rr.at[zp])

        s.start(line, rl.at[zp], sl.at[zp], right, lambda: zp > g.z)
        s.start(line, rr.at[zp], sr.at[zp], left, lambda: zp < g.z)


def line_scratch(shards, block, dtype):
    v, dma = pltpu.VMEM, pltpu.SemaphoreType.DMA
    return [v((shards,) + block, dtype), v((shards,) + block, dtype), dma((shards,)), dma((shards,))]


def wait_for(copies, k):
    for copy in copies(k):
        copy.wait()


hbm = pl.BlockSpec(memory_space=pl.ANY)
vmem = pl.BlockSpec(memory_space=pltpu.VMEM)


def params(ident):
    return pltpu.CompilerParams(collective_id=ident, has_side_effects=True, vmem_limit_bytes=vmem_cap)


def scatter_all_kernel(reps, shards, slabbed, *refs):
    if slabbed:
        (
            p_ref, slab_ref, x_ref, c_ref, gg_ref, gu_ref, act_ref, out_ref, slabs_ref, wg_ref, wu_ref, wd_ref,
            xt, ct, og, ou, od, tile_sems, out_sems, *rest,
        ) = refs
    else:
        p_ref, out_ref, *rest = refs
    sems, ps, pr, slab_sem, *rest = rest
    g = Grid(reps, shards).here()
    s = Sends(sems)
    n = g.shards
    scatter = ScatterAll(g, s, p_ref, out_ref, *rest)
    half = pl.ds(0, out_ref.shape[0] // 2)
    own = scatter.plane.owned
    s.samples = [own.at[0, 0], own.at[0, 0, half], own.at[0, pl.ds(0, g.los), half]]
    scatter.load()
    if not slabbed:
        greet_all(g)
        scatter.to_partner()
        for turn in range(n + 2):
            scatter.step(turn)
        s.drain()
        return

    tile = xt.shape[2]
    tiles = x_ref.shape[1] // tile

    def tile_in(j, slot):
        span = pl.ds(pl.multiple_of(j * tile, tile), tile)
        return [
            pltpu.make_async_copy(x_ref.at[:, span], xt.at[slot], tile_sems.at[slot, 0]),
            pltpu.make_async_copy(c_ref.at[:, span], ct.at[slot], tile_sems.at[slot, 1]),
        ]

    def tile_out(j):
        span = pl.ds(pl.multiple_of(j * tile, tile), tile)
        return [
            pltpu.make_async_copy(og, wg_ref.at[span, :], out_sems.at[0]),
            pltpu.make_async_copy(ou, wu_ref.at[span, :], out_sems.at[1]),
            pltpu.make_async_copy(od, wd_ref.at[:, span], out_sems.at[2]),
        ]

    for copy in tile_in(0, 0):
        copy.start()
    greet_all(g)
    scatter.to_partner()
    push_rows(g, slab_ref, slabs_ref, ps, pr)
    me = g.r * n + g.z
    keep_slab = pltpu.make_async_copy(slab_ref.at[me], slabs_ref.at[me], slab_sem.at[0])
    keep_slab.start()

    def next_tiles(j):
        for copy in tile_in(j + 1, (j + 1) % 2):
            copy.start()

    def weight_grads(j, carry):
        for turn in range(n):
            pl.when(j == turn * tiles // n)(functools.partial(scatter.step, turn))
        pl.when(j + 1 < tiles)(functools.partial(next_tiles, j))
        slot = j % 2
        for copy in tile_in(j, slot):
            copy.wait()
        pl.when(j > 0)(functools.partial(wait_for, tile_out, j))
        og[...] = t_dot(xt[slot], gg_ref[...])
        ou[...] = t_dot(xt[slot], gu_ref[...])
        od[...] = t_dot(act_ref[...], ct[slot])
        for copy in tile_out(j):
            copy.start()
        return carry

    lax.fori_loop(0, tiles, weight_grads, 0)
    scatter.step(n)
    scatter.step(n + 1)
    wait_for(tile_out, 0)
    keep_slab.wait()
    push_wait(g, slab_ref, slabs_ref, ps, pr)
    s.drain()


def scatter_all(reps, shards, p, slab, fill, ident):
    g = Grid(reps, shards)
    n = shards
    _, rows, width = p.shape
    dma, v = pltpu.SemaphoreType.DMA, pltpu.VMEM
    slabbed = slab is not None
    out_shape = (jax.ShapeDtypeStruct((rows, width), f32),)
    out_specs, in_specs, extra, scratch = (vmem,), [hbm], [], []
    if slabbed:
        x, c, gg, gu, act = fill
        count, wide = x.shape
        inner = gg.shape[1]
        tile = 256
        narrow = jax.ShapeDtypeStruct((wide, inner), f32)
        out_shape += (
            jax.ShapeDtypeStruct(slab.shape, slab.dtype), narrow, narrow, jax.ShapeDtypeStruct((inner, wide), f32)
        )
        out_specs += (vmem, hbm, hbm, hbm)
        in_specs += [vmem, hbm, hbm, vmem, vmem, vmem]
        extra = [slab, *fill]
        scratch = [
            v((2, count, tile), bf16), v((2, count, tile), bf16),
            v((tile, inner), f32), v((tile, inner), f32), v((inner, tile), f32),
            dma((2, 2)), dma((3,)),
        ]
    done = pl.pallas_call(
        functools.partial(scatter_all_kernel, reps, shards, slabbed),
        out_shape=out_shape,
        in_specs=in_specs,
        out_specs=out_specs,
        scratch_shapes=scratch
        + [dma((ScatterAll.sends(g),)), dma((g.devices,)), dma((g.devices,)), dma((1,))]
        + ScatterAll.scratch(g, (rows, width), p.dtype),
        compiler_params=params(ident),
        name="scatter_all",
    )(p.reshape(g.places, 2, n, rows, width), *extra)
    return done if slabbed else done[0]


def scatter_wide(reps, shards, p, slab, fill, ident, chunks):
    if chunks == 1:
        return scatter_all(reps, shards, p, slab, fill, ident)
    step = p.shape[2] // chunks
    parts = [
        scatter_all(reps, shards, p[:, :, i * step : (i + 1) * step], slab if i == 0 else None, fill, ident + i)
        for i in range(chunks)
    ]
    if slab is None:
        return jnp.concatenate(parts, axis=1)
    first, *others = parts[0]
    return jnp.concatenate([first] + parts[1:], axis=1), *others


def deliver_kernel(reps, shards, split, *refs):
    (
        gqkv_ref, small_ref, qsum_ref, ksum_ref, wo_sum_ref, w_in, hid_in, xs_in,
        out_ref, q_out, rest_out, wo_out,
        w_ref, hid_ref, xs_ref, both, acc, ws_ref, wo_all, line_own, rl, rr, sl, sr,
        sems, wr, small_sem, keep_sem, ls, *rest,
    ) = refs
    q_cols, experts, part = split
    g = Grid(reps, shards).here()
    s = Sends(sems)
    n, places = g.shards, g.places
    gather_refs, wo_refs, scatter_refs = rest[:4], rest[4:8], rest[8:]
    length = out_ref.shape[0]
    total, cols = ws_ref.shape[-1], gqkv_ref.shape[1]
    piece = ws_ref.shape[2]
    deep = hid_ref.shape[1] // n
    first = total // 2 // 128 * 128
    spans = {0: pl.ds(0, first), 1: pl.ds(first, total - first), None: pl.ds(0, total)}
    owned = wo_sum_ref.shape[0]
    halves = {0: pl.ds(0, owned // 2), 1: pl.ds(owned // 2, owned // 2), None: pl.ds(0, owned)}
    order = g.nearest()[::-1]
    scatter = PlaneScatter(g, s, None, lambda p: (slice(None), spans[p]), both.at[g.core], *scatter_refs)
    scatter.loads = [None] * n
    gather = PlaneGather(
        g, s, lambda u, hi, lo, core, p: ws_ref.at[u, g.rep_of(hi, lo, core), :, spans[p]], *gather_refs
    )
    out_weight = PlaneGather(g, s, lambda u, hi, lo, core, p: wo_all.at[g.rep_of(hi, lo, core), halves[p]], *wo_refs)
    loads = [
        pltpu.make_async_copy(hid_in, hid_ref, ls.at[0]),
        pltpu.make_async_copy(w_in, w_ref, ls.at[1]),
        pltpu.make_async_copy(xs_in, xs_ref, ls.at[2]),
    ]
    for copy in loads:
        copy.start()
    barrier = pltpu.get_barrier_semaphore()
    peers = [g.device(g.r, (g.z + step) % n) for step in range(1, n)]
    peers += [g.device(g.rep_of(g.hi, g.other_lo(step), g.core), g.z) for step in range(1, g.los)]
    peers += [g.device(g.rep_of(1 - g.hi, g.lo, g.core), g.z), g.device(g.rep_of(g.hi, g.lo, 1 - g.core), g.z)]
    for peer in peers:
        pl.semaphore_signal(barrier, inc=1, device_id=peer, device_id_type=pl.DeviceIdType.MESH)
    pl.semaphore_wait(barrier, len(peers))
    out_weight.own(0, lambda p: wo_sum_ref.at[halves[p]])

    ra = scatter.ra
    loads[0].wait()
    for zp in range(n):
        grad = t_dot(hid_ref[:, zp * deep : (zp + 1) * deep], gqkv_ref[...]).astype(bf16)
        for place in range(places):
            for core in range(2):
                row = (place * 2 + core) * piece
                both[core, zp, place, :, 0:cols] = grad[row : row + piece]
        src = both.at[1 - g.core, zp, :, :, pl.ds(0, cols)]
        s.start(src, ra.at[zp, :, :, pl.ds(0, cols)], scatter.sa.at[zp], scatter.partner())

    loads[1].wait()
    loads[2].wait()
    lane = lax.broadcasted_iota(jnp.int32, (length, total - cols), 1)
    marked = jnp.where(lane == experts, 1.0, 0.0).astype(bf16)

    def line(turn):
        send_line(g, s, order[turn], line_own.at[turn], out_ref, rl, rr, sl, sr, last=turn == n - 1)

    acc[...] = small_ref[...]
    for turn in range(n):
        at = pl.ds(pl.multiple_of(order[turn] * length, length), length)
        share = dot_t(gqkv_ref[at, :], w_ref[...])
        line_own[turn] = share.astype(bf16)
        _, unit = unit_of(xs_ref[at, :].astype(f32))
        acc[...] += t_dot((share * unit).astype(bf16), marked)
        if turn == 0:
            line(0)
    for i, ref in ((2, qsum_ref), (3, ksum_ref)):
        width = ref.shape[1]
        columns = jnp.broadcast_to(ref[...], (total - cols, width)).T
        mask = lax.broadcasted_iota(jnp.int32, (part, total - cols), 1) == experts + i
        for zp in range(n):
            acc[zp * deep : zp * deep + part] += jnp.where(mask, columns[zp * part : (zp + 1) * part], 0.0)
    for zp in range(n):
        for place in range(places):
            for core in range(2):
                row = zp * deep + (place * 2 + core) * piece
                both[core, zp, place, :, cols:total] = acc[row : row + piece].astype(bf16)
    tail = pl.ds(cols, total - cols)
    s.start(both.at[1 - g.core, :, :, :, tail], ra.at[:, :, :, tail], small_sem.at[0], scatter.partner())

    def from_partner(turn):
        if turn == 0:
            s.arrived(ra.at[:, :, :, tail], small_sem.at[0], scatter.partner())
        s.arrived(ra.at[turn, :, :, pl.ds(0, cols)], scatter.sa.at[turn], scatter.partner())

    def owner(turn):
        scatter.c(turn)
        dst = ws_ref.at[g.z, g.r]
        keep = pltpu.make_async_copy(scatter.mine(turn), dst, keep_sem.at[0])
        pl.when(g.z == turn)(keep.start)
        s.start(scatter.mine(turn), dst, wr.at[g.z], g.device(g.r, turn), lambda: g.z != turn)
        pl.when(g.z == turn)(keep.wait)

    for turn in range(n + 2):
        if turn < n:
            from_partner(turn)
            scatter.a(turn, waited=True)
        if turn == 0:
            out_weight.first(0)
        if turn == 1:
            out_weight.second(0)
        if 0 <= turn - 1 < n:
            scatter.b(turn - 1)
        if 1 <= turn < n - 1:
            line(turn)
        if 0 <= turn - 2 < n:
            owner(turn - 2)
    out_weight.from_partner(0)
    keep = pltpu.make_async_copy(wo_sum_ref, wo_all.at[g.r], keep_sem.at[0])
    keep.start()
    keep.wait()
    saves = [pltpu.make_async_copy(wo_all, wo_out, ls.at[3])]
    saves[0].start()
    gather.own(g.z)

    def unit_at(step):
        return (g.z + n - step) % n

    for step in range(1, n):
        u = unit_at(step)
        s.arrived(ws_ref.at[u, g.r], wr.at[u], g.device(g.r, u))
        gather.own(u)
        gather.first(unit_at(step - 1))
        if step > 1:
            gather.second(unit_at(step - 2))
    gather.first(unit_at(n - 1))
    gather.second(unit_at(n - 2))
    gather.second(unit_at(n - 1))
    line(n - 1)
    for step in range(n):
        u = unit_at(step)
        gather.from_partner(u)
        q_span = pl.ds(pl.multiple_of(u * q_cols, 128), q_cols)
        saves += [
            pltpu.make_async_copy(ws_ref.at[u, :, :, pl.ds(0, q_cols)], q_out.at[:, :, q_span], ls.at[4 + 2 * step]),
            pltpu.make_async_copy(
                ws_ref.at[u, :, :, pl.ds(q_cols, total - q_cols)], rest_out.at[u], ls.at[5 + 2 * step]
            ),
        ]
        saves[-1].start()
        saves[-2].start()
    for copy in saves:
        copy.wait()
    s.drain()


def deliver(reps, shards, q_cols, experts, part, gqkv, small, qsum, ksum, wo_sum, w, hid, xs, ident):
    g = Grid(reps, shards)
    n = shards
    dma, v = pltpu.SemaphoreType.DMA, pltpu.VMEM
    width = hid.shape[1]
    rows = hid.shape[0] // n
    cols = gqkv.shape[1]
    total = cols + small.shape[1]
    piece = width // n // reps
    first = total // 2 // 128 * 128
    return pl.pallas_call(
        functools.partial(deliver_kernel, reps, shards, (q_cols, experts, part)),
        out_shape=(
            jax.ShapeDtypeStruct((rows, width), f32),
            jax.ShapeDtypeStruct((reps, piece, n * q_cols), bf16),
            jax.ShapeDtypeStruct((n, reps, piece, total - q_cols), bf16),
            jax.ShapeDtypeStruct((reps,) + wo_sum.shape, bf16),
        ),
        in_specs=[vmem] * 5 + [hbm] * 3,
        out_specs=(vmem, hbm, hbm, hbm),
        scratch_shapes=[
            v(w.shape, bf16),
            v(hid.shape, bf16),
            v(xs.shape, bf16),
            v((2, n, g.places, piece, total), bf16),
            v(small.shape, f32),
            v((n, reps, piece, total), bf16),
            v((reps,) + wo_sum.shape, bf16),
            v((n, rows, width), bf16),
        ]
        + line_scratch(n, (rows, width), bf16)
        + [
            dma((PlaneGather.sends(g, n) + PlaneGather.sends(g, 1) + PlaneScatter.sends(g, n) + 4 * n + 1,)),
            dma((n,)),
            dma((1,)),
            dma((1,)),
            dma((4 + 2 * n,)),
        ]
        + PlaneGather.scratch(g, n)
        + PlaneGather.scratch(g, 1)
        + PlaneScatter.scratch(g, n, (piece, total), ((piece, first), (piece, total - first)), bf16)[1:],
        compiler_params=params(ident),
        name="deliver",
    )(gqkv, small, qsum, ksum, wo_sum, w, hid, xs)


def turned(x, cosine, sine):
    return x * cosine + pltpu.roll(x, x.shape[-1] // 2, 1) * sine


def mean_last(x):
    return jnp.sum(x, axis=-1, keepdims=True) * (1.0 / x.shape[-1])


def unit_of(x):
    inverse = lax.rsqrt(mean_last(x * x) + epsilon)
    return inverse, x * inverse


def dot_t(a, b):
    return lax.dot_general(a, b, (((1,), (1,)), ((), ())), preferred_element_type=f32)


def t_dot(a, b):
    return lax.dot_general(a, b, (((0,), (0,)), ((), ())), preferred_element_type=f32)


def softmax_rows(q_rot, k_rot, bias, head_dim):
    scores = dot_t(q_rot, k_rot) * head_dim ** (-0.5) + bias
    raised = jnp.exp(scores - jnp.max(scores, axis=-1, keepdims=True))
    return raised * (1.0 / jnp.sum(raised, axis=-1, keepdims=True))


def back_unit(grad_scaled, unit, inverse, gain):
    gained = grad_scaled * gain
    return inverse * (gained - unit * mean_last(gained * unit))


def attend_block(b, heads, x_ref, w_ref, wo_ref, gain_ref, qg_ref, kg_ref, cos_ref, sin_ref, bias_ref, hid_ref, qkv_ref, att_ref, line):
    my_heads, my_kv, head_dim = heads
    x = x_ref[b].astype(f32)
    _, unit = unit_of(x)
    hid_ref[b] = (unit * gain_ref[...]).astype(bf16)
    qkv_ref[b] = jnp.dot(hid_ref[b], w_ref[...], preferred_element_type=f32)
    cosine, sine, bias = cos_ref[b], sin_ref[b], bias_ref[b]
    group = my_heads // my_kv
    for n in range(my_kv):
        at_k = (my_heads + n) * head_dim
        at_v = (my_heads + my_kv + n) * head_dim
        _, k_unit = unit_of(qkv_ref[b, :, at_k : at_k + head_dim])
        k_rot = turned(k_unit * kg_ref[...], cosine, sine).astype(bf16)
        values = qkv_ref[b, :, at_v : at_v + head_dim].astype(bf16)
        for h in range(n * group, (n + 1) * group):
            span = slice(h * head_dim, (h + 1) * head_dim)
            _, q_unit = unit_of(qkv_ref[b, :, span])
            q_rot = turned(q_unit * qg_ref[...], cosine, sine).astype(bf16)
            probs = softmax_rows(q_rot, k_rot, bias, head_dim)
            mixed = jnp.dot(probs.astype(bf16), values, preferred_element_type=f32)
            att_ref[b, :, span] = mixed.astype(bf16)
    line[...] = jnp.dot(att_ref[b], wo_ref[...], preferred_element_type=f32).astype(bf16)


def attend_back_block(b, heads, ga_ref, qkv_ref, wo_ref, qg_ref, kg_ref, cos_ref, sin_ref, bias_ref, gm_ref, gqkv_ref, qsum_ref, ksum_ref):
    my_heads, my_kv, head_dim = heads
    gm_ref[...] = dot_t(ga_ref[b], wo_ref[...]).astype(bf16)
    cosine, sine, bias = cos_ref[b], sin_ref[b], bias_ref[b]
    group = my_heads // my_kv
    qg, kg = qg_ref[...], kg_ref[...]
    for n in range(my_kv):
        at_k = (my_heads + n) * head_dim
        at_v = (my_heads + my_kv + n) * head_dim
        k_inverse, k_unit = unit_of(qkv_ref[b, :, at_k : at_k + head_dim])
        k_rot = turned(k_unit * kg, cosine, sine).astype(bf16)
        values = qkv_ref[b, :, at_v : at_v + head_dim].astype(bf16)
        grad_k = jnp.zeros(k_unit.shape, f32)
        grad_v = jnp.zeros(k_unit.shape, f32)
        for h in range(n * group, (n + 1) * group):
            span = slice(h * head_dim, (h + 1) * head_dim)
            q_inverse, q_unit = unit_of(qkv_ref[b, :, span])
            q_rot = turned(q_unit * qg, cosine, sine).astype(bf16)
            probs = softmax_rows(q_rot, k_rot, bias, head_dim)
            grad_mixed = gm_ref[:, span]
            grad_weights = dot_t(grad_mixed, values)
            centre = jnp.sum(probs * grad_weights, axis=-1, keepdims=True)
            grad_scores = (probs * (grad_weights - centre) * head_dim ** (-0.5)).astype(bf16)
            grad_v = grad_v + t_dot(probs.astype(bf16), grad_mixed)
            grad_k = grad_k + t_dot(grad_scores, q_rot)
            grad_q = jnp.dot(grad_scores, k_rot, preferred_element_type=f32)
            grad_q = turned(grad_q, cosine, -sine)
            qsum_ref[...] += jnp.sum(grad_q * q_unit, axis=0, keepdims=True)
            gqkv_ref[b, :, span] = back_unit(grad_q, q_unit, q_inverse, qg).astype(bf16)
        grad_k = turned(grad_k, cosine, -sine)
        ksum_ref[...] += jnp.sum(grad_k * k_unit, axis=0, keepdims=True)
        gqkv_ref[b, :, at_k : at_k + head_dim] = back_unit(grad_k, k_unit, k_inverse, kg).astype(bf16)
        gqkv_ref[b, :, at_v : at_v + head_dim] = grad_v.astype(bf16)


class GatherAll:
    def __init__(self, g, s, x_ref, out_ref, zr, plane_sems):
        self.g, self.s, self.x_ref, self.out_ref, self.zr = g, s, x_ref, out_ref, zr
        half = x_ref.shape[0] // 2
        self.spans = {0: pl.ds(0, half), 1: pl.ds(half, half), None: pl.ds(0, 2 * half)}
        self.order = g.nearest()
        self.plane = PlaneGather(g, s, self.view, *plane_sems)

    @staticmethod
    def scratch(g):
        dma = pltpu.SemaphoreType.DMA
        return [dma((g.shards,))] + PlaneGather.scratch(g, g.shards)

    @staticmethod
    def sends(g):
        return PlaneGather.sends(g, g.shards) + 2 * g.shards

    def view(self, u, hi, lo, core, part):
        return self.out_ref.at[self.g.rep_of(hi, lo, core) * self.g.shards + u, self.spans[part]]

    def own(self):
        g = self.g
        return self.view(g.z, g.hi, g.lo, g.core, None)

    def line(self, turn):
        g, zp = self.g, self.order[turn]
        dst = self.view(zp, g.hi, g.lo, g.core, None)
        if turn:
            self.s.arrived(dst, self.zr.at[zp], g.device(g.r, zp))
        pass_along(g, self.s, zp, dst if turn else self.x_ref, dst, self.zr)
        self.plane.own(zp, None if turn else lambda part: self.x_ref.at[self.spans[part]])

    def first(self, turn):
        self.plane.first(self.order[turn])

    def second(self, turn):
        self.plane.second(self.order[turn])

    def finish(self):
        for turn in range(self.g.shards):
            self.plane.from_partner(self.order[turn])


class ScatterAll:
    def __init__(self, g, s, p_ref, out_ref, rl, rr, sl, sr, *plane_refs):
        self.g, self.s, self.out_ref = g, s, out_ref
        self.lines = (rl, rr, sl, sr)
        half = out_ref.shape[0] // 2
        self.order = g.nearest()[::-1]
        self.plane = PlaneScatter(
            g,
            s,
            lambda turn, core: p_ref.at[:, core, self.order[turn]],
            lambda part: (pl.ds(part * half, half),),
            *plane_refs,
        )

    @staticmethod
    def scratch(g, block, dtype):
        rows, width = block
        half = (rows // 2, width)
        return line_scratch(g.shards, block, dtype) + PlaneScatter.scratch(g, g.shards, block, (half, half), dtype)

    @staticmethod
    def sends(g):
        return PlaneScatter.sends(g, g.shards) + 2 * g.shards

    def load(self):
        self.plane.load(self.g.shards)

    def to_partner(self):
        for turn in range(self.g.shards):
            self.plane.to_partner(turn)

    def step(self, turn):
        n = self.g.shards
        if turn < n:
            self.plane.a(turn)
        if 0 <= turn - 1 < n:
            self.plane.b(turn - 1)
        if 0 <= turn - 2 < n:
            t = turn - 2
            self.plane.c(t)
            send_line(self.g, self.s, self.order[t], self.plane.mine(t), self.out_ref, *self.lines, last=t == n - 1)


def attend_back_kernel(reps, shards, heads, *refs):
    (
        ga_ref, qg_ref, kg_ref, cos_ref, sin_ref, bias_ref, qkv_in, wo_in, att_in, p_ref,
        gqkv_ref, qsum_ref, ksum_ref, out_ref, wo_sum_ref,
        gas_ref, qkv_ref, wo_ref, att_ref, both, gm, zr, sems, ls, *scatter_refs,
    ) = refs
    g = Grid(reps, shards).here()
    s = Sends(sems)
    n, rows = g.shards, ga_ref.shape[0]
    half = both.shape[3] // 2
    count = len(scatter_refs) - 11
    scatter = ScatterAll(g, s, p_ref, out_ref, *scatter_refs[:count])
    own = both.at[g.core]
    owner = PlaneScatter(
        g, s, lambda turn, core: both.at[core, turn], lambda part: (pl.ds(part * half, half),), own, *scatter_refs[count:]
    )
    scatter.load()
    loads = [
        pltpu.make_async_copy(wo_in, wo_ref, ls.at[0]),
        pltpu.make_async_copy(qkv_in, qkv_ref, ls.at[1]),
        pltpu.make_async_copy(att_in, att_ref, ls.at[2]),
    ]
    keep = pltpu.make_async_copy(ga_ref, gas_ref.at[g.z], ls.at[3])
    for copy in loads + [keep]:
        copy.start()
    qsum_ref[...] = jnp.zeros(qsum_ref.shape, f32)
    ksum_ref[...] = jnp.zeros(ksum_ref.shape, f32)
    greet_all(g)
    order = g.nearest()

    def line(turn):
        zp = order[turn]
        dst = gas_ref.at[zp]
        if turn:
            s.arrived(dst, zr.at[zp], g.device(g.r, zp))
        pass_along(g, s, zp, dst if turn else ga_ref, dst, zr)

    def out_weight():
        width = ga_ref.shape[1]
        block = att_ref.shape[2] // g.reps
        grads = gas_ref[...].reshape(n * rows, width)
        for place in range(g.places):
            for core in range(2):
                at = (place * 2 + core) * block
                mixed = att_ref[:, :, at : at + block].reshape(n * rows, block)
                both[core, 0, place] = t_dot(mixed, grads).astype(bf16)

    line(0)
    scatter.to_partner()
    for copy in loads + [keep]:
        copy.wait()
    for turn in range(n):
        scatter.step(turn)
        if turn + 1 < n:
            line(turn + 1)
        else:
            out_weight()
            owner.to_partner(0)
        attend_back_block(
            order[turn], heads, gas_ref, qkv_ref, wo_ref, qg_ref, kg_ref, cos_ref, sin_ref, bias_ref,
            gm, gqkv_ref, qsum_ref, ksum_ref,
        )
    owner.loads = [None]
    scatter.step(n)
    owner.a(0)
    scatter.step(n + 1)
    owner.b(0)
    owner.c(0)
    wo_sum_ref[...] = own[0, g.hi * g.los + g.lo]
    s.drain()


def attend_back(reps, shards, heads, ga, qkv, wo, att, qg, kg, cosine, sine, bias, p, ident):
    g = Grid(reps, shards)
    dma, v = pltpu.SemaphoreType.DMA, pltpu.VMEM
    n = shards
    rows, width = ga.shape
    out_width = p.shape[2]
    owned = wo.shape[0] // reps
    row = jax.ShapeDtypeStruct(qg.shape, f32)
    block = (owned, width)
    half = (owned // 2, width)
    return pl.pallas_call(
        functools.partial(attend_back_kernel, reps, shards, heads),
        out_shape=(
            jax.ShapeDtypeStruct(qkv.shape, bf16),
            row,
            row,
            jax.ShapeDtypeStruct((rows, out_width), f32),
            jax.ShapeDtypeStruct(block, bf16),
        ),
        in_specs=[vmem] * 6 + [hbm] * 4,
        out_specs=(vmem,) * 5,
        scratch_shapes=[
            v((n, rows, width), bf16),
            v(qkv.shape, f32),
            v(wo.shape, bf16),
            v(att.shape, bf16),
            v((2, 1, g.places) + block, bf16),
            v((rows, wo.shape[0]), bf16),
            dma((n,)),
            dma((ScatterAll.sends(g) + PlaneScatter.sends(g, 1) + 2 * n,)),
            dma((4,)),
        ]
        + ScatterAll.scratch(g, (rows, out_width), p.dtype)
        + PlaneScatter.scratch(g, 1, block, (half, half), bf16)[1:],
        compiler_params=params(ident),
        name="attend_back",
    )(ga, qg, kg, cosine, sine, bias, qkv, wo, att, p.reshape(g.places, 2, n, rows, out_width))


def tables_of(segment_column, segment_row, frequency):
    length = segment_row.shape[1]
    rows = lax.broadcasted_iota(jnp.int32, (length, length), 0).astype(f32)
    columns = lax.broadcasted_iota(jnp.int32, (length, length), 1).astype(f32)
    same = segment_column == segment_row
    first = jnp.min(jnp.where(same, columns, float(length)), axis=1, keepdims=True)
    width = frequency.shape[1]
    place = lax.broadcasted_iota(jnp.int32, (length, width), 0).astype(f32)
    angle = (place - first) * frequency
    second_half = lax.broadcasted_iota(jnp.int32, (length, width), 1) >= width // 2
    sine = jnp.sin(angle)
    bias = jnp.where(same & (columns <= rows), 0.0, masked_score)
    return jnp.cos(angle), jnp.where(second_half, sine, -sine), bias


def front_kernel(reps, shards, heads, layout, *refs):
    (
        x_ref, cot_ref, small_ref, freq_ref, wq_ref, wk_ref, wv_ref, wo_in,
        smalls_ref, gains_ref, qk_ref, cos_ref, sin_ref, bias_ref, out_ref,
        xs_out, w_out, hid_out, qkv_out, att_out, cots_ref,
        xs_ref, w_ref, wo_ref, hid_ref, qkv_ref, att_ref, own, rl, rr, sl, sr,
        sems, xr, mr, wr, ls, out_sems, lr, hr, dr, cr, *gather_sems,
    ) = refs
    g = Grid(reps, shards).here()
    s = Sends(sems)
    n = g.shards
    q_cols, kv_cols, kv_heads, experts = layout
    head_dim = heads[2]
    deep = wq_ref.shape[0]
    piece = deep // g.reps
    cols = q_cols + 2 * kv_cols
    first = cols // 2 // 128 * 128
    spans = {0: pl.ds(0, first), 1: pl.ds(first, cols - first), None: pl.ds(0, cols)}
    mine = pl.ds(pl.multiple_of(g.r * piece, piece), piece)

    def view(u, hi, lo, core, part):
        row = pl.multiple_of(u * deep + g.rep_of(hi, lo, core) * piece, piece)
        return w_ref.at[pl.ds(row, piece), spans[part]]

    def pieces(zp, u):
        row = pl.ds(pl.multiple_of(u * deep + g.r * piece, piece), piece)
        at_q = pl.ds(pl.multiple_of(zp * q_cols, 128), q_cols)
        at_kv = pl.ds(pl.multiple_of(zp * kv_heads // n * head_dim, 128), kv_cols)
        return (
            (wq_ref.at[mine, at_q], w_ref.at[row, pl.ds(0, q_cols)]),
            (wk_ref.at[mine, at_kv], w_ref.at[row, pl.ds(q_cols, kv_cols)]),
            (wv_ref.at[mine, at_kv], w_ref.at[row, pl.ds(q_cols + kv_cols, kv_cols)]),
        )

    plane = PlaneGather(g, s, view, lr, hr, dr, cr)
    gather = GatherAll(g, s, cot_ref, cots_ref, gather_sems[0], gather_sems[1:])
    locals_ = [pltpu.make_async_copy(src, dst, ls.at[i]) for i, (src, dst) in enumerate(pieces(g.z, g.z))]
    keeps = [
        pltpu.make_async_copy(x_ref, xs_ref.at[g.z], ls.at[3]),
        pltpu.make_async_copy(small_ref, smalls_ref.at[g.z], ls.at[4]),
        pltpu.make_async_copy(wo_in, wo_ref, ls.at[5]),
        pltpu.make_async_copy(cot_ref, gather.own(), ls.at[6]),
    ]
    for copy in locals_ + keeps:
        copy.start()
    barrier = pltpu.get_barrier_semaphore()
    peers = [g.device(g.r, (g.z + step) % n) for step in range(1, n)]
    peers += [g.device(g.rep_of(g.hi, g.other_lo(step), g.core), g.z) for step in range(1, g.los)]
    peers += [g.device(g.rep_of(1 - g.hi, g.lo, g.core), g.z), g.device(g.rep_of(g.hi, g.lo, 1 - g.core), g.z)]
    for peer in peers:
        pl.semaphore_signal(barrier, inc=1, device_id=peer, device_id_type=pl.DeviceIdType.MESH)
    pl.semaphore_wait(barrier, len(peers))

    order = g.nearest()

    def unit(step):
        return (g.z + n - step) % n

    def line(turn):
        zp = order[turn]
        if turn:
            s.arrived(smalls_ref.at[zp], mr.at[zp], g.device(g.r, zp))
        pass_along(g, s, zp, smalls_ref.at[zp] if turn else small_ref, smalls_ref.at[zp], mr)
        if turn:
            s.arrived(xs_ref.at[zp], xr.at[zp], g.device(g.r, zp))
        pass_along(g, s, zp, xs_ref.at[zp] if turn else x_ref, xs_ref.at[zp], xr)

    for step in range(1, n):
        zp = (g.z + step) % n
        for i, (src, dst) in enumerate(pieces(zp, g.z)):
            s.start(src, dst, wr.at[step, i], g.device(g.r, zp))
    line(0)
    for copy in locals_:
        copy.wait()
    plane.own(g.z)
    for step in range(1, n):
        u = unit(step)
        for i, (_, dst) in enumerate(pieces(g.z, u)):
            s.arrived(dst, wr.at[step, i], g.device(g.r, u))
        plane.own(u)
    gather.plane.own(g.z, lambda part: cot_ref.at[gather.spans[part]])
    line(1)
    for step in range(n):
        plane.first(unit(step))
        if step:
            plane.second(unit(step - 1))
        if 2 + step < n - 1:
            line(2 + step)
        if step == max(0, n - 4):
            pass_along(g, s, g.z, cot_ref, gather.own(), gather.zr)
    plane.second(unit(n - 1))
    for step in range(n):
        plane.from_partner(unit(step))
    for copy in keeps[:3]:
        copy.wait()

    length = x_ref.shape[0]
    smalls_late = order[n - 1]
    s.arrived(smalls_ref.at[smalls_late], mr.at[smalls_late], g.device(g.r, smalls_late))
    pass_along(g, s, smalls_late, smalls_ref.at[smalls_late], smalls_ref.at[smalls_late], mr)
    for zp in range(n):
        gains_ref[:, zp * deep : (zp + 1) * deep] = smalls_ref[zp].astype(f32)[experts : experts + 8]
    for i in range(2):
        qk_ref[i : i + 1] = sum(gains_ref[2 + i : 3 + i, zp * deep : zp * deep + head_dim] for zp in range(n))

    def compute(turn):
        zp = order[turn]
        row = gains_ref[4:5, pl.ds(pl.multiple_of(zp * deep, 128), length)]
        column = jnp.broadcast_to(row, (length, length)).T
        cos_ref[zp], sin_ref[zp], bias_ref[zp] = tables_of(column, row, freq_ref[...])
        attend_block(
            zp, heads, xs_ref, w_ref, wo_ref, gains_ref.at[0:1], qk_ref.at[0:1], qk_ref.at[1:2],
            cos_ref, sin_ref, bias_ref, hid_ref, qkv_ref, att_ref, own.at[turn],
        )

    def sums(turn):
        send_line(g, s, order[turn], own.at[turn], out_ref, rl, rr, sl, sr, last=turn == 0)

    farthest = order[n - 1]
    between = lambda: (g.z > 0) & (g.z + 1 < n)
    at_end = lambda: (g.z == 0) | (g.z + 1 == n)
    s.arrived(xs_ref.at[farthest], xr.at[farthest], g.device(g.r, farthest), between)
    pass_along(g, s, farthest, xs_ref.at[farthest], xs_ref.at[farthest], xr)
    compute(0)
    s.arrived(xs_ref.at[farthest], xr.at[farthest], g.device(g.r, farthest), at_end)
    outs = [pltpu.make_async_copy(w_ref, w_out, out_sems.at[0]), pltpu.make_async_copy(xs_ref, xs_out, out_sems.at[1])]
    for copy in outs:
        copy.start()
    compute(n - 1)
    sums(n - 1)
    gather.first(0)
    gather.line(1)
    for turn in range(n - 2, -1, -1):
        if turn > 0:
            compute(turn)
        at = n - 1 - turn
        if turn > 0:
            sums(turn)
            gather.second(at - 1)
            gather.first(at)
            if at + 1 < n:
                gather.line(at + 1)
    late = [
        pltpu.make_async_copy(hid_ref, hid_out, out_sems.at[2]),
        pltpu.make_async_copy(qkv_ref, qkv_out, out_sems.at[3]),
        pltpu.make_async_copy(att_ref, att_out, out_sems.at[4]),
    ]
    for copy in late:
        copy.start()
    gather.second(n - 2)
    gather.first(n - 1)
    gather.second(n - 1)
    sums(0)
    gather.finish()
    for copy in outs + late + keeps[3:]:
        copy.wait()
    s.drain()


def front(reps, shards, heads, layout, x, cot, small, frequency, wq, wk, wv, wo, ident):
    g = Grid(reps, shards)
    dma, v = pltpu.SemaphoreType.DMA, pltpu.VMEM
    n = shards
    rows, width = x.shape
    head_dim = heads[2]
    cols = layout[0] + 2 * layout[1]
    table = jax.ShapeDtypeStruct((n, rows, head_dim), f32)
    lines = (n, rows, width)
    return pl.pallas_call(
        functools.partial(front_kernel, reps, shards, heads, layout),
        out_shape=(
            jax.ShapeDtypeStruct((n,) + small.shape, bf16),
            jax.ShapeDtypeStruct((8, width), f32),
            jax.ShapeDtypeStruct((8, head_dim), f32),
            table,
            table,
            jax.ShapeDtypeStruct((n, rows, rows), f32),
            jax.ShapeDtypeStruct((rows, width), f32),
            jax.ShapeDtypeStruct(lines, bf16),
            jax.ShapeDtypeStruct((width, cols), bf16),
            jax.ShapeDtypeStruct(lines, bf16),
            jax.ShapeDtypeStruct((n, rows, cols), f32),
            jax.ShapeDtypeStruct((n, rows, wo.shape[0]), bf16),
            jax.ShapeDtypeStruct((g.devices, rows, width), bf16),
        ),
        in_specs=[vmem] * 4 + [hbm] * 4,
        out_specs=(vmem,) * 7 + (hbm,) * 6,
        scratch_shapes=[
            v(lines, bf16),
            v((width, cols), bf16),
            v(wo.shape, bf16),
            v(lines, bf16),
            v((n, rows, cols), f32),
            v((n, rows, wo.shape[0]), bf16),
            v(lines, bf16),
        ]
        + line_scratch(n, (rows, width), bf16)
        + [
            dma((PlaneGather.sends(g, n) + GatherAll.sends(g) + 9 * n,)),
            dma((n,)),
            dma((n,)),
            dma((n, 3)),
            dma((7,)),
            dma((5,)),
        ]
        + PlaneGather.scratch(g, n)
        + GatherAll.scratch(g),
        compiler_params=params(ident),
        name="front",
    )(x, cot, small, frequency, wq, wk, wv, wo)


def slots_of(slab, capacity):
    length = slab.shape[1]
    member = slab >= 0.0
    earlier = lax.broadcasted_iota(jnp.int32, (length, length), 0) < lax.broadcasted_iota(jnp.int32, (length, length), 1)
    ones = jnp.where(member, 1.0, 0.0).astype(bf16)
    slot = jnp.dot(ones, jnp.where(earlier, 1.0, 0.0).astype(bf16), preferred_element_type=f32)
    slot = jnp.where(member, slot, -1.0)[0:1]
    rows = lax.broadcasted_iota(jnp.int32, (capacity, length), 0).astype(f32)
    return jnp.where(rows == slot, 1.0, 0.0), slab[0:1]


def experts_kernel(reps, shards, capacity, held, *refs):
    (
        x_ref, slab_ref, cots_ref, wg_ref, wu_ref, wd_ref,
        back_ref, sums_ref, grads_ref, rows_ref, cs_ref, gg_ref, gu_ref, act_ref, all_ref,
        slabs, cot_buf, hid_buf, d_ref, x_buf, c_buf, gg_buf, gu_buf, act_buf, sum_buf, grad_buf,
        sems, ps, pr, ls, cot_sem, hid_sem, out_sems, zr, *plane_sems,
    ) = refs
    g = Grid(reps, shards).here()
    s = Sends(sems)
    n, places = g.shards, g.places
    length = x_ref.shape[0]
    hidden = hid_buf if held else all_ref
    s.samples = [x_ref, x_ref.at[pl.ds(0, length // 2)]]
    gather = GatherAll(g, s, x_ref, hidden, zr, plane_sems)
    order = gather.order
    groups = 2 * n

    def which(k):
        return jnp.where(k % 2 == 0, g.core, 1 - g.core), pick(k // 2, order)

    def cot_load(k, slot):
        core, zp = which(k)
        return pltpu.make_async_copy(cots_ref.at[:, core, zp], cot_buf.at[slot], cot_sem.at[slot])

    def onehots(k):
        core, zp = which(k)
        return [slots_of(slabs[(q * 2 + core) * n + zp], capacity) for q in range(places)]

    keep = pltpu.make_async_copy(x_ref, gather.own(), ls.at[0])
    keep.start()
    cot_load(0, 0).start()
    greet_all(g)
    push_rows(g, slab_ref, slabs, ps, pr)
    me = g.r * n + g.z
    keep_slab = pltpu.make_async_copy(slab_ref.at[me], slabs.at[me], ls.at[1])
    keep_slab.start()
    gather.line(0)
    keep_slab.wait()
    push_wait(g, slab_ref, slabs, ps, pr)
    keep.wait()

    def turns(k, steps):
        for at, step in steps:
            pl.when(k == at)(step)

    def both(*fs):
        def run():
            for f, turn in fs:
                f(turn)

        return run

    early = [(2, both((gather.first, 0))), (3, both((gather.line, 1))), (5, both((gather.second, 0)))]
    if n > 2:
        early.append((7, both((gather.line, 2))))

    def outs(k):
        return [
            pltpu.make_async_copy(x_buf, rows_ref.at[k], out_sems.at[0]),
            pltpu.make_async_copy(gg_buf, gg_ref.at[k], out_sems.at[1]),
            pltpu.make_async_copy(gu_buf, gu_ref.at[k], out_sems.at[2]),
            pltpu.make_async_copy(act_buf, act_ref.at[k], out_sems.at[3]),
        ]

    def blocks_out(k):
        core, zp = which(k)
        return [
            pltpu.make_async_copy(sum_buf, sums_ref.at[:, core, zp], out_sems.at[4]),
            pltpu.make_async_copy(grad_buf, grads_ref.at[:, core, zp], out_sems.at[5]),
        ]

    def c_out(k):
        return pltpu.make_async_copy(c_buf, cs_ref.at[k], out_sems.at[6])

    def backward_input(k, carry):
        turns(k, early)
        slot = k % 2
        pl.when(k + 1 < groups)(lambda: cot_load(k + 1, 1 - slot).start())
        cot_load(k, slot).wait()
        pl.when(k > 0)(lambda: c_out(k).wait())
        for q, (onehot, _) in enumerate(onehots(k)):
            taken = jnp.dot(onehot.astype(bf16), cot_buf[slot, q], preferred_element_type=f32)
            c_buf[q * capacity : (q + 1) * capacity, :] = taken.astype(bf16)
        c_out(k).start()
        d_ref[k] = dot_t(c_buf[...], wd_ref[...])
        return carry

    lax.fori_loop(0, groups, backward_input, 0)
    c_out(0).wait()

    def partner(turn):
        gather.plane.from_partner(order[turn])

    late = [(0, both((gather.first, 1)))]
    for turn in range(n):
        if 0 < turn < n - 1:
            late.append((2 * turn, both((gather.second, turn))))
        steps = [(partner, turn)]
        if turn + 3 < n:
            steps.append((gather.line, turn + 3))
        if turn + 2 < n:
            steps.append((gather.first, turn + 2))
        if turn == n - 2:
            steps.append((gather.second, n - 1))
        late.append((2 * turn + 1, both(*steps)))

    def expert(k, carry):
        turns(k, late)
        core, zp = which(k)
        if not held:
            fetch = pltpu.make_async_copy(all_ref.at[pl.ds(0, places)], hid_buf, hid_sem.at[0])
            for q in range(places):
                pltpu.make_async_copy(all_ref.at[(q * 2 + core) * n + zp], hid_buf.at[q], hid_sem.at[0]).start()
            fetch.wait()
        hots = onehots(k)
        pl.when(k > 0)(functools.partial(wait_for, outs, k))
        for q, (onehot, _) in enumerate(hots):
            block = hid_buf[(q * 2 + core) * n + zp] if held else hid_buf[q]
            taken = jnp.dot(onehot.astype(bf16), block, preferred_element_type=f32)
            x_buf[q * capacity : (q + 1) * capacity, :] = taken.astype(bf16)
        weight = jnp.concatenate(
            [jnp.sum(onehot * share, axis=1, keepdims=True) for onehot, share in hots], axis=0
        )
        gate = jnp.dot(x_buf[...], wg_ref[...], preferred_element_type=f32)
        up = jnp.dot(x_buf[...], wu_ref[...], preferred_element_type=f32)
        sigmoid = 1.0 / (1.0 + jnp.exp(-gate))
        silu = gate * sigmoid
        activated = silu * up
        grad = d_ref[k]
        row_mix = jnp.sum(activated * grad, axis=1, keepdims=True)
        grad = grad * weight
        act_buf[...] = (activated * weight).astype(bf16)
        gg_buf[...] = (grad * up * sigmoid * (1.0 + gate * (1.0 - sigmoid))).astype(bf16)
        gu_buf[...] = (grad * silu).astype(bf16)
        for copy in outs(k):
            copy.start()
        for q, (onehot, _) in enumerate(hots):
            back = jnp.sum(onehot * row_mix[q * capacity : (q + 1) * capacity], axis=0, keepdims=True)
            back_ref[(q * 2 + core) * n + zp] = jnp.broadcast_to(back, slab_ref.shape[1:])
        produced = jnp.dot(act_buf[...], wd_ref[...], preferred_element_type=f32).astype(bf16)
        pl.when(k > 0)(functools.partial(wait_for, blocks_out, k))
        for q, (onehot, _) in enumerate(hots):
            part = produced[q * capacity : (q + 1) * capacity]
            sum_buf[q] = t_dot(onehot.astype(bf16), part).astype(bf16)
        grad_in = (dot_t(gg_buf[...], wg_ref[...]) + dot_t(gu_buf[...], wu_ref[...])).astype(bf16)
        for q, (onehot, _) in enumerate(hots):
            part = grad_in[q * capacity : (q + 1) * capacity]
            grad_buf[q] = t_dot(onehot.astype(bf16), part).astype(bf16)
        for copy in blocks_out(k):
            copy.start()
        return carry

    lax.fori_loop(0, groups, expert, 0)
    for copy in outs(0) + blocks_out(0):
        copy.wait()
    s.drain()


def experts_all(reps, shards, capacity, x, slab, cots, wg, wu, wd, ident):
    g = Grid(reps, shards)
    dma, v = pltpu.SemaphoreType.DMA, pltpu.VMEM
    n, places = shards, g.places
    length, width = x.shape
    inner = wg.shape[1]
    rows = places * capacity
    held = g.devices <= 32
    blocks = jax.ShapeDtypeStruct((places, 2, n, length, width), bf16)
    wide = jax.ShapeDtypeStruct((2 * n, rows, width), bf16)
    narrow = jax.ShapeDtypeStruct((2 * n, rows, inner), bf16)
    gathered = (g.devices, length, width)
    return pl.pallas_call(
        functools.partial(experts_kernel, reps, shards, capacity, held),
        out_shape=(
            jax.ShapeDtypeStruct(slab.shape, f32),
            blocks,
            blocks,
            wide,
            wide,
            narrow,
            narrow,
            narrow,
            jax.ShapeDtypeStruct((1, 16, 128) if held else gathered, bf16),
        ),
        in_specs=[vmem, vmem, hbm, vmem, vmem, vmem],
        out_specs=(vmem,) + (hbm,) * 8,
        scratch_shapes=[
            v(slab.shape, f32),
            v((2, places, length, width), bf16),
            v(gathered if held else (places, length, width), bf16),
            v((2 * n, rows, inner), f32),
            v((rows, width), bf16),
            v((rows, width), bf16),
            v((rows, inner), bf16),
            v((rows, inner), bf16),
            v((rows, inner), bf16),
            v((places, length, width), bf16),
            v((places, length, width), bf16),
            dma((GatherAll.sends(g),)),
            dma((g.devices,)),
            dma((g.devices,)),
            dma((2,)),
            dma((2,)),
            dma((1,)),
            dma((7,)),
        ]
        + GatherAll.scratch(g),
        compiler_params=params(ident),
        name="experts_all",
    )(x, slab, cots.reshape(places, 2, n, length, width), wg, wu, wd)[:-1]


def inverse_rms(values):
    return lax.rsqrt(jnp.mean(values * values, axis=-1, keepdims=True) + epsilon)


def norm_back(grad_scaled, unit, inverse, gain):
    gained = grad_scaled * gain
    return inverse * (gained - unit * jnp.mean(gained * unit, axis=-1, keepdims=True))


def matmul(a, b, dims=((1,), (0,))):
    return lax.dot_general(a, b, (dims, ((), ())), preferred_element_type=f32)


def local(
    tokens,
    segments,
    routes,
    attn_gain,
    w_query,
    key_weight,
    value_weight,
    w_out,
    query_gain,
    key_gain,
    ffn_gain,
    w_router,
    w_gate,
    w_up,
    w_down,
    cotangent,
):
    reps, shards = lax.axis_size("rep"), lax.axis_size("shard")
    devices = reps * shards
    r, z = lax.axis_index("rep"), lax.axis_index("shard")
    length, width = tokens.shape
    deep = w_query.shape[0]
    head_dim = query_gain.shape[0] * shards
    heads = w_query.shape[1] // head_dim
    kv_heads = key_weight.shape[1] // head_dim
    experts = w_router.shape[1]
    top = routes.shape[1]
    capacity = 2 * length * top // experts
    my_heads = heads // shards
    my_kv = max(1, kv_heads // shards)
    shared_by = max(1, shards // kv_heads)
    q_cols, kv_cols = my_heads * head_dim, my_kv * head_dim
    cols = q_cols + 2 * kv_cols
    piece = deep // reps
    chunks = max(1, devices // 32)
    part = head_dim // shards

    spot = lax.broadcasted_iota(jnp.int32, (1, deep), 1) // part == z

    def row_of(values):
        return jnp.pad(values.reshape(1, -1), ((0, 0), (0, deep - values.size)))

    def spotted(values):
        return jnp.where(spot, jnp.tile(values.reshape(1, part), (1, deep // part)), 0)

    small = jnp.concatenate(
        [
            w_router.T,
            row_of(attn_gain),
            row_of(ffn_gain),
            spotted(query_gain),
            spotted(key_gain),
            row_of(segments[0].astype(bf16)),
        ],
        axis=0,
    )
    small = jnp.pad(small, ((0, -(-(experts + 8) // 16) * 16 - small.shape[0]), (0, 0)))
    small_cols = -(-(experts + 8) // 128) * 128
    half = rope_base ** (-2.0 * jnp.arange(head_dim // 2, dtype=f32) / head_dim)
    frequency = jnp.concatenate([half, half]).reshape(1, head_dim)
    head_sizes = (my_heads, my_kv, head_dim)
    layout = (q_cols, kv_cols, kv_heads, experts)
    (
        small_all, gains, qk_gains, cosine, sine, bias, mixed,
        block_tokens, w_in, hidden_in, qkv, attn_out, cotangents,
    ) = front(
        reps, shards, head_sizes, layout, tokens, cotangent, small, frequency,
        w_query, key_weight, value_weight, w_out, 1,
    )
    router = small_all[:, :experts].transpose(1, 0, 2).reshape(experts, width)
    gain_one, gain_two = gains[0:1], gains[1:2]
    qgain, kgain = qk_gains[0:1], qk_gains[1:2]
    own_tokens = tokens.astype(f32)
    resid = own_tokens + mixed

    inverse_two = inverse_rms(resid)
    normed_two = resid * inverse_two
    hidden_two = (normed_two * gain_two).astype(bf16)
    logits = matmul(hidden_two, router, ((1,), (1,)))
    gate_probs = jax.nn.softmax(logits, axis=-1)
    chosen = jnp.any(routes[:, :, None] == jnp.arange(experts, dtype=jnp.int32)[None, None, :], axis=1)
    picked = jnp.where(chosen, gate_probs, 0.0)
    picked_total = jnp.sum(picked, axis=-1, keepdims=True)
    mix = picked / picked_total
    slab = jnp.where(chosen, mix, -1.0).T.reshape(experts, 1, length)
    slab = jnp.broadcast_to(slab, (experts, 8, length))
    back_mix, sums, grad_sums, rows, row_grads, grad_gate, grad_up, activated = experts_all(
        reps, shards, capacity, hidden_two, slab, cotangents, w_gate[0], w_up[0], w_down[0], 4
    )
    sums = sums.reshape(devices, length, width)
    grad_sums = grad_sums.reshape(devices, length, width)
    rows, row_grads = rows.reshape(-1, width), row_grads.reshape(-1, width)
    fill = (rows, row_grads) + tuple(a.reshape(rows.shape[0], -1) for a in (grad_gate, grad_up, activated))
    grad_hidden, mixes, grad_w_gate, grad_w_up, grad_w_down = scatter_wide(
        reps, shards, grad_sums, back_mix, fill, 8, chunks
    )

    grad_out = cotangent.astype(f32)
    grad_mix = mixes[:, 0, :].T
    grad_picked = jnp.where(chosen, grad_mix - jnp.sum(grad_mix * mix, axis=-1, keepdims=True), 0.0) / picked_total
    grad_logits = (gate_probs * (grad_picked - jnp.sum(grad_picked * picked, axis=-1, keepdims=True))).astype(bf16)
    grad_hidden = grad_hidden + matmul(grad_logits, router)
    grad_ffn_gain = jnp.sum(grad_hidden * normed_two, axis=0)
    grad_resid = grad_out + norm_back(grad_hidden, normed_two, inverse_two, gain_two)
    grad_w_router = matmul(hidden_two, grad_logits, ((0,), (0,)))

    fused = width // chunks
    grad_qkv, grad_query_gain, grad_key_gain, moe, out_grad = attend_back(
        reps, shards, head_sizes, grad_resid.astype(bf16), qkv, w_out, attn_out, qgain, kgain, cosine, sine, bias,
        sums[:, :, :fused], 5,
    )
    if chunks > 1:
        rest = scatter_wide(reps, shards, sums[:, :, fused:], None, None, 16, chunks - 1)
        moe = jnp.concatenate([moe, rest], axis=1)
    output = (resid + moe).astype(bf16)

    small_grads = jnp.concatenate(
        [grad_w_router, jnp.zeros((width, 1), f32), grad_ffn_gain.reshape(width, 1)], axis=1
    )
    small_grads = jnp.pad(small_grads, ((0, 0), (0, small_cols - small_grads.shape[1])))
    grad_hidden_in, sent_q, sent, sent_out = deliver(
        reps, shards, q_cols, experts, part, grad_qkv.reshape(shards * length, cols), small_grads,
        grad_query_gain, grad_key_gain, out_grad, w_in, hidden_in.reshape(shards * length, width),
        block_tokens.reshape(shards * length, width), 6,
    )
    own_inverse, own_normed = unit_of(own_tokens)
    grad_tokens = grad_resid + norm_back(grad_hidden_in, own_normed, own_inverse, gain_one)
    sent = sent.reshape(shards, deep, 2 * kv_cols + small_cols)

    def joined(values):
        if shared_by > 1:
            values = values.astype(f32).reshape(-1, shared_by, deep, values.shape[-1]).sum(axis=1)
        return values.transpose(1, 0, 2).reshape(deep, -1).astype(f32)

    owned_small = jnp.sum(sent[:, :, 2 * kv_cols :].astype(f32), axis=0)
    return (
        output,
        grad_tokens,
        owned_small[:, experts],
        sent_q.reshape(deep, -1).astype(f32),
        joined(sent[:, :, :kv_cols]),
        joined(sent[:, :, kv_cols : 2 * kv_cols]),
        sent_out.reshape(w_out.shape).astype(f32),
        owned_small[:part, experts + 2],
        owned_small[:part, experts + 3],
        owned_small[:, experts + 1],
        owned_small[:, :experts],
        grad_w_gate[None],
        grad_w_up[None],
        grad_w_down[None],
    )


def solution(mesh):
    split = P(("rep", "shard"))
    row = P("shard")
    return jax.shard_map(
        local,
        mesh=mesh,
        in_specs=(split,) * 3 + (row,) * 9 + (split,) * 4,
        out_specs=(split,) * 2 + (row,) * 9 + (split,) * 3,
        check_vma=False,
    )
```

```python
import functools
import jax
import jax.numpy as jnp
from jax import lax
from jax.experimental import pallas as pl
from jax.experimental.pallas import tpu as pltpu
from jax.sharding import PartitionSpec as P

bf16 = jnp.bfloat16
f32 = jnp.float32
vmem_cap = 62 * 1024 * 1024
epsilon = 1e-06
rope_base = 1000000.0
masked_score = -1e30
tuned_front = {
    4: [
        ("w", 0), ("m", 0), ("w", 1), ("x", 0), ("cz", 0), ("pf", 1), ("co", 0), ("m", 1), ("w", 2), ("pf", 0),
        ("xe", 1), ("w", 3), ("m", 2), ("xm", 2), ("ps", 0), ("xm", 1), ("pf", 3), ("gf", 0), ("pf", 2), ("ps", 1),
        ("m", 3), ("glm", 1), ("glm", 2), ("ps", 2), ("gle", 1), ("xm", 3), ("ps", 3), ("pp", 3), ("g", 0),
        ("glm", 3), ("gle", 2), ("pp", 2), ("xe", 3), ("pp", 0), ("pp", 1), ("c", 3), ("gf", 1), ("r", 3), ("c", 1),
        ("xe", 2), ("gf", 2), ("c", 2), ("r", 2), ("o", 0), ("gs", 1), ("gle", 3), ("r", 1), ("gf", 3), ("gs", 2),
        ("c", 0), ("gs", 0), ("gs", 3), ("o", 1), ("r", 0),
    ]
}
tuned_back = {
    4: [
        ("a", 0), ("l", 1), ("a", 1), ("l", 2), ("a", 2), ("k", 0), ("b", 0), ("l", 3), ("a", 3), ("w", 0), ("b", 1),
        ("k", 2), ("c", 0), ("b", 2), ("wa", 0), ("s", 0), ("k", 1), ("k", 3), ("c", 1), ("s", 1), ("c", 2), ("s", 2),
        ("b", 3), ("wb", 0), ("c", 3), ("s", 3), ("wc", 0),
    ]
}
tuned_deliver = {
    4: [
        ("wi", 0), ("pt", 0), ("pt", 3), ("l", 0), ("pt", 2), ("of", 0), ("pt", 1), ("sm", 0), ("wi", 1), ("a", 0),
        ("wi", 2), ("a", 1), ("l", 1), ("os", 0), ("b", 0), ("a", 2), ("wi", 3), ("o", 0), ("a", 3), ("op", 0),
        ("b", 1), ("b", 2), ("b", 3), ("o", 1), ("o", 3), ("o", 2), ("u", 0), ("l", 2), ("u", 3), ("f", 0), ("f", 3),
        ("u", 2), ("f", 2), ("u", 1), ("s", 3), ("l", 3), ("s", 0), ("s", 2), ("f", 1), ("s", 1), ("p", 0), ("p", 2),
        ("p", 1), ("p", 3),
    ]
}
tuned_experts = {
    4: [
        (5, "s", 0), (13, "p", 2), (10, "s", 1), (9, "f", 2), (12, "s", 2), (14, "s", 3), (11, "p", 1), (11, "e", 3),
        (15, "p", 3), (0, "f", 0), (9, "l", 3), (0, "l", 1), (7, "f", 1), (2, "e", 1), (5, "e", 2), (5, "p", 0),
        (1, "l", 2), (13, "f", 3),
    ]
}
tuned_sum = {(4, 8): [0, 2, 3, 5, 6, 7, 7, 6, 8, 8, 8, 8, 8, 8, 8, 8]}


class Grid:
    def __init__(self, reps, shards):
        self.reps, self.shards = reps, shards
        self.devices = reps * shards
        self.places = reps // 2
        self.los = self.places // 2

    def here(self):
        self.r = lax.axis_index("rep")
        self.z = lax.axis_index("shard")
        self.core = self.r % 2
        place = self.r // 2
        self.hi = place // self.los
        self.lo = place % self.los
        return self

    def rep_of(self, hi, lo, core):
        return (hi * self.los + lo) * 2 + core

    def device(self, rep, shard):
        return {"rep": rep, "shard": shard}

    def other_lo(self, step):
        return (self.lo + step) % self.los

    def inside(self):
        return (self.z > 0) & (self.z + 1 < self.shards)

    def outside(self):
        return (self.z == 0) | (self.z + 1 == self.shards)

    def nearest(self):
        n = self.shards
        rows = [sorted(range(n), key=lambda p: (abs(p - z), p)) for z in range(n)]
        return [pick(self.z, [rows[z][turn] for z in range(n)]) for turn in range(n)]


def pick(index, values):
    out = jnp.int32(values[0])
    for i in range(1, len(values)):
        out = jnp.where(index == i, jnp.int32(values[i]), out)
    return out


class Sends:
    def __init__(self, sems):
        self.sems, self.used, self.open, self.samples, self.guard = sems, 0, [], [], None

    def under(self, guard, task):
        self.guard = guard
        task()
        self.guard = None

    def all_of(self, when):
        guard = self.guard
        if guard is None or when is None:
            return guard or when
        return lambda: guard() & when()

    def copy(self, src, dst, sem, recv, device):
        return pltpu.make_async_remote_copy(
            src_ref=src,
            dst_ref=dst,
            send_sem=self.sems.at[sem],
            recv_sem=recv,
            device_id=device,
            device_id_type=pl.DeviceIdType.MESH,
        )

    def start(self, src, dst, recv, device, when=None):
        copy = self.copy(src, dst, self.used, recv, device)
        sample = src
        for other in self.samples:
            if other.shape == src.shape:
                sample = other
        when = self.all_of(when)
        self.open.append((self.used, sample, when))
        self.used += 1
        if when is None:
            copy.start()
        else:
            pl.when(when())(copy.start)

    def arrived(self, dst, recv, device, when=None):
        copy = self.copy(dst, dst, 0, recv, device)
        when = self.all_of(when)
        if when is None:
            copy.wait_recv()
        else:
            pl.when(when())(copy.wait_recv)

    def drain(self):
        here = {"rep": lax.axis_index("rep"), "shard": lax.axis_index("shard")}
        for sem, sample, when in self.open:
            copy = self.copy(sample, sample, sem, self.sems.at[sem], here)
            if when is None:
                copy.wait_send()
            else:
                pl.when(when())(copy.wait_send)
        self.open = []


def greet_all(g):
    barrier = pltpu.get_barrier_semaphore()
    me = g.r * g.shards + g.z

    def one(step, carry):
        peer = (me + step) % g.devices
        pl.semaphore_signal(
            barrier,
            inc=1,
            device_id=g.device(peer // g.shards, peer % g.shards),
            device_id_type=pl.DeviceIdType.MESH,
        )
        return carry

    lax.fori_loop(1, g.devices, one, 0)
    pl.semaphore_wait(barrier, g.devices - 1)


def push_rows(g, src, dst, send_sems, recv_sems):
    me = g.r * g.shards + g.z

    def one(step, carry):
        peer = (me + step) % g.devices
        pltpu.make_async_remote_copy(
            src_ref=src.at[peer],
            dst_ref=dst.at[me],
            send_sem=send_sems.at[step],
            recv_sem=recv_sems.at[step],
            device_id=g.device(peer // g.shards, peer % g.shards),
            device_id_type=pl.DeviceIdType.MESH,
        ).start()
        return carry

    lax.fori_loop(1, g.devices, one, 0)


def push_wait(g, src, dst, send_sems, recv_sems):
    me = g.r * g.shards + g.z

    def one(step, carry):
        peer = (me + g.devices - step) % g.devices
        copy = pltpu.make_async_remote_copy(
            src_ref=src.at[peer],
            dst_ref=dst.at[peer],
            send_sem=send_sems.at[step],
            recv_sem=recv_sems.at[step],
            device_id=g.device(peer // g.shards, peer % g.shards),
            device_id_type=pl.DeviceIdType.MESH,
        )
        copy.wait_send()
        copy.wait_recv()
        return carry

    lax.fori_loop(1, g.devices, one, 0)


class PlaneGather:
    def __init__(self, g, s, view, lr, hr, dr, cr):
        self.g, self.s, self.view = g, s, view
        self.lr, self.hr, self.dr, self.cr = lr, hr, dr, cr

    @staticmethod
    def scratch(g, units):
        dma, others = pltpu.SemaphoreType.DMA, max(1, g.los - 1)
        return [dma((units, 2, others)), dma((units, 2)), dma((units, 2, others)), dma((units, 5 * g.los))]

    @staticmethod
    def sends(g, units):
        return 9 * g.los * units

    def at(self, hi, lo):
        return self.g.device(self.g.rep_of(hi, lo, self.g.core), self.g.z)

    def partner(self):
        g = self.g
        return g.device(g.rep_of(g.hi, g.lo, 1 - g.core), g.z)

    def own(self, u, src=None):
        g, s = self.g, self.s

        def dst(part):
            return self.view(u, g.hi, g.lo, g.core, part)

        src = src or dst
        for part in (0, 1):
            for step in range(1, g.los):
                s.start(src(part), dst(part), self.lr.at[u, part, step - 1], self.at(g.hi, g.other_lo(step)))
            s.start(src(1 - part), dst(1 - part), self.hr.at[u, 1 - part], self.at(1 - g.hi, g.lo))
        s.start(src(None), dst(None), self.cr.at[u, 0], self.partner())

    def take(self, u, hi, lo, part, recv, frm, partner_slot, onward=()):
        ref = self.view(u, hi, lo, self.g.core, part)
        self.s.arrived(ref, recv, frm)
        for sem, device in onward:
            self.s.start(ref, ref, sem, device)
        self.s.start(ref, ref, self.cr.at[u, partner_slot], self.partner())

    def first(self, u):
        g = self.g
        far = 1 - g.hi
        for step in range(1, g.los):
            frm = (g.lo + g.los - step) % g.los
            onward = [(self.dr.at[u, 0, step - 1], self.at(far, g.lo))]
            self.take(u, g.hi, frm, 0, self.lr.at[u, 0, step - 1], self.at(g.hi, frm), 5 * step, onward)
        onward = [(self.dr.at[u, 1, step - 1], self.at(g.hi, g.other_lo(step))) for step in range(1, g.los)]
        self.take(u, far, g.lo, 1, self.hr.at[u, 1], self.at(far, g.lo), 1, onward)
        for step in range(1, g.los):
            frm = (g.lo + g.los - step) % g.los
            self.take(u, g.hi, frm, 1, self.lr.at[u, 1, step - 1], self.at(g.hi, frm), 5 * step + 1)
        self.take(u, far, g.lo, 0, self.hr.at[u, 0], self.at(far, g.lo), 2)

    def second(self, u):
        g = self.g
        far = 1 - g.hi
        for step in range(1, g.los):
            frm = (g.lo + g.los - step) % g.los
            self.take(u, far, frm, 0, self.dr.at[u, 0, step - 1], self.at(far, g.lo), 5 * step + 2)
            self.take(u, far, frm, 1, self.dr.at[u, 1, step - 1], self.at(g.hi, frm), 5 * step + 3)

    def from_partner(self, u):
        g = self.g
        far, other = 1 - g.hi, 1 - g.core

        def got(hi, lo, part, slot):
            self.s.arrived(self.view(u, hi, lo, other, part), self.cr.at[u, slot], self.partner())

        got(g.hi, g.lo, None, 0)
        got(far, g.lo, 1, 1)
        got(far, g.lo, 0, 2)
        for step in range(1, g.los):
            frm = (g.lo + g.los - step) % g.los
            got(g.hi, frm, 0, 5 * step)
            got(g.hi, frm, 1, 5 * step + 1)
            got(far, frm, 0, 5 * step + 2)
            got(far, frm, 1, 5 * step + 3)


def add_rows(dst, *srcs, step=16):
    def one(i, carry):
        at = pl.ds(pl.multiple_of(i * step, step), step)
        total = srcs[0][at, :].astype(f32)
        for src in srcs[1:]:
            total = total + src[at, :].astype(f32)
        dst[at, :] = total.astype(dst.dtype)
        return carry

    lax.fori_loop(0, dst.shape[0] // step, one, 0)


class PlaneScatter:
    def __init__(self, g, s, p, cut, own, ra, rb0, rb1, rc0, rc1, sa, sb0, sb1, sc0, sc1, ls):
        self.g, self.s, self.p, self.cut, self.owned = g, s, p, cut, own
        self.ra, self.rb0, self.rb1, self.rc0, self.rc1 = ra, rb0, rb1, rc0, rc1
        self.sa, self.sb0, self.sb1, self.sc0, self.sc1, self.ls = sa, sb0, sb1, sc0, sc1, ls

    @staticmethod
    def scratch(g, units, block, halves, dtype):
        dma, others, v = pltpu.SemaphoreType.DMA, max(1, g.los - 1), pltpu.VMEM
        first, second = halves
        return [
            v((units, g.places) + block, dtype),
            v((units, g.places) + block, dtype),
            v((units, g.los) + first, dtype),
            v((units, others, 2) + second, dtype),
            v((units, others) + first, dtype),
            v((units,) + second, dtype),
            dma((units,)),
            dma((units,)),
            dma((units, others, 2)),
            dma((units, others)),
            dma((units,)),
            dma((units,)),
        ]

    @staticmethod
    def sends(g, units):
        return units * (3 * g.los + 2)

    def at(self, hi, lo):
        return self.g.device(self.g.rep_of(hi, lo, self.g.core), self.g.z)

    def partner(self):
        g = self.g
        return g.device(g.rep_of(g.hi, g.lo, 1 - g.core), g.z)

    def load(self, units):
        self.loads = []
        for turn in range(units):
            load = pltpu.make_async_copy(self.p(turn, self.g.core), self.owned.at[turn], self.ls.at[turn])
            load.start()
            self.loads.append(load)

    def to_partner(self, turn):
        self.s.start(self.p(turn, 1 - self.g.core), self.ra.at[turn], self.sa.at[turn], self.partner())

    def half(self, turn, place, part):
        return self.owned.at[(turn, place) + self.cut(part)]

    def mine(self, turn):
        return self.owned.at[turn, self.g.hi * self.g.los + self.g.lo]

    def a(self, turn, waited=False):
        g, s = self.g, self.s
        far = 1 - g.hi
        if self.loads[turn] is not None:
            self.loads[turn].wait()
        if not waited:
            s.arrived(self.ra.at[turn], self.sa.at[turn], self.partner())

        def one(q, carry):
            line = self.owned.at[turn, q]
            add_rows(line, line, self.ra.at[turn, q])
            return carry

        lax.fori_loop(0, g.places, one, 0)
        block = self.owned.at[(turn, pl.ds(far * g.los, g.los)) + self.cut(0)]
        s.start(block, self.rb0.at[turn], self.sb0.at[turn], self.at(far, g.lo))
        for step in range(1, g.los):
            to = g.other_lo(step)
            for hi in range(2):
                sem = self.sb1.at[turn, step - 1, hi]
                s.start(self.half(turn, hi * g.los + to, 1), self.rb1.at[turn, step - 1, hi], sem, self.at(g.hi, to))

    def b(self, turn):
        g, s = self.g, self.s
        far = 1 - g.hi
        s.arrived(self.rb0.at[turn], self.sb0.at[turn], self.at(far, g.lo))
        for lo in range(g.los):
            line = self.half(turn, g.hi * g.los + lo, 0)
            add_rows(line, line, self.rb0.at[turn, lo])
        for step in range(1, g.los):
            to = g.other_lo(step)
            sem = self.sc0.at[turn, step - 1]
            s.start(self.half(turn, g.hi * g.los + to, 0), self.rc0.at[turn, step - 1], sem, self.at(g.hi, to))
        for step in range(1, g.los):
            frm = (g.lo + g.los - step) % g.los
            for hi in range(2):
                s.arrived(self.rb1.at[turn, step - 1, hi], self.sb1.at[turn, step - 1, hi], self.at(g.hi, frm))
        for hi in range(2):
            line = self.half(turn, hi * g.los + g.lo, 1)
            add_rows(line, line, *[self.rb1.at[turn, step, hi] for step in range(g.los - 1)])
        s.start(self.half(turn, far * g.los + g.lo, 1), self.rc1.at[turn], self.sc1.at[turn], self.at(far, g.lo))

    def c(self, turn):
        g, s = self.g, self.s
        place = g.hi * g.los + g.lo
        for step in range(1, g.los):
            frm = (g.lo + g.los - step) % g.los
            s.arrived(self.rc0.at[turn, step - 1], self.sc0.at[turn, step - 1], self.at(g.hi, frm))
        line = self.half(turn, place, 0)
        add_rows(line, line, *[self.rc0.at[turn, step] for step in range(g.los - 1)])
        s.arrived(self.rc1.at[turn], self.sc1.at[turn], self.at(1 - g.hi, g.lo))
        line = self.half(turn, place, 1)
        add_rows(line, line, self.rc1.at[turn])


def pass_along(g, s, zp, src, dst, zr):
    n = g.shards
    right, left = g.device(g.r, jnp.minimum(g.z + 1, n - 1)), g.device(g.r, jnp.maximum(g.z - 1, 0))
    s.start(src, dst, zr.at[zp], right, lambda: (zp <= g.z) & (g.z + 1 < n))
    s.start(src, dst, zr.at[zp], left, lambda: (zp >= g.z) & (g.z > 0))


def send_line(g, s, zp, line, out_ref, rl, rr, sl, sr, last):
    n = g.shards
    left, right = g.device(g.r, jnp.maximum(g.z - 1, 0)), g.device(g.r, jnp.minimum(g.z + 1, n - 1))
    has_left, has_right = g.z > 0, g.z + 1 < n
    if last:
        s.arrived(rl.at[g.z], sl.at[g.z], left, lambda: g.z > 0)
        s.arrived(rr.at[g.z], sr.at[g.z], right, lambda: g.z + 1 < n)

        @pl.when(has_left & has_right)
        def _():
            add_rows(out_ref, line, rl.at[g.z], rr.at[g.z])

        @pl.when(has_left & jnp.logical_not(has_right))
        def _():
            add_rows(out_ref, line, rl.at[g.z])

        @pl.when(has_right & jnp.logical_not(has_left))
        def _():
            add_rows(out_ref, line, rr.at[g.z])
    else:
        onward_right, onward_left = zp > g.z, zp < g.z

        @pl.when(onward_right & has_left)
        def _():
            s.arrived(rl.at[zp], sl.at[zp], left)
            add_rows(line, line, rl.at[zp])

        @pl.when(onward_left & has_right)
        def _():
            s.arrived(rr.at[zp], sr.at[zp], right)
            add_rows(line, line, rr.at[zp])

        s.start(line, rl.at[zp], sl.at[zp], right, lambda: zp > g.z)
        s.start(line, rr.at[zp], sr.at[zp], left, lambda: zp < g.z)


def line_scratch(shards, block, dtype):
    v, dma = pltpu.VMEM, pltpu.SemaphoreType.DMA
    return [v((shards,) + block, dtype), v((shards,) + block, dtype), dma((shards,)), dma((shards,))]


def wait_for(copies, k):
    for copy in copies(k):
        copy.wait()


def run_all(steps):
    for step in steps:
        step()


def in_order(tasks, default, tuned, n):
    order = tuned.get(n, default)
    assert sorted(order) == sorted(tasks), "task list"
    for key in order:
        tasks[key]()


def staged(n):
    steps = []
    for turn in range(n + 2):
        if turn < n:
            steps.append(("a", turn))
        if 0 <= turn - 1 < n:
            steps.append(("b", turn - 1))
        if 0 <= turn - 2 < n:
            steps += [("c", turn - 2), ("s", turn - 2)]
    return steps


def sum_steps(n, tiles):
    tuned = tuned_sum.get((n, tiles))
    if tuned is None:
        tuned = [min(tiles, (turn + {"a": 0, "b": 1, "c": 2, "s": 2}[name]) * tiles // n) for name, turn in staged(n)]
    timed = {at: [] for at in range(tiles + 1)}
    for at, step in zip(tuned, staged(n)):
        timed[at].append(step)
    return timed


hbm = pl.BlockSpec(memory_space=pl.ANY)
vmem = pl.BlockSpec(memory_space=pltpu.VMEM)


def params(ident):
    return pltpu.CompilerParams(collective_id=ident, has_side_effects=True, vmem_limit_bytes=vmem_cap)


def scatter_all_kernel(reps, shards, slabbed, *refs):
    if slabbed:
        (
            p_ref, slab_ref, x_ref, c_ref, gg_ref, gu_ref, act_ref, out_ref, slabs_ref, wg_ref, wu_ref, wd_ref,
            xt, ct, og, ou, od, tile_sems, out_sems, *rest,
        ) = refs
    else:
        p_ref, out_ref, *rest = refs
    sems, ps, pr, slab_sem, *rest = rest
    g = Grid(reps, shards).here()
    s = Sends(sems)
    n = g.shards
    scatter = ScatterAll(g, s, p_ref, out_ref, *rest)
    half = pl.ds(0, out_ref.shape[0] // 2)
    own = scatter.plane.owned
    s.samples = [own.at[0, 0], own.at[0, 0, half], own.at[0, pl.ds(0, g.los), half]]
    scatter.load()
    if not slabbed:
        greet_all(g)
        scatter.to_partner()
        for name, turn in staged(n):
            scatter.stage(name, turn)
        s.drain()
        return

    tile = xt.shape[2]
    tiles = x_ref.shape[1] // tile

    def tile_in(j, slot):
        span = pl.ds(pl.multiple_of(j * tile, tile), tile)
        return [
            pltpu.make_async_copy(x_ref.at[:, span], xt.at[slot], tile_sems.at[slot, 0]),
            pltpu.make_async_copy(c_ref.at[:, span], ct.at[slot], tile_sems.at[slot, 1]),
        ]

    def tile_out(j):
        span = pl.ds(pl.multiple_of(j * tile, tile), tile)
        return [
            pltpu.make_async_copy(og, wg_ref.at[span, :], out_sems.at[0]),
            pltpu.make_async_copy(ou, wu_ref.at[span, :], out_sems.at[1]),
            pltpu.make_async_copy(od, wd_ref.at[:, span], out_sems.at[2]),
        ]

    for copy in tile_in(0, 0):
        copy.start()
    greet_all(g)
    scatter.to_partner()
    push_rows(g, slab_ref, slabs_ref, ps, pr)
    me = g.r * n + g.z
    keep_slab = pltpu.make_async_copy(slab_ref.at[me], slabs_ref.at[me], slab_sem.at[0])
    keep_slab.start()

    timed = sum_steps(n, tiles)

    def next_tiles(j):
        for copy in tile_in(j + 1, (j + 1) % 2):
            copy.start()

    def weight_grads(j, carry):
        for at, steps in timed.items():
            if at < tiles:
                pl.when(j == at)(functools.partial(run_all, [functools.partial(scatter.stage, *step) for step in steps]))
        pl.when(j + 1 < tiles)(functools.partial(next_tiles, j))
        slot = j % 2
        for copy in tile_in(j, slot):
            copy.wait()
        pl.when(j > 0)(functools.partial(wait_for, tile_out, j))
        og[...] = t_dot(xt[slot], gg_ref[...])
        ou[...] = t_dot(xt[slot], gu_ref[...])
        od[...] = t_dot(act_ref[...], ct[slot])
        for copy in tile_out(j):
            copy.start()
        return carry

    lax.fori_loop(0, tiles, weight_grads, 0)
    for step in timed[tiles]:
        scatter.stage(*step)
    wait_for(tile_out, 0)
    keep_slab.wait()
    push_wait(g, slab_ref, slabs_ref, ps, pr)
    s.drain()


def scatter_all(reps, shards, p, slab, fill, ident):
    g = Grid(reps, shards)
    n = shards
    _, rows, width = p.shape
    dma, v = pltpu.SemaphoreType.DMA, pltpu.VMEM
    slabbed = slab is not None
    out_shape = (jax.ShapeDtypeStruct((rows, width), f32),)
    out_specs, in_specs, extra, scratch = (vmem,), [hbm], [], []
    if slabbed:
        x, c, gg, gu, act = fill
        count, wide = x.shape
        inner = gg.shape[1]
        tile = 256
        narrow = jax.ShapeDtypeStruct((wide, inner), f32)
        out_shape += (
            jax.ShapeDtypeStruct(slab.shape, slab.dtype), narrow, narrow, jax.ShapeDtypeStruct((inner, wide), f32)
        )
        out_specs += (vmem, hbm, hbm, hbm)
        in_specs += [vmem, hbm, hbm, vmem, vmem, vmem]
        extra = [slab, *fill]
        scratch = [
            v((2, count, tile), bf16), v((2, count, tile), bf16),
            v((tile, inner), f32), v((tile, inner), f32), v((inner, tile), f32),
            dma((2, 2)), dma((3,)),
        ]
    done = pl.pallas_call(
        functools.partial(scatter_all_kernel, reps, shards, slabbed),
        out_shape=out_shape,
        in_specs=in_specs,
        out_specs=out_specs,
        scratch_shapes=scratch
        + [dma((ScatterAll.sends(g),)), dma((g.devices,)), dma((g.devices,)), dma((1,))]
        + ScatterAll.scratch(g, (rows, width), p.dtype),
        compiler_params=params(ident),
        name="scatter_all",
    )(p.reshape(g.places, 2, n, rows, width), *extra)
    return done if slabbed else done[0]


def scatter_wide(reps, shards, p, slab, fill, ident, chunks):
    if chunks == 1:
        return scatter_all(reps, shards, p, slab, fill, ident)
    step = p.shape[2] // chunks
    parts = [
        scatter_all(reps, shards, p[:, :, i * step : (i + 1) * step], slab if i == 0 else None, fill, ident + i)
        for i in range(chunks)
    ]
    if slab is None:
        return jnp.concatenate(parts, axis=1)
    first, *others = parts[0]
    return jnp.concatenate([first] + parts[1:], axis=1), *others


def deliver_kernel(reps, shards, split, *refs):
    (
        gqkv_ref, small_ref, qsum_ref, ksum_ref, wo_sum_ref, w_in, hid_in, xs_in,
        out_ref, q_out, rest_out, wo_out,
        w_ref, hid_ref, xs_ref, both, acc, ws_ref, wo_all, line_own, rl, rr, sl, sr,
        sems, wr, small_sem, keep_sem, ls, *rest,
    ) = refs
    q_cols, experts, part = split
    g = Grid(reps, shards).here()
    s = Sends(sems)
    n, places = g.shards, g.places
    gather_refs, wo_refs, scatter_refs = rest[:4], rest[4:8], rest[8:]
    length = out_ref.shape[0]
    total, cols = ws_ref.shape[-1], gqkv_ref.shape[1]
    piece = ws_ref.shape[2]
    deep = hid_ref.shape[1] // n
    first = total // 2 // 128 * 128
    spans = {0: pl.ds(0, first), 1: pl.ds(first, total - first), None: pl.ds(0, total)}
    owned = wo_sum_ref.shape[0]
    halves = {0: pl.ds(0, owned // 2), 1: pl.ds(owned // 2, owned // 2), None: pl.ds(0, owned)}
    order = g.nearest()[::-1]
    scatter = PlaneScatter(g, s, None, lambda p: (slice(None), spans[p]), both.at[g.core], *scatter_refs)
    scatter.loads = [None] * n
    gather = PlaneGather(
        g, s, lambda u, hi, lo, core, p: ws_ref.at[u, g.rep_of(hi, lo, core), :, spans[p]], *gather_refs
    )
    out_weight = PlaneGather(g, s, lambda u, hi, lo, core, p: wo_all.at[g.rep_of(hi, lo, core), halves[p]], *wo_refs)
    loads = [
        pltpu.make_async_copy(hid_in, hid_ref, ls.at[0]),
        pltpu.make_async_copy(w_in, w_ref, ls.at[1]),
        pltpu.make_async_copy(xs_in, xs_ref, ls.at[2]),
    ]
    for copy in loads:
        copy.start()
    barrier = pltpu.get_barrier_semaphore()
    peers = [g.device(g.r, (g.z + step) % n) for step in range(1, n)]
    peers += [g.device(g.rep_of(g.hi, g.other_lo(step), g.core), g.z) for step in range(1, g.los)]
    peers += [g.device(g.rep_of(1 - g.hi, g.lo, g.core), g.z), g.device(g.rep_of(g.hi, g.lo, 1 - g.core), g.z)]
    for peer in peers:
        pl.semaphore_signal(barrier, inc=1, device_id=peer, device_id_type=pl.DeviceIdType.MESH)
    pl.semaphore_wait(barrier, len(peers))
    out_weight.own(0, lambda p: wo_sum_ref.at[halves[p]])

    ra = scatter.ra
    tail = pl.ds(cols, total - cols)

    def projection(zp):
        if zp == 0:
            loads[0].wait()
        grad = t_dot(hid_ref[:, zp * deep : (zp + 1) * deep], gqkv_ref[...]).astype(bf16)
        for place in range(places):
            for core in range(2):
                row = (place * 2 + core) * piece
                both[core, zp, place, :, 0:cols] = grad[row : row + piece]
        src = both.at[1 - g.core, zp, :, :, pl.ds(0, cols)]
        s.start(src, ra.at[zp, :, :, pl.ds(0, cols)], scatter.sa.at[zp], scatter.partner())

    def share(turn):
        if turn == 0:
            loads[1].wait()
            loads[2].wait()
            acc[...] = small_ref[...]
        lane = lax.broadcasted_iota(jnp.int32, (length, total - cols), 1)
        marked = jnp.where(lane == experts, 1.0, 0.0).astype(bf16)
        at = pl.ds(pl.multiple_of(order[turn] * length, length), length)
        grad = dot_t(gqkv_ref[at, :], w_ref[...])
        line_own[turn] = grad.astype(bf16)
        _, unit = unit_of(xs_ref[at, :].astype(f32))
        acc[...] += t_dot((grad * unit).astype(bf16), marked)

    def small_grads():
        for i, ref in ((2, qsum_ref), (3, ksum_ref)):
            width = ref.shape[1]
            columns = jnp.broadcast_to(ref[...], (total - cols, width)).T
            mask = lax.broadcasted_iota(jnp.int32, (part, total - cols), 1) == experts + i
            for zp in range(n):
                acc[zp * deep : zp * deep + part] += jnp.where(mask, columns[zp * part : (zp + 1) * part], 0.0)
        for zp in range(n):
            for place in range(places):
                for core in range(2):
                    row = zp * deep + (place * 2 + core) * piece
                    both[core, zp, place, :, cols:total] = acc[row : row + piece].astype(bf16)
        s.start(both.at[1 - g.core, :, :, :, tail], ra.at[:, :, :, tail], small_sem.at[0], scatter.partner())

    def line(turn):
        send_line(g, s, order[turn], line_own.at[turn], out_ref, rl, rr, sl, sr, last=turn == n - 1)

    def from_partner(turn):
        if turn == 0:
            s.arrived(ra.at[:, :, :, tail], small_sem.at[0], scatter.partner())
        s.arrived(ra.at[turn, :, :, pl.ds(0, cols)], scatter.sa.at[turn], scatter.partner())
        scatter.a(turn, waited=True)

    def owner(turn):
        scatter.c(turn)
        dst = ws_ref.at[g.z, g.r]
        keep = pltpu.make_async_copy(scatter.mine(turn), dst, keep_sem.at[0])
        pl.when(g.z == turn)(keep.start)
        s.start(scatter.mine(turn), dst, wr.at[g.z], g.device(g.r, turn), lambda: g.z != turn)
        pl.when(g.z == turn)(keep.wait)

    saves = [pltpu.make_async_copy(wo_all, wo_out, ls.at[3])]

    def weight_done():
        out_weight.from_partner(0)
        keep = pltpu.make_async_copy(wo_sum_ref, wo_all.at[g.r], keep_sem.at[0])
        keep.start()
        keep.wait()
        saves[0].start()

    def unit_at(step):
        return (g.z + n - step) % n

    def hand_out(step):
        u = unit_at(step)
        if step:
            s.arrived(ws_ref.at[u, g.r], wr.at[u], g.device(g.r, u))
        gather.own(u)

    def save(step):
        u = unit_at(step)
        gather.from_partner(u)
        q_span = pl.ds(pl.multiple_of(u * q_cols, 128), q_cols)
        rest_span = pl.ds(q_cols, total - q_cols)
        pair = [
            pltpu.make_async_copy(ws_ref.at[u, :, :, pl.ds(0, q_cols)], q_out.at[:, :, q_span], ls.at[4 + 2 * step]),
            pltpu.make_async_copy(ws_ref.at[u, :, :, rest_span], rest_out.at[u], ls.at[5 + 2 * step]),
        ]
        for copy in pair:
            copy.start()
        saves.extend(pair)

    tasks = {
        ("sm", 0): small_grads,
        ("of", 0): functools.partial(out_weight.first, 0),
        ("os", 0): functools.partial(out_weight.second, 0),
        ("op", 0): weight_done,
    }
    for k in range(n):
        tasks["wi", k] = functools.partial(projection, k)
        tasks["pt", k] = functools.partial(share, k)
        tasks["l", k] = functools.partial(line, k)
        tasks["a", k] = functools.partial(from_partner, k)
        tasks["b", k] = functools.partial(scatter.b, k)
        tasks["o", k] = functools.partial(owner, k)
        tasks["u", k] = functools.partial(hand_out, k)
        tasks["f", k] = functools.partial(gather.first, unit_at(k))
        tasks["s", k] = functools.partial(gather.second, unit_at(k))
        tasks["p", k] = functools.partial(save, k)
    default = [("wi", k) for k in range(n)] + [("pt", 0), ("l", 0)] + [("pt", k) for k in range(1, n)] + [("sm", 0)]
    for turn in range(n + 2):
        if turn < n:
            default.append(("a", turn))
        if turn < 2:
            default.append((("of", "os")[turn], 0))
        if 0 <= turn - 1 < n:
            default.append(("b", turn - 1))
        if 1 <= turn < n - 1:
            default.append(("l", turn))
        if 0 <= turn - 2 < n:
            default.append(("o", turn - 2))
    default += [("op", 0), ("u", 0)]
    for k in range(1, n):
        default += [("u", k), ("f", k - 1)]
        if k > 1:
            default.append(("s", k - 2))
    default += [("f", n - 1), ("s", n - 2), ("s", n - 1), ("l", n - 1)] + [("p", k) for k in range(n)]
    in_order(tasks, default, tuned_deliver, n)
    for copy in saves:
        copy.wait()
    s.drain()


def deliver(reps, shards, q_cols, experts, part, gqkv, small, qsum, ksum, wo_sum, w, hid, xs, ident):
    g = Grid(reps, shards)
    n = shards
    dma, v = pltpu.SemaphoreType.DMA, pltpu.VMEM
    width = hid.shape[1]
    rows = hid.shape[0] // n
    cols = gqkv.shape[1]
    total = cols + small.shape[1]
    piece = width // n // reps
    first = total // 2 // 128 * 128
    return pl.pallas_call(
        functools.partial(deliver_kernel, reps, shards, (q_cols, experts, part)),
        out_shape=(
            jax.ShapeDtypeStruct((rows, width), f32),
            jax.ShapeDtypeStruct((reps, piece, n * q_cols), bf16),
            jax.ShapeDtypeStruct((n, reps, piece, total - q_cols), bf16),
            jax.ShapeDtypeStruct((reps,) + wo_sum.shape, bf16),
        ),
        in_specs=[vmem] * 5 + [hbm] * 3,
        out_specs=(vmem, hbm, hbm, hbm),
        scratch_shapes=[
            v(w.shape, bf16),
            v(hid.shape, bf16),
            v(xs.shape, bf16),
            v((2, n, g.places, piece, total), bf16),
            v(small.shape, f32),
            v((n, reps, piece, total), bf16),
            v((reps,) + wo_sum.shape, bf16),
            v((n, rows, width), bf16),
        ]
        + line_scratch(n, (rows, width), bf16)
        + [
            dma((PlaneGather.sends(g, n) + PlaneGather.sends(g, 1) + PlaneScatter.sends(g, n) + 4 * n + 1,)),
            dma((n,)),
            dma((1,)),
            dma((1,)),
            dma((4 + 2 * n,)),
        ]
        + PlaneGather.scratch(g, n)
        + PlaneGather.scratch(g, 1)
        + PlaneScatter.scratch(g, n, (piece, total), ((piece, first), (piece, total - first)), bf16)[1:],
        compiler_params=params(ident),
        name="deliver",
    )(gqkv, small, qsum, ksum, wo_sum, w, hid, xs)


def turned(x, cosine, sine):
    return x * cosine + pltpu.roll(x, x.shape[-1] // 2, 1) * sine


def mean_last(x):
    return jnp.sum(x, axis=-1, keepdims=True) * (1.0 / x.shape[-1])


def unit_of(x):
    inverse = lax.rsqrt(mean_last(x * x) + epsilon)
    return inverse, x * inverse


def dot_t(a, b):
    return lax.dot_general(a, b, (((1,), (1,)), ((), ())), preferred_element_type=f32)


def t_dot(a, b):
    return lax.dot_general(a, b, (((0,), (0,)), ((), ())), preferred_element_type=f32)


def softmax_rows(q_rot, k_rot, bias, head_dim):
    scores = dot_t(q_rot, k_rot) * head_dim ** (-0.5) + bias
    raised = jnp.exp(scores - jnp.max(scores, axis=-1, keepdims=True))
    return raised * (1.0 / jnp.sum(raised, axis=-1, keepdims=True))


def back_unit(grad_scaled, unit, inverse, gain):
    gained = grad_scaled * gain
    return inverse * (gained - unit * mean_last(gained * unit))


def attend_block(b, heads, x_ref, w_ref, wo_ref, gain_ref, qg_ref, kg_ref, cos_ref, sin_ref, bias_ref, hid_ref, qkv_ref, att_ref, line):
    my_heads, my_kv, head_dim = heads
    x = x_ref[b].astype(f32)
    _, unit = unit_of(x)
    hid_ref[b] = (unit * gain_ref[...]).astype(bf16)
    qkv_ref[b] = jnp.dot(hid_ref[b], w_ref[...], preferred_element_type=f32)
    cosine, sine, bias = cos_ref[b], sin_ref[b], bias_ref[b]
    group = my_heads // my_kv
    for n in range(my_kv):
        at_k = (my_heads + n) * head_dim
        at_v = (my_heads + my_kv + n) * head_dim
        _, k_unit = unit_of(qkv_ref[b, :, at_k : at_k + head_dim])
        k_rot = turned(k_unit * kg_ref[...], cosine, sine).astype(bf16)
        values = qkv_ref[b, :, at_v : at_v + head_dim].astype(bf16)
        for h in range(n * group, (n + 1) * group):
            span = slice(h * head_dim, (h + 1) * head_dim)
            _, q_unit = unit_of(qkv_ref[b, :, span])
            q_rot = turned(q_unit * qg_ref[...], cosine, sine).astype(bf16)
            probs = softmax_rows(q_rot, k_rot, bias, head_dim)
            mixed = jnp.dot(probs.astype(bf16), values, preferred_element_type=f32)
            att_ref[b, :, span] = mixed.astype(bf16)
    line[...] = jnp.dot(att_ref[b], wo_ref[...], preferred_element_type=f32).astype(bf16)


def attend_back_block(b, heads, ga_ref, qkv_ref, wo_ref, qg_ref, kg_ref, cos_ref, sin_ref, bias_ref, gm_ref, gqkv_ref, qsum_ref, ksum_ref):
    my_heads, my_kv, head_dim = heads
    gm_ref[...] = dot_t(ga_ref[b], wo_ref[...]).astype(bf16)
    cosine, sine, bias = cos_ref[b], sin_ref[b], bias_ref[b]
    group = my_heads // my_kv
    qg, kg = qg_ref[...], kg_ref[...]
    for n in range(my_kv):
        at_k = (my_heads + n) * head_dim
        at_v = (my_heads + my_kv + n) * head_dim
        k_inverse, k_unit = unit_of(qkv_ref[b, :, at_k : at_k + head_dim])
        k_rot = turned(k_unit * kg, cosine, sine).astype(bf16)
        values = qkv_ref[b, :, at_v : at_v + head_dim].astype(bf16)
        grad_k = jnp.zeros(k_unit.shape, f32)
        grad_v = jnp.zeros(k_unit.shape, f32)
        for h in range(n * group, (n + 1) * group):
            span = slice(h * head_dim, (h + 1) * head_dim)
            q_inverse, q_unit = unit_of(qkv_ref[b, :, span])
            q_rot = turned(q_unit * qg, cosine, sine).astype(bf16)
            probs = softmax_rows(q_rot, k_rot, bias, head_dim)
            grad_mixed = gm_ref[:, span]
            grad_weights = dot_t(grad_mixed, values)
            centre = jnp.sum(probs * grad_weights, axis=-1, keepdims=True)
            grad_scores = (probs * (grad_weights - centre) * head_dim ** (-0.5)).astype(bf16)
            grad_v = grad_v + t_dot(probs.astype(bf16), grad_mixed)
            grad_k = grad_k + t_dot(grad_scores, q_rot)
            grad_q = jnp.dot(grad_scores, k_rot, preferred_element_type=f32)
            grad_q = turned(grad_q, cosine, -sine)
            qsum_ref[...] += jnp.sum(grad_q * q_unit, axis=0, keepdims=True)
            gqkv_ref[b, :, span] = back_unit(grad_q, q_unit, q_inverse, qg).astype(bf16)
        grad_k = turned(grad_k, cosine, -sine)
        ksum_ref[...] += jnp.sum(grad_k * k_unit, axis=0, keepdims=True)
        gqkv_ref[b, :, at_k : at_k + head_dim] = back_unit(grad_k, k_unit, k_inverse, kg).astype(bf16)
        gqkv_ref[b, :, at_v : at_v + head_dim] = grad_v.astype(bf16)


class GatherAll:
    def __init__(self, g, s, x_ref, out_ref, zr, plane_sems):
        self.g, self.s, self.x_ref, self.out_ref, self.zr = g, s, x_ref, out_ref, zr
        half = x_ref.shape[0] // 2
        self.spans = {0: pl.ds(0, half), 1: pl.ds(half, half), None: pl.ds(0, 2 * half)}
        self.order = g.nearest()
        self.plane = PlaneGather(g, s, self.view, *plane_sems)

    @staticmethod
    def scratch(g):
        dma = pltpu.SemaphoreType.DMA
        return [dma((g.shards,))] + PlaneGather.scratch(g, g.shards)

    @staticmethod
    def sends(g):
        return PlaneGather.sends(g, g.shards) + 2 * g.shards

    def view(self, u, hi, lo, core, part):
        return self.out_ref.at[self.g.rep_of(hi, lo, core) * self.g.shards + u, self.spans[part]]

    def own(self):
        g = self.g
        return self.view(g.z, g.hi, g.lo, g.core, None)

    def line(self, turn):
        g, zp = self.g, self.order[turn]
        dst = self.view(zp, g.hi, g.lo, g.core, None)
        if turn:
            self.s.arrived(dst, self.zr.at[zp], g.device(g.r, zp))
        pass_along(g, self.s, zp, dst if turn else self.x_ref, dst, self.zr)
        self.plane.own(zp, None if turn else lambda part: self.x_ref.at[self.spans[part]])

    def first(self, turn):
        self.plane.first(self.order[turn])

    def second(self, turn):
        self.plane.second(self.order[turn])

    def finish(self):
        for turn in range(self.g.shards):
            self.plane.from_partner(self.order[turn])


class ScatterAll:
    def __init__(self, g, s, p_ref, out_ref, rl, rr, sl, sr, *plane_refs):
        self.g, self.s, self.out_ref = g, s, out_ref
        self.lines = (rl, rr, sl, sr)
        half = out_ref.shape[0] // 2
        self.order = g.nearest()[::-1]
        self.plane = PlaneScatter(
            g,
            s,
            lambda turn, core: p_ref.at[:, core, self.order[turn]],
            lambda part: (pl.ds(part * half, half),),
            *plane_refs,
        )

    @staticmethod
    def scratch(g, block, dtype):
        rows, width = block
        half = (rows // 2, width)
        return line_scratch(g.shards, block, dtype) + PlaneScatter.scratch(g, g.shards, block, (half, half), dtype)

    @staticmethod
    def sends(g):
        return PlaneScatter.sends(g, g.shards) + 2 * g.shards

    def load(self):
        self.plane.load(self.g.shards)

    def to_partner(self):
        for turn in range(self.g.shards):
            self.plane.to_partner(turn)

    def stage(self, name, turn):
        if name == "s":
            last = turn == self.g.shards - 1
            line = self.plane.mine(turn)
            send_line(self.g, self.s, self.order[turn], line, self.out_ref, *self.lines, last=last)
        else:
            getattr(self.plane, name)(turn)


def attend_back_kernel(reps, shards, heads, *refs):
    (
        ga_ref, qg_ref, kg_ref, cos_ref, sin_ref, bias_ref, qkv_in, wo_in, att_in, p_ref,
        gqkv_ref, qsum_ref, ksum_ref, out_ref, wo_sum_ref,
        gas_ref, qkv_ref, wo_ref, att_ref, both, gm, zr, sems, ls, *scatter_refs,
    ) = refs
    g = Grid(reps, shards).here()
    s = Sends(sems)
    n, rows = g.shards, ga_ref.shape[0]
    half = both.shape[3] // 2
    count = len(scatter_refs) - 11
    scatter = ScatterAll(g, s, p_ref, out_ref, *scatter_refs[:count])
    own = both.at[g.core]
    owner = PlaneScatter(
        g, s, lambda turn, core: both.at[core, turn], lambda part: (pl.ds(part * half, half),), own, *scatter_refs[count:]
    )
    scatter.load()
    loads = [
        pltpu.make_async_copy(wo_in, wo_ref, ls.at[0]),
        pltpu.make_async_copy(qkv_in, qkv_ref, ls.at[1]),
        pltpu.make_async_copy(att_in, att_ref, ls.at[2]),
    ]
    keep = pltpu.make_async_copy(ga_ref, gas_ref.at[g.z], ls.at[3])
    for copy in loads + [keep]:
        copy.start()
    qsum_ref[...] = jnp.zeros(qsum_ref.shape, f32)
    ksum_ref[...] = jnp.zeros(ksum_ref.shape, f32)
    greet_all(g)
    order = g.nearest()

    def line(turn):
        zp = order[turn]
        dst = gas_ref.at[zp]
        if turn:
            s.arrived(dst, zr.at[zp], g.device(g.r, zp))
        pass_along(g, s, zp, dst if turn else ga_ref, dst, zr)

    def out_weight():
        width = ga_ref.shape[1]
        block = att_ref.shape[2] // g.reps
        grads = gas_ref[...].reshape(n * rows, width)
        for place in range(g.places):
            for core in range(2):
                at = (place * 2 + core) * block
                mixed = att_ref[:, :, at : at + block].reshape(n * rows, block)
                both[core, 0, place] = t_dot(mixed, grads).astype(bf16)

    line(0)
    scatter.to_partner()
    for copy in loads + [keep]:
        copy.wait()
    owner.loads = [None]

    def block(turn):
        attend_back_block(
            order[turn], heads, gas_ref, qkv_ref, wo_ref, qg_ref, kg_ref, cos_ref, sin_ref, bias_ref,
            gm, gqkv_ref, qsum_ref, ksum_ref,
        )

    def weigh():
        out_weight()
        owner.to_partner(0)

    tasks = {("w", 0): weigh}
    for name in "abc":
        tasks["w" + name, 0] = functools.partial(getattr(owner, name), 0)
    for turn in range(n):
        if turn:
            tasks["l", turn] = functools.partial(line, turn)
        tasks["k", turn] = functools.partial(block, turn)
        for name in "abcs":
            tasks[name, turn] = functools.partial(scatter.stage, name, turn)
    default = []
    for turn in range(n + 2):
        default += [step for step in staged(n) if step[1] + {"a": 0, "b": 1, "c": 2, "s": 2}[step[0]] == turn]
        if turn + 1 < n:
            default.append(("l", turn + 1))
        elif turn + 1 == n:
            default.append(("w", 0))
        if turn < n:
            default.append(("k", turn))
        elif turn == n:
            default.append(("wa", 0))
        else:
            default += [("wb", 0), ("wc", 0)]
    in_order(tasks, default, tuned_back, n)
    wo_sum_ref[...] = own[0, g.hi * g.los + g.lo]
    s.drain()


def attend_back(reps, shards, heads, ga, qkv, wo, att, qg, kg, cosine, sine, bias, p, ident):
    g = Grid(reps, shards)
    dma, v = pltpu.SemaphoreType.DMA, pltpu.VMEM
    n = shards
    rows, width = ga.shape
    out_width = p.shape[2]
    owned = wo.shape[0] // reps
    row = jax.ShapeDtypeStruct(qg.shape, f32)
    block = (owned, width)
    half = (owned // 2, width)
    return pl.pallas_call(
        functools.partial(attend_back_kernel, reps, shards, heads),
        out_shape=(
            jax.ShapeDtypeStruct(qkv.shape, bf16),
            row,
            row,
            jax.ShapeDtypeStruct((rows, out_width), f32),
            jax.ShapeDtypeStruct(block, bf16),
        ),
        in_specs=[vmem] * 6 + [hbm] * 4,
        out_specs=(vmem,) * 5,
        scratch_shapes=[
            v((n, rows, width), bf16),
            v(qkv.shape, f32),
            v(wo.shape, bf16),
            v(att.shape, bf16),
            v((2, 1, g.places) + block, bf16),
            v((rows, wo.shape[0]), bf16),
            dma((n,)),
            dma((ScatterAll.sends(g) + PlaneScatter.sends(g, 1) + 2 * n,)),
            dma((4,)),
        ]
        + ScatterAll.scratch(g, (rows, out_width), p.dtype)
        + PlaneScatter.scratch(g, 1, block, (half, half), bf16)[1:],
        compiler_params=params(ident),
        name="attend_back",
    )(ga, qg, kg, cosine, sine, bias, qkv, wo, att, p.reshape(g.places, 2, n, rows, out_width))


def tables_of(segment_column, segment_row, frequency):
    length = segment_row.shape[1]
    rows = lax.broadcasted_iota(jnp.int32, (length, length), 0).astype(f32)
    columns = lax.broadcasted_iota(jnp.int32, (length, length), 1).astype(f32)
    same = segment_column == segment_row
    first = jnp.min(jnp.where(same, columns, float(length)), axis=1, keepdims=True)
    width = frequency.shape[1]
    place = lax.broadcasted_iota(jnp.int32, (length, width), 0).astype(f32)
    angle = (place - first) * frequency
    second_half = lax.broadcasted_iota(jnp.int32, (length, width), 1) >= width // 2
    sine = jnp.sin(angle)
    bias = jnp.where(same & (columns <= rows), 0.0, masked_score)
    return jnp.cos(angle), jnp.where(second_half, sine, -sine), bias


def front_kernel(reps, shards, heads, layout, *refs):
    (
        x_ref, cot_ref, small_ref, freq_ref, wq_ref, wk_ref, wv_ref, wo_in,
        smalls_ref, gains_ref, qk_ref, cos_ref, sin_ref, bias_ref, out_ref,
        xs_out, w_out, hid_out, qkv_out, att_out, cots_ref,
        xs_ref, w_ref, wo_ref, hid_ref, qkv_ref, att_ref, own, rl, rr, sl, sr,
        sems, xr, mr, wr, ls, out_sems, lr, hr, dr, cr, *gather_sems,
    ) = refs
    g = Grid(reps, shards).here()
    s = Sends(sems)
    n = g.shards
    q_cols, kv_cols, kv_heads, experts = layout
    head_dim = heads[2]
    deep = wq_ref.shape[0]
    piece = deep // g.reps
    cols = q_cols + 2 * kv_cols
    first = cols // 2 // 128 * 128
    spans = {0: pl.ds(0, first), 1: pl.ds(first, cols - first), None: pl.ds(0, cols)}
    mine = pl.ds(pl.multiple_of(g.r * piece, piece), piece)

    def view(u, hi, lo, core, part):
        row = pl.multiple_of(u * deep + g.rep_of(hi, lo, core) * piece, piece)
        return w_ref.at[pl.ds(row, piece), spans[part]]

    def pieces(zp, u):
        row = pl.ds(pl.multiple_of(u * deep + g.r * piece, piece), piece)
        at_q = pl.ds(pl.multiple_of(zp * q_cols, 128), q_cols)
        at_kv = pl.ds(pl.multiple_of(zp * kv_heads // n * head_dim, 128), kv_cols)
        return (
            (wq_ref.at[mine, at_q], w_ref.at[row, pl.ds(0, q_cols)]),
            (wk_ref.at[mine, at_kv], w_ref.at[row, pl.ds(q_cols, kv_cols)]),
            (wv_ref.at[mine, at_kv], w_ref.at[row, pl.ds(q_cols + kv_cols, kv_cols)]),
        )

    plane = PlaneGather(g, s, view, lr, hr, dr, cr)
    gather = GatherAll(g, s, cot_ref, cots_ref, gather_sems[0], gather_sems[1:])
    locals_ = [pltpu.make_async_copy(src, dst, ls.at[i]) for i, (src, dst) in enumerate(pieces(g.z, g.z))]
    keeps = [
        pltpu.make_async_copy(x_ref, xs_ref.at[g.z], ls.at[3]),
        pltpu.make_async_copy(small_ref, smalls_ref.at[g.z], ls.at[4]),
        pltpu.make_async_copy(wo_in, wo_ref, ls.at[5]),
        pltpu.make_async_copy(cot_ref, gather.own(), ls.at[6]),
    ]
    for copy in locals_ + keeps:
        copy.start()
    barrier = pltpu.get_barrier_semaphore()
    peers = [g.device(g.r, (g.z + step) % n) for step in range(1, n)]
    peers += [g.device(g.rep_of(g.hi, g.other_lo(step), g.core), g.z) for step in range(1, g.los)]
    peers += [g.device(g.rep_of(1 - g.hi, g.lo, g.core), g.z), g.device(g.rep_of(g.hi, g.lo, 1 - g.core), g.z)]
    for peer in peers:
        pl.semaphore_signal(barrier, inc=1, device_id=peer, device_id_type=pl.DeviceIdType.MESH)
    pl.semaphore_wait(barrier, len(peers))

    order = g.nearest()

    def unit(step):
        return (g.z + n - step) % n

    def small_line(turn):
        zp = order[turn]
        if turn:
            s.arrived(smalls_ref.at[zp], mr.at[zp], g.device(g.r, zp))
        pass_along(g, s, zp, smalls_ref.at[zp] if turn else small_ref, smalls_ref.at[zp], mr)

    def token_line(turn):
        zp = order[turn]
        here = xs_ref.at[zp]
        if turn:
            s.arrived(here, xr.at[zp], g.device(g.r, zp))
        pass_along(g, s, zp, here if turn else x_ref, here, xr)

    for step in range(1, n):
        zp = (g.z + step) % n
        for i, (src, dst) in enumerate(pieces(zp, g.z)):
            s.start(src, dst, wr.at[step, i], g.device(g.r, zp))
    def own_pieces():
        for copy in locals_:
            copy.wait()
        plane.own(g.z)

    def other_pieces(step):
        u = unit(step)
        for i, (_, dst) in enumerate(pieces(g.z, u)):
            s.arrived(dst, wr.at[step, i], g.device(g.r, u))
        plane.own(u)

    length = x_ref.shape[0]

    def gains():
        for copy in keeps[:3]:
            copy.wait()
        for zp in range(n):
            gains_ref[:, zp * deep : (zp + 1) * deep] = smalls_ref[zp].astype(f32)[experts : experts + 8]
        for i in range(2):
            qk_ref[i : i + 1] = sum(gains_ref[2 + i : 3 + i, zp * deep : zp * deep + head_dim] for zp in range(n))

    def compute(turn):
        zp = order[turn]
        row = gains_ref[4:5, pl.ds(pl.multiple_of(zp * deep, 128), length)]
        column = jnp.broadcast_to(row, (length, length)).T
        cos_ref[zp], sin_ref[zp], bias_ref[zp] = tables_of(column, row, freq_ref[...])
        attend_block(
            zp, heads, xs_ref, w_ref, wo_ref, gains_ref.at[0:1], qk_ref.at[0:1], qk_ref.at[1:2],
            cos_ref, sin_ref, bias_ref, hid_ref, qkv_ref, att_ref, own.at[turn],
        )

    def sums(turn):
        send_line(g, s, order[turn], own.at[turn], out_ref, rl, rr, sl, sr, last=turn == 0)

    outs = [
        pltpu.make_async_copy(w_ref, w_out, out_sems.at[0]),
        pltpu.make_async_copy(xs_ref, xs_out, out_sems.at[1]),
        pltpu.make_async_copy(hid_ref, hid_out, out_sems.at[2]),
        pltpu.make_async_copy(qkv_ref, qkv_out, out_sems.at[3]),
        pltpu.make_async_copy(att_ref, att_out, out_sems.at[4]),
    ]
    tasks = {
        ("w", 0): own_pieces,
        ("g", 0): gains,
        ("co", 0): functools.partial(gather.plane.own, g.z, lambda part: cot_ref.at[gather.spans[part]]),
        ("cz", 0): functools.partial(pass_along, g, s, g.z, cot_ref, gather.own(), gather.zr),
        ("o", 0): functools.partial(run_all, [copy.start for copy in outs[:2]]),
        ("o", 1): functools.partial(run_all, [copy.start for copy in outs[2:]]),
    }
    for k in range(n):
        tasks["m", k] = functools.partial(small_line, k)
        tasks["c", k] = functools.partial(compute, k)
        tasks["r", k] = functools.partial(sums, k)
        tasks["pf", k] = functools.partial(plane.first, unit(k))
        tasks["ps", k] = functools.partial(plane.second, unit(k))
        tasks["pp", k] = functools.partial(plane.from_partner, unit(k))
        tasks["gf", k] = functools.partial(gather.first, k)
        tasks["gs", k] = functools.partial(gather.second, k)
        if k:
            tasks["w", k] = functools.partial(other_pieces, k)
            for name, guard in (("m", g.inside), ("e", g.outside)):
                tasks["x" + name, k] = functools.partial(s.under, guard, functools.partial(token_line, k))
                tasks["gl" + name, k] = functools.partial(s.under, guard, functools.partial(gather.line, k))
    tasks["x", 0] = functools.partial(token_line, 0)
    default = [("m", 0), ("x", 0)] + [("w", k) for k in range(n)] + [("co", 0), ("m", 1), ("xm", 1), ("xe", 1)]
    for k in range(n):
        default.append(("pf", k))
        if k:
            default.append(("ps", k - 1))
        if 2 + k < n - 1:
            default += [("m", 2 + k), ("xm", 2 + k), ("xe", 2 + k)]
        if k == max(0, n - 4):
            default.append(("cz", 0))
    default += [("ps", n - 1)] + [("pp", k) for k in range(n)]
    default += [("m", n - 1), ("g", 0), ("xm", n - 1), ("c", 0), ("xe", n - 1), ("o", 0), ("c", n - 1), ("r", n - 1)]
    default += [("gf", 0), ("glm", 1), ("gle", 1)]
    for k in range(n - 2, 0, -1):
        at = n - 1 - k
        default += [("c", k), ("r", k), ("gs", at - 1), ("gf", at), ("glm", at + 1), ("gle", at + 1)]
    default += [("o", 1), ("gs", n - 2), ("gf", n - 1), ("gs", n - 1), ("r", 0)]
    in_order(tasks, default, tuned_front, n)
    gather.finish()
    for copy in outs + keeps[3:]:
        copy.wait()
    s.drain()


def front(reps, shards, heads, layout, x, cot, small, frequency, wq, wk, wv, wo, ident):
    g = Grid(reps, shards)
    dma, v = pltpu.SemaphoreType.DMA, pltpu.VMEM
    n = shards
    rows, width = x.shape
    head_dim = heads[2]
    cols = layout[0] + 2 * layout[1]
    table = jax.ShapeDtypeStruct((n, rows, head_dim), f32)
    lines = (n, rows, width)
    return pl.pallas_call(
        functools.partial(front_kernel, reps, shards, heads, layout),
        out_shape=(
            jax.ShapeDtypeStruct((n,) + small.shape, bf16),
            jax.ShapeDtypeStruct((8, width), f32),
            jax.ShapeDtypeStruct((8, head_dim), f32),
            table,
            table,
            jax.ShapeDtypeStruct((n, rows, rows), f32),
            jax.ShapeDtypeStruct((rows, width), f32),
            jax.ShapeDtypeStruct(lines, bf16),
            jax.ShapeDtypeStruct((width, cols), bf16),
            jax.ShapeDtypeStruct(lines, bf16),
            jax.ShapeDtypeStruct((n, rows, cols), f32),
            jax.ShapeDtypeStruct((n, rows, wo.shape[0]), bf16),
            jax.ShapeDtypeStruct((g.devices, rows, width), bf16),
        ),
        in_specs=[vmem] * 4 + [hbm] * 4,
        out_specs=(vmem,) * 7 + (hbm,) * 6,
        scratch_shapes=[
            v(lines, bf16),
            v((width, cols), bf16),
            v(wo.shape, bf16),
            v(lines, bf16),
            v((n, rows, cols), f32),
            v((n, rows, wo.shape[0]), bf16),
            v(lines, bf16),
        ]
        + line_scratch(n, (rows, width), bf16)
        + [
            dma((PlaneGather.sends(g, n) + 2 * GatherAll.sends(g) + 11 * n,)),
            dma((n,)),
            dma((n,)),
            dma((n, 3)),
            dma((7,)),
            dma((5,)),
        ]
        + PlaneGather.scratch(g, n)
        + GatherAll.scratch(g),
        compiler_params=params(ident),
        name="front",
    )(x, cot, small, frequency, wq, wk, wv, wo)


def slots_of(slab, capacity):
    length = slab.shape[1]
    member = slab >= 0.0
    earlier = lax.broadcasted_iota(jnp.int32, (length, length), 0) < lax.broadcasted_iota(jnp.int32, (length, length), 1)
    ones = jnp.where(member, 1.0, 0.0).astype(bf16)
    slot = jnp.dot(ones, jnp.where(earlier, 1.0, 0.0).astype(bf16), preferred_element_type=f32)
    slot = jnp.where(member, slot, -1.0)[0:1]
    rows = lax.broadcasted_iota(jnp.int32, (capacity, length), 0).astype(f32)
    return jnp.where(rows == slot, 1.0, 0.0), slab[0:1]


def expert_steps(n):
    base = 2 * n
    steps = [(2, "f", 0), (3, "l", 1), (3, "e", 1), (5, "s", 0)]
    steps += [(7, "l", 2), (7, "e", 2)] * (n > 2) + [(base, "f", 1)]
    for turn in range(n):
        if 0 < turn < n - 1:
            steps.append((base + 2 * turn, "s", turn))
        at = base + 2 * turn + 1
        steps.append((at, "p", turn))
        if turn + 3 < n:
            steps += [(at, "l", turn + 3), (at, "e", turn + 3)]
        if turn + 2 < n:
            steps.append((at, "f", turn + 2))
        if turn == n - 2:
            steps.append((at, "s", n - 1))
    return steps


def experts_kernel(reps, shards, capacity, held, *refs):
    (
        x_ref, slab_ref, cots_ref, wg_ref, wu_ref, wd_ref,
        back_ref, sums_ref, grads_ref, rows_ref, cs_ref, gg_ref, gu_ref, act_ref, all_ref,
        slabs, cot_buf, hid_buf, d_ref, x_buf, c_buf, gg_buf, gu_buf, act_buf, sum_buf, grad_buf,
        sems, ps, pr, ls, cot_sem, hid_sem, out_sems, zr, *plane_sems,
    ) = refs
    g = Grid(reps, shards).here()
    s = Sends(sems)
    n, places = g.shards, g.places
    length = x_ref.shape[0]
    hidden = hid_buf if held else all_ref
    s.samples = [x_ref, x_ref.at[pl.ds(0, length // 2)]]
    gather = GatherAll(g, s, x_ref, hidden, zr, plane_sems)
    order = gather.order
    groups = 2 * n

    def which(k):
        return jnp.where(k % 2 == 0, g.core, 1 - g.core), pick(k // 2, order)

    def cot_load(k, slot):
        core, zp = which(k)
        return pltpu.make_async_copy(cots_ref.at[:, core, zp], cot_buf.at[slot], cot_sem.at[slot])

    def onehots(k):
        core, zp = which(k)
        return [slots_of(slabs[(q * 2 + core) * n + zp], capacity) for q in range(places)]

    keep = pltpu.make_async_copy(x_ref, gather.own(), ls.at[0])
    keep.start()
    cot_load(0, 0).start()
    greet_all(g)
    push_rows(g, slab_ref, slabs, ps, pr)
    me = g.r * n + g.z
    keep_slab = pltpu.make_async_copy(slab_ref.at[me], slabs.at[me], ls.at[1])
    keep_slab.start()
    gather.line(0)
    keep_slab.wait()
    push_wait(g, slab_ref, slabs, ps, pr)
    keep.wait()

    def turns(k, steps):
        for at, step in steps:
            pl.when(k == at)(step)

    def split(guard, turn):
        s.under(guard, functools.partial(gather.line, turn))

    named = {
        "l": functools.partial(split, g.inside),
        "e": functools.partial(split, g.outside),
        "f": gather.first,
        "s": gather.second,
        "p": lambda turn: gather.plane.from_partner(order[turn]),
    }
    early, late = [], []
    for at, name, turn in tuned_experts.get(n) or expert_steps(n):
        step = functools.partial(named[name], turn)
        if at < groups:
            early.append((at, step))
        else:
            late.append((at - groups, step))

    def outs(k):
        return [
            pltpu.make_async_copy(x_buf, rows_ref.at[k], out_sems.at[0]),
            pltpu.make_async_copy(gg_buf, gg_ref.at[k], out_sems.at[1]),
            pltpu.make_async_copy(gu_buf, gu_ref.at[k], out_sems.at[2]),
            pltpu.make_async_copy(act_buf, act_ref.at[k], out_sems.at[3]),
        ]

    def blocks_out(k):
        core, zp = which(k)
        return [
            pltpu.make_async_copy(sum_buf, sums_ref.at[:, core, zp], out_sems.at[4]),
            pltpu.make_async_copy(grad_buf, grads_ref.at[:, core, zp], out_sems.at[5]),
        ]

    def c_out(k):
        return pltpu.make_async_copy(c_buf, cs_ref.at[k], out_sems.at[6])

    def backward_input(k, carry):
        turns(k, early)
        slot = k % 2
        pl.when(k + 1 < groups)(lambda: cot_load(k + 1, 1 - slot).start())
        cot_load(k, slot).wait()
        pl.when(k > 0)(lambda: c_out(k).wait())
        for q, (onehot, _) in enumerate(onehots(k)):
            taken = jnp.dot(onehot.astype(bf16), cot_buf[slot, q], preferred_element_type=f32)
            c_buf[q * capacity : (q + 1) * capacity, :] = taken.astype(bf16)
        c_out(k).start()
        d_ref[k] = dot_t(c_buf[...], wd_ref[...])
        return carry

    lax.fori_loop(0, groups, backward_input, 0)
    c_out(0).wait()

    def expert(k, carry):
        turns(k, late)
        core, zp = which(k)
        if not held:
            fetch = pltpu.make_async_copy(all_ref.at[pl.ds(0, places)], hid_buf, hid_sem.at[0])
            for q in range(places):
                pltpu.make_async_copy(all_ref.at[(q * 2 + core) * n + zp], hid_buf.at[q], hid_sem.at[0]).start()
            fetch.wait()
        hots = onehots(k)
        pl.when(k > 0)(functools.partial(wait_for, outs, k))
        for q, (onehot, _) in enumerate(hots):
            block = hid_buf[(q * 2 + core) * n + zp] if held else hid_buf[q]
            taken = jnp.dot(onehot.astype(bf16), block, preferred_element_type=f32)
            x_buf[q * capacity : (q + 1) * capacity, :] = taken.astype(bf16)
        weight = jnp.concatenate(
            [jnp.sum(onehot * share, axis=1, keepdims=True) for onehot, share in hots], axis=0
        )
        gate = jnp.dot(x_buf[...], wg_ref[...], preferred_element_type=f32)
        up = jnp.dot(x_buf[...], wu_ref[...], preferred_element_type=f32)
        sigmoid = 1.0 / (1.0 + jnp.exp(-gate))
        silu = gate * sigmoid
        activated = silu * up
        grad = d_ref[k]
        row_mix = jnp.sum(activated * grad, axis=1, keepdims=True)
        grad = grad * weight
        act_buf[...] = (activated * weight).astype(bf16)
        gg_buf[...] = (grad * up * sigmoid * (1.0 + gate * (1.0 - sigmoid))).astype(bf16)
        gu_buf[...] = (grad * silu).astype(bf16)
        for copy in outs(k):
            copy.start()
        for q, (onehot, _) in enumerate(hots):
            back = jnp.sum(onehot * row_mix[q * capacity : (q + 1) * capacity], axis=0, keepdims=True)
            back_ref[(q * 2 + core) * n + zp] = jnp.broadcast_to(back, slab_ref.shape[1:])
        produced = jnp.dot(act_buf[...], wd_ref[...], preferred_element_type=f32).astype(bf16)
        pl.when(k > 0)(functools.partial(wait_for, blocks_out, k))
        for q, (onehot, _) in enumerate(hots):
            part = produced[q * capacity : (q + 1) * capacity]
            sum_buf[q] = t_dot(onehot.astype(bf16), part).astype(bf16)
        grad_in = (dot_t(gg_buf[...], wg_ref[...]) + dot_t(gu_buf[...], wu_ref[...])).astype(bf16)
        for q, (onehot, _) in enumerate(hots):
            part = grad_in[q * capacity : (q + 1) * capacity]
            grad_buf[q] = t_dot(onehot.astype(bf16), part).astype(bf16)
        for copy in blocks_out(k):
            copy.start()
        return carry

    lax.fori_loop(0, groups, expert, 0)
    for copy in outs(0) + blocks_out(0):
        copy.wait()
    s.drain()


def experts_all(reps, shards, capacity, x, slab, cots, wg, wu, wd, ident):
    g = Grid(reps, shards)
    dma, v = pltpu.SemaphoreType.DMA, pltpu.VMEM
    n, places = shards, g.places
    length, width = x.shape
    inner = wg.shape[1]
    rows = places * capacity
    held = g.devices <= 32
    blocks = jax.ShapeDtypeStruct((places, 2, n, length, width), bf16)
    wide = jax.ShapeDtypeStruct((2 * n, rows, width), bf16)
    narrow = jax.ShapeDtypeStruct((2 * n, rows, inner), bf16)
    gathered = (g.devices, length, width)
    return pl.pallas_call(
        functools.partial(experts_kernel, reps, shards, capacity, held),
        out_shape=(
            jax.ShapeDtypeStruct(slab.shape, f32),
            blocks,
            blocks,
            wide,
            wide,
            narrow,
            narrow,
            narrow,
            jax.ShapeDtypeStruct((1, 16, 128) if held else gathered, bf16),
        ),
        in_specs=[vmem, vmem, hbm, vmem, vmem, vmem],
        out_specs=(vmem,) + (hbm,) * 8,
        scratch_shapes=[
            v(slab.shape, f32),
            v((2, places, length, width), bf16),
            v(gathered if held else (places, length, width), bf16),
            v((2 * n, rows, inner), f32),
            v((rows, width), bf16),
            v((rows, width), bf16),
            v((rows, inner), bf16),
            v((rows, inner), bf16),
            v((rows, inner), bf16),
            v((places, length, width), bf16),
            v((places, length, width), bf16),
            dma((2 * GatherAll.sends(g),)),
            dma((g.devices,)),
            dma((g.devices,)),
            dma((2,)),
            dma((2,)),
            dma((1,)),
            dma((7,)),
        ]
        + GatherAll.scratch(g),
        compiler_params=params(ident),
        name="experts_all",
    )(x, slab, cots.reshape(places, 2, n, length, width), wg, wu, wd)[:-1]


def inverse_rms(values):
    return lax.rsqrt(jnp.mean(values * values, axis=-1, keepdims=True) + epsilon)


def norm_back(grad_scaled, unit, inverse, gain):
    gained = grad_scaled * gain
    return inverse * (gained - unit * jnp.mean(gained * unit, axis=-1, keepdims=True))


def matmul(a, b, dims=((1,), (0,))):
    return lax.dot_general(a, b, (dims, ((), ())), preferred_element_type=f32)


def local(
    tokens,
    segments,
    routes,
    attn_gain,
    w_query,
    key_weight,
    value_weight,
    w_out,
    query_gain,
    key_gain,
    ffn_gain,
    w_router,
    w_gate,
    w_up,
    w_down,
    cotangent,
):
    reps, shards = lax.axis_size("rep"), lax.axis_size("shard")
    devices = reps * shards
    r, z = lax.axis_index("rep"), lax.axis_index("shard")
    length, width = tokens.shape
    deep = w_query.shape[0]
    head_dim = query_gain.shape[0] * shards
    heads = w_query.shape[1] // head_dim
    kv_heads = key_weight.shape[1] // head_dim
    experts = w_router.shape[1]
    top = routes.shape[1]
    capacity = 2 * length * top // experts
    my_heads = heads // shards
    my_kv = max(1, kv_heads // shards)
    shared_by = max(1, shards // kv_heads)
    q_cols, kv_cols = my_heads * head_dim, my_kv * head_dim
    cols = q_cols + 2 * kv_cols
    piece = deep // reps
    chunks = max(1, devices // 32)
    part = head_dim // shards

    spot = lax.broadcasted_iota(jnp.int32, (1, deep), 1) // part == z

    def row_of(values):
        return jnp.pad(values.reshape(1, -1), ((0, 0), (0, deep - values.size)))

    def spotted(values):
        return jnp.where(spot, jnp.tile(values.reshape(1, part), (1, deep // part)), 0)

    small = jnp.concatenate(
        [
            w_router.T,
            row_of(attn_gain),
            row_of(ffn_gain),
            spotted(query_gain),
            spotted(key_gain),
            row_of(segments[0].astype(bf16)),
        ],
        axis=0,
    )
    small = jnp.pad(small, ((0, -(-(experts + 8) // 16) * 16 - small.shape[0]), (0, 0)))
    small_cols = -(-(experts + 8) // 128) * 128
    half = rope_base ** (-2.0 * jnp.arange(head_dim // 2, dtype=f32) / head_dim)
    frequency = jnp.concatenate([half, half]).reshape(1, head_dim)
    head_sizes = (my_heads, my_kv, head_dim)
    layout = (q_cols, kv_cols, kv_heads, experts)
    (
        small_all, gains, qk_gains, cosine, sine, bias, mixed,
        block_tokens, w_in, hidden_in, qkv, attn_out, cotangents,
    ) = front(
        reps, shards, head_sizes, layout, tokens, cotangent, small, frequency,
        w_query, key_weight, value_weight, w_out, 1,
    )
    router = small_all[:, :experts].transpose(1, 0, 2).reshape(experts, width)
    gain_one, gain_two = gains[0:1], gains[1:2]
    qgain, kgain = qk_gains[0:1], qk_gains[1:2]
    own_tokens = tokens.astype(f32)
    resid = own_tokens + mixed

    inverse_two = inverse_rms(resid)
    normed_two = resid * inverse_two
    hidden_two = (normed_two * gain_two).astype(bf16)
    logits = matmul(hidden_two, router, ((1,), (1,)))
    gate_probs = jax.nn.softmax(logits, axis=-1)
    chosen = jnp.any(routes[:, :, None] == jnp.arange(experts, dtype=jnp.int32)[None, None, :], axis=1)
    picked = jnp.where(chosen, gate_probs, 0.0)
    picked_total = jnp.sum(picked, axis=-1, keepdims=True)
    mix = picked / picked_total
    slab = jnp.where(chosen, mix, -1.0).T.reshape(experts, 1, length)
    slab = jnp.broadcast_to(slab, (experts, 8, length))
    back_mix, sums, grad_sums, rows, row_grads, grad_gate, grad_up, activated = experts_all(
        reps, shards, capacity, hidden_two, slab, cotangents, w_gate[0], w_up[0], w_down[0], 4
    )
    sums = sums.reshape(devices, length, width)
    grad_sums = grad_sums.reshape(devices, length, width)
    rows, row_grads = rows.reshape(-1, width), row_grads.reshape(-1, width)
    fill = (rows, row_grads) + tuple(a.reshape(rows.shape[0], -1) for a in (grad_gate, grad_up, activated))
    grad_hidden, mixes, grad_w_gate, grad_w_up, grad_w_down = scatter_wide(
        reps, shards, grad_sums, back_mix, fill, 8, chunks
    )

    grad_out = cotangent.astype(f32)
    grad_mix = mixes[:, 0, :].T
    grad_picked = jnp.where(chosen, grad_mix - jnp.sum(grad_mix * mix, axis=-1, keepdims=True), 0.0) / picked_total
    grad_logits = (gate_probs * (grad_picked - jnp.sum(grad_picked * picked, axis=-1, keepdims=True))).astype(bf16)
    grad_hidden = grad_hidden + matmul(grad_logits, router)
    grad_ffn_gain = jnp.sum(grad_hidden * normed_two, axis=0)
    grad_resid = grad_out + norm_back(grad_hidden, normed_two, inverse_two, gain_two)
    grad_w_router = matmul(hidden_two, grad_logits, ((0,), (0,)))

    fused = width // chunks
    grad_qkv, grad_query_gain, grad_key_gain, moe, out_grad = attend_back(
        reps, shards, head_sizes, grad_resid.astype(bf16), qkv, w_out, attn_out, qgain, kgain, cosine, sine, bias,
        sums[:, :, :fused], 5,
    )
    if chunks > 1:
        rest = scatter_wide(reps, shards, sums[:, :, fused:], None, None, 16, chunks - 1)
        moe = jnp.concatenate([moe, rest], axis=1)
    output = (resid + moe).astype(bf16)

    small_grads = jnp.concatenate(
        [grad_w_router, jnp.zeros((width, 1), f32), grad_ffn_gain.reshape(width, 1)], axis=1
    )
    small_grads = jnp.pad(small_grads, ((0, 0), (0, small_cols - small_grads.shape[1])))
    grad_hidden_in, sent_q, sent, sent_out = deliver(
        reps, shards, q_cols, experts, part, grad_qkv.reshape(shards * length, cols), small_grads,
        grad_query_gain, grad_key_gain, out_grad, w_in, hidden_in.reshape(shards * length, width),
        block_tokens.reshape(shards * length, width), 6,
    )
    own_inverse, own_normed = unit_of(own_tokens)
    grad_tokens = grad_resid + norm_back(grad_hidden_in, own_normed, own_inverse, gain_one)
    sent = sent.reshape(shards, deep, 2 * kv_cols + small_cols)

    def joined(values):
        if shared_by > 1:
            values = values.astype(f32).reshape(-1, shared_by, deep, values.shape[-1]).sum(axis=1)
        return values.transpose(1, 0, 2).reshape(deep, -1).astype(f32)

    owned_small = jnp.sum(sent[:, :, 2 * kv_cols :].astype(f32), axis=0)
    return (
        output,
        grad_tokens,
        owned_small[:, experts],
        sent_q.reshape(deep, -1).astype(f32),
        joined(sent[:, :, :kv_cols]),
        joined(sent[:, :, kv_cols : 2 * kv_cols]),
        sent_out.reshape(w_out.shape).astype(f32),
        owned_small[:part, experts + 2],
        owned_small[:part, experts + 3],
        owned_small[:, experts + 1],
        owned_small[:, :experts],
        grad_w_gate[None],
        grad_w_up[None],
        grad_w_down[None],
    )


def solution(mesh):
    split = P(("rep", "shard"))
    row = P("shard")
    return jax.shard_map(
        local,
        mesh=mesh,
        in_specs=(split,) * 3 + (row,) * 9 + (split,) * 4,
        out_specs=(split,) * 2 + (row,) * 9 + (split,) * 3,
        check_vma=False,
    )
```

```python
import functools
import jax
import jax.numpy as jnp
from jax import lax
from jax.experimental import pallas as pl
from jax.experimental.pallas import tpu as pltpu
from jax.sharding import PartitionSpec as P

bf16 = jnp.bfloat16
f32 = jnp.float32
vmem_cap = 62 * 1024 * 1024
epsilon = 1e-06
rope_base = 1000000.0
masked_score = -1e30
tuned_front = {
    4: [
        ("w", 1), ("w", 0), ("x", 0), ("pf", 0), ("w", 3), ("m", 0), ("pf", 3), ("xm", 1), ("co", 0), ("xe", 1),
        ("xm", 2), ("m", 2), ("ps", 3), ("pf", 1), ("ps", 0), ("m", 1), ("cz", 0), ("pp", 3), ("gf", 0), ("w", 2),
        ("ps", 1), ("m", 3), ("xm", 3), ("pp", 1), ("g", 0), ("pf", 2), ("glm", 1), ("glm", 2), ("ps", 2), ("pp", 2),
        ("pp", 0), ("gle", 1), ("xe", 3), ("c", 3), ("xe", 2), ("glm", 3), ("r", 3), ("gf", 1), ("c", 1), ("gle", 2),
        ("c", 2), ("gs", 1), ("r", 2), ("gs", 0), ("gf", 2), ("gle", 3), ("o", 0), ("r", 1), ("c", 0), ("gf", 3),
        ("gs", 2), ("o", 1), ("gs", 3), ("r", 0),
    ]
}
tuned_back = {
    4: [
        ("a", 0), ("k", 0), ("a", 1), ("a", 2), ("l", 2), ("l", 1), ("b", 0), ("k", 2), ("l", 3), ("w", 0), ("b", 2),
        ("b", 1), ("c", 0), ("a", 3), ("s", 0), ("wa", 0), ("k", 3), ("c", 1), ("k", 1), ("s", 1), ("c", 2), ("s", 2),
        ("b", 3), ("wb", 0), ("c", 3), ("s", 3), ("wc", 0),
    ]
}
tuned_deliver = {
    4: [
        ("wi", 0), ("pt", 0), ("pt", 3), ("pt", 1), ("pt", 2), ("sm", 0), ("l", 0), ("a", 0), ("wi", 1), ("wi", 3),
        ("a", 3), ("wi", 2), ("b", 0), ("a", 2), ("l", 1), ("o", 0), ("a", 1), ("b", 3), ("b", 2), ("b", 1), ("o", 3),
        ("of", 0), ("o", 1), ("o", 2), ("u", 0), ("os", 0), ("u", 3), ("l", 2), ("f", 3), ("u", 2), ("f", 2),
        ("f", 0), ("u", 1), ("s", 2), ("s", 3), ("p", 3), ("s", 0), ("p", 0), ("p", 2), ("op", 0), ("f", 1), ("s", 1),
        ("l", 3), ("p", 1),
    ]
}
tuned_experts = {
    4: [
        (1, "l", 1), (11, "e", 3), (14, "s", 3), (12, "s", 2), (13, "f", 3), (9, "f", 2), (15, "p", 3), (1, "e", 1),
        (10, "s", 1), (6, "e", 2), (0, "f", 0), (11, "p", 1), (7, "p", 0), (13, "p", 2), (7, "f", 1), (1, "l", 2),
        (5, "s", 0), (9, "l", 3),
    ]
}
tuned_sum = {(4, 8): [0, 0, 3, 3, 4, 5, 5, 5, 7, 8, 8, 8, 8, 8, 8, 8]}


class Grid:
    def __init__(self, reps, shards):
        self.reps, self.shards = reps, shards
        self.devices = reps * shards
        self.places = reps // 2
        self.los = self.places // 2

    def here(self):
        self.r = lax.axis_index("rep")
        self.z = lax.axis_index("shard")
        self.core = self.r % 2
        place = self.r // 2
        self.hi = place // self.los
        self.lo = place % self.los
        return self

    def rep_of(self, hi, lo, core):
        return (hi * self.los + lo) * 2 + core

    def device(self, rep, shard):
        return {"rep": rep, "shard": shard}

    def other_lo(self, step):
        return (self.lo + step) % self.los

    def inside(self):
        return (self.z > 0) & (self.z + 1 < self.shards)

    def outside(self):
        return (self.z == 0) | (self.z + 1 == self.shards)

    def nearest(self):
        n = self.shards
        rows = [sorted(range(n), key=lambda p: (abs(p - z), p)) for z in range(n)]
        return [pick(self.z, [rows[z][turn] for z in range(n)]) for turn in range(n)]


def pick(index, values):
    out = jnp.int32(values[0])
    for i in range(1, len(values)):
        out = jnp.where(index == i, jnp.int32(values[i]), out)
    return out


class Sends:
    def __init__(self, sems):
        self.sems, self.used, self.open, self.samples, self.guard = sems, 0, [], [], None

    def under(self, guard, task):
        self.guard = guard
        task()
        self.guard = None

    def all_of(self, when):
        guard = self.guard
        if guard is None or when is None:
            return guard or when
        return lambda: guard() & when()

    def copy(self, src, dst, sem, recv, device):
        return pltpu.make_async_remote_copy(
            src_ref=src,
            dst_ref=dst,
            send_sem=self.sems.at[sem],
            recv_sem=recv,
            device_id=device,
            device_id_type=pl.DeviceIdType.MESH,
        )

    def start(self, src, dst, recv, device, when=None):
        copy = self.copy(src, dst, self.used, recv, device)
        sample = src
        for other in self.samples:
            if other.shape == src.shape:
                sample = other
        when = self.all_of(when)
        self.open.append((self.used, sample, when))
        self.used += 1
        if when is None:
            copy.start()
        else:
            pl.when(when())(copy.start)

    def arrived(self, dst, recv, device, when=None):
        copy = self.copy(dst, dst, 0, recv, device)
        when = self.all_of(when)
        if when is None:
            copy.wait_recv()
        else:
            pl.when(when())(copy.wait_recv)

    def drain(self):
        here = {"rep": lax.axis_index("rep"), "shard": lax.axis_index("shard")}
        for sem, sample, when in self.open:
            copy = self.copy(sample, sample, sem, self.sems.at[sem], here)
            if when is None:
                copy.wait_send()
            else:
                pl.when(when())(copy.wait_send)
        self.open = []


def greet_all(g):
    barrier = pltpu.get_barrier_semaphore()
    me = g.r * g.shards + g.z

    def one(step, carry):
        peer = (me + step) % g.devices
        pl.semaphore_signal(
            barrier,
            inc=1,
            device_id=g.device(peer // g.shards, peer % g.shards),
            device_id_type=pl.DeviceIdType.MESH,
        )
        return carry

    lax.fori_loop(1, g.devices, one, 0)
    pl.semaphore_wait(barrier, g.devices - 1)


def push_rows(g, src, dst, send_sems, recv_sems):
    me = g.r * g.shards + g.z

    def one(step, carry):
        peer = (me + step) % g.devices
        pltpu.make_async_remote_copy(
            src_ref=src.at[peer],
            dst_ref=dst.at[me],
            send_sem=send_sems.at[step],
            recv_sem=recv_sems.at[step],
            device_id=g.device(peer // g.shards, peer % g.shards),
            device_id_type=pl.DeviceIdType.MESH,
        ).start()
        return carry

    lax.fori_loop(1, g.devices, one, 0)


def push_wait(g, src, dst, send_sems, recv_sems):
    me = g.r * g.shards + g.z

    def one(step, carry):
        peer = (me + g.devices - step) % g.devices
        copy = pltpu.make_async_remote_copy(
            src_ref=src.at[peer],
            dst_ref=dst.at[peer],
            send_sem=send_sems.at[step],
            recv_sem=recv_sems.at[step],
            device_id=g.device(peer // g.shards, peer % g.shards),
            device_id_type=pl.DeviceIdType.MESH,
        )
        copy.wait_send()
        copy.wait_recv()
        return carry

    lax.fori_loop(1, g.devices, one, 0)


class PlaneGather:
    def __init__(self, g, s, view, lr, hr, dr, cr):
        self.g, self.s, self.view = g, s, view
        self.lr, self.hr, self.dr, self.cr = lr, hr, dr, cr

    @staticmethod
    def scratch(g, units):
        dma, others = pltpu.SemaphoreType.DMA, max(1, g.los - 1)
        return [dma((units, 2, others)), dma((units, 2)), dma((units, 2, others)), dma((units, 5 * g.los))]

    @staticmethod
    def sends(g, units):
        return 9 * g.los * units

    def at(self, hi, lo):
        return self.g.device(self.g.rep_of(hi, lo, self.g.core), self.g.z)

    def partner(self):
        g = self.g
        return g.device(g.rep_of(g.hi, g.lo, 1 - g.core), g.z)

    def own(self, u, src=None):
        g, s = self.g, self.s

        def dst(part):
            return self.view(u, g.hi, g.lo, g.core, part)

        src = src or dst
        for part in (0, 1):
            for step in range(1, g.los):
                s.start(src(part), dst(part), self.lr.at[u, part, step - 1], self.at(g.hi, g.other_lo(step)))
            s.start(src(1 - part), dst(1 - part), self.hr.at[u, 1 - part], self.at(1 - g.hi, g.lo))
        s.start(src(None), dst(None), self.cr.at[u, 0], self.partner())

    def take(self, u, hi, lo, part, recv, frm, partner_slot, onward=()):
        ref = self.view(u, hi, lo, self.g.core, part)
        self.s.arrived(ref, recv, frm)
        for sem, device in onward:
            self.s.start(ref, ref, sem, device)
        self.s.start(ref, ref, self.cr.at[u, partner_slot], self.partner())

    def first(self, u):
        g = self.g
        far = 1 - g.hi
        for step in range(1, g.los):
            frm = (g.lo + g.los - step) % g.los
            onward = [(self.dr.at[u, 0, step - 1], self.at(far, g.lo))]
            self.take(u, g.hi, frm, 0, self.lr.at[u, 0, step - 1], self.at(g.hi, frm), 5 * step, onward)
        onward = [(self.dr.at[u, 1, step - 1], self.at(g.hi, g.other_lo(step))) for step in range(1, g.los)]
        self.take(u, far, g.lo, 1, self.hr.at[u, 1], self.at(far, g.lo), 1, onward)
        for step in range(1, g.los):
            frm = (g.lo + g.los - step) % g.los
            self.take(u, g.hi, frm, 1, self.lr.at[u, 1, step - 1], self.at(g.hi, frm), 5 * step + 1)
        self.take(u, far, g.lo, 0, self.hr.at[u, 0], self.at(far, g.lo), 2)

    def second(self, u):
        g = self.g
        far = 1 - g.hi
        for step in range(1, g.los):
            frm = (g.lo + g.los - step) % g.los
            self.take(u, far, frm, 0, self.dr.at[u, 0, step - 1], self.at(far, g.lo), 5 * step + 2)
            self.take(u, far, frm, 1, self.dr.at[u, 1, step - 1], self.at(g.hi, frm), 5 * step + 3)

    def from_partner(self, u):
        g = self.g
        far, other = 1 - g.hi, 1 - g.core

        def got(hi, lo, part, slot):
            self.s.arrived(self.view(u, hi, lo, other, part), self.cr.at[u, slot], self.partner())

        got(g.hi, g.lo, None, 0)
        got(far, g.lo, 1, 1)
        got(far, g.lo, 0, 2)
        for step in range(1, g.los):
            frm = (g.lo + g.los - step) % g.los
            got(g.hi, frm, 0, 5 * step)
            got(g.hi, frm, 1, 5 * step + 1)
            got(far, frm, 0, 5 * step + 2)
            got(far, frm, 1, 5 * step + 3)


def add_rows(dst, *srcs, step=16):
    def one(i, carry):
        at = pl.ds(pl.multiple_of(i * step, step), step)
        total = srcs[0][at, :].astype(f32)
        for src in srcs[1:]:
            total = total + src[at, :].astype(f32)
        dst[at, :] = total.astype(dst.dtype)
        return carry

    lax.fori_loop(0, dst.shape[0] // step, one, 0)


class PlaneScatter:
    def __init__(self, g, s, p, cut, own, ra, rb0, rb1, rc0, rc1, sa, sb0, sb1, sc0, sc1, ls):
        self.g, self.s, self.p, self.cut, self.owned = g, s, p, cut, own
        self.ra, self.rb0, self.rb1, self.rc0, self.rc1 = ra, rb0, rb1, rc0, rc1
        self.sa, self.sb0, self.sb1, self.sc0, self.sc1, self.ls = sa, sb0, sb1, sc0, sc1, ls

    @staticmethod
    def scratch(g, units, block, halves, dtype):
        dma, others, v = pltpu.SemaphoreType.DMA, max(1, g.los - 1), pltpu.VMEM
        first, second = halves
        return [
            v((units, g.places) + block, dtype),
            v((units, g.places) + block, dtype),
            v((units, g.los) + first, dtype),
            v((units, others, 2) + second, dtype),
            v((units, others) + first, dtype),
            v((units,) + second, dtype),
            dma((units,)),
            dma((units,)),
            dma((units, others, 2)),
            dma((units, others)),
            dma((units,)),
            dma((units,)),
        ]

    @staticmethod
    def sends(g, units):
        return units * (3 * g.los + 2)

    def at(self, hi, lo):
        return self.g.device(self.g.rep_of(hi, lo, self.g.core), self.g.z)

    def partner(self):
        g = self.g
        return g.device(g.rep_of(g.hi, g.lo, 1 - g.core), g.z)

    def load(self, units):
        self.loads = []
        for turn in range(units):
            load = pltpu.make_async_copy(self.p(turn, self.g.core), self.owned.at[turn], self.ls.at[turn])
            load.start()
            self.loads.append(load)

    def to_partner(self, turn):
        self.s.start(self.p(turn, 1 - self.g.core), self.ra.at[turn], self.sa.at[turn], self.partner())

    def half(self, turn, place, part):
        return self.owned.at[(turn, place) + self.cut(part)]

    def mine(self, turn):
        return self.owned.at[turn, self.g.hi * self.g.los + self.g.lo]

    def a(self, turn, waited=False):
        g, s = self.g, self.s
        far = 1 - g.hi
        if self.loads[turn] is not None:
            self.loads[turn].wait()
        if not waited:
            s.arrived(self.ra.at[turn], self.sa.at[turn], self.partner())

        def one(q, carry):
            line = self.owned.at[turn, q]
            add_rows(line, line, self.ra.at[turn, q])
            return carry

        lax.fori_loop(0, g.places, one, 0)
        block = self.owned.at[(turn, pl.ds(far * g.los, g.los)) + self.cut(0)]
        s.start(block, self.rb0.at[turn], self.sb0.at[turn], self.at(far, g.lo))
        for step in range(1, g.los):
            to = g.other_lo(step)
            for hi in range(2):
                sem = self.sb1.at[turn, step - 1, hi]
                s.start(self.half(turn, hi * g.los + to, 1), self.rb1.at[turn, step - 1, hi], sem, self.at(g.hi, to))

    def b(self, turn):
        g, s = self.g, self.s
        far = 1 - g.hi
        s.arrived(self.rb0.at[turn], self.sb0.at[turn], self.at(far, g.lo))
        for lo in range(g.los):
            line = self.half(turn, g.hi * g.los + lo, 0)
            add_rows(line, line, self.rb0.at[turn, lo])
        for step in range(1, g.los):
            to = g.other_lo(step)
            sem = self.sc0.at[turn, step - 1]
            s.start(self.half(turn, g.hi * g.los + to, 0), self.rc0.at[turn, step - 1], sem, self.at(g.hi, to))
        for step in range(1, g.los):
            frm = (g.lo + g.los - step) % g.los
            for hi in range(2):
                s.arrived(self.rb1.at[turn, step - 1, hi], self.sb1.at[turn, step - 1, hi], self.at(g.hi, frm))
        for hi in range(2):
            line = self.half(turn, hi * g.los + g.lo, 1)
            add_rows(line, line, *[self.rb1.at[turn, step, hi] for step in range(g.los - 1)])
        s.start(self.half(turn, far * g.los + g.lo, 1), self.rc1.at[turn], self.sc1.at[turn], self.at(far, g.lo))

    def c(self, turn):
        g, s = self.g, self.s
        place = g.hi * g.los + g.lo
        for step in range(1, g.los):
            frm = (g.lo + g.los - step) % g.los
            s.arrived(self.rc0.at[turn, step - 1], self.sc0.at[turn, step - 1], self.at(g.hi, frm))
        line = self.half(turn, place, 0)
        add_rows(line, line, *[self.rc0.at[turn, step] for step in range(g.los - 1)])
        s.arrived(self.rc1.at[turn], self.sc1.at[turn], self.at(1 - g.hi, g.lo))
        line = self.half(turn, place, 1)
        add_rows(line, line, self.rc1.at[turn])


def pass_along(g, s, zp, src, dst, zr):
    n = g.shards
    right, left = g.device(g.r, jnp.minimum(g.z + 1, n - 1)), g.device(g.r, jnp.maximum(g.z - 1, 0))
    s.start(src, dst, zr.at[zp], right, lambda: (zp <= g.z) & (g.z + 1 < n))
    s.start(src, dst, zr.at[zp], left, lambda: (zp >= g.z) & (g.z > 0))


def send_line(g, s, zp, line, out_ref, rl, rr, sl, sr, last):
    n = g.shards
    left, right = g.device(g.r, jnp.maximum(g.z - 1, 0)), g.device(g.r, jnp.minimum(g.z + 1, n - 1))
    has_left, has_right = g.z > 0, g.z + 1 < n
    if last:
        s.arrived(rl.at[g.z], sl.at[g.z], left, lambda: g.z > 0)
        s.arrived(rr.at[g.z], sr.at[g.z], right, lambda: g.z + 1 < n)

        @pl.when(has_left & has_right)
        def _():
            add_rows(out_ref, line, rl.at[g.z], rr.at[g.z])

        @pl.when(has_left & jnp.logical_not(has_right))
        def _():
            add_rows(out_ref, line, rl.at[g.z])

        @pl.when(has_right & jnp.logical_not(has_left))
        def _():
            add_rows(out_ref, line, rr.at[g.z])
    else:
        onward_right, onward_left = zp > g.z, zp < g.z

        @pl.when(onward_right & has_left)
        def _():
            s.arrived(rl.at[zp], sl.at[zp], left)
            add_rows(line, line, rl.at[zp])

        @pl.when(onward_left & has_right)
        def _():
            s.arrived(rr.at[zp], sr.at[zp], right)
            add_rows(line, line, rr.at[zp])

        s.start(line, rl.at[zp], sl.at[zp], right, lambda: zp > g.z)
        s.start(line, rr.at[zp], sr.at[zp], left, lambda: zp < g.z)


def line_scratch(shards, block, dtype):
    v, dma = pltpu.VMEM, pltpu.SemaphoreType.DMA
    return [v((shards,) + block, dtype), v((shards,) + block, dtype), dma((shards,)), dma((shards,))]


def wait_for(copies, k):
    for copy in copies(k):
        copy.wait()


def run_all(steps):
    for step in steps:
        step()


def in_order(tasks, default, tuned, n):
    order = tuned.get(n, default)
    assert sorted(order) == sorted(tasks), "task list"
    for key in order:
        tasks[key]()


def staged(n):
    steps = []
    for turn in range(n + 2):
        if turn < n:
            steps.append(("a", turn))
        if 0 <= turn - 1 < n:
            steps.append(("b", turn - 1))
        if 0 <= turn - 2 < n:
            steps += [("c", turn - 2), ("s", turn - 2)]
    return steps


def sum_steps(n, tiles):
    tuned = tuned_sum.get((n, tiles))
    if tuned is None:
        tuned = [min(tiles, (turn + {"a": 0, "b": 1, "c": 2, "s": 2}[name]) * tiles // n) for name, turn in staged(n)]
    timed = {at: [] for at in range(tiles + 1)}
    for at, step in zip(tuned, staged(n)):
        timed[at].append(step)
    return timed


hbm = pl.BlockSpec(memory_space=pl.ANY)
vmem = pl.BlockSpec(memory_space=pltpu.VMEM)


def params(ident):
    return pltpu.CompilerParams(collective_id=ident, has_side_effects=True, vmem_limit_bytes=vmem_cap)


def scatter_all_kernel(reps, shards, slabbed, *refs):
    if slabbed:
        (
            p_ref, slab_ref, x_ref, c_ref, gg_ref, gu_ref, act_ref, out_ref, slabs_ref, wg_ref, wu_ref, wd_ref,
            gg_buf, gu_buf, act_buf, xt, ct, og, ou, od, tile_sems, out_sems, in_sems, *rest,
        ) = refs
    else:
        p_ref, out_ref, *rest = refs
    sems, ps, pr, slab_sem, *rest = rest
    g = Grid(reps, shards).here()
    s = Sends(sems)
    n = g.shards
    scatter = ScatterAll(g, s, p_ref, out_ref, *rest)
    half = pl.ds(0, out_ref.shape[0] // 2)
    own = scatter.plane.owned
    s.samples = [own.at[0, 0], own.at[0, 0, half], own.at[0, pl.ds(0, g.los), half]]
    scatter.load()
    if not slabbed:
        greet_all(g)
        scatter.to_partner()
        for name, turn in staged(n):
            scatter.stage(name, turn)
        s.drain()
        return

    tile = xt.shape[2]
    tiles = x_ref.shape[1] // tile

    def tile_in(j, slot):
        span = pl.ds(pl.multiple_of(j * tile, tile), tile)
        return [
            pltpu.make_async_copy(x_ref.at[:, span], xt.at[slot], tile_sems.at[slot, 0]),
            pltpu.make_async_copy(c_ref.at[:, span], ct.at[slot], tile_sems.at[slot, 1]),
        ]

    def tile_out(j):
        span = pl.ds(pl.multiple_of(j * tile, tile), tile)
        return [
            pltpu.make_async_copy(og, wg_ref.at[span, :], out_sems.at[0]),
            pltpu.make_async_copy(ou, wu_ref.at[span, :], out_sems.at[1]),
            pltpu.make_async_copy(od, wd_ref.at[:, span], out_sems.at[2]),
        ]

    inner = [
        pltpu.make_async_copy(src, dst, in_sems.at[i])
        for i, (src, dst) in enumerate(((gg_ref, gg_buf), (gu_ref, gu_buf), (act_ref, act_buf)))
    ]
    for copy in tile_in(0, 0) + inner:
        copy.start()
    greet_all(g)
    scatter.to_partner()
    push_rows(g, slab_ref, slabs_ref, ps, pr)
    me = g.r * n + g.z
    keep_slab = pltpu.make_async_copy(slab_ref.at[me], slabs_ref.at[me], slab_sem.at[0])
    keep_slab.start()

    timed = sum_steps(n, tiles)

    def next_tiles(j):
        for copy in tile_in(j + 1, (j + 1) % 2):
            copy.start()

    def weight_grads(j, carry):
        for at, steps in timed.items():
            if at < tiles:
                pl.when(j == at)(functools.partial(run_all, [functools.partial(scatter.stage, *step) for step in steps]))
        pl.when(j + 1 < tiles)(functools.partial(next_tiles, j))
        slot = j % 2
        for copy in tile_in(j, slot):
            copy.wait()
        pl.when(j == 0)(functools.partial(run_all, [copy.wait for copy in inner]))
        pl.when(j > 0)(functools.partial(wait_for, tile_out, j))
        og[...] = t_dot(xt[slot], gg_buf[...])
        ou[...] = t_dot(xt[slot], gu_buf[...])
        od[...] = t_dot(act_buf[...], ct[slot])
        for copy in tile_out(j):
            copy.start()
        return carry

    lax.fori_loop(0, tiles, weight_grads, 0)
    for step in timed[tiles]:
        scatter.stage(*step)
    wait_for(tile_out, 0)
    keep_slab.wait()
    push_wait(g, slab_ref, slabs_ref, ps, pr)
    s.drain()


def scatter_all(reps, shards, p, slab, fill, ident):
    g = Grid(reps, shards)
    n = shards
    _, rows, width = p.shape
    dma, v = pltpu.SemaphoreType.DMA, pltpu.VMEM
    slabbed = slab is not None
    out_shape = (jax.ShapeDtypeStruct((rows, width), f32),)
    out_specs, in_specs, extra, scratch = (vmem,), [hbm], [], []
    if slabbed:
        x, c, gg, gu, act = fill
        count, wide = x.shape
        inner = gg.shape[1]
        tile = 256
        narrow = jax.ShapeDtypeStruct((wide, inner), f32)
        out_shape += (
            jax.ShapeDtypeStruct(slab.shape, slab.dtype), narrow, narrow, jax.ShapeDtypeStruct((inner, wide), f32)
        )
        out_specs += (vmem, hbm, hbm, hbm)
        in_specs += [vmem] + [hbm] * 5
        extra = [slab, *fill]
        scratch = [v((count, inner), bf16)] * 3 + [
            v((2, count, tile), bf16), v((2, count, tile), bf16),
            v((tile, inner), f32), v((tile, inner), f32), v((inner, tile), f32),
            dma((2, 2)), dma((3,)), dma((3,)),
        ]
    done = pl.pallas_call(
        functools.partial(scatter_all_kernel, reps, shards, slabbed),
        out_shape=out_shape,
        in_specs=in_specs,
        out_specs=out_specs,
        scratch_shapes=scratch
        + [dma((ScatterAll.sends(g),)), dma((g.devices,)), dma((g.devices,)), dma((1,))]
        + ScatterAll.scratch(g, (rows, width), p.dtype),
        compiler_params=params(ident),
        name="scatter_all",
    )(p.reshape(g.places, 2, n, rows, width), *extra)
    return done if slabbed else done[0]


def scatter_wide(reps, shards, p, slab, fill, ident, chunks):
    if chunks == 1:
        return scatter_all(reps, shards, p, slab, fill, ident)
    step = p.shape[2] // chunks
    parts = [
        scatter_all(reps, shards, p[:, :, i * step : (i + 1) * step], slab if i == 0 else None, fill, ident + i)
        for i in range(chunks)
    ]
    if slab is None:
        return jnp.concatenate(parts, axis=1)
    first, *others = parts[0]
    return jnp.concatenate([first] + parts[1:], axis=1), *others


def deliver_kernel(reps, shards, split, *refs):
    (
        gqkv_ref, small_ref, qsum_ref, ksum_ref, wo_sum_ref, w_in, hid_in, xs_in,
        out_ref, q_out, rest_out, wo_out,
        w_ref, hid_ref, xs_ref, both, acc, ws_ref, wo_all, line_own, rl, rr, sl, sr,
        sems, wr, small_sem, keep_sem, ls, *rest,
    ) = refs
    q_cols, experts, part = split
    g = Grid(reps, shards).here()
    s = Sends(sems)
    n, places = g.shards, g.places
    gather_refs, wo_refs, scatter_refs = rest[:4], rest[4:8], rest[8:]
    length = out_ref.shape[0]
    total, cols = ws_ref.shape[-1], gqkv_ref.shape[1]
    piece = ws_ref.shape[2]
    deep = hid_ref.shape[1] // n
    first = total // 2 // 128 * 128
    spans = {0: pl.ds(0, first), 1: pl.ds(first, total - first), None: pl.ds(0, total)}
    owned = wo_sum_ref.shape[0]
    halves = {0: pl.ds(0, owned // 2), 1: pl.ds(owned // 2, owned // 2), None: pl.ds(0, owned)}
    order = g.nearest()[::-1]
    scatter = PlaneScatter(g, s, None, lambda p: (slice(None), spans[p]), both.at[g.core], *scatter_refs)
    scatter.loads = [None] * n
    gather = PlaneGather(
        g, s, lambda u, hi, lo, core, p: ws_ref.at[u, g.rep_of(hi, lo, core), :, spans[p]], *gather_refs
    )
    out_weight = PlaneGather(g, s, lambda u, hi, lo, core, p: wo_all.at[g.rep_of(hi, lo, core), halves[p]], *wo_refs)
    loads = [
        pltpu.make_async_copy(hid_in, hid_ref, ls.at[0]),
        pltpu.make_async_copy(w_in, w_ref, ls.at[1]),
        pltpu.make_async_copy(xs_in, xs_ref, ls.at[2]),
    ]
    for copy in loads:
        copy.start()
    barrier = pltpu.get_barrier_semaphore()
    peers = [g.device(g.r, (g.z + step) % n) for step in range(1, n)]
    peers += [g.device(g.rep_of(g.hi, g.other_lo(step), g.core), g.z) for step in range(1, g.los)]
    peers += [g.device(g.rep_of(1 - g.hi, g.lo, g.core), g.z), g.device(g.rep_of(g.hi, g.lo, 1 - g.core), g.z)]
    for peer in peers:
        pl.semaphore_signal(barrier, inc=1, device_id=peer, device_id_type=pl.DeviceIdType.MESH)
    pl.semaphore_wait(barrier, len(peers))
    out_weight.own(0, lambda p: wo_sum_ref.at[halves[p]])

    ra = scatter.ra
    tail = pl.ds(cols, total - cols)

    def projection(zp):
        if zp == 0:
            loads[0].wait()
        grad = t_dot(hid_ref[:, zp * deep : (zp + 1) * deep], gqkv_ref[...]).astype(bf16)
        for place in range(places):
            for core in range(2):
                row = (place * 2 + core) * piece
                both[core, zp, place, :, 0:cols] = grad[row : row + piece]
        src = both.at[1 - g.core, zp, :, :, pl.ds(0, cols)]
        s.start(src, ra.at[zp, :, :, pl.ds(0, cols)], scatter.sa.at[zp], scatter.partner())

    def share(turn):
        if turn == 0:
            loads[1].wait()
            loads[2].wait()
            acc[...] = small_ref[...]
        lane = lax.broadcasted_iota(jnp.int32, (length, total - cols), 1)
        marked = jnp.where(lane == experts, 1.0, 0.0).astype(bf16)
        at = pl.ds(pl.multiple_of(order[turn] * length, length), length)
        grad = dot_t(gqkv_ref[at, :], w_ref[...])
        line_own[turn] = grad.astype(bf16)
        _, unit = unit_of(xs_ref[at, :].astype(f32))
        acc[...] += t_dot((grad * unit).astype(bf16), marked)

    def small_grads():
        for i, ref in ((2, qsum_ref), (3, ksum_ref)):
            width = ref.shape[1]
            columns = jnp.broadcast_to(ref[...], (total - cols, width)).T
            mask = lax.broadcasted_iota(jnp.int32, (part, total - cols), 1) == experts + i
            for zp in range(n):
                acc[zp * deep : zp * deep + part] += jnp.where(mask, columns[zp * part : (zp + 1) * part], 0.0)
        for zp in range(n):
            for place in range(places):
                for core in range(2):
                    row = zp * deep + (place * 2 + core) * piece
                    both[core, zp, place, :, cols:total] = acc[row : row + piece].astype(bf16)
        s.start(both.at[1 - g.core, :, :, :, tail], ra.at[:, :, :, tail], small_sem.at[0], scatter.partner())

    def line(turn):
        send_line(g, s, order[turn], line_own.at[turn], out_ref, rl, rr, sl, sr, last=turn == n - 1)

    def from_partner(turn):
        if turn == 0:
            s.arrived(ra.at[:, :, :, tail], small_sem.at[0], scatter.partner())
        s.arrived(ra.at[turn, :, :, pl.ds(0, cols)], scatter.sa.at[turn], scatter.partner())
        scatter.a(turn, waited=True)

    def owner(turn):
        scatter.c(turn)
        dst = ws_ref.at[g.z, g.r]
        keep = pltpu.make_async_copy(scatter.mine(turn), dst, keep_sem.at[0])
        pl.when(g.z == turn)(keep.start)
        s.start(scatter.mine(turn), dst, wr.at[g.z], g.device(g.r, turn), lambda: g.z != turn)
        pl.when(g.z == turn)(keep.wait)

    saves = [pltpu.make_async_copy(wo_all, wo_out, ls.at[3])]

    def weight_done():
        out_weight.from_partner(0)
        keep = pltpu.make_async_copy(wo_sum_ref, wo_all.at[g.r], keep_sem.at[0])
        keep.start()
        keep.wait()
        saves[0].start()

    def unit_at(step):
        return (g.z + n - step) % n

    def hand_out(step):
        u = unit_at(step)
        if step:
            s.arrived(ws_ref.at[u, g.r], wr.at[u], g.device(g.r, u))
        gather.own(u)

    def save(step):
        u = unit_at(step)
        gather.from_partner(u)
        q_span = pl.ds(pl.multiple_of(u * q_cols, 128), q_cols)
        rest_span = pl.ds(q_cols, total - q_cols)
        pair = [
            pltpu.make_async_copy(ws_ref.at[u, :, :, pl.ds(0, q_cols)], q_out.at[:, :, q_span], ls.at[4 + 2 * step]),
            pltpu.make_async_copy(ws_ref.at[u, :, :, rest_span], rest_out.at[u], ls.at[5 + 2 * step]),
        ]
        for copy in pair:
            copy.start()
        saves.extend(pair)

    tasks = {
        ("sm", 0): small_grads,
        ("of", 0): functools.partial(out_weight.first, 0),
        ("os", 0): functools.partial(out_weight.second, 0),
        ("op", 0): weight_done,
    }
    for k in range(n):
        tasks["wi", k] = functools.partial(projection, k)
        tasks["pt", k] = functools.partial(share, k)
        tasks["l", k] = functools.partial(line, k)
        tasks["a", k] = functools.partial(from_partner, k)
        tasks["b", k] = functools.partial(scatter.b, k)
        tasks["o", k] = functools.partial(owner, k)
        tasks["u", k] = functools.partial(hand_out, k)
        tasks["f", k] = functools.partial(gather.first, unit_at(k))
        tasks["s", k] = functools.partial(gather.second, unit_at(k))
        tasks["p", k] = functools.partial(save, k)
    default = [("wi", k) for k in range(n)] + [("pt", 0), ("l", 0)] + [("pt", k) for k in range(1, n)] + [("sm", 0)]
    for turn in range(n + 2):
        if turn < n:
            default.append(("a", turn))
        if turn < 2:
            default.append((("of", "os")[turn], 0))
        if 0 <= turn - 1 < n:
            default.append(("b", turn - 1))
        if 1 <= turn < n - 1:
            default.append(("l", turn))
        if 0 <= turn - 2 < n:
            default.append(("o", turn - 2))
    default += [("op", 0), ("u", 0)]
    for k in range(1, n):
        default += [("u", k), ("f", k - 1)]
        if k > 1:
            default.append(("s", k - 2))
    default += [("f", n - 1), ("s", n - 2), ("s", n - 1), ("l", n - 1)] + [("p", k) for k in range(n)]
    in_order(tasks, default, tuned_deliver, n)
    for copy in saves:
        copy.wait()
    s.drain()


def deliver(reps, shards, q_cols, experts, part, gqkv, small, qsum, ksum, wo_sum, w, hid, xs, ident):
    g = Grid(reps, shards)
    n = shards
    dma, v = pltpu.SemaphoreType.DMA, pltpu.VMEM
    width = hid.shape[1]
    rows = hid.shape[0] // n
    cols = gqkv.shape[1]
    total = cols + small.shape[1]
    piece = width // n // reps
    first = total // 2 // 128 * 128
    return pl.pallas_call(
        functools.partial(deliver_kernel, reps, shards, (q_cols, experts, part)),
        out_shape=(
            jax.ShapeDtypeStruct((rows, width), f32),
            jax.ShapeDtypeStruct((reps, piece, n * q_cols), bf16),
            jax.ShapeDtypeStruct((n, reps, piece, total - q_cols), bf16),
            jax.ShapeDtypeStruct((reps,) + wo_sum.shape, bf16),
        ),
        in_specs=[vmem] * 5 + [hbm] * 3,
        out_specs=(vmem, hbm, hbm, hbm),
        scratch_shapes=[
            v(w.shape, bf16),
            v(hid.shape, bf16),
            v(xs.shape, bf16),
            v((2, n, g.places, piece, total), bf16),
            v(small.shape, f32),
            v((n, reps, piece, total), bf16),
            v((reps,) + wo_sum.shape, bf16),
            v((n, rows, width), bf16),
        ]
        + line_scratch(n, (rows, width), bf16)
        + [
            dma((PlaneGather.sends(g, n) + PlaneGather.sends(g, 1) + PlaneScatter.sends(g, n) + 4 * n + 1,)),
            dma((n,)),
            dma((1,)),
            dma((1,)),
            dma((4 + 2 * n,)),
        ]
        + PlaneGather.scratch(g, n)
        + PlaneGather.scratch(g, 1)
        + PlaneScatter.scratch(g, n, (piece, total), ((piece, first), (piece, total - first)), bf16)[1:],
        compiler_params=params(ident),
        name="deliver",
    )(gqkv, small, qsum, ksum, wo_sum, w, hid, xs)


def turned(x, cosine, sine):
    return x * cosine + pltpu.roll(x, x.shape[-1] // 2, 1) * sine


def mean_last(x):
    return jnp.sum(x, axis=-1, keepdims=True) * (1.0 / x.shape[-1])


def unit_of(x):
    inverse = lax.rsqrt(mean_last(x * x) + epsilon)
    return inverse, x * inverse


def dot_t(a, b):
    return lax.dot_general(a, b, (((1,), (1,)), ((), ())), preferred_element_type=f32)


def t_dot(a, b):
    return lax.dot_general(a, b, (((0,), (0,)), ((), ())), preferred_element_type=f32)


def softmax_rows(q_rot, k_rot, bias, head_dim):
    scores = dot_t(q_rot, k_rot) * head_dim ** (-0.5) + bias
    raised = jnp.exp(scores - jnp.max(scores, axis=-1, keepdims=True))
    return raised * (1.0 / jnp.sum(raised, axis=-1, keepdims=True))


def back_unit(grad_scaled, unit, inverse, gain):
    gained = grad_scaled * gain
    return inverse * (gained - unit * mean_last(gained * unit))


def loop_heads(first, last, head, carry):
    width = 4 if (last - first) % 4 == 0 else 1

    def some(i, carry):
        for j in range(width):
            carry = head(first + i * width + j, carry)
        return carry

    return lax.fori_loop(0, (last - first) // width, some, carry)


def attend_block(b, heads, x_ref, w_ref, wo_ref, gain_ref, qg_ref, kg_ref, cos_ref, sin_ref, bias_ref, hid_ref, qkv_ref, att_ref, line):
    my_heads, my_kv, head_dim = heads
    x = x_ref[b].astype(f32)
    _, unit = unit_of(x)
    hid_ref[b] = (unit * gain_ref[...]).astype(bf16)
    qkv_ref[b] = jnp.dot(hid_ref[b], w_ref[...], preferred_element_type=f32)
    cosine, sine, bias = cos_ref[b], sin_ref[b], bias_ref[b]
    group = my_heads // my_kv
    for n in range(my_kv):
        at_k = (my_heads + n) * head_dim
        at_v = (my_heads + my_kv + n) * head_dim
        _, k_unit = unit_of(qkv_ref[b, :, at_k : at_k + head_dim])
        k_rot = turned(k_unit * kg_ref[...], cosine, sine).astype(bf16)
        values = qkv_ref[b, :, at_v : at_v + head_dim].astype(bf16)

        def head(h, carry):
            span = pl.ds(pl.multiple_of(h * head_dim, head_dim), head_dim)
            _, q_unit = unit_of(qkv_ref[b, :, span])
            q_rot = turned(q_unit * qg_ref[...], cosine, sine).astype(bf16)
            probs = softmax_rows(q_rot, k_rot, bias, head_dim)
            mixed = jnp.dot(probs.astype(bf16), values, preferred_element_type=f32)
            att_ref[b, :, span] = mixed.astype(bf16)
            return carry

        loop_heads(n * group, (n + 1) * group, head, 0)
    line[...] = jnp.dot(att_ref[b], wo_ref[...], preferred_element_type=f32).astype(bf16)


def attend_back_block(b, heads, ga_ref, qkv_ref, wo_ref, qg_ref, kg_ref, cos_ref, sin_ref, bias_ref, gm_ref, gqkv_ref, qsum_ref, ksum_ref):
    my_heads, my_kv, head_dim = heads
    gm_ref[...] = dot_t(ga_ref[b], wo_ref[...]).astype(bf16)
    cosine, sine, bias = cos_ref[b], sin_ref[b], bias_ref[b]
    group = my_heads // my_kv
    qg, kg = qg_ref[...], kg_ref[...]
    for n in range(my_kv):
        at_k = (my_heads + n) * head_dim
        at_v = (my_heads + my_kv + n) * head_dim
        k_inverse, k_unit = unit_of(qkv_ref[b, :, at_k : at_k + head_dim])
        k_rot = turned(k_unit * kg, cosine, sine).astype(bf16)
        values = qkv_ref[b, :, at_v : at_v + head_dim].astype(bf16)
        nothing = jnp.zeros(k_unit.shape, f32)

        def head(h, carry):
            grad_k, grad_v = carry
            span = pl.ds(pl.multiple_of(h * head_dim, head_dim), head_dim)
            q_inverse, q_unit = unit_of(qkv_ref[b, :, span])
            q_rot = turned(q_unit * qg, cosine, sine).astype(bf16)
            probs = softmax_rows(q_rot, k_rot, bias, head_dim)
            grad_mixed = gm_ref[:, span]
            grad_weights = dot_t(grad_mixed, values)
            centre = jnp.sum(probs * grad_weights, axis=-1, keepdims=True)
            grad_scores = (probs * (grad_weights - centre) * head_dim ** (-0.5)).astype(bf16)
            grad_v = grad_v + t_dot(probs.astype(bf16), grad_mixed)
            grad_k = grad_k + t_dot(grad_scores, q_rot)
            grad_q = jnp.dot(grad_scores, k_rot, preferred_element_type=f32)
            grad_q = turned(grad_q, cosine, -sine)
            qsum_ref[...] += jnp.sum(grad_q * q_unit, axis=0, keepdims=True)
            gqkv_ref[b, :, span] = back_unit(grad_q, q_unit, q_inverse, qg).astype(bf16)
            return grad_k, grad_v

        grad_k, grad_v = loop_heads(n * group, (n + 1) * group, head, (nothing, nothing))
        grad_k = turned(grad_k, cosine, -sine)
        ksum_ref[...] += jnp.sum(grad_k * k_unit, axis=0, keepdims=True)
        gqkv_ref[b, :, at_k : at_k + head_dim] = back_unit(grad_k, k_unit, k_inverse, kg).astype(bf16)
        gqkv_ref[b, :, at_v : at_v + head_dim] = grad_v.astype(bf16)


class GatherAll:
    def __init__(self, g, s, x_ref, out_ref, zr, plane_sems):
        self.g, self.s, self.x_ref, self.out_ref, self.zr = g, s, x_ref, out_ref, zr
        half = x_ref.shape[0] // 2
        self.spans = {0: pl.ds(0, half), 1: pl.ds(half, half), None: pl.ds(0, 2 * half)}
        self.order = g.nearest()
        self.plane = PlaneGather(g, s, self.view, *plane_sems)

    @staticmethod
    def scratch(g):
        dma = pltpu.SemaphoreType.DMA
        return [dma((g.shards,))] + PlaneGather.scratch(g, g.shards)

    @staticmethod
    def sends(g):
        return PlaneGather.sends(g, g.shards) + 2 * g.shards

    def view(self, u, hi, lo, core, part):
        return self.out_ref.at[self.g.rep_of(hi, lo, core) * self.g.shards + u, self.spans[part]]

    def own(self):
        g = self.g
        return self.view(g.z, g.hi, g.lo, g.core, None)

    def line(self, turn):
        g, zp = self.g, self.order[turn]
        dst = self.view(zp, g.hi, g.lo, g.core, None)
        if turn:
            self.s.arrived(dst, self.zr.at[zp], g.device(g.r, zp))
        pass_along(g, self.s, zp, dst if turn else self.x_ref, dst, self.zr)
        self.plane.own(zp, None if turn else lambda part: self.x_ref.at[self.spans[part]])

    def first(self, turn):
        self.plane.first(self.order[turn])

    def second(self, turn):
        self.plane.second(self.order[turn])

    def finish(self):
        for turn in range(self.g.shards):
            self.plane.from_partner(self.order[turn])


class ScatterAll:
    def __init__(self, g, s, p_ref, out_ref, rl, rr, sl, sr, *plane_refs):
        self.g, self.s, self.out_ref = g, s, out_ref
        self.lines = (rl, rr, sl, sr)
        half = out_ref.shape[0] // 2
        self.order = g.nearest()[::-1]
        self.plane = PlaneScatter(
            g,
            s,
            lambda turn, core: p_ref.at[:, core, self.order[turn]],
            lambda part: (pl.ds(part * half, half),),
            *plane_refs,
        )

    @staticmethod
    def scratch(g, block, dtype):
        rows, width = block
        half = (rows // 2, width)
        return line_scratch(g.shards, block, dtype) + PlaneScatter.scratch(g, g.shards, block, (half, half), dtype)

    @staticmethod
    def sends(g):
        return PlaneScatter.sends(g, g.shards) + 2 * g.shards

    def load(self):
        self.plane.load(self.g.shards)

    def to_partner(self):
        for turn in range(self.g.shards):
            self.plane.to_partner(turn)

    def stage(self, name, turn):
        if name == "s":
            last = turn == self.g.shards - 1
            line = self.plane.mine(turn)
            send_line(self.g, self.s, self.order[turn], line, self.out_ref, *self.lines, last=last)
        else:
            getattr(self.plane, name)(turn)


def attend_back_kernel(reps, shards, heads, *refs):
    (
        ga_ref, qg_ref, kg_ref, cos_ref, sin_ref, bias_ref, qkv_in, wo_in, att_in, p_ref,
        gqkv_ref, qsum_ref, ksum_ref, out_ref, wo_sum_ref,
        gas_ref, qkv_ref, wo_ref, att_ref, both, gm, zr, sems, ls, *scatter_refs,
    ) = refs
    g = Grid(reps, shards).here()
    s = Sends(sems)
    n, rows = g.shards, ga_ref.shape[0]
    half = both.shape[3] // 2
    count = len(scatter_refs) - 11
    scatter = ScatterAll(g, s, p_ref, out_ref, *scatter_refs[:count])
    own = both.at[g.core]
    owner = PlaneScatter(
        g, s, lambda turn, core: both.at[core, turn], lambda part: (pl.ds(part * half, half),), own, *scatter_refs[count:]
    )
    scatter.load()
    loads = [
        pltpu.make_async_copy(wo_in, wo_ref, ls.at[0]),
        pltpu.make_async_copy(qkv_in, qkv_ref, ls.at[1]),
        pltpu.make_async_copy(att_in, att_ref, ls.at[2]),
    ]
    keep = pltpu.make_async_copy(ga_ref, gas_ref.at[g.z], ls.at[3])
    for copy in loads + [keep]:
        copy.start()
    qsum_ref[...] = jnp.zeros(qsum_ref.shape, f32)
    ksum_ref[...] = jnp.zeros(ksum_ref.shape, f32)
    greet_all(g)
    order = g.nearest()

    def line(turn):
        zp = order[turn]
        dst = gas_ref.at[zp]
        if turn:
            s.arrived(dst, zr.at[zp], g.device(g.r, zp))
        pass_along(g, s, zp, dst if turn else ga_ref, dst, zr)

    def out_weight():
        width = ga_ref.shape[1]
        block = att_ref.shape[2] // g.reps
        grads = gas_ref[...].reshape(n * rows, width)
        def one(i, carry):
            at = pl.ds(pl.multiple_of(i * block, 128), block) if block % 128 == 0 else slice(i * block, (i + 1) * block)
            mixed = att_ref[:, :, at].reshape(n * rows, block)
            both[i % 2, 0, i // 2] = t_dot(mixed, grads).astype(bf16)
            return carry

        if block % 128 == 0:
            lax.fori_loop(0, g.reps, one, 0)
        else:
            for i in range(g.reps):
                one(i, 0)

    line(0)
    scatter.to_partner()
    for copy in loads + [keep]:
        copy.wait()
    owner.loads = [None]

    def block(turn):
        attend_back_block(
            order[turn], heads, gas_ref, qkv_ref, wo_ref, qg_ref, kg_ref, cos_ref, sin_ref, bias_ref,
            gm, gqkv_ref, qsum_ref, ksum_ref,
        )

    def weigh():
        out_weight()
        owner.to_partner(0)

    tasks = {("w", 0): weigh}
    for name in "abc":
        tasks["w" + name, 0] = functools.partial(getattr(owner, name), 0)
    for turn in range(n):
        if turn:
            tasks["l", turn] = functools.partial(line, turn)
        tasks["k", turn] = functools.partial(block, turn)
        for name in "abcs":
            tasks[name, turn] = functools.partial(scatter.stage, name, turn)
    default = []
    for turn in range(n + 2):
        default += [step for step in staged(n) if step[1] + {"a": 0, "b": 1, "c": 2, "s": 2}[step[0]] == turn]
        if turn + 1 < n:
            default.append(("l", turn + 1))
        elif turn + 1 == n:
            default.append(("w", 0))
        if turn < n:
            default.append(("k", turn))
        elif turn == n:
            default.append(("wa", 0))
        else:
            default += [("wb", 0), ("wc", 0)]
    in_order(tasks, default, tuned_back, n)
    wo_sum_ref[...] = own[0, g.hi * g.los + g.lo]
    s.drain()


def attend_back(reps, shards, heads, ga, qkv, wo, att, qg, kg, cosine, sine, bias, p, ident):
    g = Grid(reps, shards)
    dma, v = pltpu.SemaphoreType.DMA, pltpu.VMEM
    n = shards
    rows, width = ga.shape
    out_width = p.shape[2]
    owned = wo.shape[0] // reps
    row = jax.ShapeDtypeStruct(qg.shape, f32)
    block = (owned, width)
    half = (owned // 2, width)
    return pl.pallas_call(
        functools.partial(attend_back_kernel, reps, shards, heads),
        out_shape=(
            jax.ShapeDtypeStruct(qkv.shape, bf16),
            row,
            row,
            jax.ShapeDtypeStruct((rows, out_width), f32),
            jax.ShapeDtypeStruct(block, bf16),
        ),
        in_specs=[vmem] * 6 + [hbm] * 4,
        out_specs=(vmem,) * 5,
        scratch_shapes=[
            v((n, rows, width), bf16),
            v(qkv.shape, f32),
            v(wo.shape, bf16),
            v(att.shape, bf16),
            v((2, 1, g.places) + block, bf16),
            v((rows, wo.shape[0]), bf16),
            dma((n,)),
            dma((ScatterAll.sends(g) + PlaneScatter.sends(g, 1) + 2 * n,)),
            dma((4,)),
        ]
        + ScatterAll.scratch(g, (rows, out_width), p.dtype)
        + PlaneScatter.scratch(g, 1, block, (half, half), bf16)[1:],
        compiler_params=params(ident),
        name="attend_back",
    )(ga, qg, kg, cosine, sine, bias, qkv, wo, att, p.reshape(g.places, 2, n, rows, out_width))


def tables_of(segment_column, segment_row, frequency):
    length = segment_row.shape[1]
    rows = lax.broadcasted_iota(jnp.int32, (length, length), 0).astype(f32)
    columns = lax.broadcasted_iota(jnp.int32, (length, length), 1).astype(f32)
    same = segment_column == segment_row
    first = jnp.min(jnp.where(same, columns, float(length)), axis=1, keepdims=True)
    width = frequency.shape[1]
    place = lax.broadcasted_iota(jnp.int32, (length, width), 0).astype(f32)
    angle = (place - first) * frequency
    second_half = lax.broadcasted_iota(jnp.int32, (length, width), 1) >= width // 2
    sine = jnp.sin(angle)
    bias = jnp.where(same & (columns <= rows), 0.0, masked_score)
    return jnp.cos(angle), jnp.where(second_half, sine, -sine), bias


def front_kernel(reps, shards, heads, layout, *refs):
    (
        x_ref, cot_ref, small_ref, freq_ref, wq_ref, wk_ref, wv_ref, wo_in,
        smalls_ref, gains_ref, qk_ref, cos_ref, sin_ref, bias_ref, out_ref,
        xs_out, w_out, hid_out, qkv_out, att_out, cots_ref,
        xs_ref, w_ref, wo_ref, hid_ref, qkv_ref, att_ref, own, rl, rr, sl, sr,
        sems, xr, mr, wr, ls, out_sems, lr, hr, dr, cr, *gather_sems,
    ) = refs
    g = Grid(reps, shards).here()
    s = Sends(sems)
    n = g.shards
    q_cols, kv_cols, kv_heads, experts = layout
    head_dim = heads[2]
    deep = wq_ref.shape[0]
    piece = deep // g.reps
    cols = q_cols + 2 * kv_cols
    first = cols // 2 // 128 * 128
    spans = {0: pl.ds(0, first), 1: pl.ds(first, cols - first), None: pl.ds(0, cols)}
    mine = pl.ds(pl.multiple_of(g.r * piece, piece), piece)

    def view(u, hi, lo, core, part):
        row = pl.multiple_of(u * deep + g.rep_of(hi, lo, core) * piece, piece)
        return w_ref.at[pl.ds(row, piece), spans[part]]

    def pieces(zp, u):
        row = pl.ds(pl.multiple_of(u * deep + g.r * piece, piece), piece)
        at_q = pl.ds(pl.multiple_of(zp * q_cols, 128), q_cols)
        at_kv = pl.ds(pl.multiple_of(zp * kv_heads // n * head_dim, 128), kv_cols)
        return (
            (wq_ref.at[mine, at_q], w_ref.at[row, pl.ds(0, q_cols)]),
            (wk_ref.at[mine, at_kv], w_ref.at[row, pl.ds(q_cols, kv_cols)]),
            (wv_ref.at[mine, at_kv], w_ref.at[row, pl.ds(q_cols + kv_cols, kv_cols)]),
        )

    plane = PlaneGather(g, s, view, lr, hr, dr, cr)
    gather = GatherAll(g, s, cot_ref, cots_ref, gather_sems[0], gather_sems[1:])
    locals_ = [pltpu.make_async_copy(src, dst, ls.at[i]) for i, (src, dst) in enumerate(pieces(g.z, g.z))]
    keeps = [
        pltpu.make_async_copy(x_ref, xs_ref.at[g.z], ls.at[3]),
        pltpu.make_async_copy(small_ref, smalls_ref.at[g.z], ls.at[4]),
        pltpu.make_async_copy(wo_in, wo_ref, ls.at[5]),
        pltpu.make_async_copy(cot_ref, gather.own(), ls.at[6]),
    ]
    for copy in locals_ + keeps:
        copy.start()
    barrier = pltpu.get_barrier_semaphore()
    peers = [g.device(g.r, (g.z + step) % n) for step in range(1, n)]
    peers += [g.device(g.rep_of(g.hi, g.other_lo(step), g.core), g.z) for step in range(1, g.los)]
    peers += [g.device(g.rep_of(1 - g.hi, g.lo, g.core), g.z), g.device(g.rep_of(g.hi, g.lo, 1 - g.core), g.z)]
    for peer in peers:
        pl.semaphore_signal(barrier, inc=1, device_id=peer, device_id_type=pl.DeviceIdType.MESH)
    pl.semaphore_wait(barrier, len(peers))

    order = g.nearest()

    def unit(step):
        return (g.z + n - step) % n

    def small_line(turn):
        zp = order[turn]
        if turn:
            s.arrived(smalls_ref.at[zp], mr.at[zp], g.device(g.r, zp))
        pass_along(g, s, zp, smalls_ref.at[zp] if turn else small_ref, smalls_ref.at[zp], mr)

    def token_line(turn):
        zp = order[turn]
        here = xs_ref.at[zp]
        if turn:
            s.arrived(here, xr.at[zp], g.device(g.r, zp))
        pass_along(g, s, zp, here if turn else x_ref, here, xr)

    for step in range(1, n):
        zp = (g.z + step) % n
        for i, (src, dst) in enumerate(pieces(zp, g.z)):
            s.start(src, dst, wr.at[step, i], g.device(g.r, zp))
    def own_pieces():
        for copy in locals_:
            copy.wait()
        plane.own(g.z)

    def other_pieces(step):
        u = unit(step)
        for i, (_, dst) in enumerate(pieces(g.z, u)):
            s.arrived(dst, wr.at[step, i], g.device(g.r, u))
        plane.own(u)

    length = x_ref.shape[0]

    def gains():
        for copy in keeps[:3]:
            copy.wait()
        for zp in range(n):
            gains_ref[:, zp * deep : (zp + 1) * deep] = smalls_ref[zp].astype(f32)[experts : experts + 8]
        for i in range(2):
            qk_ref[i : i + 1] = sum(gains_ref[2 + i : 3 + i, zp * deep : zp * deep + head_dim] for zp in range(n))

    def compute(turn):
        zp = order[turn]
        row = gains_ref[4:5, pl.ds(pl.multiple_of(zp * deep, 128), length)]
        column = jnp.broadcast_to(row, (length, length)).T
        cos_ref[zp], sin_ref[zp], bias_ref[zp] = tables_of(column, row, freq_ref[...])
        attend_block(
            zp, heads, xs_ref, w_ref, wo_ref, gains_ref.at[0:1], qk_ref.at[0:1], qk_ref.at[1:2],
            cos_ref, sin_ref, bias_ref, hid_ref, qkv_ref, att_ref, own.at[turn],
        )

    def sums(turn):
        send_line(g, s, order[turn], own.at[turn], out_ref, rl, rr, sl, sr, last=turn == 0)

    outs = [
        pltpu.make_async_copy(w_ref, w_out, out_sems.at[0]),
        pltpu.make_async_copy(xs_ref, xs_out, out_sems.at[1]),
        pltpu.make_async_copy(hid_ref, hid_out, out_sems.at[2]),
        pltpu.make_async_copy(qkv_ref, qkv_out, out_sems.at[3]),
        pltpu.make_async_copy(att_ref, att_out, out_sems.at[4]),
    ]
    tasks = {
        ("w", 0): own_pieces,
        ("g", 0): gains,
        ("co", 0): functools.partial(gather.plane.own, g.z, lambda part: cot_ref.at[gather.spans[part]]),
        ("cz", 0): functools.partial(pass_along, g, s, g.z, cot_ref, gather.own(), gather.zr),
        ("o", 0): functools.partial(run_all, [copy.start for copy in outs[:2]]),
        ("o", 1): functools.partial(run_all, [copy.start for copy in outs[2:]]),
    }
    for k in range(n):
        tasks["m", k] = functools.partial(small_line, k)
        tasks["c", k] = functools.partial(compute, k)
        tasks["r", k] = functools.partial(sums, k)
        tasks["pf", k] = functools.partial(plane.first, unit(k))
        tasks["ps", k] = functools.partial(plane.second, unit(k))
        tasks["pp", k] = functools.partial(plane.from_partner, unit(k))
        tasks["gf", k] = functools.partial(gather.first, k)
        tasks["gs", k] = functools.partial(gather.second, k)
        if k:
            tasks["w", k] = functools.partial(other_pieces, k)
            for name, guard in (("m", g.inside), ("e", g.outside)):
                tasks["x" + name, k] = functools.partial(s.under, guard, functools.partial(token_line, k))
                tasks["gl" + name, k] = functools.partial(s.under, guard, functools.partial(gather.line, k))
    tasks["x", 0] = functools.partial(token_line, 0)
    default = [("m", 0), ("x", 0)] + [("w", k) for k in range(n)] + [("co", 0), ("m", 1), ("xm", 1), ("xe", 1)]
    for k in range(n):
        default.append(("pf", k))
        if k:
            default.append(("ps", k - 1))
        if 2 + k < n - 1:
            default += [("m", 2 + k), ("xm", 2 + k), ("xe", 2 + k)]
        if k == max(0, n - 4):
            default.append(("cz", 0))
    default += [("ps", n - 1)] + [("pp", k) for k in range(n)]
    default += [("m", n - 1), ("g", 0), ("xm", n - 1), ("c", 0), ("xe", n - 1), ("o", 0), ("c", n - 1), ("r", n - 1)]
    default += [("gf", 0), ("glm", 1), ("gle", 1)]
    for k in range(n - 2, 0, -1):
        at = n - 1 - k
        default += [("c", k), ("r", k), ("gs", at - 1), ("gf", at), ("glm", at + 1), ("gle", at + 1)]
    default += [("o", 1), ("gs", n - 2), ("gf", n - 1), ("gs", n - 1), ("r", 0)]
    in_order(tasks, default, tuned_front, n)
    gather.finish()
    for copy in outs + keeps[3:]:
        copy.wait()
    s.drain()


def front(reps, shards, heads, layout, x, cot, small, frequency, wq, wk, wv, wo, ident):
    g = Grid(reps, shards)
    dma, v = pltpu.SemaphoreType.DMA, pltpu.VMEM
    n = shards
    rows, width = x.shape
    head_dim = heads[2]
    cols = layout[0] + 2 * layout[1]
    table = jax.ShapeDtypeStruct((n, rows, head_dim), f32)
    lines = (n, rows, width)
    return pl.pallas_call(
        functools.partial(front_kernel, reps, shards, heads, layout),
        out_shape=(
            jax.ShapeDtypeStruct((n,) + small.shape, bf16),
            jax.ShapeDtypeStruct((8, width), f32),
            jax.ShapeDtypeStruct((8, head_dim), f32),
            table,
            table,
            jax.ShapeDtypeStruct((n, rows, rows), f32),
            jax.ShapeDtypeStruct((rows, width), f32),
            jax.ShapeDtypeStruct(lines, bf16),
            jax.ShapeDtypeStruct((width, cols), bf16),
            jax.ShapeDtypeStruct(lines, bf16),
            jax.ShapeDtypeStruct((n, rows, cols), f32),
            jax.ShapeDtypeStruct((n, rows, wo.shape[0]), bf16),
            jax.ShapeDtypeStruct((g.devices, rows, width), bf16),
        ),
        in_specs=[vmem] * 4 + [hbm] * 4,
        out_specs=(vmem,) * 7 + (hbm,) * 6,
        scratch_shapes=[
            v(lines, bf16),
            v((width, cols), bf16),
            v(wo.shape, bf16),
            v(lines, bf16),
            v((n, rows, cols), f32),
            v((n, rows, wo.shape[0]), bf16),
            v(lines, bf16),
        ]
        + line_scratch(n, (rows, width), bf16)
        + [
            dma((PlaneGather.sends(g, n) + 2 * GatherAll.sends(g) + 11 * n,)),
            dma((n,)),
            dma((n,)),
            dma((n, 3)),
            dma((7,)),
            dma((5,)),
        ]
        + PlaneGather.scratch(g, n)
        + GatherAll.scratch(g),
        compiler_params=params(ident),
        name="front",
    )(x, cot, small, frequency, wq, wk, wv, wo)


def slots_of(slab, capacity):
    length = slab.shape[1]
    member = slab >= 0.0
    earlier = lax.broadcasted_iota(jnp.int32, (length, length), 0) < lax.broadcasted_iota(jnp.int32, (length, length), 1)
    ones = jnp.where(member, 1.0, 0.0).astype(bf16)
    slot = jnp.dot(ones, jnp.where(earlier, 1.0, 0.0).astype(bf16), preferred_element_type=f32)
    slot = jnp.where(member, slot, -1.0)[0:1]
    rows = lax.broadcasted_iota(jnp.int32, (capacity, length), 0).astype(f32)
    return jnp.where(rows == slot, 1.0, 0.0), slab[0:1]


def expert_steps(n):
    base = 2 * n
    steps = [(2, "f", 0), (3, "l", 1), (3, "e", 1), (5, "s", 0)]
    steps += [(7, "l", 2), (7, "e", 2)] * (n > 2) + [(base, "f", 1)]
    for turn in range(n):
        if 0 < turn < n - 1:
            steps.append((base + 2 * turn, "s", turn))
        at = base + 2 * turn + 1
        steps.append((at, "p", turn))
        if turn + 3 < n:
            steps += [(at, "l", turn + 3), (at, "e", turn + 3)]
        if turn + 2 < n:
            steps.append((at, "f", turn + 2))
        if turn == n - 2:
            steps.append((at, "s", n - 1))
    return steps


def experts_kernel(reps, shards, capacity, held, *refs):
    (
        x_ref, slab_ref, cots_ref, wg_in, wu_in, wd_in,
        back_ref, sums_ref, grads_ref, rows_ref, cs_ref, gg_ref, gu_ref, act_ref, all_ref,
        slabs, cot_buf, hid_buf, d_ref, x_buf, c_buf, gg_buf, gu_buf, act_buf, sum_buf, grad_buf,
        wg_ref, wu_ref, wd_ref,
        sems, ps, pr, ls, cot_sem, hid_sem, out_sems, zr, *plane_sems,
    ) = refs
    g = Grid(reps, shards).here()
    s = Sends(sems)
    n, places = g.shards, g.places
    length = x_ref.shape[0]
    hidden = hid_buf if held else all_ref
    s.samples = [x_ref, x_ref.at[pl.ds(0, length // 2)]]
    gather = GatherAll(g, s, x_ref, hidden, zr, plane_sems)
    order = gather.order
    groups = 2 * n

    def which(k):
        return jnp.where(k % 2 == 0, g.core, 1 - g.core), pick(k // 2, order)

    def cot_load(k, slot):
        core, zp = which(k)
        return pltpu.make_async_copy(cots_ref.at[:, core, zp], cot_buf.at[slot], cot_sem.at[slot])

    def onehots(k):
        core, zp = which(k)
        return [slots_of(slabs[(q * 2 + core) * n + zp], capacity) for q in range(places)]

    keep = pltpu.make_async_copy(x_ref, gather.own(), ls.at[0])
    weights = [
        pltpu.make_async_copy(src, dst, ls.at[2 + i])
        for i, (src, dst) in enumerate(((wd_in, wd_ref), (wg_in, wg_ref), (wu_in, wu_ref)))
    ]
    for copy in [keep] + weights:
        copy.start()
    cot_load(0, 0).start()
    greet_all(g)
    push_rows(g, slab_ref, slabs, ps, pr)
    me = g.r * n + g.z
    keep_slab = pltpu.make_async_copy(slab_ref.at[me], slabs.at[me], ls.at[1])
    keep_slab.start()
    gather.line(0)
    keep_slab.wait()
    push_wait(g, slab_ref, slabs, ps, pr)
    keep.wait()
    for copy in weights:
        copy.wait()

    def turns(k, steps):
        for at, step in steps:
            pl.when(k == at)(step)

    def split(guard, turn):
        s.under(guard, functools.partial(gather.line, turn))

    named = {
        "l": functools.partial(split, g.inside),
        "e": functools.partial(split, g.outside),
        "f": gather.first,
        "s": gather.second,
        "p": lambda turn: gather.plane.from_partner(order[turn]),
    }
    early, late = [], []
    for at, name, turn in tuned_experts.get(n) or expert_steps(n):
        step = functools.partial(named[name], turn)
        if at < groups:
            early.append((at, step))
        else:
            late.append((at - groups, step))

    def outs(k):
        return [
            pltpu.make_async_copy(x_buf, rows_ref.at[k], out_sems.at[0]),
            pltpu.make_async_copy(gg_buf, gg_ref.at[k], out_sems.at[1]),
            pltpu.make_async_copy(gu_buf, gu_ref.at[k], out_sems.at[2]),
            pltpu.make_async_copy(act_buf, act_ref.at[k], out_sems.at[3]),
        ]

    def blocks_out(k):
        core, zp = which(k)
        return [
            pltpu.make_async_copy(sum_buf, sums_ref.at[:, core, zp], out_sems.at[4]),
            pltpu.make_async_copy(grad_buf, grads_ref.at[:, core, zp], out_sems.at[5]),
        ]

    def c_out(k):
        return pltpu.make_async_copy(c_buf, cs_ref.at[k], out_sems.at[6])

    def backward_input(k, carry):
        turns(k, early)
        slot = k % 2
        pl.when(k + 1 < groups)(lambda: cot_load(k + 1, 1 - slot).start())
        cot_load(k, slot).wait()
        pl.when(k > 0)(lambda: c_out(k).wait())
        for q, (onehot, _) in enumerate(onehots(k)):
            taken = jnp.dot(onehot.astype(bf16), cot_buf[slot, q], preferred_element_type=f32)
            c_buf[q * capacity : (q + 1) * capacity, :] = taken.astype(bf16)
        c_out(k).start()
        d_ref[k] = dot_t(c_buf[...], wd_ref[...])
        return carry

    lax.fori_loop(0, groups, backward_input, 0)
    c_out(0).wait()

    def expert(k, carry):
        turns(k, late)
        core, zp = which(k)
        if not held:
            fetch = pltpu.make_async_copy(all_ref.at[pl.ds(0, places)], hid_buf, hid_sem.at[0])
            for q in range(places):
                pltpu.make_async_copy(all_ref.at[(q * 2 + core) * n + zp], hid_buf.at[q], hid_sem.at[0]).start()
            fetch.wait()
        hots = onehots(k)
        pl.when(k > 0)(functools.partial(wait_for, outs, k))
        for q, (onehot, _) in enumerate(hots):
            block = hid_buf[(q * 2 + core) * n + zp] if held else hid_buf[q]
            taken = jnp.dot(onehot.astype(bf16), block, preferred_element_type=f32)
            x_buf[q * capacity : (q + 1) * capacity, :] = taken.astype(bf16)
        weight = jnp.concatenate(
            [jnp.sum(onehot * share, axis=1, keepdims=True) for onehot, share in hots], axis=0
        )
        gate = jnp.dot(x_buf[...], wg_ref[...], preferred_element_type=f32)
        up = jnp.dot(x_buf[...], wu_ref[...], preferred_element_type=f32)
        sigmoid = 1.0 / (1.0 + jnp.exp(-gate))
        silu = gate * sigmoid
        activated = silu * up
        grad = d_ref[k]
        row_mix = jnp.sum(activated * grad, axis=1, keepdims=True)
        grad = grad * weight
        act_buf[...] = (activated * weight).astype(bf16)
        gg_buf[...] = (grad * up * sigmoid * (1.0 + gate * (1.0 - sigmoid))).astype(bf16)
        gu_buf[...] = (grad * silu).astype(bf16)
        for copy in outs(k):
            copy.start()
        for q, (onehot, _) in enumerate(hots):
            back = jnp.sum(onehot * row_mix[q * capacity : (q + 1) * capacity], axis=0, keepdims=True)
            back_ref[(q * 2 + core) * n + zp] = jnp.broadcast_to(back, slab_ref.shape[1:])
        produced = jnp.dot(act_buf[...], wd_ref[...], preferred_element_type=f32).astype(bf16)
        pl.when(k > 0)(functools.partial(wait_for, blocks_out, k))
        for q, (onehot, _) in enumerate(hots):
            part = produced[q * capacity : (q + 1) * capacity]
            sum_buf[q] = t_dot(onehot.astype(bf16), part).astype(bf16)
        grad_in = (dot_t(gg_buf[...], wg_ref[...]) + dot_t(gu_buf[...], wu_ref[...])).astype(bf16)
        for q, (onehot, _) in enumerate(hots):
            part = grad_in[q * capacity : (q + 1) * capacity]
            grad_buf[q] = t_dot(onehot.astype(bf16), part).astype(bf16)
        for copy in blocks_out(k):
            copy.start()
        return carry

    lax.fori_loop(0, groups, expert, 0)
    for copy in outs(0) + blocks_out(0):
        copy.wait()
    s.drain()


def experts_all(reps, shards, capacity, x, slab, cots, wg, wu, wd, ident):
    g = Grid(reps, shards)
    dma, v = pltpu.SemaphoreType.DMA, pltpu.VMEM
    n, places = shards, g.places
    length, width = x.shape
    inner = wg.shape[1]
    rows = places * capacity
    held = g.devices <= 32
    blocks = jax.ShapeDtypeStruct((places, 2, n, length, width), bf16)
    wide = jax.ShapeDtypeStruct((2 * n, rows, width), bf16)
    narrow = jax.ShapeDtypeStruct((2 * n, rows, inner), bf16)
    gathered = (g.devices, length, width)
    return pl.pallas_call(
        functools.partial(experts_kernel, reps, shards, capacity, held),
        out_shape=(
            jax.ShapeDtypeStruct(slab.shape, f32),
            blocks,
            blocks,
            wide,
            wide,
            narrow,
            narrow,
            narrow,
            jax.ShapeDtypeStruct((1, 16, 128) if held else gathered, bf16),
        ),
        in_specs=[vmem, vmem, hbm, hbm, hbm, hbm],
        out_specs=(vmem,) + (hbm,) * 8,
        scratch_shapes=[
            v(slab.shape, f32),
            v((2, places, length, width), bf16),
            v(gathered if held else (places, length, width), bf16),
            v((2 * n, rows, inner), f32),
            v((rows, width), bf16),
            v((rows, width), bf16),
            v((rows, inner), bf16),
            v((rows, inner), bf16),
            v((rows, inner), bf16),
            v((places, length, width), bf16),
            v((places, length, width), bf16),
            v(wg.shape, bf16),
            v(wu.shape, bf16),
            v(wd.shape, bf16),
            dma((2 * GatherAll.sends(g),)),
            dma((g.devices,)),
            dma((g.devices,)),
            dma((5,)),
            dma((2,)),
            dma((1,)),
            dma((7,)),
        ]
        + GatherAll.scratch(g),
        compiler_params=params(ident),
        name="experts_all",
    )(x, slab, cots.reshape(places, 2, n, length, width), wg, wu, wd)[:-1]


def inverse_rms(values):
    return lax.rsqrt(jnp.mean(values * values, axis=-1, keepdims=True) + epsilon)


def norm_back(grad_scaled, unit, inverse, gain):
    gained = grad_scaled * gain
    return inverse * (gained - unit * jnp.mean(gained * unit, axis=-1, keepdims=True))


def matmul(a, b, dims=((1,), (0,))):
    return lax.dot_general(a, b, (dims, ((), ())), preferred_element_type=f32)


def local(
    tokens,
    segments,
    routes,
    attn_gain,
    w_query,
    key_weight,
    value_weight,
    w_out,
    query_gain,
    key_gain,
    ffn_gain,
    w_router,
    w_gate,
    w_up,
    w_down,
    cotangent,
):
    reps, shards = lax.axis_size("rep"), lax.axis_size("shard")
    devices = reps * shards
    r, z = lax.axis_index("rep"), lax.axis_index("shard")
    length, width = tokens.shape
    deep = w_query.shape[0]
    head_dim = query_gain.shape[0] * shards
    heads = w_query.shape[1] // head_dim
    kv_heads = key_weight.shape[1] // head_dim
    experts = w_router.shape[1]
    top = routes.shape[1]
    capacity = 2 * length * top // experts
    my_heads = heads // shards
    my_kv = max(1, kv_heads // shards)
    shared_by = max(1, shards // kv_heads)
    q_cols, kv_cols = my_heads * head_dim, my_kv * head_dim
    cols = q_cols + 2 * kv_cols
    piece = deep // reps
    chunks = max(1, devices // 32)
    part = head_dim // shards

    spot = lax.broadcasted_iota(jnp.int32, (1, deep), 1) // part == z

    def row_of(values):
        return jnp.pad(values.reshape(1, -1), ((0, 0), (0, deep - values.size)))

    def spotted(values):
        return jnp.where(spot, jnp.tile(values.reshape(1, part), (1, deep // part)), 0)

    small = jnp.concatenate(
        [
            w_router.T,
            row_of(attn_gain),
            row_of(ffn_gain),
            spotted(query_gain),
            spotted(key_gain),
            row_of(segments[0].astype(bf16)),
        ],
        axis=0,
    )
    small = jnp.pad(small, ((0, -(-(experts + 8) // 16) * 16 - small.shape[0]), (0, 0)))
    small_cols = -(-(experts + 8) // 128) * 128
    half = rope_base ** (-2.0 * jnp.arange(head_dim // 2, dtype=f32) / head_dim)
    frequency = jnp.concatenate([half, half]).reshape(1, head_dim)
    head_sizes = (my_heads, my_kv, head_dim)
    layout = (q_cols, kv_cols, kv_heads, experts)
    (
        small_all, gains, qk_gains, cosine, sine, bias, mixed,
        block_tokens, w_in, hidden_in, qkv, attn_out, cotangents,
    ) = front(
        reps, shards, head_sizes, layout, tokens, cotangent, small, frequency,
        w_query, key_weight, value_weight, w_out, 1,
    )
    router = small_all[:, :experts].transpose(1, 0, 2).reshape(experts, width)
    gain_one, gain_two = gains[0:1], gains[1:2]
    qgain, kgain = qk_gains[0:1], qk_gains[1:2]
    own_tokens = tokens.astype(f32)
    resid = own_tokens + mixed

    inverse_two = inverse_rms(resid)
    normed_two = resid * inverse_two
    hidden_two = (normed_two * gain_two).astype(bf16)
    logits = matmul(hidden_two, router, ((1,), (1,)))
    gate_probs = jax.nn.softmax(logits, axis=-1)
    chosen = jnp.any(routes[:, :, None] == jnp.arange(experts, dtype=jnp.int32)[None, None, :], axis=1)
    picked = jnp.where(chosen, gate_probs, 0.0)
    picked_total = jnp.sum(picked, axis=-1, keepdims=True)
    mix = picked / picked_total
    slab = jnp.where(chosen, mix, -1.0).T.reshape(experts, 1, length)
    slab = jnp.broadcast_to(slab, (experts, 8, length))
    back_mix, sums, grad_sums, rows, row_grads, grad_gate, grad_up, activated = experts_all(
        reps, shards, capacity, hidden_two, slab, cotangents, w_gate[0], w_up[0], w_down[0], 4
    )
    sums = sums.reshape(devices, length, width)
    grad_sums = grad_sums.reshape(devices, length, width)
    rows, row_grads = rows.reshape(-1, width), row_grads.reshape(-1, width)
    fill = (rows, row_grads) + tuple(a.reshape(rows.shape[0], -1) for a in (grad_gate, grad_up, activated))
    grad_hidden, mixes, grad_w_gate, grad_w_up, grad_w_down = scatter_wide(
        reps, shards, grad_sums, back_mix, fill, 8, chunks
    )

    grad_out = cotangent.astype(f32)
    grad_mix = mixes[:, 0, :].T
    grad_picked = jnp.where(chosen, grad_mix - jnp.sum(grad_mix * mix, axis=-1, keepdims=True), 0.0) / picked_total
    grad_logits = (gate_probs * (grad_picked - jnp.sum(grad_picked * picked, axis=-1, keepdims=True))).astype(bf16)
    grad_hidden = grad_hidden + matmul(grad_logits, router)
    grad_ffn_gain = jnp.sum(grad_hidden * normed_two, axis=0)
    grad_resid = grad_out + norm_back(grad_hidden, normed_two, inverse_two, gain_two)
    grad_w_router = matmul(hidden_two, grad_logits, ((0,), (0,)))

    fused = width // chunks
    grad_qkv, grad_query_gain, grad_key_gain, moe, out_grad = attend_back(
        reps, shards, head_sizes, grad_resid.astype(bf16), qkv, w_out, attn_out, qgain, kgain, cosine, sine, bias,
        sums[:, :, :fused], 5,
    )
    if chunks > 1:
        rest = scatter_wide(reps, shards, sums[:, :, fused:], None, None, 16, chunks - 1)
        moe = jnp.concatenate([moe, rest], axis=1)
    output = (resid + moe).astype(bf16)

    small_grads = jnp.concatenate(
        [grad_w_router, jnp.zeros((width, 1), f32), grad_ffn_gain.reshape(width, 1)], axis=1
    )
    small_grads = jnp.pad(small_grads, ((0, 0), (0, small_cols - small_grads.shape[1])))
    grad_hidden_in, sent_q, sent, sent_out = deliver(
        reps, shards, q_cols, experts, part, grad_qkv.reshape(shards * length, cols), small_grads,
        grad_query_gain, grad_key_gain, out_grad, w_in, hidden_in.reshape(shards * length, width),
        block_tokens.reshape(shards * length, width), 6,
    )
    own_inverse, own_normed = unit_of(own_tokens)
    grad_tokens = grad_resid + norm_back(grad_hidden_in, own_normed, own_inverse, gain_one)
    sent = sent.reshape(shards, deep, 2 * kv_cols + small_cols)

    def joined(values):
        if shared_by > 1:
            values = values.astype(f32).reshape(-1, shared_by, deep, values.shape[-1]).sum(axis=1)
        return values.transpose(1, 0, 2).reshape(deep, -1).astype(f32)

    owned_small = jnp.sum(sent[:, :, 2 * kv_cols :].astype(f32), axis=0)
    return (
        output,
        grad_tokens,
        owned_small[:, experts],
        sent_q.reshape(deep, -1).astype(f32),
        joined(sent[:, :, :kv_cols]),
        joined(sent[:, :, kv_cols : 2 * kv_cols]),
        sent_out.reshape(w_out.shape).astype(f32),
        owned_small[:part, experts + 2],
        owned_small[:part, experts + 3],
        owned_small[:, experts + 1],
        owned_small[:, :experts],
        grad_w_gate[None],
        grad_w_up[None],
        grad_w_down[None],
    )


def solution(mesh):
    split = P(("rep", "shard"))
    row = P("shard")
    return jax.shard_map(
        local,
        mesh=mesh,
        in_specs=(split,) * 3 + (row,) * 9 + (split,) * 4,
        out_specs=(split,) * 2 + (row,) * 9 + (split,) * 3,
        check_vma=False,
    )
```
